32 devices in a mesh: data: 4 (over z), model: 8 (over y, x, core).
Axes of the slice: x: 2, y: 2, z: 4, core: 2. Of those that a mesh axis runs over, the one named last changes fastest.
Arguments:
- x_saved: bfloat16 [2, 4, 4096, 2048], P(None, 'data', 'model')
- h_saved: bfloat16 [2, 4, 4096, 8192], P(None, 'data', None, 'model')
- w_up: bfloat16 [2, 2048, 8192], P(None, None, 'model')
- w_down: bfloat16 [2, 8192, 2048], P(None, 'model')
- grad_out: bfloat16 [4, 4096, 2048], P('data', 'model')
Outputs:
- output 1: bfloat16 [4, 4096, 2048], P('data', 'model')
- output 2: float32 [2, 2048, 8192], P(None, None, 'model')
- output 3: float32 [2, 8192, 2048], P(None, 'model')
All inputs are finite; a program needn't handle non-finite values.
Results may differ from the reference program's by a relative error of at most 0.0134317.
Values are sent between devices in bfloat16 or wider.
A program may use at most 1 GiB of HBM per device.

```python
import jax
import jax.numpy as jnp
from jax import lax

HIDDEN = 2048
FFN_DIM = 8192
BATCH_SIZE = 4
SEQ_LEN = 4096
LAYERS = 2


def setup_inputs(seed: int = 0) -> dict:
    keys = jax.random.split(jax.random.key(seed), 5)
    x_saved = jax.random.normal(keys[0], (LAYERS, BATCH_SIZE, SEQ_LEN, HIDDEN), jnp.float32)
    h_saved = jax.random.normal(keys[1], (LAYERS, BATCH_SIZE, SEQ_LEN, FFN_DIM), jnp.float32)
    w_up = jax.random.normal(keys[2], (LAYERS, HIDDEN, FFN_DIM), jnp.float32) * HIDDEN ** -0.5
    w_down = jax.random.normal(keys[3], (LAYERS, FFN_DIM, HIDDEN), jnp.float32) * FFN_DIM ** -0.5
    grad_out = jax.random.normal(keys[4], (BATCH_SIZE, SEQ_LEN, HIDDEN), jnp.float32)
    return {
        "x_saved": x_saved.astype(jnp.bfloat16),
        "h_saved": h_saved.astype(jnp.bfloat16),
        "w_up": w_up.astype(jnp.bfloat16),
        "w_down": w_down.astype(jnp.bfloat16),
        "grad_out": grad_out.astype(jnp.bfloat16),
    }


def gelu_parts(pre_act):
    inner = 0.7978845608028654 * (pre_act + 0.044715 * pre_act * pre_act * pre_act)
    tanh_val = jnp.tanh(inner)
    gelu_out = 0.5 * pre_act * (1.0 + tanh_val)
    gelu_slope = 0.5 * (1.0 + tanh_val) + 0.5 * pre_act * (1.0 - tanh_val * tanh_val) * 0.7978845608028654 * (1.0 + 0.134145 * pre_act * pre_act)
    return gelu_out, gelu_slope


def reference(x_saved, h_saved, w_up, w_down, grad_out):
    def block_back(grad_next, layer_in):
        x_layer, h_layer, up_layer, down_layer = layer_in
        grad_f32 = grad_next.astype(jnp.float32)
        d_act = jnp.einsum("bsd,fd->bsf", grad_f32, down_layer.astype(jnp.float32))
        gelu_out, gelu_slope = gelu_parts(h_layer.astype(jnp.float32))
        d_pre = (d_act * gelu_slope).astype(jnp.bfloat16).astype(jnp.float32)
        branch = jnp.einsum("bsf,df->bsd", d_pre, up_layer.astype(jnp.float32))
        grad_in = (grad_f32 + branch).astype(jnp.bfloat16)
        act_rounded = gelu_out.astype(jnp.bfloat16).astype(jnp.float32)
        grad_down = jnp.einsum("bsf,bsd->fd", act_rounded, grad_f32)
        grad_up = jnp.einsum("bsd,bsf->df", x_layer.astype(jnp.float32), d_pre)
        return grad_in, (grad_up, grad_down)

    grad_x, (grad_up, grad_down) = lax.scan(block_back, grad_out, (x_saved, h_saved, w_up, w_down), reverse=True)
    return grad_x, grad_up, grad_down
```

```python
import functools

import jax
import jax.numpy as jnp
from jax import lax
from jax.experimental import pallas as pl
from jax.experimental.pallas import tpu as pltpu
from jax.sharding import PartitionSpec as P

MESH = pl.DeviceIdType.MESH
F32, BF16 = jnp.float32, jnp.bfloat16
NT = (((1,), (1,)), ((), ()))

LAYERS = 2
CHUNKS = 8
PER_LAYER = 4 * CHUNKS
PIECES = LAYERS * PER_LAYER
SLOTS = 8
FIRST_SLOTS = 4
LAST_SLOTS = 16
LAG_SUM = 3
LAG_FREE = 5
LAG_LAST = 10
UNIT_STEP = 8
FINAL_STEP = 23


def gelu_tanh(pre):
    return jnp.tanh(0.7978845608028654 * (pre + 0.044715 * pre * pre * pre))


def gelu(pre):
    return 0.5 * pre * (1.0 + gelu_tanh(pre))


def gelu_slope(pre):
    tanh_val = gelu_tanh(pre)
    return 0.5 * (1.0 + tanh_val) + 0.5 * pre * (1.0 - tanh_val * tanh_val) * 0.7978845608028654 * (1.0 + 0.134145 * pre * pre)


def kernel(x_ref, h_ref, wu_ref, wd_ref, g_ref, gx_ref, up_ref, down_ref, gb_ref, rxh_ref,
           lt, wd, wu, cbuf, gr, hr, dh, ha, gown, xown, pm, pp, pb, rxo, rxv, zp, z1, z2,
           zs, z_r1, z_r2, z_ts, z_tl, z_rt, c1, c2, c3,
           ag_r, ag_p, ag_s, ag_f, ag_l, pp_s, pb_r, pm_s, rx_r, pbc,
           ld_c, ld_g, ld_h, ld_a, ld_w, ld_o, ld_rx, st_gx):
    rows, hidden = gown.shape
    ffn = lt.shape[1]
    half_rows = rows // 2
    cw = hidden // CHUNKS
    fb = ffn // 4
    half_ffn = ffn // 2

    me = lax.axis_index("model")
    spot = lax.axis_index("data")
    core = lax.rem(me, 2)
    px = lax.rem(me // 2, 2)
    py = me // 4
    partner = me + 1 - 2 * core
    step_x, step_y = 2 * (1 - 2 * px), 4 * (1 - 2 * py)
    peers = (me + step_x, me + step_y, me + step_x + step_y)
    is_end = jnp.logical_or(spot == 0, spot == 3)
    is_mid = jnp.logical_not(is_end)
    line_mid = jnp.where(spot < 2, 1, 2)
    line_end = jnp.where(spot < 2, 0, 3)
    line_across = 3 - spot

    def model(i):
        return {"model": i}

    def data(i):
        return {"data": i}

    def signal(sem, where):
        pl.semaphore_signal(sem, inc=1, device_id=where, device_id_type=MESH)

    def remote(src, dst, send, recv, where):
        return pltpu.make_async_remote_copy(src_ref=src, dst_ref=dst, send_sem=send, recv_sem=recv, device_id=where, device_id_type=MESH)

    def take(ref, sem):
        pltpu.make_async_copy(ref, ref, sem).wait()

    def chunk_columns(c):
        return pl.ds(pl.multiple_of(c * cw, cw), cw)

    def row_block(i):
        return pl.ds(pl.multiple_of(i * rows, rows), rows)

    def gather_keep(gid, own):
        for c in range(CHUNKS):
            pltpu.make_async_copy(own.at[:, pl.ds(c * cw, cw)], gb_ref.at[gid, c, row_block(me)], ag_l.at[gid]).start()

    def gather_send(gid, c, own):
        src = own.at[:, chunk_columns(c)]
        dst = gb_ref.at[gid, c, row_block(me)]
        for peer in peers:
            remote(src, dst, ag_s.at[gid], ag_r.at[gid, c], model(peer)).start()
        remote(src, dst, ag_s.at[gid], ag_p.at[gid, c], model(partner)).start()

    def gather_forward(gid, c):
        take(gb_ref.at[gid, c, pl.ds(0, 3 * rows)], ag_r.at[gid, c])
        for peer in peers:
            block = gb_ref.at[gid, c, row_block(peer)]
            remote(block, block, ag_f.at[gid], ag_p.at[gid, c], model(partner)).start()

    def gather_wait(gid, c):
        take(gb_ref.at[gid, c, pl.ds(0, 4 * rows)], ag_p.at[gid, c])

    def chunk_load(gid, c, slot):
        return pltpu.make_async_copy(gb_ref.at[gid, c], cbuf.at[slot], ld_c.at[slot])

    def act_load(layer, b):
        return pltpu.make_async_copy(h_ref.at[layer, row_block(b)], ha, ld_a)

    def act_block(b):
        @pl.loop(0, 4)
        def _(f):
            cols = pl.ds(pl.multiple_of(f * fb, fb), fb)
            a = gelu(ha[:, cols].astype(F32)).astype(BF16).astype(F32)
            lt[0, cols, row_block(b)] = a.T.astype(BF16)

    def weight_loads(layer):
        return (pltpu.make_async_copy(wd_ref.at[layer], wd, ld_w.at[0]), pltpu.make_async_copy(wu_ref.at[layer], wu, ld_w.at[1]))

    def unit_place(u):
        r = lax.rem(u // 2 + 1, 4)
        chip = lax.rem(py + r // 2, 2) * 2 + lax.rem(px + lax.rem(r, 2), 2)
        return r, chip

    def unit_rows(u):
        _, chip = unit_place(u)
        start = (chip * 2 + core) * rows + lax.rem(u, 2) * half_rows
        other = (chip * 2 + 1 - core) * rows + lax.rem(u, 2) * half_rows
        return tuple(pl.ds(pl.multiple_of(s, half_rows), half_rows) for s in (start, other))

    def unit_load(gid, layer, u):
        for n, block in enumerate(unit_rows(u)):
            here = pl.ds(n * half_rows, half_rows)
            for c in range(CHUNKS):
                pltpu.make_async_copy(gb_ref.at[gid, c, block], gr.at[here, pl.ds(c * cw, cw)], ld_g).start()
            pltpu.make_async_copy(h_ref.at[layer, block], hr.at[here], ld_h).start()

    def unit(lp, u):
        order = lp * 8 + u
        slot = lax.rem(order, 2)
        take(gr, ld_g)
        take(hr, ld_h)
        mine, other = unit_rows(u)

        @pl.loop(0, 4)
        def _(f):
            cols = pl.ds(pl.multiple_of(f * fb, fb), fb)
            d_act = lax.dot_general(gr[...], wd[cols, :], NT, preferred_element_type=F32)
            d_pre = (d_act * gelu_slope(hr[:, cols].astype(F32))).astype(BF16)
            dh[:, cols] = d_pre
            flipped = d_pre.astype(F32).T.astype(BF16)
            lt[1, cols, mine] = flipped[:, :half_rows]
            lt[1, cols, other] = flipped[:, half_rows:]

        @pl.when(order >= 2)
        def _():
            take(pp.at[slot], pp_s.at[slot])

            @pl.when(lax.rem(order - 2, 8) < 6)
            def _():
                take(pm.at[slot], pm_s.at[slot])

        @pl.loop(0, CHUNKS)
        def _(d):
            cols = chunk_columns(d)
            part = lax.dot_general(dh[...], wu[cols, :], NT, preferred_element_type=F32).astype(BF16)
            pm[slot, :, cols] = part[:half_rows]
            pp[slot, :, cols] = part[half_rows:]

        @pl.when(order >= 2)
        def _():
            pl.semaphore_wait(pbc, 1)

        remote(pp.at[slot], pb.at[slot], pp_s.at[slot], pb_r.at[slot], model(partner)).start()

    def unit_finish(lp, u):
        order = lp * 8 + u
        slot = lax.rem(order, 2)
        r, chip = unit_place(u)
        here = pl.ds(pl.multiple_of(lax.rem(u, 2) * half_rows, half_rows), half_rows)
        take(pb.at[slot], pb_r.at[slot])

        @pl.when(r != 0)
        def _():
            @pl.loop(0, CHUNKS)
            def _(d):
                cols = chunk_columns(d)
                pm[slot, :, cols] = (pm[slot, :, cols].astype(F32) + pb[slot, :, cols].astype(F32)).astype(BF16)

            remote(pm.at[slot], rxh_ref.at[lp, r - 1, here], pm_s.at[slot], rx_r.at[lp * 6 + (r - 1) * 2 + lax.rem(u, 2)],
                   model(chip * 2 + core)).start()

        @pl.when(r == 0)
        def _():
            @pl.loop(0, CHUNKS)
            def _(d):
                cols = chunk_columns(d)
                rxo[here, cols] = (pm[slot, :, cols].astype(F32) + pb[slot, :, cols].astype(F32)).astype(BF16)

        @pl.when(order < 8 * LAYERS - 2)
        def _():
            signal(pbc, model(partner))

    def new_gradient(lp):
        take(gb_ref.at[2 * lp, pl.ds(0, 4)], ag_s.at[2 * lp])
        for n in range(2):
            here = pl.ds(n * half_rows, half_rows)
            for r in range(3):
                take(rxv.at[r], rx_r.at[lp * 6 + r * 2 + n])
                pltpu.make_async_copy(rxh_ref.at[lp, r, here], rxv.at[r], ld_rx.at[r]).start()
            for r in range(3):
                take(rxv.at[r], ld_rx.at[r])

            @pl.loop(0, CHUNKS)
            def _(d):
                cols = chunk_columns(d)
                total = rxo[here, cols].astype(F32)
                for r in range(3):
                    total += rxv[r, :, cols].astype(F32)
                gown[here, cols] = (gown[here, cols].astype(F32) + total).astype(BF16)

    def piece_place(i):
        return LAYERS - 1 - i // PER_LAYER, lax.rem(i // (2 * CHUNKS), 2), lax.rem(i, 2 * CHUNKS) // 2, lax.rem(i, 2)

    def piece(i):
        _, phase, c, half = piece_place(i)
        slot = lax.rem(i, SLOTS)
        held = lax.rem(i // 2, 2)

        @pl.when(jnp.logical_and(is_end, i >= SLOTS))
        def _():
            take(zp.at[slot], zs.at[slot])

        part = jnp.dot(lt[phase, pl.ds(pl.multiple_of(half * half_ffn, half_ffn), half_ffn), :], cbuf[held], preferred_element_type=F32)

        @pl.when(phase == 0)
        def _():
            zp[slot] = part

        @pl.when(phase == 1)
        def _():
            zp[slot, :fb, :] = part[:fb].T
            zp[slot, fb:, :] = part[fb:].T

    def finished_copies(j):
        layer, _, c, half = piece_place(j)
        slot = lax.rem(j, SLOTS)
        f0 = half * half_ffn
        down = [(z2.at[slot], down_ref.at[layer, pl.ds(pl.multiple_of(f0, half_ffn), half_ffn), chunk_columns(c)])]
        up = [(z2.at[slot, pl.ds(b * fb, fb)], up_ref.at[layer, chunk_columns(c), pl.ds(pl.multiple_of(f0 + b * fb, fb), fb)]) for b in range(2)]
        return down, up

    def line_step(i):
        @pl.when(is_end)
        def _():
            @pl.when(i < PIECES)
            def _():
                slot, there = lax.rem(i, SLOTS), lax.rem(i, FIRST_SLOTS)

                @pl.when(i >= FIRST_SLOTS)
                def _():
                    pl.semaphore_wait(c1, 1)

                remote(zp.at[slot], z1.at[there], zs.at[slot], z_r1.at[there], data(line_mid)).start()

            j = i - LAG_LAST

            @pl.when(jnp.logical_and(j >= 0, j < PIECES))
            def _():
                take(zp.at[0], z_rt.at[lax.rem(j, LAST_SLOTS)])

                @pl.when(j + LAST_SLOTS < PIECES)
                def _():
                    signal(c3, data(line_mid))

        @pl.when(is_mid)
        def _():
            slot, there = lax.rem(i, SLOTS), lax.rem(i, FIRST_SLOTS)
            j = i - LAG_SUM
            old = lax.rem(j + SLOTS, SLOTS)

            @pl.when(i < PIECES)
            def _():
                take(z1.at[there], z_r1.at[there])
                zp[slot] = zp[slot] + z1[there]

            @pl.when(jnp.logical_and(j >= 0, j < PIECES))
            def _():
                take(z2.at[old], z_r2.at[old])
                z2[old] = z2[old] + zp[old]

            @pl.when(i < PIECES)
            def _():
                @pl.when(i + FIRST_SLOTS < PIECES)
                def _():
                    signal(c1, data(line_end))

                @pl.when(i >= SLOTS)
                def _():
                    pl.semaphore_wait(c2, 1)

                remote(zp.at[slot], z2.at[slot], zs.at[slot], z_r2.at[slot], data(line_across)).start()

            @pl.when(jnp.logical_and(j >= 0, j < PIECES))
            def _():
                take(zp.at[old], zs.at[old])

                @pl.when(j >= LAST_SLOTS)
                def _():
                    pl.semaphore_wait(c3, 1)

                down, up = finished_copies(j)
                _, phase, _, _ = piece_place(j)
                for kind, copies in enumerate((down, up)):
                    @pl.when(phase == kind)
                    def _():
                        for src, dst in copies:
                            remote(src, dst, z_ts.at[old], z_rt.at[lax.rem(j, LAST_SLOTS)], data(line_end)).start()
                            pltpu.make_async_copy(src, dst, z_tl.at[old]).start()

            k = i - LAG_FREE

            @pl.when(jnp.logical_and(k >= 0, k < PIECES))
            def _():
                free = lax.rem(k, SLOTS)
                take(z2.at[free], z_ts.at[free])
                take(z2.at[free], z_tl.at[free])

                @pl.when(k + SLOTS < PIECES)
                def _():
                    signal(c2, data(line_across))

    load_g = pltpu.make_async_copy(g_ref, gown, ld_o)
    load_g.start()
    act_load(LAYERS - 1, 0).start()
    for load in weight_loads(LAYERS - 1):
        load.start()

    barrier = pltpu.get_barrier_semaphore()
    for peer in peers + (partner,):
        signal(barrier, model(peer))

    @pl.when(is_end)
    def _():
        signal(barrier, data(line_mid))
        pl.semaphore_wait(barrier, 5)

    @pl.when(is_mid)
    def _():
        signal(barrier, data(line_end))
        signal(barrier, data(line_across))
        pl.semaphore_wait(barrier, 6)

    load_g.wait()
    for c in range(CHUNKS):
        gather_send(0, c, gown)
    gather_keep(0, gown)

    @pl.loop(0, 8)
    def _(b):
        act_load(LAYERS - 1, 0).wait()
        act_block(b)

        @pl.when(b < 7)
        def _():
            act_load(LAYERS - 1, b + 1).start()

    load_x = pltpu.make_async_copy(x_ref.at[LAYERS - 1], xown, ld_o)
    load_x.start()
    load_x.wait()
    gather_forward(0, 0)
    take(gown, ag_l.at[0])
    gather_wait(0, 0)
    chunk_load(0, 0, 0).start()

    @pl.loop(0, PIECES + LAG_LAST)
    def _(i):
        lp = i // PER_LAYER
        layer = LAYERS - 1 - lp
        il = lax.rem(i, PER_LAYER)
        odd = lax.rem(i, 2) == 1
        ggid, xgid = 2 * lp, 2 * lp + 1
        live = i < PIECES

        @pl.when(live)
        def _():
            @pl.when(jnp.logical_not(odd))
            def _():
                take(cbuf.at[0], ld_c.at[lax.rem(i // 2, 2)])

            piece(i)

        line_step(i)

        def when(cond):
            return pl.when(jnp.logical_and(live, cond))

        @when(jnp.logical_and(lp == 0, jnp.logical_and(il >= 1, il < CHUNKS)))
        def _():
            gather_forward(0, il)

        @when(il == 8)
        def _():
            gather_keep(xgid, xown)
            gather_send(xgid, 0, xown)

        @when(jnp.logical_and(odd, jnp.logical_and(il >= 9, il < 23)))
        def _():
            gather_send(xgid, (il - 7) // 2, xown)

        @when(jnp.logical_and(jnp.logical_not(odd), jnp.logical_and(il >= 14, il < 30)))
        def _():
            gather_forward(xgid, (il - 14) // 2)

        @when(jnp.logical_and(lp == 0, il == 24))
        def _():
            gather_keep(2, gown)

        @when(jnp.logical_and(lp == 0, il >= 24))
        def _():
            gather_send(2, il - 24, gown)

        @when(jnp.logical_and(i >= 27, i < 35))
        def _():
            gather_forward(2, i - 27)

        @when(jnp.logical_and(lp == 0, jnp.logical_and(il >= 1, il < CHUNKS)))
        def _():
            gather_wait(0, il)

        @when(i == 28)
        def _():
            take(gown, ag_l.at[2])

        @when(jnp.logical_and(i >= 28, i < 36))
        def _():
            gather_wait(2, i - 28)

        @when(il == 15)
        def _():
            take(xown, ag_l.at[xgid])

        @when(jnp.logical_and(odd, jnp.logical_and(il >= 15, il < 31)))
        def _():
            gather_wait(xgid, (il - 15) // 2)

        @when(jnp.logical_and(odd, i + 1 < PIECES))
        def _():
            nxt = i + 1
            chunk_load(nxt // (2 * CHUNKS), lax.rem(nxt, 2 * CHUNKS) // 2, lax.rem(nxt // 2, 2)).start()

        @when(jnp.logical_and(il > UNIT_STEP, il <= UNIT_STEP + 8))
        def _():
            unit_finish(lp, il - UNIT_STEP - 1)

        @when(il == UNIT_STEP)
        def _():
            for load in weight_loads(0):
                load.wait()

        @when(jnp.logical_and(il >= UNIT_STEP, il < UNIT_STEP + 8))
        def _():
            unit(lp, il - UNIT_STEP)

        @when(jnp.logical_and(il >= UNIT_STEP - 1, il < UNIT_STEP + 7))
        def _():
            unit_load(ggid, layer, il - UNIT_STEP + 1)

        @when(il == FINAL_STEP)
        def _():
            new_gradient(lp)

        @when(i == PER_LAYER + FINAL_STEP)
        def _():
            pltpu.make_async_copy(gown, gx_ref, st_gx).start()

        @when(jnp.logical_and(lp == 0, il == 17))
        def _():
            for load in weight_loads(0):
                load.start()

        @when(jnp.logical_and(lp == 0, il >= 16))
        def _():
            @pl.when(jnp.logical_not(odd))
            def _():
                act_load(0, (il - 16) // 2).start()

            @pl.when(odd)
            def _():
                act_load(0, 0).wait()
                act_block((il - 16) // 2)

        @when(il == 31)
        def _():
            take(gb_ref.at[xgid, pl.ds(0, 4)], ag_s.at[xgid])

            @pl.when(lp == 0)
            def _():
                load = pltpu.make_async_copy(x_ref.at[0], xown, ld_o)
                load.start()
                load.wait()

    for gid in range(2 * LAYERS):
        take(gb_ref.at[gid, pl.ds(0, 3)], ag_f.at[gid])
    for slot in range(2):
        take(pp.at[slot], pp_s.at[slot])
    take(gown, st_gx)

    @pl.when(is_end)
    def _():
        for slot in range(SLOTS):
            take(zp.at[slot], zs.at[slot])


def solution(mesh):
    def device_step(x_saved, h_saved, w_up, w_down, grad_out):
        layers, hidden, ffn = w_up.shape
        rows = grad_out.shape[1]
        tokens = h_saved.shape[2]
        cw, half_ffn = hidden // CHUNKS, ffn // 2
        half_rows = rows // 2
        any_space = pl.BlockSpec(memory_space=pl.ANY)
        dma = pltpu.SemaphoreType.DMA
        vmem = pltpu.VMEM
        grad_x, grad_up, grad_down, _, _ = pl.pallas_call(
            kernel,
            name="backward",
            out_shape=(
                jax.ShapeDtypeStruct((rows, hidden), BF16),
                jax.ShapeDtypeStruct(w_up.shape, F32),
                jax.ShapeDtypeStruct(w_down.shape, F32),
                jax.ShapeDtypeStruct((2 * layers, CHUNKS, tokens, cw), BF16),
                jax.ShapeDtypeStruct((layers, 3, rows, hidden), BF16),
            ),
            in_specs=[any_space] * 5,
            out_specs=(any_space,) * 5,
            scratch_shapes=[
                vmem((2, ffn, tokens), BF16),
                vmem((ffn, hidden), BF16),
                vmem((hidden, ffn), BF16),
                vmem((2, tokens, cw), BF16),
                vmem((rows, hidden), BF16),
                vmem((rows, ffn), BF16),
                vmem((rows, ffn), BF16),
                vmem((rows, ffn), BF16),
                vmem((rows, hidden), BF16),
                vmem((rows, hidden), BF16),
                vmem((2, half_rows, hidden), BF16),
                vmem((2, half_rows, hidden), BF16),
                vmem((2, half_rows, hidden), BF16),
                vmem((rows, hidden), BF16),
                vmem((3, half_rows, hidden), BF16),
                vmem((SLOTS, half_ffn, cw), F32),
                vmem((FIRST_SLOTS, half_ffn, cw), F32),
                vmem((SLOTS, half_ffn, cw), F32),
                dma((SLOTS,)), dma((FIRST_SLOTS,)), dma((SLOTS,)), dma((SLOTS,)), dma((SLOTS,)), dma((LAST_SLOTS,)),
                pltpu.SemaphoreType.REGULAR, pltpu.SemaphoreType.REGULAR, pltpu.SemaphoreType.REGULAR,
                dma((2 * layers, CHUNKS)), dma((2 * layers, CHUNKS)), dma((2 * layers,)), dma((2 * layers,)), dma((2 * layers,)),
                dma((2,)), dma((2,)), dma((2,)), dma((6 * layers,)), pltpu.SemaphoreType.REGULAR,
                dma((2,)), dma(()), dma(()), dma(()), dma((2,)), dma(()), dma((3,)), dma(()),
            ],
            compiler_params=pltpu.CompilerParams(collective_id=0, has_side_effects=True, vmem_limit_bytes=67043328),
        )(x_saved[:, 0], h_saved[:, 0], w_up, w_down, grad_out[0])
        return grad_x[None], grad_up, grad_down

    return jax.shard_map(
        device_step,
        mesh=mesh,
        in_specs=(P(None, "data", "model", None), P(None, "data", None, "model"), P(None, None, "model"), P(None, "model", None), P("data", "model", None)),
        out_specs=(P("data", "model", None), P(None, None, "model"), P(None, "model", None)),
        check_vma=False,
    )
```

```python
import functools

import jax
import jax.numpy as jnp
from jax import lax
from jax.experimental import pallas as pl
from jax.experimental.pallas import tpu as pltpu
from jax.sharding import PartitionSpec as P

MESH = pl.DeviceIdType.MESH
F32, BF16 = jnp.float32, jnp.bfloat16
NT = (((1,), (1,)), ((), ()))

LAYERS = 2
CHUNKS = 8
PER_LAYER = 4 * CHUNKS
PIECES = LAYERS * PER_LAYER
SLOTS = 8
FIRST_SLOTS = 4
LAST_SLOTS = 16
LAG_SUM = 3
LAG_FREE = 5
LAG_LAST = 10
UNIT_STEP = 8
FINAL_STEP = 23
SUMS = 6


def gelu_tanh(pre):
    return jnp.tanh(0.7978845608028654 * (pre + 0.044715 * pre * pre * pre))


def gelu(pre):
    return 0.5 * pre * (1.0 + gelu_tanh(pre))


def gelu_slope(pre):
    tanh_val = gelu_tanh(pre)
    return 0.5 * (1.0 + tanh_val) + 0.5 * pre * (1.0 - tanh_val * tanh_val) * 0.7978845608028654 * (1.0 + 0.134145 * pre * pre)


def kernel(x_ref, h_ref, wu_ref, wd_ref, g_ref, gx_ref, up_ref, down_ref, gb_ref, rxh_ref,
           lt, wd, wu, cbuf, gr, hr, dh, ha, gown, xown, pm, pp, pb, rxo, zp, z1, z2,
           zs, z_r1, z_r2, z_ts, z_tl, z_rt, c1, c2, c3,
           ag_r, ag_p, ag_s, ag_f, ag_l, pp_s, pb_r, pm_s, rx_r, pbc,
           ld_c, ld_g, ld_h, ld_a, ld_w, ld_o, ld_rx, st_gx):
    rows, hidden = gown.shape
    ffn = lt.shape[1]
    half_rows = rows // 2
    cw = hidden // CHUNKS
    fb = ffn // 4
    half_ffn = ffn // 2

    me = lax.axis_index("model")
    spot = lax.axis_index("data")
    core = lax.rem(me, 2)
    px = lax.rem(me // 2, 2)
    py = me // 4
    partner = me + 1 - 2 * core
    step_x, step_y = 2 * (1 - 2 * px), 4 * (1 - 2 * py)
    peers = (me + step_x, me + step_y, me + step_x + step_y)
    is_end = jnp.logical_or(spot == 0, spot == 3)
    is_mid = jnp.logical_not(is_end)
    line_mid = jnp.where(spot < 2, 1, 2)
    line_end = jnp.where(spot < 2, 0, 3)
    line_across = 3 - spot

    def model(i):
        return {"model": i}

    def data(i):
        return {"data": i}

    def signal(sem, where):
        pl.semaphore_signal(sem, inc=1, device_id=where, device_id_type=MESH)

    def remote(src, dst, send, recv, where):
        return pltpu.make_async_remote_copy(src_ref=src, dst_ref=dst, send_sem=send, recv_sem=recv, device_id=where, device_id_type=MESH)

    def take(ref, sem):
        pltpu.make_async_copy(ref, ref, sem).wait()

    def chunk_columns(c):
        return pl.ds(pl.multiple_of(c * cw, cw), cw)

    def row_block(i):
        return pl.ds(pl.multiple_of(i * rows, rows), rows)

    def gather_keep(gid, own):
        for c in range(CHUNKS):
            pltpu.make_async_copy(own.at[:, pl.ds(c * cw, cw)], gb_ref.at[gid, c, row_block(me)], ag_l.at[gid]).start()

    def gather_send(gid, c, own):
        src = own.at[:, chunk_columns(c)]
        dst = gb_ref.at[gid, c, row_block(me)]
        for peer in peers:
            remote(src, dst, ag_s.at[gid], ag_r.at[gid, c], model(peer)).start()
        remote(src, dst, ag_s.at[gid], ag_p.at[gid, c], model(partner)).start()

    def gather_forward(gid, c):
        take(gb_ref.at[gid, c, pl.ds(0, 3 * rows)], ag_r.at[gid, c])
        for peer in peers:
            block = gb_ref.at[gid, c, row_block(peer)]
            remote(block, block, ag_f.at[gid], ag_p.at[gid, c], model(partner)).start()

    def gather_wait(gid, c):
        take(gb_ref.at[gid, c, pl.ds(0, 4 * rows)], ag_p.at[gid, c])

    def chunk_load(gid, c, slot):
        return pltpu.make_async_copy(gb_ref.at[gid, c], cbuf.at[slot], ld_c.at[slot])

    def act_load(layer, b):
        return pltpu.make_async_copy(h_ref.at[layer, row_block(b)], ha, ld_a)

    def act_block(b):
        @pl.loop(0, 4)
        def _(f):
            cols = pl.ds(pl.multiple_of(f * fb, fb), fb)
            a = gelu(ha[:, cols].astype(F32)).astype(BF16).astype(F32)
            lt[0, cols, row_block(b)] = a.T.astype(BF16)

    def weight_loads(layer):
        return (pltpu.make_async_copy(wd_ref.at[layer], wd, ld_w.at[0]), pltpu.make_async_copy(wu_ref.at[layer], wu, ld_w.at[1]))

    def unit_place(u):
        r = lax.rem(u // 2 + 1, 4)
        chip = lax.rem(py + r // 2, 2) * 2 + lax.rem(px + lax.rem(r, 2), 2)
        return r, chip

    def unit_rows(u):
        _, chip = unit_place(u)
        start = (chip * 2 + core) * rows + lax.rem(u, 2) * half_rows
        other = (chip * 2 + 1 - core) * rows + lax.rem(u, 2) * half_rows
        return tuple(pl.ds(pl.multiple_of(s, half_rows), half_rows) for s in (start, other))

    def unit_load(gid, layer, u):
        for n, block in enumerate(unit_rows(u)):
            here = pl.ds(n * half_rows, half_rows)
            for c in range(CHUNKS):
                pltpu.make_async_copy(gb_ref.at[gid, c, block], gr.at[here, pl.ds(c * cw, cw)], ld_g).start()
            pltpu.make_async_copy(h_ref.at[layer, block], hr.at[here], ld_h).start()

    def unit(lp, u):
        order = lp * 8 + u
        slot = lax.rem(order, 2)
        take(gr, ld_g)
        take(hr, ld_h)
        mine, other = unit_rows(u)

        @pl.loop(0, 4)
        def _(f):
            cols = pl.ds(pl.multiple_of(f * fb, fb), fb)
            d_act = lax.dot_general(gr[...], wd[cols, :], NT, preferred_element_type=F32)
            d_pre = (d_act * gelu_slope(hr[:, cols].astype(F32))).astype(BF16)
            dh[:, cols] = d_pre
            flipped = d_pre.astype(F32).T.astype(BF16)
            lt[1, cols, mine] = flipped[:, :half_rows]
            lt[1, cols, other] = flipped[:, half_rows:]

        kept = lax.rem(u, SUMS)

        @pl.when(order >= 2)
        def _():
            take(pp.at[slot], pp_s.at[slot])

        @pl.when(jnp.logical_or(u >= SUMS, jnp.logical_and(lp > 0, u >= 8 - SUMS)))
        def _():
            take(pm.at[kept], pm_s.at[kept])

        @pl.loop(0, CHUNKS)
        def _(d):
            cols = chunk_columns(d)
            part = lax.dot_general(dh[...], wu[cols, :], NT, preferred_element_type=F32).astype(BF16)
            pm[kept, :, cols] = part[:half_rows]
            pp[slot, :, cols] = part[half_rows:]

        @pl.when(order >= 2)
        def _():
            pl.semaphore_wait(pbc, 1)

        remote(pp.at[slot], pb.at[slot], pp_s.at[slot], pb_r.at[slot], model(partner)).start()

    def unit_finish(lp, u):
        order = lp * 8 + u
        slot = lax.rem(order, 2)
        kept = lax.rem(u, SUMS)
        r, chip = unit_place(u)
        here = pl.ds(pl.multiple_of(lax.rem(u, 2) * half_rows, half_rows), half_rows)
        take(pb.at[slot], pb_r.at[slot])

        @pl.when(r != 0)
        def _():
            @pl.loop(0, CHUNKS)
            def _(d):
                cols = chunk_columns(d)
                pm[kept, :, cols] = (pm[kept, :, cols].astype(F32) + pb[slot, :, cols].astype(F32)).astype(BF16)

            remote(pm.at[kept], rxh_ref.at[lp, r - 1, here], pm_s.at[kept], rx_r.at[lp * 6 + (r - 1) * 2 + lax.rem(u, 2)],
                   model(chip * 2 + core)).start()

        @pl.when(r == 0)
        def _():
            @pl.loop(0, CHUNKS)
            def _(d):
                cols = chunk_columns(d)
                rxo[here, cols] = (pm[kept, :, cols].astype(F32) + pb[slot, :, cols].astype(F32)).astype(BF16)

        @pl.when(order < 8 * LAYERS - 2)
        def _():
            signal(pbc, model(partner))

    def new_gradient(lp):
        take(gb_ref.at[2 * lp, pl.ds(0, 4)], ag_s.at[2 * lp])
        part = rows // 4
        for n in range(4):
            here = pl.ds(n * part, part)
            for r in range(3):
                if n % 2 == 0:
                    take(pm.at[0], rx_r.at[lp * 6 + r * 2 + n // 2])
                pltpu.make_async_copy(rxh_ref.at[lp, r, here], gr.at[pl.ds(r * part, part)], ld_rx.at[r]).start()
            for r in range(3):
                take(gr.at[pl.ds(0, part)], ld_rx.at[r])

            @pl.loop(0, CHUNKS)
            def _(d):
                cols = chunk_columns(d)
                total = rxo[here, cols].astype(F32)
                for r in range(3):
                    total += gr[pl.ds(r * part, part), cols].astype(F32)
                gown[here, cols] = (gown[here, cols].astype(F32) + total).astype(BF16)

    def piece_place(i):
        return LAYERS - 1 - i // PER_LAYER, lax.rem(i // (2 * CHUNKS), 2), lax.rem(i, 2 * CHUNKS) // 2, lax.rem(i, 2)

    def piece(i):
        _, phase, c, half = piece_place(i)
        slot = lax.rem(i, SLOTS)
        held = lax.rem(i // 2, 2)

        @pl.when(jnp.logical_and(is_end, i >= SLOTS))
        def _():
            take(zp.at[slot], zs.at[slot])

        part = jnp.dot(lt[phase, pl.ds(pl.multiple_of(half * half_ffn, half_ffn), half_ffn), :], cbuf[held], preferred_element_type=F32)

        @pl.when(phase == 0)
        def _():
            zp[slot] = part

        @pl.when(phase == 1)
        def _():
            zp[slot, :fb, :] = part[:fb].T
            zp[slot, fb:, :] = part[fb:].T

    def finished_copies(j):
        layer, _, c, half = piece_place(j)
        slot = lax.rem(j, SLOTS)
        f0 = half * half_ffn
        down = [(z2.at[slot], down_ref.at[layer, pl.ds(pl.multiple_of(f0, half_ffn), half_ffn), chunk_columns(c)])]
        up = [(z2.at[slot, pl.ds(b * fb, fb)], up_ref.at[layer, chunk_columns(c), pl.ds(pl.multiple_of(f0 + b * fb, fb), fb)]) for b in range(2)]
        return down, up

    def line_step(i):
        @pl.when(is_end)
        def _():
            @pl.when(i < PIECES)
            def _():
                slot, there = lax.rem(i, SLOTS), lax.rem(i, FIRST_SLOTS)

                @pl.when(i >= FIRST_SLOTS)
                def _():
                    pl.semaphore_wait(c1, 1)

                remote(zp.at[slot], z1.at[there], zs.at[slot], z_r1.at[there], data(line_mid)).start()

            j = i - LAG_LAST

            @pl.when(jnp.logical_and(j >= 0, j < PIECES))
            def _():
                take(zp.at[0], z_rt.at[lax.rem(j, LAST_SLOTS)])

                @pl.when(j + LAST_SLOTS < PIECES)
                def _():
                    signal(c3, data(line_mid))

        @pl.when(is_mid)
        def _():
            slot, there = lax.rem(i, SLOTS), lax.rem(i, FIRST_SLOTS)
            j = i - LAG_SUM
            old = lax.rem(j + SLOTS, SLOTS)

            @pl.when(i < PIECES)
            def _():
                take(z1.at[there], z_r1.at[there])
                zp[slot] = zp[slot] + z1[there]

            @pl.when(jnp.logical_and(j >= 0, j < PIECES))
            def _():
                take(z2.at[old], z_r2.at[old])
                z2[old] = z2[old] + zp[old]

            @pl.when(i < PIECES)
            def _():
                @pl.when(i + FIRST_SLOTS < PIECES)
                def _():
                    signal(c1, data(line_end))

                @pl.when(i >= SLOTS)
                def _():
                    pl.semaphore_wait(c2, 1)

                remote(zp.at[slot], z2.at[slot], zs.at[slot], z_r2.at[slot], data(line_across)).start()

            @pl.when(jnp.logical_and(j >= 0, j < PIECES))
            def _():
                take(zp.at[old], zs.at[old])

                @pl.when(j >= LAST_SLOTS)
                def _():
                    pl.semaphore_wait(c3, 1)

                down, up = finished_copies(j)
                _, phase, _, _ = piece_place(j)
                for kind, copies in enumerate((down, up)):
                    @pl.when(phase == kind)
                    def _():
                        for src, dst in copies:
                            remote(src, dst, z_ts.at[old], z_rt.at[lax.rem(j, LAST_SLOTS)], data(line_end)).start()
                            pltpu.make_async_copy(src, dst, z_tl.at[old]).start()

            k = i - LAG_FREE

            @pl.when(jnp.logical_and(k >= 0, k < PIECES))
            def _():
                free = lax.rem(k, SLOTS)
                take(z2.at[free], z_ts.at[free])
                take(z2.at[free], z_tl.at[free])

                @pl.when(k + SLOTS < PIECES)
                def _():
                    signal(c2, data(line_across))

    load_g = pltpu.make_async_copy(g_ref, gown, ld_o)
    load_g.start()
    act_load(LAYERS - 1, 0).start()
    for load in weight_loads(LAYERS - 1):
        load.start()

    barrier = pltpu.get_barrier_semaphore()
    for peer in peers + (partner,):
        signal(barrier, model(peer))

    @pl.when(is_end)
    def _():
        signal(barrier, data(line_mid))
        pl.semaphore_wait(barrier, 5)

    @pl.when(is_mid)
    def _():
        signal(barrier, data(line_end))
        signal(barrier, data(line_across))
        pl.semaphore_wait(barrier, 6)

    load_g.wait()
    for c in range(CHUNKS):
        gather_send(0, c, gown)
    gather_keep(0, gown)

    @pl.loop(0, 8)
    def _(b):
        act_load(LAYERS - 1, 0).wait()
        act_block(b)

        @pl.when(b < 7)
        def _():
            act_load(LAYERS - 1, b + 1).start()

    load_x = pltpu.make_async_copy(x_ref.at[LAYERS - 1], xown, ld_o)
    load_x.start()
    load_x.wait()
    gather_forward(0, 0)
    take(gown, ag_l.at[0])
    gather_wait(0, 0)
    chunk_load(0, 0, 0).start()

    @pl.loop(0, PIECES + LAG_LAST)
    def _(i):
        lp = i // PER_LAYER
        layer = LAYERS - 1 - lp
        il = lax.rem(i, PER_LAYER)
        odd = lax.rem(i, 2) == 1
        ggid, xgid = 2 * lp, 2 * lp + 1
        live = i < PIECES

        @pl.when(live)
        def _():
            @pl.when(jnp.logical_not(odd))
            def _():
                take(cbuf.at[0], ld_c.at[lax.rem(i // 2, 2)])

            piece(i)

        line_step(i)

        def when(cond):
            return pl.when(jnp.logical_and(live, cond))

        @when(jnp.logical_and(lp == 0, jnp.logical_and(il >= 1, il < CHUNKS)))
        def _():
            gather_forward(0, il)

        @when(il == 8)
        def _():
            gather_keep(xgid, xown)
            gather_send(xgid, 0, xown)

        @when(jnp.logical_and(odd, jnp.logical_and(il >= 9, il < 23)))
        def _():
            gather_send(xgid, (il - 7) // 2, xown)

        @when(jnp.logical_and(jnp.logical_not(odd), jnp.logical_and(il >= 14, il < 30)))
        def _():
            gather_forward(xgid, (il - 14) // 2)

        @when(jnp.logical_and(lp == 0, il == 24))
        def _():
            gather_keep(2, gown)

        @when(jnp.logical_and(lp == 0, il >= 24))
        def _():
            gather_send(2, il - 24, gown)

        @when(jnp.logical_and(i >= 27, i < 35))
        def _():
            gather_forward(2, i - 27)

        @when(jnp.logical_and(lp == 0, jnp.logical_and(il >= 1, il < CHUNKS)))
        def _():
            gather_wait(0, il)

        @when(i == 28)
        def _():
            take(gown, ag_l.at[2])

        @when(jnp.logical_and(i >= 28, i < 36))
        def _():
            gather_wait(2, i - 28)

        @when(il == 15)
        def _():
            take(xown, ag_l.at[xgid])

        @when(jnp.logical_and(odd, jnp.logical_and(il >= 15, il < 31)))
        def _():
            gather_wait(xgid, (il - 15) // 2)

        @when(jnp.logical_and(odd, i + 1 < PIECES))
        def _():
            nxt = i + 1
            chunk_load(nxt // (2 * CHUNKS), lax.rem(nxt, 2 * CHUNKS) // 2, lax.rem(nxt // 2, 2)).start()

        @when(jnp.logical_and(il > UNIT_STEP, il <= UNIT_STEP + 8))
        def _():
            unit_finish(lp, il - UNIT_STEP - 1)

        @when(il == UNIT_STEP)
        def _():
            for load in weight_loads(0):
                load.wait()

        @when(jnp.logical_and(il >= UNIT_STEP, il < UNIT_STEP + 8))
        def _():
            unit(lp, il - UNIT_STEP)

        @when(jnp.logical_and(il >= UNIT_STEP - 1, il < UNIT_STEP + 7))
        def _():
            unit_load(ggid, layer, il - UNIT_STEP + 1)

        @when(il == FINAL_STEP)
        def _():
            new_gradient(lp)

        @when(i == PER_LAYER + FINAL_STEP)
        def _():
            pltpu.make_async_copy(gown, gx_ref, st_gx).start()

        @when(jnp.logical_and(lp == 0, il == 17))
        def _():
            for load in weight_loads(0):
                load.start()

        @when(jnp.logical_and(lp == 0, il >= 16))
        def _():
            @pl.when(jnp.logical_not(odd))
            def _():
                act_load(0, (il - 16) // 2).start()

            @pl.when(odd)
            def _():
                act_load(0, 0).wait()
                act_block((il - 16) // 2)

        @when(il == 31)
        def _():
            take(gb_ref.at[xgid, pl.ds(0, 4)], ag_s.at[xgid])

            @pl.when(lp == 0)
            def _():
                load = pltpu.make_async_copy(x_ref.at[0], xown, ld_o)
                load.start()
                load.wait()

    for gid in range(2 * LAYERS):
        take(gb_ref.at[gid, pl.ds(0, 3)], ag_f.at[gid])
    for slot in range(2):
        take(pp.at[slot], pp_s.at[slot])
    for kept in range(8 - SUMS, SUMS):
        take(pm.at[kept], pm_s.at[kept])
    take(gown, st_gx)

    @pl.when(is_end)
    def _():
        for slot in range(SLOTS):
            take(zp.at[slot], zs.at[slot])


def solution(mesh):
    def device_step(x_saved, h_saved, w_up, w_down, grad_out):
        layers, hidden, ffn = w_up.shape
        rows = grad_out.shape[1]
        tokens = h_saved.shape[2]
        cw, half_ffn = hidden // CHUNKS, ffn // 2
        half_rows = rows // 2
        any_space = pl.BlockSpec(memory_space=pl.ANY)
        dma = pltpu.SemaphoreType.DMA
        vmem = pltpu.VMEM
        grad_x, grad_up, grad_down, _, _ = pl.pallas_call(
            kernel,
            name="backward",
            out_shape=(
                jax.ShapeDtypeStruct((rows, hidden), BF16),
                jax.ShapeDtypeStruct(w_up.shape, F32),
                jax.ShapeDtypeStruct(w_down.shape, F32),
                jax.ShapeDtypeStruct((2 * layers, CHUNKS, tokens, cw), BF16),
                jax.ShapeDtypeStruct((layers, 3, rows, hidden), BF16),
            ),
            in_specs=[any_space] * 5,
            out_specs=(any_space,) * 5,
            scratch_shapes=[
                vmem((2, ffn, tokens), BF16),
                vmem((ffn, hidden), BF16),
                vmem((hidden, ffn), BF16),
                vmem((2, tokens, cw), BF16),
                vmem((rows, hidden), BF16),
                vmem((rows, ffn), BF16),
                vmem((rows, ffn), BF16),
                vmem((rows, ffn), BF16),
                vmem((rows, hidden), BF16),
                vmem((rows, hidden), BF16),
                vmem((SUMS, half_rows, hidden), BF16),
                vmem((2, half_rows, hidden), BF16),
                vmem((2, half_rows, hidden), BF16),
                vmem((rows, hidden), BF16),
                vmem((SLOTS, half_ffn, cw), F32),
                vmem((FIRST_SLOTS, half_ffn, cw), F32),
                vmem((SLOTS, half_ffn, cw), F32),
                dma((SLOTS,)), dma((FIRST_SLOTS,)), dma((SLOTS,)), dma((SLOTS,)), dma((SLOTS,)), dma((LAST_SLOTS,)),
                pltpu.SemaphoreType.REGULAR, pltpu.SemaphoreType.REGULAR, pltpu.SemaphoreType.REGULAR,
                dma((2 * layers, CHUNKS)), dma((2 * layers, CHUNKS)), dma((2 * layers,)), dma((2 * layers,)), dma((2 * layers,)),
                dma((2,)), dma((2,)), dma((SUMS,)), dma((6 * layers,)), pltpu.SemaphoreType.REGULAR,
                dma((2,)), dma(()), dma(()), dma(()), dma((2,)), dma(()), dma((3,)), dma(()),
            ],
            compiler_params=pltpu.CompilerParams(collective_id=0, has_side_effects=True, vmem_limit_bytes=67043328),
        )(x_saved[:, 0], h_saved[:, 0], w_up, w_down, grad_out[0])
        return grad_x[None], grad_up, grad_down

    return jax.shard_map(
        device_step,
        mesh=mesh,
        in_specs=(P(None, "data", "model", None), P(None, "data", None, "model"), P(None, None, "model"), P(None, "model", None), P("data", "model", None)),
        out_specs=(P("data", "model", None), P(None, None, "model"), P(None, "model", None)),
        check_vma=False,
    )
```

```python
import functools

import jax
import jax.numpy as jnp
from jax import lax
from jax.experimental import pallas as pl
from jax.experimental.pallas import tpu as pltpu
from jax.sharding import PartitionSpec as P

MESH = pl.DeviceIdType.MESH
F32, BF16 = jnp.float32, jnp.bfloat16
NT = (((1,), (1,)), ((), ()))

LAYERS = 2
CHUNKS = 8
PARTS = 4
PHASE = CHUNKS * PARTS
PER_LAYER = 2 * PHASE
PIECES = LAYERS * PER_LAYER
SLOTS = 16
FIRST_SLOTS = 8
LAST_SLOTS = 32
LAG_SUM = 2
LAG_FREE = 6
LAG_LAST = 20
UNIT_STEP = 8
FINAL_STEP = 46
SUMS = 6


def gelu_tanh(pre):
    return jnp.tanh(0.7978845608028654 * (pre + 0.044715 * pre * pre * pre))


def gelu(pre):
    return 0.5 * pre * (1.0 + gelu_tanh(pre))


def gelu_slope(pre):
    tanh_val = gelu_tanh(pre)
    return 0.5 * (1.0 + tanh_val) + 0.5 * pre * (1.0 - tanh_val * tanh_val) * 0.7978845608028654 * (1.0 + 0.134145 * pre * pre)


def kernel(x_ref, h_ref, wu_ref, wd_ref, g_ref, gx_ref, up_ref, down_ref, gb_ref, rxh_ref,
           lt, wd, wu, cbuf, gr, hr, dh, ha, gown, xown, pm, pp, pb, rxo, zp, z1, z2,
           zs, z_r1, z_r2, z_ts, z_tl, z_rt, c1, c2, c3,
           ag_r, ag_p, ag_s, ag_f, ag_l, pp_s, pb_r, pm_s, rx_r, pbc,
           ld_c, ld_g, ld_h, ld_a, ld_w, ld_o, ld_rx, st_gx):
    rows, hidden = gown.shape
    ffn = lt.shape[1]
    half_rows = rows // 2
    cw = hidden // CHUNKS
    fb = ffn // 4

    me = lax.axis_index("model")
    spot = lax.axis_index("data")
    core = lax.rem(me, 2)
    px = lax.rem(me // 2, 2)
    py = me // 4
    partner = me + 1 - 2 * core
    step_x, step_y = 2 * (1 - 2 * px), 4 * (1 - 2 * py)
    peers = (me + step_x, me + step_y, me + step_x + step_y)
    is_end = jnp.logical_or(spot == 0, spot == 3)
    is_mid = jnp.logical_not(is_end)
    line_mid = jnp.where(spot < 2, 1, 2)
    line_end = jnp.where(spot < 2, 0, 3)
    line_across = 3 - spot

    def model(i):
        return {"model": i}

    def data(i):
        return {"data": i}

    def signal(sem, where):
        pl.semaphore_signal(sem, inc=1, device_id=where, device_id_type=MESH)

    def remote(src, dst, send, recv, where):
        return pltpu.make_async_remote_copy(src_ref=src, dst_ref=dst, send_sem=send, recv_sem=recv, device_id=where, device_id_type=MESH)

    def take(ref, sem):
        pltpu.make_async_copy(ref, ref, sem).wait()

    def chunk_columns(c):
        return pl.ds(pl.multiple_of(c * cw, cw), cw)

    def row_block(i):
        return pl.ds(pl.multiple_of(i * rows, rows), rows)

    def gather_keep(gid, own):
        for c in range(CHUNKS):
            pltpu.make_async_copy(own.at[:, pl.ds(c * cw, cw)], gb_ref.at[gid, c, row_block(me)], ag_l.at[gid]).start()

    def gather_send(gid, c, own):
        src = own.at[:, chunk_columns(c)]
        dst = gb_ref.at[gid, c, row_block(me)]
        for peer in peers:
            remote(src, dst, ag_s.at[gid], ag_r.at[gid, c], model(peer)).start()
        remote(src, dst, ag_s.at[gid], ag_p.at[gid, c], model(partner)).start()

    def gather_forward(gid, c):
        take(gb_ref.at[gid, c, pl.ds(0, 3 * rows)], ag_r.at[gid, c])
        for peer in peers:
            block = gb_ref.at[gid, c, row_block(peer)]
            remote(block, block, ag_f.at[gid], ag_p.at[gid, c], model(partner)).start()

    def gather_wait(gid, c):
        take(gb_ref.at[gid, c, pl.ds(0, 4 * rows)], ag_p.at[gid, c])

    def chunk_load(gid, c, slot):
        return pltpu.make_async_copy(gb_ref.at[gid, c], cbuf.at[slot], ld_c.at[slot])

    def act_load(layer, b, ref, sem):
        return pltpu.make_async_copy(h_ref.at[layer, row_block(b)], ref, sem)

    def act_block(b, ref):
        @pl.loop(0, 4)
        def _(f):
            cols = pl.ds(pl.multiple_of(f * fb, fb), fb)
            a = gelu(ref[:, cols].astype(F32)).astype(BF16).astype(F32)
            lt[0, cols, row_block(b)] = a.T.astype(BF16)

    def weight_loads(layer):
        return (pltpu.make_async_copy(wd_ref.at[layer], wd, ld_w.at[0]), pltpu.make_async_copy(wu_ref.at[layer], wu, ld_w.at[1]))

    def unit_place(u):
        r = lax.rem(u // 2 + 1, 4)
        chip = lax.rem(py + r // 2, 2) * 2 + lax.rem(px + lax.rem(r, 2), 2)
        return r, chip

    def unit_rows(u):
        _, chip = unit_place(u)
        start = (chip * 2 + core) * rows + lax.rem(u, 2) * half_rows
        other = (chip * 2 + 1 - core) * rows + lax.rem(u, 2) * half_rows
        return tuple(pl.ds(pl.multiple_of(s, half_rows), half_rows) for s in (start, other))

    def unit_load(gid, layer, u):
        for n, block in enumerate(unit_rows(u)):
            here = pl.ds(n * half_rows, half_rows)
            for c in range(CHUNKS):
                pltpu.make_async_copy(gb_ref.at[gid, c, block], gr.at[here, pl.ds(c * cw, cw)], ld_g).start()
            pltpu.make_async_copy(h_ref.at[layer, block], hr.at[here], ld_h).start()

    def unit_first(u):
        take(gr, ld_g)
        take(hr, ld_h)
        mine, other = unit_rows(u)

        @pl.loop(0, 4)
        def _(f):
            cols = pl.ds(pl.multiple_of(f * fb, fb), fb)
            d_act = lax.dot_general(gr[...], wd[cols, :], NT, preferred_element_type=F32)
            d_pre = (d_act * gelu_slope(hr[:, cols].astype(F32))).astype(BF16)
            dh[:, cols] = d_pre
            flipped = d_pre.astype(F32).T.astype(BF16)
            lt[1, cols, mine] = flipped[:, :half_rows]
            lt[1, cols, other] = flipped[:, half_rows:]

    def unit_second(lp, u):
        order = lp * 8 + u
        slot = lax.rem(order, 2)
        kept = lax.rem(u, SUMS)

        @pl.when(order >= 2)
        def _():
            take(pp.at[slot], pp_s.at[slot])

        @pl.when(jnp.logical_or(u >= SUMS, jnp.logical_and(lp > 0, u >= 8 - SUMS)))
        def _():
            take(pm.at[kept], pm_s.at[kept])

        @pl.loop(0, CHUNKS)
        def _(d):
            cols = chunk_columns(d)
            part = lax.dot_general(dh[...], wu[cols, :], NT, preferred_element_type=F32).astype(BF16)
            pm[kept, :, cols] = part[:half_rows]
            pp[slot, :, cols] = part[half_rows:]

        @pl.when(order >= 2)
        def _():
            pl.semaphore_wait(pbc, 1)

        remote(pp.at[slot], pb.at[slot], pp_s.at[slot], pb_r.at[slot], model(partner)).start()

    def unit_finish(lp, u):
        order = lp * 8 + u
        slot = lax.rem(order, 2)
        kept = lax.rem(u, SUMS)
        r, chip = unit_place(u)
        here = pl.ds(pl.multiple_of(lax.rem(u, 2) * half_rows, half_rows), half_rows)
        take(pb.at[slot], pb_r.at[slot])

        @pl.when(r != 0)
        def _():
            @pl.loop(0, CHUNKS)
            def _(d):
                cols = chunk_columns(d)
                pm[kept, :, cols] = (pm[kept, :, cols].astype(F32) + pb[slot, :, cols].astype(F32)).astype(BF16)

            remote(pm.at[kept], rxh_ref.at[lp, r - 1, here], pm_s.at[kept], rx_r.at[lp * 6 + (r - 1) * 2 + lax.rem(u, 2)],
                   model(chip * 2 + core)).start()

        @pl.when(r == 0)
        def _():
            @pl.loop(0, CHUNKS)
            def _(d):
                cols = chunk_columns(d)
                rxo[here, cols] = (pm[kept, :, cols].astype(F32) + pb[slot, :, cols].astype(F32)).astype(BF16)

        @pl.when(order < 8 * LAYERS - 2)
        def _():
            signal(pbc, model(partner))

    def quarter(n):
        part = rows // 4
        return pl.ds(pl.multiple_of(n * part, part), part)

    def new_gradient_load(lp, n):
        @pl.when(lax.rem(n, 2) == 0)
        def _():
            for r in range(3):
                take(pm.at[0], rx_r.at[lp * 6 + r * 2 + n // 2])

        for r in range(3):
            pltpu.make_async_copy(rxh_ref.at[lp, r, quarter(n)], gr.at[quarter(r)], ld_rx.at[r]).start()

    def new_gradient(n):
        for r in range(3):
            take(gr.at[quarter(0)], ld_rx.at[r])

        @pl.loop(0, CHUNKS)
        def _(d):
            cols = chunk_columns(d)
            total = rxo[quarter(n), cols].astype(F32)
            for r in range(3):
                total += gr[quarter(r), cols].astype(F32)
            gown[quarter(n), cols] = (gown[quarter(n), cols].astype(F32) + total).astype(BF16)

    def piece_place(i):
        return LAYERS - 1 - i // PER_LAYER, lax.rem(i // PHASE, 2), lax.rem(i, PHASE) // PARTS, lax.rem(i, PARTS)

    def part_columns(n):
        return pl.ds(pl.multiple_of(n * fb, fb), fb)

    def piece(i):
        _, phase, _, n = piece_place(i)
        slot = lax.rem(i, SLOTS)

        @pl.when(jnp.logical_and(is_end, i >= SLOTS))
        def _():
            take(zp.at[slot], zs.at[slot])

        part = jnp.dot(lt[phase, part_columns(n), :], cbuf[lax.rem(i // PARTS, 2)], preferred_element_type=F32)

        @pl.when(phase == 0)
        def _():
            zp[slot] = part

        @pl.when(phase == 1)
        def _():
            zp[slot] = part.T

    def total_place(j):
        layer, _, c, n = piece_place(j)
        return down_ref.at[layer, part_columns(n), chunk_columns(c)], up_ref.at[layer, chunk_columns(c), part_columns(n)]

    def line_step(i):
        @pl.when(is_end)
        def _():
            @pl.when(i < PIECES)
            def _():
                slot, there = lax.rem(i, SLOTS), lax.rem(i, FIRST_SLOTS)

                @pl.when(i >= FIRST_SLOTS)
                def _():
                    pl.semaphore_wait(c1, 1)

                remote(zp.at[slot], z1.at[there], zs.at[slot], z_r1.at[there], data(line_mid)).start()

            j = i - LAG_LAST

            @pl.when(jnp.logical_and(j >= 0, j < PIECES))
            def _():
                take(zp.at[0], z_rt.at[lax.rem(j, LAST_SLOTS)])

                @pl.when(j + LAST_SLOTS < PIECES)
                def _():
                    signal(c3, data(line_mid))

        @pl.when(is_mid)
        def _():
            slot, there = lax.rem(i, SLOTS), lax.rem(i, FIRST_SLOTS)
            j = i - LAG_SUM
            old = lax.rem(j + SLOTS, SLOTS)

            @pl.when(jnp.logical_and(j >= 0, j < PIECES))
            def _():
                take(z2.at[old], z_r2.at[old])
                z2[old] = z2[old] + zp[old]
                take(zp.at[old], zs.at[old])

                @pl.when(j >= LAST_SLOTS)
                def _():
                    pl.semaphore_wait(c3, 1)

            @pl.when(i < PIECES)
            def _():
                take(z1.at[there], z_r1.at[there])
                zp[slot] = zp[slot] + z1[there]

            @pl.when(jnp.logical_and(j >= 0, j < PIECES))
            def _():
                _, phase, _, _ = piece_place(j)
                for kind, place in enumerate(total_place(j)):
                    @pl.when(phase == kind)
                    def _():
                        remote(z2.at[old], place, z_ts.at[old], z_rt.at[lax.rem(j, LAST_SLOTS)], data(line_end)).start()
                        pltpu.make_async_copy(z2.at[old], place, z_tl.at[old]).start()

            @pl.when(i < PIECES)
            def _():
                @pl.when(i + FIRST_SLOTS < PIECES)
                def _():
                    signal(c1, data(line_end))

                @pl.when(i >= SLOTS)
                def _():
                    pl.semaphore_wait(c2, 1)

                remote(zp.at[slot], z2.at[slot], zs.at[slot], z_r2.at[slot], data(line_across)).start()

            k = i - LAG_FREE

            @pl.when(jnp.logical_and(k >= 0, k < PIECES))
            def _():
                free = lax.rem(k, SLOTS)
                take(z2.at[free], z_ts.at[free])
                take(z2.at[free], z_tl.at[free])

                @pl.when(k + SLOTS < PIECES)
                def _():
                    signal(c2, data(line_across))

    top = LAYERS - 1
    load_g = pltpu.make_async_copy(g_ref, gown, ld_o)
    load_g.start()
    held = ((ha, ld_a), (hr, ld_h))
    for n, (ref, sem) in enumerate(held):
        act_load(top, n, ref, sem).start()
    barrier = pltpu.get_barrier_semaphore()
    for peer in peers + (partner,):
        signal(barrier, model(peer))

    @pl.when(is_end)
    def _():
        signal(barrier, data(line_mid))
        pl.semaphore_wait(barrier, 5)

    @pl.when(is_mid)
    def _():
        signal(barrier, data(line_end))
        signal(barrier, data(line_across))
        pl.semaphore_wait(barrier, 6)

    load_g.wait()
    for c in range(CHUNKS):
        gather_send(0, c, gown)
    gather_keep(0, gown)
    load_x = pltpu.make_async_copy(x_ref.at[top], xown, ld_o)
    load_x.start()
    for load in weight_loads(top):
        load.start()

    @pl.loop(0, 4)
    def _(b):
        for n, (ref, sem) in enumerate(held):
            act_load(top, 0, ref, sem).wait()
            act_block(2 * b + n, ref)

            @pl.when(b < 3)
            def _():
                act_load(top, 2 * b + n + 2, ref, sem).start()

    load_x.wait()
    take(gown, ag_l.at[0])
    gather_forward(0, 0)
    gather_wait(0, 0)
    chunk_load(0, 0, 0).start()

    @pl.loop(0, PIECES + LAG_LAST)
    def _(i):
        lp = i // PER_LAYER
        layer = LAYERS - 1 - lp
        s = i // 2
        sl = lax.rem(s, PER_LAYER // 2)
        il = lax.rem(i, PER_LAYER)
        even = lax.rem(i, 2) == 0
        odd = jnp.logical_not(even)
        odd_pair = lax.rem(s, 2) == 1
        ggid, xgid = 2 * lp, 2 * lp + 1
        live = i < PIECES

        @pl.when(live)
        def _():
            @pl.when(lax.rem(i, PARTS) == 0)
            def _():
                take(cbuf.at[0], ld_c.at[lax.rem(i // PARTS, 2)])

            piece(i)

        line_step(i)

        def when(*conds):
            return pl.when(functools.reduce(jnp.logical_and, conds, live))

        @when(even, s >= 1, s < CHUNKS)
        def _():
            gather_forward(0, s)

        @when(odd, s >= 1, s < CHUNKS)
        def _():
            gather_wait(0, s)

        @when(even, sl == 8)
        def _():
            gather_keep(xgid, xown)
            gather_send(xgid, 0, xown)

        @when(even, odd_pair, sl >= 9, sl < 23)
        def _():
            gather_send(xgid, (sl - 7) // 2, xown)

        @when(even, jnp.logical_not(odd_pair), sl >= 14, sl < 30)
        def _():
            gather_forward(xgid, (sl - 14) // 2)

        @when(odd, sl == 15)
        def _():
            take(xown, ag_l.at[xgid])

        @when(odd, odd_pair, sl >= 15, sl < 31)
        def _():
            gather_wait(xgid, (sl - 15) // 2)

        @when(even, s == 25)
        def _():
            gather_keep(2, gown)

        @when(even, s >= 25, s < 25 + CHUNKS)
        def _():
            gather_send(2, s - 25, gown)

        @when(even, s >= 28, s < 28 + CHUNKS)
        def _():
            gather_forward(2, s - 28)

        @when(odd, s == 29)
        def _():
            take(gown, ag_l.at[2])

        @when(odd, s >= 29, s < 29 + CHUNKS)
        def _():
            gather_wait(2, s - 29)

        @when(lax.rem(i, PARTS) == PARTS - 1, i + 1 < PIECES)
        def _():
            nxt = i + 1
            chunk_load(nxt // PHASE, lax.rem(nxt, PHASE) // PARTS, lax.rem(nxt // PARTS, 2)).start()

        @when(even, sl == UNIT_STEP)
        def _():
            for load in weight_loads(0):
                load.wait()

        @when(even, sl >= UNIT_STEP, sl < UNIT_STEP + 8)
        def _():
            unit_first(sl - UNIT_STEP)

        @when(even, sl > UNIT_STEP, sl <= UNIT_STEP + 8)
        def _():
            unit_finish(lp, sl - UNIT_STEP - 1)

        @when(odd, sl >= UNIT_STEP - 1, sl < UNIT_STEP + 7)
        def _():
            unit_load(ggid, layer, sl - UNIT_STEP + 1)

        @when(odd, sl >= UNIT_STEP, sl < UNIT_STEP + 8)
        def _():
            unit_second(lp, sl - UNIT_STEP)

        @when(il == FINAL_STEP - 1)
        def _():
            take(gb_ref.at[ggid, pl.ds(0, 4)], ag_s.at[ggid])
            new_gradient_load(lp, 0)

        @when(il >= FINAL_STEP, il < FINAL_STEP + 4)
        def _():
            new_gradient(il - FINAL_STEP)

            @pl.when(il < FINAL_STEP + 3)
            def _():
                new_gradient_load(lp, il - FINAL_STEP + 1)

        @when(i == PER_LAYER + FINAL_STEP + 4)
        def _():
            pltpu.make_async_copy(gown, gx_ref, st_gx).start()

        @when(lp == 0, even, sl == 17)
        def _():
            for load in weight_loads(0):
                load.start()

        @when(lp == 0, even, jnp.logical_not(odd_pair), sl >= 16)
        def _():
            act_load(0, (sl - 16) // 2, ha, ld_a).start()

        @when(lp == 0, odd, odd_pair, sl >= 16)
        def _():
            act_load(0, 0, ha, ld_a).wait()
            act_block((sl - 16) // 2, ha)

        @when(even, sl == 31)
        def _():
            take(gb_ref.at[xgid, pl.ds(0, 4)], ag_s.at[xgid])

            @pl.when(lp == 0)
            def _():
                pltpu.make_async_copy(x_ref.at[0], xown, ld_o).start()

        @when(lp == 0, odd, sl == 31)
        def _():
            pltpu.make_async_copy(x_ref.at[0], xown, ld_o).wait()

    for gid in range(2 * LAYERS):
        take(gb_ref.at[gid, pl.ds(0, 3)], ag_f.at[gid])
    for slot in range(2):
        take(pp.at[slot], pp_s.at[slot])
    for kept in range(8 - SUMS, SUMS):
        take(pm.at[kept], pm_s.at[kept])
    take(gown, st_gx)

    @pl.when(is_end)
    def _():
        for slot in range(SLOTS):
            take(zp.at[slot], zs.at[slot])


def solution(mesh):
    def device_step(x_saved, h_saved, w_up, w_down, grad_out):
        layers, hidden, ffn = w_up.shape
        rows = grad_out.shape[1]
        tokens = h_saved.shape[2]
        cw, fb = hidden // CHUNKS, ffn // PARTS
        half_rows = rows // 2
        any_space = pl.BlockSpec(memory_space=pl.ANY)
        dma = pltpu.SemaphoreType.DMA
        vmem = pltpu.VMEM
        grad_x, grad_up, grad_down, _, _ = pl.pallas_call(
            kernel,
            name="backward",
            out_shape=(
                jax.ShapeDtypeStruct((rows, hidden), BF16),
                jax.ShapeDtypeStruct(w_up.shape, F32),
                jax.ShapeDtypeStruct(w_down.shape, F32),
                jax.ShapeDtypeStruct((2 * layers, CHUNKS, tokens, cw), BF16),
                jax.ShapeDtypeStruct((layers, 3, rows, hidden), BF16),
            ),
            in_specs=[any_space] * 5,
            out_specs=(any_space,) * 5,
            scratch_shapes=[
                vmem((2, ffn, tokens), BF16),
                vmem((ffn, hidden), BF16),
                vmem((hidden, ffn), BF16),
                vmem((2, tokens, cw), BF16),
                vmem((rows, hidden), BF16),
                vmem((rows, ffn), BF16),
                vmem((rows, ffn), BF16),
                vmem((rows, ffn), BF16),
                vmem((rows, hidden), BF16),
                vmem((rows, hidden), BF16),
                vmem((SUMS, half_rows, hidden), BF16),
                vmem((2, half_rows, hidden), BF16),
                vmem((2, half_rows, hidden), BF16),
                vmem((rows, hidden), BF16),
                vmem((SLOTS, fb, cw), F32),
                vmem((FIRST_SLOTS, fb, cw), F32),
                vmem((SLOTS, fb, cw), F32),
                dma((SLOTS,)), dma((FIRST_SLOTS,)), dma((SLOTS,)), dma((SLOTS,)), dma((SLOTS,)), dma((LAST_SLOTS,)),
                pltpu.SemaphoreType.REGULAR, pltpu.SemaphoreType.REGULAR, pltpu.SemaphoreType.REGULAR,
                dma((2 * layers, CHUNKS)), dma((2 * layers, CHUNKS)), dma((2 * layers,)), dma((2 * layers,)), dma((2 * layers,)),
                dma((2,)), dma((2,)), dma((SUMS,)), dma((6 * layers,)), pltpu.SemaphoreType.REGULAR,
                dma((2,)), dma(()), dma(()), dma(()), dma((2,)), dma(()), dma((3,)), dma(()),
            ],
            compiler_params=pltpu.CompilerParams(collective_id=0, has_side_effects=True, vmem_limit_bytes=67043328),
        )(x_saved[:, 0], h_saved[:, 0], w_up, w_down, grad_out[0])
        return grad_x[None], grad_up, grad_down

    return jax.shard_map(
        device_step,
        mesh=mesh,
        in_specs=(P(None, "data", "model", None), P(None, "data", None, "model"), P(None, None, "model"), P(None, "model", None), P("data", "model", None)),
        out_specs=(P("data", "model", None), P(None, None, "model"), P(None, "model", None)),
        check_vma=False,
    )
```

```python
import functools

import jax
import jax.numpy as jnp
from jax import lax
from jax.experimental import pallas as pl
from jax.experimental.pallas import tpu as pltpu
from jax.sharding import PartitionSpec as P

MESH = pl.DeviceIdType.MESH
F32, BF16 = jnp.float32, jnp.bfloat16
NT = (((1,), (1,)), ((), ()))

LAYERS = 2
CHUNKS = 8
PARTS = 4
PHASE = CHUNKS * PARTS
PER_LAYER = 2 * PHASE
PIECES = LAYERS * PER_LAYER
SLOTS = 16
FIRST_SLOTS = 8
LAST_SLOTS = 32
LAG_SUM = 2
LAG_FREE = 6
LAG_LAST = 20
UNIT_STEP = 8
FINAL_STEP = 46
SUMS = 6


def gelu_tanh(pre):
    return jnp.tanh(0.7978845608028654 * (pre + 0.044715 * pre * pre * pre))


def gelu(pre):
    return 0.5 * pre * (1.0 + gelu_tanh(pre))


def gelu_slope(pre):
    tanh_val = gelu_tanh(pre)
    return 0.5 * (1.0 + tanh_val) + 0.5 * pre * (1.0 - tanh_val * tanh_val) * 0.7978845608028654 * (1.0 + 0.134145 * pre * pre)


def kernel(x_ref, h_ref, wu_ref, wd_ref, g_ref, gx_ref, up_ref, down_ref, gb_ref, rxh_ref,
           lt, wd, wu, cbuf, gr, hr, dh, ha, gown, xown, pm, pp, pb, rxo, zp, z1, z2,
           zs, z_r1, z_r2, z_ts, z_tl, z_rt, c1, c2, c3,
           ag_x, ag_y, ag_d, ag_p, ag_s, ag_f, ag_l, pp_s, pb_r, pm_s, rx_r, pbc,
           ld_c, ld_g, ld_h, ld_a, ld_w, ld_o, ld_rx, st_gx):
    rows, hidden = gown.shape
    ffn = lt.shape[1]
    half_rows = rows // 2
    cw = hidden // CHUNKS
    fb = ffn // 4

    me = lax.axis_index("model")
    spot = lax.axis_index("data")
    core = lax.rem(me, 2)
    px = lax.rem(me // 2, 2)
    py = me // 4
    partner = me + 1 - 2 * core
    step_x, step_y = 2 * (1 - 2 * px), 4 * (1 - 2 * py)
    near_x, near_y, far = me + step_x, me + step_y, me + step_x + step_y
    is_end = jnp.logical_or(spot == 0, spot == 3)
    is_mid = jnp.logical_not(is_end)
    line_mid = jnp.where(spot < 2, 1, 2)
    line_end = jnp.where(spot < 2, 0, 3)
    line_across = 3 - spot

    def model(i):
        return {"model": i}

    def data(i):
        return {"data": i}

    def signal(sem, where):
        pl.semaphore_signal(sem, inc=1, device_id=where, device_id_type=MESH)

    def remote(src, dst, send, recv, where):
        return pltpu.make_async_remote_copy(src_ref=src, dst_ref=dst, send_sem=send, recv_sem=recv, device_id=where, device_id_type=MESH)

    def take(ref, sem):
        pltpu.make_async_copy(ref, ref, sem).wait()

    def chunk_columns(c):
        return pl.ds(pl.multiple_of(c * cw, cw), cw)

    def row_block(i):
        return pl.ds(pl.multiple_of(i * rows, rows), rows)

    def gather_keep(gid, own):
        for c in range(CHUNKS):
            pltpu.make_async_copy(own.at[:, pl.ds(c * cw, cw)], gb_ref.at[gid, c, row_block(me)], ag_l.at[gid]).start()

    def gather_send(gid, c, own):
        src = own.at[:, chunk_columns(c)]
        dst = gb_ref.at[gid, c, row_block(me)]
        remote(src, dst, ag_s.at[gid], ag_x.at[gid, c], model(near_x)).start()
        remote(src, dst, ag_s.at[gid], ag_y.at[gid, c], model(near_y)).start()
        remote(src, dst, ag_s.at[gid], ag_p.at[gid, c], model(partner)).start()

    def gather_relay(gid, c):
        take(gb_ref.at[gid, c, row_block(0)], ag_x.at[gid, c])
        take(gb_ref.at[gid, c, row_block(0)], ag_y.at[gid, c])
        for n, (source, target) in enumerate(((near_x, near_y), (near_y, near_x))):
            @pl.when(core == n)
            def _():
                block = gb_ref.at[gid, c, row_block(source)]
                remote(block, block, ag_s.at[gid], ag_d.at[gid, c], model(target)).start()

    def gather_forward(gid, c):
        take(gb_ref.at[gid, c, row_block(0)], ag_d.at[gid, c])
        for peer in (near_x, near_y, far):
            block = gb_ref.at[gid, c, row_block(peer)]
            remote(block, block, ag_f.at[gid], ag_p.at[gid, c], model(partner)).start()

    def gather_wait(gid, c):
        take(gb_ref.at[gid, c, pl.ds(0, 4 * rows)], ag_p.at[gid, c])

    def chunk_load(gid, c, slot):
        return pltpu.make_async_copy(gb_ref.at[gid, c], cbuf.at[slot], ld_c.at[slot])

    def act_load(layer, b, ref, sem):
        return pltpu.make_async_copy(h_ref.at[layer, row_block(b)], ref, sem)

    def act_block(b, ref):
        @pl.loop(0, 4)
        def _(f):
            cols = pl.ds(pl.multiple_of(f * fb, fb), fb)
            a = gelu(ref[:, cols].astype(F32)).astype(BF16).astype(F32)
            lt[0, cols, row_block(b)] = a.T.astype(BF16)

    def weight_loads(layer):
        return (pltpu.make_async_copy(wd_ref.at[layer], wd, ld_w.at[0]), pltpu.make_async_copy(wu_ref.at[layer], wu, ld_w.at[1]))

    def unit_place(u):
        r = lax.rem(u // 2 + 1, 4)
        chip = lax.rem(py + r // 2, 2) * 2 + lax.rem(px + lax.rem(r, 2), 2)
        return r, chip

    def unit_rows(u):
        _, chip = unit_place(u)
        start = (chip * 2 + core) * rows + lax.rem(u, 2) * half_rows
        other = (chip * 2 + 1 - core) * rows + lax.rem(u, 2) * half_rows
        return tuple(pl.ds(pl.multiple_of(s, half_rows), half_rows) for s in (start, other))

    def unit_load(gid, layer, u):
        for n, block in enumerate(unit_rows(u)):
            here = pl.ds(n * half_rows, half_rows)
            for c in range(CHUNKS):
                pltpu.make_async_copy(gb_ref.at[gid, c, block], gr.at[here, pl.ds(c * cw, cw)], ld_g).start()
            pltpu.make_async_copy(h_ref.at[layer, block], hr.at[here], ld_h).start()

    def unit_first(u):
        take(gr, ld_g)
        take(hr, ld_h)
        mine, other = unit_rows(u)

        @pl.loop(0, 4)
        def _(f):
            cols = pl.ds(pl.multiple_of(f * fb, fb), fb)
            d_act = lax.dot_general(gr[...], wd[cols, :], NT, preferred_element_type=F32)
            d_pre = (d_act * gelu_slope(hr[:, cols].astype(F32))).astype(BF16)
            dh[:, cols] = d_pre
            flipped = d_pre.astype(F32).T.astype(BF16)
            lt[1, cols, mine] = flipped[:, :half_rows]
            lt[1, cols, other] = flipped[:, half_rows:]

    def unit_second(lp, u):
        order = lp * 8 + u
        slot = lax.rem(order, 2)
        kept = lax.rem(u, SUMS)

        @pl.when(order >= 2)
        def _():
            take(pp.at[slot], pp_s.at[slot])

        @pl.when(jnp.logical_or(u >= SUMS, jnp.logical_and(lp > 0, u >= 8 - SUMS)))
        def _():
            take(pm.at[kept], pm_s.at[kept])

        @pl.loop(0, CHUNKS)
        def _(d):
            cols = chunk_columns(d)
            part = lax.dot_general(dh[...], wu[cols, :], NT, preferred_element_type=F32).astype(BF16)
            pm[kept, :, cols] = part[:half_rows]
            pp[slot, :, cols] = part[half_rows:]

        @pl.when(order >= 2)
        def _():
            pl.semaphore_wait(pbc, 1)

        remote(pp.at[slot], pb.at[slot], pp_s.at[slot], pb_r.at[slot], model(partner)).start()

    def unit_finish(lp, u):
        order = lp * 8 + u
        slot = lax.rem(order, 2)
        kept = lax.rem(u, SUMS)
        r, chip = unit_place(u)
        here = pl.ds(pl.multiple_of(lax.rem(u, 2) * half_rows, half_rows), half_rows)
        take(pb.at[slot], pb_r.at[slot])

        @pl.when(r != 0)
        def _():
            @pl.loop(0, CHUNKS)
            def _(d):
                cols = chunk_columns(d)
                pm[kept, :, cols] = (pm[kept, :, cols].astype(F32) + pb[slot, :, cols].astype(F32)).astype(BF16)

            remote(pm.at[kept], rxh_ref.at[lp, r - 1, here], pm_s.at[kept], rx_r.at[lp * 6 + (r - 1) * 2 + lax.rem(u, 2)],
                   model(chip * 2 + core)).start()

        @pl.when(r == 0)
        def _():
            @pl.loop(0, CHUNKS)
            def _(d):
                cols = chunk_columns(d)
                rxo[here, cols] = (pm[kept, :, cols].astype(F32) + pb[slot, :, cols].astype(F32)).astype(BF16)

        @pl.when(order < 8 * LAYERS - 2)
        def _():
            signal(pbc, model(partner))

    def quarter(n):
        part = rows // 4
        return pl.ds(pl.multiple_of(n * part, part), part)

    def new_gradient_load(lp, n):
        @pl.when(lax.rem(n, 2) == 0)
        def _():
            for r in range(3):
                take(pm.at[0], rx_r.at[lp * 6 + r * 2 + n // 2])

        for r in range(3):
            pltpu.make_async_copy(rxh_ref.at[lp, r, quarter(n)], gr.at[quarter(r)], ld_rx.at[r]).start()

    def new_gradient(n):
        for r in range(3):
            take(gr.at[quarter(0)], ld_rx.at[r])

        @pl.loop(0, CHUNKS)
        def _(d):
            cols = chunk_columns(d)
            total = rxo[quarter(n), cols].astype(F32)
            for r in range(3):
                total += gr[quarter(r), cols].astype(F32)
            gown[quarter(n), cols] = (gown[quarter(n), cols].astype(F32) + total).astype(BF16)

    def piece_place(i):
        return LAYERS - 1 - i // PER_LAYER, lax.rem(i // PHASE, 2), lax.rem(i, PHASE) // PARTS, lax.rem(i, PARTS)

    def part_columns(n):
        return pl.ds(pl.multiple_of(n * fb, fb), fb)

    def piece(i):
        _, phase, _, n = piece_place(i)
        slot = lax.rem(i, SLOTS)

        @pl.when(jnp.logical_and(is_end, i >= SLOTS))
        def _():
            take(zp.at[slot], zs.at[slot])

        part = jnp.dot(lt[phase, part_columns(n), :], cbuf[lax.rem(i // PARTS, 2)], preferred_element_type=F32)

        @pl.when(phase == 0)
        def _():
            zp[slot] = part

        @pl.when(phase == 1)
        def _():
            zp[slot] = part.T

    def total_place(j):
        layer, _, c, n = piece_place(j)
        return down_ref.at[layer, part_columns(n), chunk_columns(c)], up_ref.at[layer, chunk_columns(c), part_columns(n)]

    def line_step(i):
        @pl.when(is_end)
        def _():
            @pl.when(i < PIECES)
            def _():
                slot, there = lax.rem(i, SLOTS), lax.rem(i, FIRST_SLOTS)

                @pl.when(i >= FIRST_SLOTS)
                def _():
                    pl.semaphore_wait(c1, 1)

                remote(zp.at[slot], z1.at[there], zs.at[slot], z_r1.at[there], data(line_mid)).start()

            j = i - LAG_LAST

            @pl.when(jnp.logical_and(j >= 0, j < PIECES))
            def _():
                take(zp.at[0], z_rt.at[lax.rem(j, LAST_SLOTS)])

                @pl.when(j + LAST_SLOTS < PIECES)
                def _():
                    signal(c3, data(line_mid))

        @pl.when(is_mid)
        def _():
            slot, there = lax.rem(i, SLOTS), lax.rem(i, FIRST_SLOTS)
            j = i - LAG_SUM
            old = lax.rem(j + SLOTS, SLOTS)

            @pl.when(jnp.logical_and(j >= 0, j < PIECES))
            def _():
                take(z2.at[old], z_r2.at[old])
                z2[old] = z2[old] + zp[old]
                take(zp.at[old], zs.at[old])

                @pl.when(j >= LAST_SLOTS)
                def _():
                    pl.semaphore_wait(c3, 1)

            @pl.when(i < PIECES)
            def _():
                take(z1.at[there], z_r1.at[there])
                zp[slot] = zp[slot] + z1[there]

            @pl.when(jnp.logical_and(j >= 0, j < PIECES))
            def _():
                _, phase, _, _ = piece_place(j)
                for kind, place in enumerate(total_place(j)):
                    @pl.when(phase == kind)
                    def _():
                        remote(z2.at[old], place, z_ts.at[old], z_rt.at[lax.rem(j, LAST_SLOTS)], data(line_end)).start()
                        pltpu.make_async_copy(z2.at[old], place, z_tl.at[old]).start()

            @pl.when(i < PIECES)
            def _():
                @pl.when(i + FIRST_SLOTS < PIECES)
                def _():
                    signal(c1, data(line_end))

                @pl.when(i >= SLOTS)
                def _():
                    pl.semaphore_wait(c2, 1)

                remote(zp.at[slot], z2.at[slot], zs.at[slot], z_r2.at[slot], data(line_across)).start()

            k = i - LAG_FREE

            @pl.when(jnp.logical_and(k >= 0, k < PIECES))
            def _():
                free = lax.rem(k, SLOTS)
                take(z2.at[free], z_ts.at[free])
                take(z2.at[free], z_tl.at[free])

                @pl.when(k + SLOTS < PIECES)
                def _():
                    signal(c2, data(line_across))

    top = LAYERS - 1
    load_g = pltpu.make_async_copy(g_ref, gown, ld_o)
    load_g.start()
    held = ((ha, ld_a), (hr, ld_h))
    for n, (ref, sem) in enumerate(held):
        act_load(top, n, ref, sem).start()
    barrier = pltpu.get_barrier_semaphore()
    for peer in (near_x, near_y, far, partner):
        signal(barrier, model(peer))

    @pl.when(is_end)
    def _():
        signal(barrier, data(line_mid))
        pl.semaphore_wait(barrier, 5)

    @pl.when(is_mid)
    def _():
        signal(barrier, data(line_end))
        signal(barrier, data(line_across))
        pl.semaphore_wait(barrier, 6)

    load_g.wait()
    gather_send(0, 0, gown)
    gather_keep(0, gown)
    load_x = pltpu.make_async_copy(x_ref.at[top], xown, ld_o)
    load_x.start()
    for load in weight_loads(top):
        load.start()

    @pl.loop(0, 4)
    def _(b):
        for n, (ref, sem) in enumerate(held):
            act_load(top, 0, ref, sem).wait()
            act_block(2 * b + n, ref)

            @pl.when(b < 3)
            def _():
                act_load(top, 2 * b + n + 2, ref, sem).start()

        @pl.when(b == 2)
        def _():
            gather_relay(0, 0)
            gather_send(0, 1, gown)

    load_x.wait()
    take(gown, ag_l.at[0])
    gather_forward(0, 0)
    gather_wait(0, 0)
    chunk_load(0, 0, 0).start()

    @pl.loop(0, PIECES + LAG_LAST)
    def _(i):
        lp = i // PER_LAYER
        layer = LAYERS - 1 - lp
        s = i // 2
        sl = lax.rem(s, PER_LAYER // 2)
        il = lax.rem(i, PER_LAYER)
        even = lax.rem(i, 2) == 0
        odd = jnp.logical_not(even)
        odd_pair = lax.rem(s, 2) == 1
        even_pair = jnp.logical_not(odd_pair)
        ggid, xgid = 2 * lp, 2 * lp + 1
        live = i < PIECES

        @pl.when(live)
        def _():
            @pl.when(lax.rem(i, PARTS) == 0)
            def _():
                take(cbuf.at[0], ld_c.at[lax.rem(i // PARTS, 2)])

            piece(i)

        line_step(i)

        def when(*conds):
            return pl.when(functools.reduce(jnp.logical_and, conds, live))

        @when(even, s < CHUNKS - 1)
        def _():
            gather_relay(0, s + 1)

        @when(even, s < CHUNKS - 2)
        def _():
            gather_send(0, s + 2, gown)

        @when(even, s >= 1, s < CHUNKS)
        def _():
            gather_forward(0, s)

        @when(odd, s >= 1, s < CHUNKS)
        def _():
            gather_wait(0, s)

        @when(even, sl == 8)
        def _():
            gather_keep(xgid, xown)

        @when(even, even_pair, sl >= 8, sl < 24)
        def _():
            gather_send(xgid, (sl - 8) // 2, xown)

        @when(even, even_pair, sl >= 10, sl < 26)
        def _():
            gather_relay(xgid, (sl - 10) // 2)

        @when(even, odd_pair, sl >= 13, sl < 29)
        def _():
            gather_forward(xgid, (sl - 13) // 2)

        @when(odd, sl == 15)
        def _():
            take(xown, ag_l.at[xgid])

        @when(odd, odd_pair, sl >= 15, sl < 31)
        def _():
            gather_wait(xgid, (sl - 15) // 2)

        @when(even, s == 25)
        def _():
            gather_keep(2, gown)

        @when(even, s >= 25, s < 25 + CHUNKS)
        def _():
            gather_send(2, s - 25, gown)

        @when(even, s >= 27, s < 27 + CHUNKS)
        def _():
            gather_relay(2, s - 27)

        @when(even, s >= 29, s < 29 + CHUNKS)
        def _():
            gather_forward(2, s - 29)

        @when(odd, s == 30)
        def _():
            take(gown, ag_l.at[2])

        @when(odd, s >= 30, s < 30 + CHUNKS)
        def _():
            gather_wait(2, s - 30)

        @when(lax.rem(i, PARTS) == PARTS - 1, i + 1 < PIECES)
        def _():
            nxt = i + 1
            chunk_load(nxt // PHASE, lax.rem(nxt, PHASE) // PARTS, lax.rem(nxt // PARTS, 2)).start()

        @when(even, sl == UNIT_STEP)
        def _():
            for load in weight_loads(0):
                load.wait()

        @when(even, sl >= UNIT_STEP, sl < UNIT_STEP + 8)
        def _():
            unit_first(sl - UNIT_STEP)

        @when(even, sl > UNIT_STEP, sl <= UNIT_STEP + 8)
        def _():
            unit_finish(lp, sl - UNIT_STEP - 1)

        @when(odd, sl >= UNIT_STEP - 1, sl < UNIT_STEP + 7)
        def _():
            unit_load(ggid, layer, sl - UNIT_STEP + 1)

        @when(odd, sl >= UNIT_STEP, sl < UNIT_STEP + 8)
        def _():
            unit_second(lp, sl - UNIT_STEP)

        @when(il == FINAL_STEP - 1)
        def _():
            take(gb_ref.at[ggid, pl.ds(0, 4)], ag_s.at[ggid])
            new_gradient_load(lp, 0)

        @when(il >= FINAL_STEP, il < FINAL_STEP + 4)
        def _():
            new_gradient(il - FINAL_STEP)

            @pl.when(il < FINAL_STEP + 3)
            def _():
                new_gradient_load(lp, il - FINAL_STEP + 1)

        @when(i == PER_LAYER + FINAL_STEP + 4)
        def _():
            pltpu.make_async_copy(gown, gx_ref, st_gx).start()

        @when(lp == 0, even, sl == 17)
        def _():
            for load in weight_loads(0):
                load.start()

        @when(lp == 0, even, even_pair, sl >= 16)
        def _():
            act_load(0, (sl - 16) // 2, ha, ld_a).start()

        @when(lp == 0, odd, odd_pair, sl >= 16)
        def _():
            act_load(0, 0, ha, ld_a).wait()
            act_block((sl - 16) // 2, ha)

        @when(even, sl == 31)
        def _():
            take(gb_ref.at[xgid, pl.ds(0, 4)], ag_s.at[xgid])

            @pl.when(lp == 0)
            def _():
                pltpu.make_async_copy(x_ref.at[0], xown, ld_o).start()

        @when(lp == 0, odd, sl == 31)
        def _():
            pltpu.make_async_copy(x_ref.at[0], xown, ld_o).wait()

    for gid in range(2 * LAYERS):
        take(gb_ref.at[gid, pl.ds(0, 3)], ag_f.at[gid])
    for slot in range(2):
        take(pp.at[slot], pp_s.at[slot])
    for kept in range(8 - SUMS, SUMS):
        take(pm.at[kept], pm_s.at[kept])
    take(gown, st_gx)

    @pl.when(is_end)
    def _():
        for slot in range(SLOTS):
            take(zp.at[slot], zs.at[slot])


def solution(mesh):
    def device_step(x_saved, h_saved, w_up, w_down, grad_out):
        layers, hidden, ffn = w_up.shape
        rows = grad_out.shape[1]
        tokens = h_saved.shape[2]
        cw, fb = hidden // CHUNKS, ffn // PARTS
        half_rows = rows // 2
        any_space = pl.BlockSpec(memory_space=pl.ANY)
        dma = pltpu.SemaphoreType.DMA
        vmem = pltpu.VMEM
        grad_x, grad_up, grad_down, _, _ = pl.pallas_call(
            kernel,
            name="backward",
            out_shape=(
                jax.ShapeDtypeStruct((rows, hidden), BF16),
                jax.ShapeDtypeStruct(w_up.shape, F32),
                jax.ShapeDtypeStruct(w_down.shape, F32),
                jax.ShapeDtypeStruct((2 * layers, CHUNKS, tokens, cw), BF16),
                jax.ShapeDtypeStruct((layers, 3, rows, hidden), BF16),
            ),
            in_specs=[any_space] * 5,
            out_specs=(any_space,) * 5,
            scratch_shapes=[
                vmem((2, ffn, tokens), BF16),
                vmem((ffn, hidden), BF16),
                vmem((hidden, ffn), BF16),
                vmem((2, tokens, cw), BF16),
                vmem((rows, hidden), BF16),
                vmem((rows, ffn), BF16),
                vmem((rows, ffn), BF16),
                vmem((rows, ffn), BF16),
                vmem((rows, hidden), BF16),
                vmem((rows, hidden), BF16),
                vmem((SUMS, half_rows, hidden), BF16),
                vmem((2, half_rows, hidden), BF16),
                vmem((2, half_rows, hidden), BF16),
                vmem((rows, hidden), BF16),
                vmem((SLOTS, fb, cw), F32),
                vmem((FIRST_SLOTS, fb, cw), F32),
                vmem((SLOTS, fb, cw), F32),
                dma((SLOTS,)), dma((FIRST_SLOTS,)), dma((SLOTS,)), dma((SLOTS,)), dma((SLOTS,)), dma((LAST_SLOTS,)),
                pltpu.SemaphoreType.REGULAR, pltpu.SemaphoreType.REGULAR, pltpu.SemaphoreType.REGULAR,
                dma((2 * layers, CHUNKS)), dma((2 * layers, CHUNKS)), dma((2 * layers, CHUNKS)), dma((2 * layers, CHUNKS)),
                dma((2 * layers,)), dma((2 * layers,)), dma((2 * layers,)),
                dma((2,)), dma((2,)), dma((SUMS,)), dma((6 * layers,)), pltpu.SemaphoreType.REGULAR,
                dma((2,)), dma(()), dma(()), dma(()), dma((2,)), dma(()), dma((3,)), dma(()),
            ],
            compiler_params=pltpu.CompilerParams(collective_id=0, has_side_effects=True, vmem_limit_bytes=67043328),
        )(x_saved[:, 0], h_saved[:, 0], w_up, w_down, grad_out[0])
        return grad_x[None], grad_up, grad_down

    return jax.shard_map(
        device_step,
        mesh=mesh,
        in_specs=(P(None, "data", "model", None), P(None, "data", None, "model"), P(None, None, "model"), P(None, "model", None), P("data", "model", None)),
        out_specs=(P("data", "model", None), P(None, None, "model"), P(None, "model", None)),
        check_vma=False,
    )
```

```python
import functools

import jax
import jax.numpy as jnp
from jax import lax
from jax.experimental import pallas as pl
from jax.experimental.pallas import tpu as pltpu
from jax.sharding import PartitionSpec as P

MESH = pl.DeviceIdType.MESH
F32, BF16 = jnp.float32, jnp.bfloat16
NT = (((1,), (1,)), ((), ()))

LAYERS = 2
CHUNKS = 8
PARTS = 4
PHASE = CHUNKS * PARTS
PER_LAYER = 2 * PHASE
PIECES = LAYERS * PER_LAYER
SLOTS = 16
FIRST_SLOTS = 8
LAST_SLOTS = 32
LAG_SUM = 2
LAG_FREE = 6
LAG_LAST = 20
UNIT_STEP = 8
X_RUNS = ((0, 5, 5, 3, 7), (5, 3, 20, 3, 5))
FINAL_STEP = 46
SUMS = 6


def gelu_tanh(pre):
    return jnp.tanh(0.7978845608028654 * (pre + 0.044715 * pre * pre * pre))


def gelu(pre):
    return 0.5 * pre * (1.0 + gelu_tanh(pre))


def gelu_slope(pre):
    tanh_val = gelu_tanh(pre)
    return 0.5 * (1.0 + tanh_val) + 0.5 * pre * (1.0 - tanh_val * tanh_val) * 0.7978845608028654 * (1.0 + 0.134145 * pre * pre)


def kernel(x_ref, h_ref, wu_ref, wd_ref, g_ref, gx_ref, up_ref, down_ref, gb_ref, rxh_ref,
           lt, wd, wu, cbuf, gr, hr, dh, ha, gown, xown, pm, pp, pb, rxo, zp, z1, z2,
           zs, z_r1, z_r2, z_ts, z_tl, z_rt, c1, c2, c3,
           ag_x, ag_y, ag_d, ag_p, ag_s, ag_f, ag_l, pp_s, pb_r, pm_s, rx_r, pbc,
           ld_c, ld_g, ld_h, ld_a, ld_w, ld_o, ld_rx, st_gx):
    rows, hidden = gown.shape
    ffn = lt.shape[1]
    half_rows = rows // 2
    cw = hidden // CHUNKS
    fb = ffn // 4

    me = lax.axis_index("model")
    spot = lax.axis_index("data")
    core = lax.rem(me, 2)
    px = lax.rem(me // 2, 2)
    py = me // 4
    partner = me + 1 - 2 * core
    step_x, step_y = 2 * (1 - 2 * px), 4 * (1 - 2 * py)
    near_x, near_y, far = me + step_x, me + step_y, me + step_x + step_y
    is_end = jnp.logical_or(spot == 0, spot == 3)
    is_mid = jnp.logical_not(is_end)
    line_mid = jnp.where(spot < 2, 1, 2)
    line_end = jnp.where(spot < 2, 0, 3)
    line_across = 3 - spot

    def model(i):
        return {"model": i}

    def data(i):
        return {"data": i}

    def signal(sem, where):
        pl.semaphore_signal(sem, inc=1, device_id=where, device_id_type=MESH)

    def remote(src, dst, send, recv, where):
        return pltpu.make_async_remote_copy(src_ref=src, dst_ref=dst, send_sem=send, recv_sem=recv, device_id=where, device_id_type=MESH)

    def take(ref, sem):
        pltpu.make_async_copy(ref, ref, sem).wait()

    def chunk_columns(c):
        return pl.ds(pl.multiple_of(c * cw, cw), cw)

    def row_block(i):
        return pl.ds(pl.multiple_of(i * rows, rows), rows)

    def gather_keep(gid, own):
        for c in range(CHUNKS):
            pltpu.make_async_copy(own.at[:, pl.ds(c * cw, cw)], gb_ref.at[gid, c, row_block(me)], ag_l.at[gid]).start()

    def gather_send(gid, c, own):
        src = own.at[:, chunk_columns(c)]
        dst = gb_ref.at[gid, c, row_block(me)]
        remote(src, dst, ag_s.at[gid], ag_x.at[gid, c], model(near_x)).start()
        remote(src, dst, ag_s.at[gid], ag_y.at[gid, c], model(near_y)).start()
        remote(src, dst, ag_s.at[gid], ag_p.at[gid, c], model(partner)).start()

    def gather_relay(gid, c):
        take(gb_ref.at[gid, c, row_block(0)], ag_x.at[gid, c])
        take(gb_ref.at[gid, c, row_block(0)], ag_y.at[gid, c])
        for n, (source, target) in enumerate(((near_x, near_y), (near_y, near_x))):
            @pl.when(core == n)
            def _():
                block = gb_ref.at[gid, c, row_block(source)]
                remote(block, block, ag_s.at[gid], ag_d.at[gid, c], model(target)).start()

    def gather_forward(gid, c):
        take(gb_ref.at[gid, c, row_block(0)], ag_d.at[gid, c])
        for peer in (near_x, near_y, far):
            block = gb_ref.at[gid, c, row_block(peer)]
            remote(block, block, ag_f.at[gid], ag_p.at[gid, c], model(partner)).start()

    def gather_wait(gid, c):
        take(gb_ref.at[gid, c, pl.ds(0, 4 * rows)], ag_p.at[gid, c])

    def chunk_load(gid, c, slot):
        return pltpu.make_async_copy(gb_ref.at[gid, c], cbuf.at[slot], ld_c.at[slot])

    def act_load(layer, b, ref, sem):
        return pltpu.make_async_copy(h_ref.at[layer, row_block(b)], ref, sem)

    def act_block(b, ref):
        @pl.loop(0, 4)
        def _(f):
            cols = pl.ds(pl.multiple_of(f * fb, fb), fb)
            a = gelu(ref[:, cols].astype(F32)).astype(BF16).astype(F32)
            lt[0, cols, row_block(b)] = a.T.astype(BF16)

    def weight_loads(layer):
        return (pltpu.make_async_copy(wd_ref.at[layer], wd, ld_w.at[0]), pltpu.make_async_copy(wu_ref.at[layer], wu, ld_w.at[1]))

    def unit_place(u):
        r = lax.rem(u // 2 + 1, 4)
        chip = lax.rem(py + r // 2, 2) * 2 + lax.rem(px + lax.rem(r, 2), 2)
        return r, chip

    def unit_rows(u):
        _, chip = unit_place(u)
        start = (chip * 2 + core) * rows + lax.rem(u, 2) * half_rows
        other = (chip * 2 + 1 - core) * rows + lax.rem(u, 2) * half_rows
        return tuple(pl.ds(pl.multiple_of(s, half_rows), half_rows) for s in (start, other))

    def unit_load(gid, layer, u):
        for n, block in enumerate(unit_rows(u)):
            here = pl.ds(n * half_rows, half_rows)
            for c in range(CHUNKS):
                pltpu.make_async_copy(gb_ref.at[gid, c, block], gr.at[here, pl.ds(c * cw, cw)], ld_g).start()
            pltpu.make_async_copy(h_ref.at[layer, block], hr.at[here], ld_h).start()

    def unit_first(u):
        take(gr, ld_g)
        take(hr, ld_h)
        mine, other = unit_rows(u)

        @pl.loop(0, 4)
        def _(f):
            cols = pl.ds(pl.multiple_of(f * fb, fb), fb)
            d_act = lax.dot_general(gr[...], wd[cols, :], NT, preferred_element_type=F32)
            d_pre = (d_act * gelu_slope(hr[:, cols].astype(F32))).astype(BF16)
            dh[:, cols] = d_pre
            flipped = d_pre.astype(F32).T.astype(BF16)
            lt[1, cols, mine] = flipped[:, :half_rows]
            lt[1, cols, other] = flipped[:, half_rows:]

    def unit_second(lp, u):
        order = lp * 8 + u
        slot = lax.rem(order, 2)
        kept = lax.rem(u, SUMS)

        @pl.when(order >= 2)
        def _():
            take(pp.at[slot], pp_s.at[slot])

        @pl.when(jnp.logical_or(u >= SUMS, jnp.logical_and(lp > 0, u >= 8 - SUMS)))
        def _():
            take(pm.at[kept], pm_s.at[kept])

        @pl.loop(0, CHUNKS)
        def _(d):
            cols = chunk_columns(d)
            part = lax.dot_general(dh[...], wu[cols, :], NT, preferred_element_type=F32).astype(BF16)
            pm[kept, :, cols] = part[:half_rows]
            pp[slot, :, cols] = part[half_rows:]

        @pl.when(order >= 2)
        def _():
            pl.semaphore_wait(pbc, 1)

        remote(pp.at[slot], pb.at[slot], pp_s.at[slot], pb_r.at[slot], model(partner)).start()

    def unit_finish(lp, u):
        order = lp * 8 + u
        slot = lax.rem(order, 2)
        kept = lax.rem(u, SUMS)
        r, chip = unit_place(u)
        here = pl.ds(pl.multiple_of(lax.rem(u, 2) * half_rows, half_rows), half_rows)
        take(pb.at[slot], pb_r.at[slot])

        @pl.when(r != 0)
        def _():
            @pl.loop(0, CHUNKS)
            def _(d):
                cols = chunk_columns(d)
                pm[kept, :, cols] = (pm[kept, :, cols].astype(F32) + pb[slot, :, cols].astype(F32)).astype(BF16)

            remote(pm.at[kept], rxh_ref.at[lp, r - 1, here], pm_s.at[kept], rx_r.at[lp * 6 + (r - 1) * 2 + lax.rem(u, 2)],
                   model(chip * 2 + core)).start()

        @pl.when(r == 0)
        def _():
            @pl.loop(0, CHUNKS)
            def _(d):
                cols = chunk_columns(d)
                rxo[here, cols] = (pm[kept, :, cols].astype(F32) + pb[slot, :, cols].astype(F32)).astype(BF16)

        @pl.when(order < 8 * LAYERS - 2)
        def _():
            signal(pbc, model(partner))

    def quarter(n):
        part = rows // 4
        return pl.ds(pl.multiple_of(n * part, part), part)

    def new_gradient_load(lp, n):
        @pl.when(lax.rem(n, 2) == 0)
        def _():
            for r in range(3):
                take(pm.at[0], rx_r.at[lp * 6 + r * 2 + n // 2])

        for r in range(3):
            pltpu.make_async_copy(rxh_ref.at[lp, r, quarter(n)], gr.at[quarter(r)], ld_rx.at[r]).start()

    def new_gradient(n):
        for r in range(3):
            take(gr.at[quarter(0)], ld_rx.at[r])

        @pl.loop(0, CHUNKS)
        def _(d):
            cols = chunk_columns(d)
            total = rxo[quarter(n), cols].astype(F32)
            for r in range(3):
                total += gr[quarter(r), cols].astype(F32)
            gown[quarter(n), cols] = (gown[quarter(n), cols].astype(F32) + total).astype(BF16)

    def piece_place(i):
        return LAYERS - 1 - i // PER_LAYER, lax.rem(i // PHASE, 2), lax.rem(i, PHASE) // PARTS, lax.rem(i, PARTS)

    def part_columns(n):
        return pl.ds(pl.multiple_of(n * fb, fb), fb)

    def piece(i):
        _, phase, _, n = piece_place(i)
        slot = lax.rem(i, SLOTS)

        @pl.when(jnp.logical_and(is_end, i >= SLOTS))
        def _():
            take(zp.at[slot], zs.at[slot])

        part = jnp.dot(lt[phase, part_columns(n), :], cbuf[lax.rem(i // PARTS, 2)], preferred_element_type=F32)

        @pl.when(phase == 0)
        def _():
            zp[slot] = part

        @pl.when(phase == 1)
        def _():
            zp[slot] = part.T

    def total_place(j):
        layer, _, c, n = piece_place(j)
        return down_ref.at[layer, part_columns(n), chunk_columns(c)], up_ref.at[layer, chunk_columns(c), part_columns(n)]

    def line_step(i):
        @pl.when(is_end)
        def _():
            @pl.when(i < PIECES)
            def _():
                slot, there = lax.rem(i, SLOTS), lax.rem(i, FIRST_SLOTS)

                @pl.when(i >= FIRST_SLOTS)
                def _():
                    pl.semaphore_wait(c1, 1)

                remote(zp.at[slot], z1.at[there], zs.at[slot], z_r1.at[there], data(line_mid)).start()

            j = i - LAG_LAST

            @pl.when(jnp.logical_and(j >= 0, j < PIECES))
            def _():
                take(zp.at[0], z_rt.at[lax.rem(j, LAST_SLOTS)])

                @pl.when(j + LAST_SLOTS < PIECES)
                def _():
                    signal(c3, data(line_mid))

        @pl.when(is_mid)
        def _():
            slot, there = lax.rem(i, SLOTS), lax.rem(i, FIRST_SLOTS)
            j = i - LAG_SUM
            old = lax.rem(j + SLOTS, SLOTS)

            @pl.when(jnp.logical_and(j >= 0, j < PIECES))
            def _():
                take(z2.at[old], z_r2.at[old])
                z2[old] = z2[old] + zp[old]
                take(zp.at[old], zs.at[old])

                @pl.when(j >= LAST_SLOTS)
                def _():
                    pl.semaphore_wait(c3, 1)

            @pl.when(i < PIECES)
            def _():
                take(z1.at[there], z_r1.at[there])
                zp[slot] = zp[slot] + z1[there]

            @pl.when(jnp.logical_and(j >= 0, j < PIECES))
            def _():
                _, phase, _, _ = piece_place(j)
                for kind, place in enumerate(total_place(j)):
                    @pl.when(phase == kind)
                    def _():
                        remote(z2.at[old], place, z_ts.at[old], z_rt.at[lax.rem(j, LAST_SLOTS)], data(line_end)).start()
                        pltpu.make_async_copy(z2.at[old], place, z_tl.at[old]).start()

            @pl.when(i < PIECES)
            def _():
                @pl.when(i + FIRST_SLOTS < PIECES)
                def _():
                    signal(c1, data(line_end))

                @pl.when(i >= SLOTS)
                def _():
                    pl.semaphore_wait(c2, 1)

                remote(zp.at[slot], z2.at[slot], zs.at[slot], z_r2.at[slot], data(line_across)).start()

            k = i - LAG_FREE

            @pl.when(jnp.logical_and(k >= 0, k < PIECES))
            def _():
                free = lax.rem(k, SLOTS)
                take(z2.at[free], z_ts.at[free])
                take(z2.at[free], z_tl.at[free])

                @pl.when(k + SLOTS < PIECES)
                def _():
                    signal(c2, data(line_across))

    top = LAYERS - 1
    load_g = pltpu.make_async_copy(g_ref, gown, ld_o)
    load_g.start()
    held = ((ha, ld_a), (hr, ld_h))
    for n, (ref, sem) in enumerate(held):
        act_load(top, n, ref, sem).start()
    barrier = pltpu.get_barrier_semaphore()
    for peer in (near_x, near_y, far, partner):
        signal(barrier, model(peer))

    @pl.when(is_end)
    def _():
        signal(barrier, data(line_mid))
        pl.semaphore_wait(barrier, 5)

    @pl.when(is_mid)
    def _():
        signal(barrier, data(line_end))
        signal(barrier, data(line_across))
        pl.semaphore_wait(barrier, 6)

    load_g.wait()
    gather_send(0, 0, gown)
    gather_keep(0, gown)
    load_x = pltpu.make_async_copy(x_ref.at[top], xown, ld_o)
    load_x.start()
    for load in weight_loads(top):
        load.start()

    @pl.loop(0, 4)
    def _(b):
        for n, (ref, sem) in enumerate(held):
            act_load(top, 0, ref, sem).wait()
            act_block(2 * b + n, ref)

            @pl.when(b < 3)
            def _():
                act_load(top, 2 * b + n + 2, ref, sem).start()

        @pl.when(b == 2)
        def _():
            gather_relay(0, 0)
            gather_send(0, 1, gown)

    load_x.wait()
    take(gown, ag_l.at[0])
    gather_forward(0, 0)
    gather_wait(0, 0)
    chunk_load(0, 0, 0).start()

    @pl.loop(0, PIECES + LAG_LAST)
    def _(i):
        lp = i // PER_LAYER
        layer = LAYERS - 1 - lp
        s = i // 2
        sl = lax.rem(s, PER_LAYER // 2)
        il = lax.rem(i, PER_LAYER)
        even = lax.rem(i, 2) == 0
        odd = jnp.logical_not(even)
        odd_pair = lax.rem(s, 2) == 1
        even_pair = jnp.logical_not(odd_pair)
        ggid, xgid = 2 * lp, 2 * lp + 1
        live = i < PIECES

        @pl.when(live)
        def _():
            @pl.when(lax.rem(i, PARTS) == 0)
            def _():
                take(cbuf.at[0], ld_c.at[lax.rem(i // PARTS, 2)])

            piece(i)

        line_step(i)

        def when(*conds):
            return pl.when(functools.reduce(jnp.logical_and, conds, live))

        @when(even, s < CHUNKS - 1)
        def _():
            gather_relay(0, s + 1)

        @when(even, s < CHUNKS - 2)
        def _():
            gather_send(0, s + 2, gown)

        @when(even, s >= 1, s < CHUNKS)
        def _():
            gather_forward(0, s)

        @when(odd, s >= 1, s < CHUNKS)
        def _():
            gather_wait(0, s)

        @when(even, sl == X_RUNS[0][2])
        def _():
            gather_keep(xgid, xown)

        for first, count, start, relay, forward in X_RUNS:
            @when(even, sl >= start, sl < start + count)
            def _():
                gather_send(xgid, sl - start + first, xown)

            @when(even, sl >= start + relay, sl < start + relay + count)
            def _():
                gather_relay(xgid, sl - start - relay + first)

            @when(even, sl >= start + forward, sl < start + forward + count)
            def _():
                gather_forward(xgid, sl - start - forward + first)

        @when(odd, sl == 15)
        def _():
            take(xown, ag_l.at[xgid])

        @when(odd, odd_pair, sl >= 15, sl < 31)
        def _():
            gather_wait(xgid, (sl - 15) // 2)

        @when(even, s == 25)
        def _():
            gather_keep(2, gown)

        @when(even, s >= 25, s < 25 + CHUNKS)
        def _():
            gather_send(2, s - 25, gown)

        @when(even, s >= 27, s < 27 + CHUNKS)
        def _():
            gather_relay(2, s - 27)

        @when(even, s >= 29, s < 29 + CHUNKS)
        def _():
            gather_forward(2, s - 29)

        @when(odd, s == 30)
        def _():
            take(gown, ag_l.at[2])

        @when(odd, s >= 30, s < 30 + CHUNKS)
        def _():
            gather_wait(2, s - 30)

        @when(lax.rem(i, PARTS) == PARTS - 1, i + 1 < PIECES)
        def _():
            nxt = i + 1
            chunk_load(nxt // PHASE, lax.rem(nxt, PHASE) // PARTS, lax.rem(nxt // PARTS, 2)).start()

        @when(even, sl == UNIT_STEP)
        def _():
            for load in weight_loads(0):
                load.wait()

        @when(even, sl >= UNIT_STEP, sl < UNIT_STEP + 8)
        def _():
            unit_first(sl - UNIT_STEP)

        @when(even, sl > UNIT_STEP, sl <= UNIT_STEP + 8)
        def _():
            unit_finish(lp, sl - UNIT_STEP - 1)

        @when(odd, sl >= UNIT_STEP - 1, sl < UNIT_STEP + 7)
        def _():
            unit_load(ggid, layer, sl - UNIT_STEP + 1)

        @when(odd, sl >= UNIT_STEP, sl < UNIT_STEP + 8)
        def _():
            unit_second(lp, sl - UNIT_STEP)

        @when(il == FINAL_STEP - 1)
        def _():
            take(gb_ref.at[ggid, pl.ds(0, 4)], ag_s.at[ggid])
            new_gradient_load(lp, 0)

        @when(il >= FINAL_STEP, il < FINAL_STEP + 4)
        def _():
            new_gradient(il - FINAL_STEP)

            @pl.when(il < FINAL_STEP + 3)
            def _():
                new_gradient_load(lp, il - FINAL_STEP + 1)

        @when(i == PER_LAYER + FINAL_STEP + 4)
        def _():
            pltpu.make_async_copy(gown, gx_ref, st_gx).start()

        @when(lp == 0, even, sl == 17)
        def _():
            for load in weight_loads(0):
                load.start()

        @when(lp == 0, even, even_pair, sl >= 16)
        def _():
            act_load(0, (sl - 16) // 2, ha, ld_a).start()

        @when(lp == 0, odd, odd_pair, sl >= 16)
        def _():
            act_load(0, 0, ha, ld_a).wait()
            act_block((sl - 16) // 2, ha)

        @when(even, sl == 31)
        def _():
            take(gb_ref.at[xgid, pl.ds(0, 4)], ag_s.at[xgid])

            @pl.when(lp == 0)
            def _():
                pltpu.make_async_copy(x_ref.at[0], xown, ld_o).start()

        @when(lp == 0, odd, sl == 31)
        def _():
            pltpu.make_async_copy(x_ref.at[0], xown, ld_o).wait()

    for gid in range(2 * LAYERS):
        take(gb_ref.at[gid, pl.ds(0, 3)], ag_f.at[gid])
    for slot in range(2):
        take(pp.at[slot], pp_s.at[slot])
    for kept in range(8 - SUMS, SUMS):
        take(pm.at[kept], pm_s.at[kept])
    take(gown, st_gx)

    @pl.when(is_end)
    def _():
        for slot in range(SLOTS):
            take(zp.at[slot], zs.at[slot])


def solution(mesh):
    def device_step(x_saved, h_saved, w_up, w_down, grad_out):
        layers, hidden, ffn = w_up.shape
        rows = grad_out.shape[1]
        tokens = h_saved.shape[2]
        cw, fb = hidden // CHUNKS, ffn // PARTS
        half_rows = rows // 2
        any_space = pl.BlockSpec(memory_space=pl.ANY)
        dma = pltpu.SemaphoreType.DMA
        vmem = pltpu.VMEM
        grad_x, grad_up, grad_down, _, _ = pl.pallas_call(
            kernel,
            name="backward",
            out_shape=(
                jax.ShapeDtypeStruct((rows, hidden), BF16),
                jax.ShapeDtypeStruct(w_up.shape, F32),
                jax.ShapeDtypeStruct(w_down.shape, F32),
                jax.ShapeDtypeStruct((2 * layers, CHUNKS, tokens, cw), BF16),
                jax.ShapeDtypeStruct((layers, 3, rows, hidden), BF16),
            ),
            in_specs=[any_space] * 5,
            out_specs=(any_space,) * 5,
            scratch_shapes=[
                vmem((2, ffn, tokens), BF16),
                vmem((ffn, hidden), BF16),
                vmem((hidden, ffn), BF16),
                vmem((2, tokens, cw), BF16),
                vmem((rows, hidden), BF16),
                vmem((rows, ffn), BF16),
                vmem((rows, ffn), BF16),
                vmem((rows, ffn), BF16),
                vmem((rows, hidden), BF16),
                vmem((rows, hidden), BF16),
                vmem((SUMS, half_rows, hidden), BF16),
                vmem((2, half_rows, hidden), BF16),
                vmem((2, half_rows, hidden), BF16),
                vmem((rows, hidden), BF16),
                vmem((SLOTS, fb, cw), F32),
                vmem((FIRST_SLOTS, fb, cw), F32),
                vmem((SLOTS, fb, cw), F32),
                dma((SLOTS,)), dma((FIRST_SLOTS,)), dma((SLOTS,)), dma((SLOTS,)), dma((SLOTS,)), dma((LAST_SLOTS,)),
                pltpu.SemaphoreType.REGULAR, pltpu.SemaphoreType.REGULAR, pltpu.SemaphoreType.REGULAR,
                dma((2 * layers, CHUNKS)), dma((2 * layers, CHUNKS)), dma((2 * layers, CHUNKS)), dma((2 * layers, CHUNKS)),
                dma((2 * layers,)), dma((2 * layers,)), dma((2 * layers,)),
                dma((2,)), dma((2,)), dma((SUMS,)), dma((6 * layers,)), pltpu.SemaphoreType.REGULAR,
                dma((2,)), dma(()), dma(()), dma(()), dma((2,)), dma(()), dma((3,)), dma(()),
            ],
            compiler_params=pltpu.CompilerParams(collective_id=0, has_side_effects=True, vmem_limit_bytes=67043328),
        )(x_saved[:, 0], h_saved[:, 0], w_up, w_down, grad_out[0])
        return grad_x[None], grad_up, grad_down

    return jax.shard_map(
        device_step,
        mesh=mesh,
        in_specs=(P(None, "data", "model", None), P(None, "data", None, "model"), P(None, None, "model"), P(None, "model", None), P("data", "model", None)),
        out_specs=(P("data", "model", None), P(None, None, "model"), P(None, "model", None)),
        check_vma=False,
    )
```

```python
import functools

import jax
import jax.numpy as jnp
from jax import lax
from jax.experimental import pallas as pl
from jax.experimental.pallas import tpu as pltpu
from jax.sharding import PartitionSpec as P

MESH = pl.DeviceIdType.MESH
F32, BF16 = jnp.float32, jnp.bfloat16
NT = (((1,), (1,)), ((), ()))

LAYERS = 2
CHUNKS = 8
PARTS = 4
PHASE = CHUNKS * PARTS
PER_LAYER = 2 * PHASE
PIECES = LAYERS * PER_LAYER
REST = 2
FULL = PIECES - REST
SLOTS = 16
FIRST_SLOTS = 8
LAST_SLOTS = 32
LAG_SUM = 2
LAG_FREE = 6
LAG_LAST = 20
UNIT_STEP = 8
X_RUNS = ((0, 5, 5, 3, 7), (5, 3, 20, 3, 5))
FINAL_STEP = 46
SUMS = 6

MOVE_BYTES = 1 << 20
MOVE_FLOPS = 10


def gelu_tanh(pre):
    return jnp.tanh(0.7978845608028654 * (pre + 0.044715 * pre * pre * pre))


def gelu(pre):
    return 0.5 * pre * (1.0 + gelu_tanh(pre))


def gelu_slope(pre):
    tanh_val = gelu_tanh(pre)
    return 0.5 * (1.0 + tanh_val) + 0.5 * pre * (1.0 - tanh_val * tanh_val) * 0.7978845608028654 * (1.0 + 0.134145 * pre * pre)


def kernel(x_ref, h_ref, wu_ref, wd_ref, g_ref, gx_ref, up_ref, down_ref, rest_ref, gb_ref, rxh_ref,
           lt, wd, wu, cbuf, gr, hr, dh, ha, gown, xown, pm, pp, pb, rxo, zp, z1, z2,
           zs, z_r1, z_r2, z_ts, z_tl, z_rt, c1, c2, c3,
           ag_x, ag_y, ag_d, ag_p, ag_s, ag_f, ag_l, pp_s, pb_r, pm_s, rx_r, pbc,
           ld_c, ld_g, ld_h, ld_a, ld_w, ld_o, ld_rx, st_gx, first_s, first_l):
    rows, hidden = gown.shape
    ffn = lt.shape[1]
    half_rows = rows // 2
    cw = hidden // CHUNKS
    fb = ffn // 4

    me = lax.axis_index("model")
    spot = lax.axis_index("data")
    core = lax.rem(me, 2)
    px = lax.rem(me // 2, 2)
    py = me // 4
    partner = me + 1 - 2 * core
    step_x, step_y = 2 * (1 - 2 * px), 4 * (1 - 2 * py)
    near_x, near_y, far = me + step_x, me + step_y, me + step_x + step_y
    is_end = jnp.logical_or(spot == 0, spot == 3)
    is_mid = jnp.logical_not(is_end)
    line_mid = jnp.where(spot < 2, 1, 2)
    line_end = jnp.where(spot < 2, 0, 3)
    line_across = 3 - spot

    def model(i):
        return {"model": i}

    def data(i):
        return {"data": i}

    def signal(sem, where):
        pl.semaphore_signal(sem, inc=1, device_id=where, device_id_type=MESH)

    def remote(src, dst, send, recv, where):
        return pltpu.make_async_remote_copy(src_ref=src, dst_ref=dst, send_sem=send, recv_sem=recv, device_id=where, device_id_type=MESH)

    def take(ref, sem):
        pltpu.make_async_copy(ref, ref, sem).wait()

    def chunk_columns(c):
        return pl.ds(pl.multiple_of(c * cw, cw), cw)

    def row_block(i):
        return pl.ds(pl.multiple_of(i * rows, rows), rows)

    def gather_keep(gid, own, first=0):
        for c in range(first, CHUNKS):
            pltpu.make_async_copy(own.at[:, pl.ds(c * cw, cw)], gb_ref.at[gid, c, row_block(me)], ag_l.at[gid]).start()

    def gather_send(gid, c, own, buf):
        src = own.at[:, chunk_columns(c)]
        dst = buf.at[row_block(me)]
        remote(src, dst, ag_s.at[gid], ag_x.at[gid, c], model(near_x)).start()
        remote(src, dst, ag_s.at[gid], ag_y.at[gid, c], model(near_y)).start()
        remote(src, dst, ag_s.at[gid], ag_p.at[gid, c], model(partner)).start()

    def gather_relay(gid, c, buf, sent):
        take(buf.at[row_block(0)], ag_x.at[gid, c])
        take(buf.at[row_block(0)], ag_y.at[gid, c])
        for n, (source, target) in enumerate(((near_x, near_y), (near_y, near_x))):
            @pl.when(core == n)
            def _():
                block = buf.at[row_block(source)]
                remote(block, block, sent, ag_d.at[gid, c], model(target)).start()

    def gather_forward(gid, c, buf, sent):
        take(buf.at[row_block(0)], ag_d.at[gid, c])
        for peer in (near_x, near_y, far):
            block = buf.at[row_block(peer)]
            remote(block, block, sent, ag_p.at[gid, c], model(partner)).start()

    def gather_wait(gid, c, buf):
        take(buf.at[pl.ds(0, 4 * rows)], ag_p.at[gid, c])

    def gathered(gid, c):
        return gb_ref.at[gid, c]

    def chunk_load(gid, c, slot):
        return pltpu.make_async_copy(gb_ref.at[gid, c], cbuf.at[slot], ld_c.at[slot])

    def act_load(layer, b, ref, sem):
        return pltpu.make_async_copy(h_ref.at[layer, row_block(b)], ref, sem)

    def act_block(b, ref):
        @pl.loop(0, 4)
        def _(f):
            cols = pl.ds(pl.multiple_of(f * fb, fb), fb)
            a = gelu(ref[:, cols].astype(F32)).astype(BF16).astype(F32)
            lt[0, cols, row_block(b)] = a.T.astype(BF16)

    def weight_loads(layer):
        return (pltpu.make_async_copy(wd_ref.at[layer], wd, ld_w.at[0]), pltpu.make_async_copy(wu_ref.at[layer], wu, ld_w.at[1]))

    def unit_place(u):
        r = lax.rem(u // 2 + 1, 4)
        chip = lax.rem(py + r // 2, 2) * 2 + lax.rem(px + lax.rem(r, 2), 2)
        return r, chip

    def unit_rows(u):
        _, chip = unit_place(u)
        start = (chip * 2 + core) * rows + lax.rem(u, 2) * half_rows
        other = (chip * 2 + 1 - core) * rows + lax.rem(u, 2) * half_rows
        return tuple(pl.ds(pl.multiple_of(s, half_rows), half_rows) for s in (start, other))

    def unit_load(gid, layer, u):
        for n, block in enumerate(unit_rows(u)):
            here = pl.ds(n * half_rows, half_rows)
            for c in range(CHUNKS):
                pltpu.make_async_copy(gb_ref.at[gid, c, block], gr.at[here, pl.ds(c * cw, cw)], ld_g).start()
            pltpu.make_async_copy(h_ref.at[layer, block], hr.at[here], ld_h).start()

    def unit_first(u):
        take(gr, ld_g)
        take(hr, ld_h)
        mine, other = unit_rows(u)

        @pl.loop(0, 4)
        def _(f):
            cols = pl.ds(pl.multiple_of(f * fb, fb), fb)
            d_act = lax.dot_general(gr[...], wd[cols, :], NT, preferred_element_type=F32)
            d_pre = (d_act * gelu_slope(hr[:, cols].astype(F32))).astype(BF16)
            dh[:, cols] = d_pre
            flipped = d_pre.astype(F32).T.astype(BF16)
            lt[1, cols, mine] = flipped[:, :half_rows]
            lt[1, cols, other] = flipped[:, half_rows:]

    def unit_second(lp, u):
        order = lp * 8 + u
        slot = lax.rem(order, 2)
        kept = lax.rem(u, SUMS)

        @pl.when(order >= 2)
        def _():
            take(pp.at[slot], pp_s.at[slot])

        @pl.when(jnp.logical_or(u >= SUMS, jnp.logical_and(lp > 0, u >= 8 - SUMS)))
        def _():
            take(pm.at[kept], pm_s.at[kept])

        @pl.loop(0, CHUNKS)
        def _(d):
            cols = chunk_columns(d)
            part = lax.dot_general(dh[...], wu[cols, :], NT, preferred_element_type=F32).astype(BF16)
            pm[kept, :, cols] = part[:half_rows]
            pp[slot, :, cols] = part[half_rows:]

        @pl.when(order >= 2)
        def _():
            pl.semaphore_wait(pbc, 1)

        remote(pp.at[slot], pb.at[slot], pp_s.at[slot], pb_r.at[slot], model(partner)).start()

    def unit_finish(lp, u):
        order = lp * 8 + u
        slot = lax.rem(order, 2)
        kept = lax.rem(u, SUMS)
        r, chip = unit_place(u)
        here = pl.ds(pl.multiple_of(lax.rem(u, 2) * half_rows, half_rows), half_rows)
        take(pb.at[slot], pb_r.at[slot])

        @pl.when(r != 0)
        def _():
            @pl.loop(0, CHUNKS)
            def _(d):
                cols = chunk_columns(d)
                pm[kept, :, cols] = (pm[kept, :, cols].astype(F32) + pb[slot, :, cols].astype(F32)).astype(BF16)

            remote(pm.at[kept], rxh_ref.at[lp, r - 1, here], pm_s.at[kept], rx_r.at[lp * 6 + (r - 1) * 2 + lax.rem(u, 2)],
                   model(chip * 2 + core)).start()

        @pl.when(r == 0)
        def _():
            @pl.loop(0, CHUNKS)
            def _(d):
                cols = chunk_columns(d)
                rxo[here, cols] = (pm[kept, :, cols].astype(F32) + pb[slot, :, cols].astype(F32)).astype(BF16)

        @pl.when(order < 8 * LAYERS - 2)
        def _():
            signal(pbc, model(partner))

    def quarter(n):
        part = rows // 4
        return pl.ds(pl.multiple_of(n * part, part), part)

    def new_gradient_load(lp, n):
        @pl.when(lax.rem(n, 2) == 0)
        def _():
            for r in range(3):
                take(pm.at[0], rx_r.at[lp * 6 + r * 2 + n // 2])

        for r in range(3):
            pltpu.make_async_copy(rxh_ref.at[lp, r, quarter(n)], gr.at[quarter(r)], ld_rx.at[r]).start()

    def new_gradient(n):
        for r in range(3):
            take(gr.at[quarter(0)], ld_rx.at[r])

        @pl.loop(0, CHUNKS)
        def _(d):
            cols = chunk_columns(d)
            total = rxo[quarter(n), cols].astype(F32)
            for r in range(3):
                total += gr[quarter(r), cols].astype(F32)
            gown[quarter(n), cols] = (gown[quarter(n), cols].astype(F32) + total).astype(BF16)

    def piece_place(i):
        return LAYERS - 1 - i // PER_LAYER, lax.rem(i // PHASE, 2), lax.rem(i, PHASE) // PARTS, lax.rem(i, PARTS)

    def part_columns(n):
        return pl.ds(pl.multiple_of(n * fb, fb), fb)

    def piece(i):
        _, phase, _, n = piece_place(i)
        slot = lax.rem(i, SLOTS)

        @pl.when(jnp.logical_and(is_end, i >= SLOTS))
        def _():
            take(zp.at[slot], zs.at[slot])

        part = jnp.dot(lt[phase, part_columns(n), :], cbuf[lax.rem(i // PARTS, 2)], preferred_element_type=F32)

        @pl.when(phase == 0)
        def _():
            zp[slot] = part

        @pl.when(phase == 1)
        def _():
            zp[slot] = part.T

    def total_place(j):
        layer, _, c, n = piece_place(j)
        return down_ref.at[layer, part_columns(n), chunk_columns(c)], up_ref.at[layer, chunk_columns(c), part_columns(n)]

    def line_step(i):
        @pl.when(is_end)
        def _():
            @pl.when(i < PIECES)
            def _():
                slot, there = lax.rem(i, SLOTS), lax.rem(i, FIRST_SLOTS)

                @pl.when(i >= FIRST_SLOTS)
                def _():
                    pl.semaphore_wait(c1, 1)

                remote(zp.at[slot], z1.at[there], zs.at[slot], z_r1.at[there], data(line_mid)).start()

            j = i - LAG_LAST

            @pl.when(jnp.logical_and(j >= 0, j < FULL))
            def _():
                take(zp.at[0], z_rt.at[lax.rem(j, LAST_SLOTS)])

                @pl.when(j + LAST_SLOTS < FULL)
                def _():
                    signal(c3, data(line_mid))

        @pl.when(is_mid)
        def _():
            slot, there = lax.rem(i, SLOTS), lax.rem(i, FIRST_SLOTS)
            j = i - LAG_SUM
            old = lax.rem(j + SLOTS, SLOTS)

            @pl.when(jnp.logical_and(j >= 0, j < PIECES))
            def _():
                take(z2.at[old], z_r2.at[old])
                z2[old] = z2[old] + zp[old]
                take(zp.at[old], zs.at[old])

                @pl.when(jnp.logical_and(j >= LAST_SLOTS, j < FULL))
                def _():
                    pl.semaphore_wait(c3, 1)

            @pl.when(i < PIECES)
            def _():
                take(z1.at[there], z_r1.at[there])
                zp[slot] = zp[slot] + z1[there]

            @pl.when(jnp.logical_and(j >= FULL, j < PIECES))
            def _():
                pltpu.make_async_copy(z2.at[old], rest_ref.at[:, part_columns(j - FULL)], z_tl.at[old]).start()

            @pl.when(jnp.logical_and(j >= 0, j < FULL))
            def _():
                _, phase, _, _ = piece_place(j)
                for kind, place in enumerate(total_place(j)):
                    @pl.when(phase == kind)
                    def _():
                        remote(z2.at[old], place, z_ts.at[old], z_rt.at[lax.rem(j, LAST_SLOTS)], data(line_end)).start()
                        pltpu.make_async_copy(z2.at[old], place, z_tl.at[old]).start()

            @pl.when(i < PIECES)
            def _():
                @pl.when(i + FIRST_SLOTS < PIECES)
                def _():
                    signal(c1, data(line_end))

                @pl.when(i >= SLOTS)
                def _():
                    pl.semaphore_wait(c2, 1)

                remote(zp.at[slot], z2.at[slot], zs.at[slot], z_r2.at[slot], data(line_across)).start()

            k = i - LAG_FREE

            @pl.when(jnp.logical_and(k >= 0, k < PIECES))
            def _():
                free = lax.rem(k, SLOTS)
                @pl.when(k < FULL)
                def _():
                    take(z2.at[free], z_ts.at[free])

                take(z2.at[free], z_tl.at[free])

                @pl.when(k + SLOTS < PIECES)
                def _():
                    signal(c2, data(line_across))

    top = LAYERS - 1
    load_g = pltpu.make_async_copy(g_ref, gown, ld_o)
    load_g.start()
    held = ((ha, ld_a), (hr, ld_h))
    for n, (ref, sem) in enumerate(held):
        act_load(top, n, ref, sem).start()
    barrier = pltpu.get_barrier_semaphore()
    for peer in (near_x, near_y, far, partner):
        signal(barrier, model(peer))

    @pl.when(is_end)
    def _():
        signal(barrier, data(line_mid))
        pl.semaphore_wait(barrier, 5)

    @pl.when(is_mid)
    def _():
        signal(barrier, data(line_end))
        signal(barrier, data(line_across))
        pl.semaphore_wait(barrier, 6)

    load_g.wait()
    first_chunk = cbuf.at[0]
    gather_send(0, 0, gown, first_chunk)
    gather_keep(0, gown, 1)
    cbuf[0, row_block(me), :] = gown[:, :cw]
    load_x = pltpu.make_async_copy(x_ref.at[top], xown, ld_o)
    load_x.start()
    for load in weight_loads(top):
        load.start()

    @pl.loop(0, 4)
    def _(b):
        for n, (ref, sem) in enumerate(held):
            act_load(top, 0, ref, sem).wait()
            act_block(2 * b + n, ref)

            @pl.when(b < 3)
            def _():
                act_load(top, 2 * b + n + 2, ref, sem).start()

        @pl.when(b == 2)
        def _():
            gather_relay(0, 0, first_chunk, first_s)
            gather_send(0, 1, gown, gathered(0, 1))

    load_x.wait()
    gather_forward(0, 0, first_chunk, first_s)
    gather_wait(0, 0, first_chunk)
    take(gown.at[:, pl.ds(0, hidden - cw)], ag_l.at[0])
    pltpu.make_async_copy(first_chunk, gathered(0, 0), first_l).start()

    @pl.loop(0, PIECES + LAG_LAST)
    def _(i):
        lp = i // PER_LAYER
        layer = LAYERS - 1 - lp
        s = i // 2
        sl = lax.rem(s, PER_LAYER // 2)
        il = lax.rem(i, PER_LAYER)
        even = lax.rem(i, 2) == 0
        odd = jnp.logical_not(even)
        odd_pair = lax.rem(s, 2) == 1
        even_pair = jnp.logical_not(odd_pair)
        ggid, xgid = 2 * lp, 2 * lp + 1
        live = i < PIECES

        @pl.when(live)
        def _():
            @pl.when(jnp.logical_and(i > 0, lax.rem(i, PARTS) == 0))
            def _():
                take(cbuf.at[0], ld_c.at[lax.rem(i // PARTS, 2)])

            piece(i)

        line_step(i)

        def when(*conds):
            return pl.when(functools.reduce(jnp.logical_and, conds, live))

        @when(even, s < CHUNKS - 1)
        def _():
            gather_relay(0, s + 1, gathered(0, s + 1), ag_s.at[0])

        @when(even, s < CHUNKS - 2)
        def _():
            gather_send(0, s + 2, gown, gathered(0, s + 2))

        @when(even, s >= 1, s < CHUNKS)
        def _():
            gather_forward(0, s, gathered(0, s), ag_f.at[0])

        @when(odd, s >= 1, s < CHUNKS)
        def _():
            gather_wait(0, s, gathered(0, s))

        @when(i == 2 * PARTS - 2)
        def _():
            take(cbuf.at[0, pl.ds(0, 4 * rows)], first_s)
            take(cbuf.at[0], first_l)

        @when(even, sl == X_RUNS[0][2])
        def _():
            gather_keep(xgid, xown)

        for first, count, start, relay, forward in X_RUNS:
            @when(even, sl >= start, sl < start + count)
            def _():
                gather_send(xgid, sl - start + first, xown, gathered(xgid, sl - start + first))

            @when(even, sl >= start + relay, sl < start + relay + count)
            def _():
                gather_relay(xgid, sl - start - relay + first, gathered(xgid, sl - start - relay + first), ag_s.at[xgid])

            @when(even, sl >= start + forward, sl < start + forward + count)
            def _():
                gather_forward(xgid, sl - start - forward + first, gathered(xgid, sl - start - forward + first), ag_f.at[xgid])

        @when(odd, sl == 15)
        def _():
            take(xown, ag_l.at[xgid])

        @when(odd, odd_pair, sl >= 15, sl < 31)
        def _():
            gather_wait(xgid, (sl - 15) // 2, gathered(xgid, (sl - 15) // 2))

        @when(even, s == 25)
        def _():
            gather_keep(2, gown)

        @when(even, s >= 25, s < 25 + CHUNKS)
        def _():
            gather_send(2, s - 25, gown, gathered(2, s - 25))

        @when(even, s >= 27, s < 27 + CHUNKS)
        def _():
            gather_relay(2, s - 27, gathered(2, s - 27), ag_s.at[2])

        @when(even, s >= 29, s < 29 + CHUNKS)
        def _():
            gather_forward(2, s - 29, gathered(2, s - 29), ag_f.at[2])

        @when(odd, s == 30)
        def _():
            take(gown, ag_l.at[2])

        @when(odd, s >= 30, s < 30 + CHUNKS)
        def _():
            gather_wait(2, s - 30, gathered(2, s - 30))

        @when(lax.rem(i, PARTS) == PARTS - 1, i + 1 < PIECES)
        def _():
            nxt = i + 1
            chunk_load(nxt // PHASE, lax.rem(nxt, PHASE) // PARTS, lax.rem(nxt // PARTS, 2)).start()

        @when(even, sl == UNIT_STEP)
        def _():
            for load in weight_loads(0):
                load.wait()

        @when(even, sl >= UNIT_STEP, sl < UNIT_STEP + 8)
        def _():
            unit_first(sl - UNIT_STEP)

        @when(even, sl > UNIT_STEP, sl <= UNIT_STEP + 8)
        def _():
            unit_finish(lp, sl - UNIT_STEP - 1)

        @when(odd, sl >= UNIT_STEP - 1, sl < UNIT_STEP + 7)
        def _():
            unit_load(ggid, layer, sl - UNIT_STEP + 1)

        @when(odd, sl >= UNIT_STEP, sl < UNIT_STEP + 8)
        def _():
            unit_second(lp, sl - UNIT_STEP)

        @when(il == FINAL_STEP - 1)
        def _():
            take(gb_ref.at[ggid, 0, pl.ds(0, 7 * rows)], ag_s.at[ggid])
            take(gb_ref.at[ggid, pl.ds(0, 3)], ag_s.at[ggid])

            @pl.when(lp > 0)
            def _():
                take(gb_ref.at[ggid, 0, row_block(0)], ag_s.at[ggid])

            new_gradient_load(lp, 0)

        @when(il >= FINAL_STEP, il < FINAL_STEP + 4)
        def _():
            new_gradient(il - FINAL_STEP)

            @pl.when(il < FINAL_STEP + 3)
            def _():
                new_gradient_load(lp, il - FINAL_STEP + 1)

        @when(i == PER_LAYER + FINAL_STEP + 4)
        def _():
            pltpu.make_async_copy(gown, gx_ref, st_gx).start()

        @when(lp == 0, even, sl == 17)
        def _():
            for load in weight_loads(0):
                load.start()

        @when(lp == 0, even, even_pair, sl >= 16)
        def _():
            act_load(0, (sl - 16) // 2, ha, ld_a).start()

        @when(lp == 0, odd, odd_pair, sl >= 16)
        def _():
            act_load(0, 0, ha, ld_a).wait()
            act_block((sl - 16) // 2, ha)

        @when(even, sl == 31)
        def _():
            take(gb_ref.at[xgid, pl.ds(0, 4)], ag_s.at[xgid])

            @pl.when(lp == 0)
            def _():
                pltpu.make_async_copy(x_ref.at[0], xown, ld_o).start()

        @when(lp == 0, odd, sl == 31)
        def _():
            pltpu.make_async_copy(x_ref.at[0], xown, ld_o).wait()

    take(gb_ref.at[0, 0, pl.ds(0, 5 * rows)], ag_f.at[0])
    take(gb_ref.at[0, pl.ds(0, 2)], ag_f.at[0])
    for gid in range(1, 2 * LAYERS):
        take(gb_ref.at[gid, pl.ds(0, 3)], ag_f.at[gid])
    for slot in range(2):
        take(pp.at[slot], pp_s.at[slot])
    for kept in range(8 - SUMS, SUMS):
        take(pm.at[kept], pm_s.at[kept])
    take(gown, st_gx)

    @pl.when(is_end)
    def _():
        for slot in range(SLOTS):
            take(zp.at[slot], zs.at[slot])


def move_kernel(count, *refs):
    sources, targets = refs[:count], refs[count:2 * count]
    buffers, read, written = refs[2 * count:3 * count], refs[-2], refs[-1]
    copies, slot = [], 0
    for source, target, buffer in zip(sources, targets, buffers):
        size = buffer.shape[1]
        for n in range(buffer.shape[0]):
            rows = pl.ds(n * size, size)
            copies.append((pltpu.make_async_copy(source.at[rows], buffer.at[n], read.at[slot]),
                           pltpu.make_async_copy(buffer.at[n], target.at[rows], written.at[slot])))
            slot += 1
    for first, _ in copies:
        first.start()
    for first, second in copies:
        first.wait()
        second.start()
    for _, second in copies:
        second.wait()


def move(*arrays):
    flat = [a.reshape(-1, a.shape[-1]) for a in arrays]
    parts = [max(1, a.size * a.dtype.itemsize // MOVE_BYTES) for a in flat]
    any_space = pl.BlockSpec(memory_space=pl.ANY)
    size = sum(a.size * a.dtype.itemsize for a in flat)
    moved = pl.pallas_call(
        functools.partial(move_kernel, len(flat)),
        name="move",
        out_shape=tuple(jax.ShapeDtypeStruct(a.shape, a.dtype) for a in flat),
        in_specs=[any_space] * len(flat),
        out_specs=(any_space,) * len(flat),
        scratch_shapes=[pltpu.VMEM((n, a.shape[0] // n, a.shape[1]), a.dtype) for a, n in zip(flat, parts)]
        + [pltpu.SemaphoreType.DMA((sum(parts),))] * 2,
        compiler_params=pltpu.CompilerParams(vmem_limit_bytes=67043328),
        cost_estimate=pl.CostEstimate(flops=int(size * MOVE_FLOPS), bytes_accessed=2 * size, transcendentals=0),
    )(*flat)
    return [m.reshape(a.shape) for m, a in zip(moved, arrays)]


def solution(mesh):
    def device_step(x_saved, h_saved, w_up, w_down, grad_out):
        layers, hidden, ffn = w_up.shape
        rows = grad_out.shape[1]
        tokens = h_saved.shape[2]
        cw, fb = hidden // CHUNKS, ffn // PARTS
        half_rows = rows // 2
        any_space = pl.BlockSpec(memory_space=pl.ANY)
        dma = pltpu.SemaphoreType.DMA
        vmem = pltpu.VMEM
        grad_x, grad_up, grad_down, rest, _, _ = pl.pallas_call(
            kernel,
            name="backward",
            out_shape=(
                jax.ShapeDtypeStruct((rows, hidden), BF16),
                jax.ShapeDtypeStruct(w_up.shape, F32),
                jax.ShapeDtypeStruct(w_down.shape, F32),
                jax.ShapeDtypeStruct((cw, REST * fb), F32),
                jax.ShapeDtypeStruct((2 * layers, CHUNKS, tokens, cw), BF16),
                jax.ShapeDtypeStruct((layers, 3, rows, hidden), BF16),
            ),
            in_specs=[any_space] * 5,
            out_specs=(any_space,) * 6,
            scratch_shapes=[
                vmem((2, ffn, tokens), BF16),
                vmem((ffn, hidden), BF16),
                vmem((hidden, ffn), BF16),
                vmem((2, tokens, cw), BF16),
                vmem((rows, hidden), BF16),
                vmem((rows, ffn), BF16),
                vmem((rows, ffn), BF16),
                vmem((rows, ffn), BF16),
                vmem((rows, hidden), BF16),
                vmem((rows, hidden), BF16),
                vmem((SUMS, half_rows, hidden), BF16),
                vmem((2, half_rows, hidden), BF16),
                vmem((2, half_rows, hidden), BF16),
                vmem((rows, hidden), BF16),
                vmem((SLOTS, fb, cw), F32),
                vmem((FIRST_SLOTS, fb, cw), F32),
                vmem((SLOTS, fb, cw), F32),
                dma((SLOTS,)), dma((FIRST_SLOTS,)), dma((SLOTS,)), dma((SLOTS,)), dma((SLOTS,)), dma((LAST_SLOTS,)),
                pltpu.SemaphoreType.REGULAR, pltpu.SemaphoreType.REGULAR, pltpu.SemaphoreType.REGULAR,
                dma((2 * layers, CHUNKS)), dma((2 * layers, CHUNKS)), dma((2 * layers, CHUNKS)), dma((2 * layers, CHUNKS)),
                dma((2 * layers,)), dma((2 * layers,)), dma((2 * layers,)),
                dma((2,)), dma((2,)), dma((SUMS,)), dma((6 * layers,)), pltpu.SemaphoreType.REGULAR,
                dma((2,)), dma(()), dma(()), dma(()), dma((2,)), dma(()), dma((3,)), dma(()), dma(()), dma(()),
            ],
            compiler_params=pltpu.CompilerParams(collective_id=0, has_side_effects=True, vmem_limit_bytes=67043328),
        )(x_saved[:, 0], h_saved[:, 0], w_up, w_down, grad_out[0])
        spot = lax.axis_index("data")
        is_end = (spot == 0) | (spot == 3)
        rest = jnp.where(is_end, lax.ppermute(rest, "data", [(1, 0), (2, 3)]), rest)
        grad_x, grad_up, grad_down = move(grad_x, grad_up, grad_down)
        grad_up = grad_up.at[0, hidden - cw:, ffn - REST * fb:].set(rest)
        return grad_x[None], grad_up, grad_down

    return jax.shard_map(
        device_step,
        mesh=mesh,
        in_specs=(P(None, "data", "model", None), P(None, "data", None, "model"), P(None, None, "model"), P(None, "model", None), P("data", "model", None)),
        out_specs=(P("data", "model", None), P(None, None, "model"), P(None, "model", None)),
        check_vma=False,
    )
```

```python
import functools

import jax
import jax.numpy as jnp
from jax import lax
from jax.experimental import pallas as pl
from jax.experimental.pallas import tpu as pltpu
from jax.sharding import PartitionSpec as P

MESH = pl.DeviceIdType.MESH
F32, BF16 = jnp.float32, jnp.bfloat16
NT = (((1,), (1,)), ((), ()))

LAYERS = 2
CHUNKS = 8
PARTS = 4
PHASE = CHUNKS * PARTS
PER_LAYER = 2 * PHASE
PIECES = LAYERS * PER_LAYER
REST = 2
FULL = PIECES - REST
SLOTS = 16
FIRST_SLOTS = 8
LAST_SLOTS = 32
LAG_SUM = 2
LAG_FREE = 6
LAG_LAST = 20
UNIT_STEP = 8
X_RUNS = ((0, 5, 4, 2, 8), (5, 3, 20, 3, 5))
FINAL_STEP = 46
SUMS = 6

MOVE_BYTES = 1 << 21
MOVE_FLOPS = 10


def gelu_tanh(pre):
    return jnp.tanh(0.7978845608028654 * (pre + 0.044715 * pre * pre * pre))


def gelu(pre):
    return 0.5 * pre * (1.0 + gelu_tanh(pre))


def gelu_slope(pre):
    tanh_val = gelu_tanh(pre)
    return 0.5 * (1.0 + tanh_val) + 0.5 * pre * (1.0 - tanh_val * tanh_val) * 0.7978845608028654 * (1.0 + 0.134145 * pre * pre)


def kernel(x_ref, h_ref, wu_ref, wd_ref, g_ref, gx_ref, up_ref, down_ref, rest_ref, gb_ref, rxh_ref,
           lt, wd, wu, cbuf, gr, hr, dh, ha, gown, xown, pm, pp, pb, rxo, zp, z1, z2,
           zs, z_r1, z_r2, z_ts, z_tl, z_rt, c1, c2, c3,
           ag_x, ag_y, ag_d, ag_p, ag_s, ag_f, ag_l, pp_s, pb_r, pm_s, rx_r, pbc,
           ld_c, ld_g, ld_h, ld_a, ld_w, ld_o, ld_rx, st_gx, first_s, first_l):
    rows, hidden = gown.shape
    ffn = lt.shape[1]
    half_rows = rows // 2
    cw = hidden // CHUNKS
    fb = ffn // 4

    me = lax.axis_index("model")
    spot = lax.axis_index("data")
    core = lax.rem(me, 2)
    px = lax.rem(me // 2, 2)
    py = me // 4
    partner = me + 1 - 2 * core
    step_x, step_y = 2 * (1 - 2 * px), 4 * (1 - 2 * py)
    near_x, near_y, far = me + step_x, me + step_y, me + step_x + step_y
    is_end = jnp.logical_or(spot == 0, spot == 3)
    is_mid = jnp.logical_not(is_end)
    line_mid = jnp.where(spot < 2, 1, 2)
    line_end = jnp.where(spot < 2, 0, 3)
    line_across = 3 - spot

    def model(i):
        return {"model": i}

    def data(i):
        return {"data": i}

    def signal(sem, where):
        pl.semaphore_signal(sem, inc=1, device_id=where, device_id_type=MESH)

    def remote(src, dst, send, recv, where):
        return pltpu.make_async_remote_copy(src_ref=src, dst_ref=dst, send_sem=send, recv_sem=recv, device_id=where, device_id_type=MESH)

    def take(ref, sem):
        pltpu.make_async_copy(ref, ref, sem).wait()

    def chunk_columns(c):
        return pl.ds(pl.multiple_of(c * cw, cw), cw)

    def row_block(i):
        return pl.ds(pl.multiple_of(i * rows, rows), rows)

    def gather_keep(gid, own, first=0):
        for c in range(first, CHUNKS):
            pltpu.make_async_copy(own.at[:, pl.ds(c * cw, cw)], gb_ref.at[gid, c, row_block(me)], ag_l.at[gid]).start()

    def gather_send(gid, c, own, buf):
        src = own.at[:, chunk_columns(c)]
        dst = buf.at[row_block(me)]
        remote(src, dst, ag_s.at[gid], ag_x.at[gid, c], model(near_x)).start()
        remote(src, dst, ag_s.at[gid], ag_y.at[gid, c], model(near_y)).start()
        remote(src, dst, ag_s.at[gid], ag_p.at[gid, c], model(partner)).start()

    def gather_relay(gid, c, buf, sent):
        take(buf.at[row_block(0)], ag_x.at[gid, c])
        take(buf.at[row_block(0)], ag_y.at[gid, c])
        for n, (source, target) in enumerate(((near_x, near_y), (near_y, near_x))):
            @pl.when(core == n)
            def _():
                block = buf.at[row_block(source)]
                remote(block, block, sent, ag_d.at[gid, c], model(target)).start()

    def gather_forward(gid, c, buf, sent):
        take(buf.at[row_block(0)], ag_d.at[gid, c])
        for peer in (near_x, near_y, far):
            block = buf.at[row_block(peer)]
            remote(block, block, sent, ag_p.at[gid, c], model(partner)).start()

    def gather_wait(gid, c, buf):
        take(buf.at[pl.ds(0, 4 * rows)], ag_p.at[gid, c])

    def gathered(gid, c):
        return gb_ref.at[gid, c]

    def chunk_load(gid, c, slot):
        return pltpu.make_async_copy(gb_ref.at[gid, c], cbuf.at[slot], ld_c.at[slot])

    def act_load(layer, b, ref, sem):
        return pltpu.make_async_copy(h_ref.at[layer, row_block(b)], ref, sem)

    def act_block(b, ref):
        @pl.loop(0, 4)
        def _(f):
            cols = pl.ds(pl.multiple_of(f * fb, fb), fb)
            a = gelu(ref[:, cols].astype(F32)).astype(BF16).astype(F32)
            lt[0, cols, row_block(b)] = a.T.astype(BF16)

    def weight_loads(layer):
        return (pltpu.make_async_copy(wd_ref.at[layer], wd, ld_w.at[0]), pltpu.make_async_copy(wu_ref.at[layer], wu, ld_w.at[1]))

    def unit_place(u):
        r = lax.rem(u // 2 + 1, 4)
        chip = lax.rem(py + r // 2, 2) * 2 + lax.rem(px + lax.rem(r, 2), 2)
        return r, chip

    def unit_rows(u):
        _, chip = unit_place(u)
        start = (chip * 2 + core) * rows + lax.rem(u, 2) * half_rows
        other = (chip * 2 + 1 - core) * rows + lax.rem(u, 2) * half_rows
        return tuple(pl.ds(pl.multiple_of(s, half_rows), half_rows) for s in (start, other))

    def unit_load(gid, layer, u):
        for n, block in enumerate(unit_rows(u)):
            here = pl.ds(n * half_rows, half_rows)
            for c in range(CHUNKS):
                pltpu.make_async_copy(gb_ref.at[gid, c, block], gr.at[here, pl.ds(c * cw, cw)], ld_g).start()
            pltpu.make_async_copy(h_ref.at[layer, block], hr.at[here], ld_h).start()

    def unit_first(u):
        take(gr, ld_g)
        take(hr, ld_h)
        mine, other = unit_rows(u)

        @pl.loop(0, 4)
        def _(f):
            cols = pl.ds(pl.multiple_of(f * fb, fb), fb)
            d_act = lax.dot_general(gr[...], wd[cols, :], NT, preferred_element_type=F32)
            d_pre = (d_act * gelu_slope(hr[:, cols].astype(F32))).astype(BF16)
            dh[:, cols] = d_pre
            flipped = d_pre.astype(F32).T.astype(BF16)
            lt[1, cols, mine] = flipped[:, :half_rows]
            lt[1, cols, other] = flipped[:, half_rows:]

    def unit_second(lp, u):
        order = lp * 8 + u
        slot = lax.rem(order, 2)
        kept = lax.rem(u, SUMS)

        @pl.when(order >= 2)
        def _():
            take(pp.at[slot], pp_s.at[slot])

        @pl.when(jnp.logical_or(u >= SUMS, jnp.logical_and(lp > 0, u >= 8 - SUMS)))
        def _():
            take(pm.at[kept], pm_s.at[kept])

        @pl.loop(0, CHUNKS)
        def _(d):
            cols = chunk_columns(d)
            part = lax.dot_general(dh[...], wu[cols, :], NT, preferred_element_type=F32).astype(BF16)
            pm[kept, :, cols] = part[:half_rows]
            pp[slot, :, cols] = part[half_rows:]

        @pl.when(order >= 2)
        def _():
            pl.semaphore_wait(pbc, 1)

        remote(pp.at[slot], pb.at[slot], pp_s.at[slot], pb_r.at[slot], model(partner)).start()

    def unit_finish(lp, u):
        order = lp * 8 + u
        slot = lax.rem(order, 2)
        kept = lax.rem(u, SUMS)
        r, chip = unit_place(u)
        here = pl.ds(pl.multiple_of(lax.rem(u, 2) * half_rows, half_rows), half_rows)
        take(pb.at[slot], pb_r.at[slot])

        @pl.when(r != 0)
        def _():
            @pl.loop(0, CHUNKS)
            def _(d):
                cols = chunk_columns(d)
                pm[kept, :, cols] = (pm[kept, :, cols].astype(F32) + pb[slot, :, cols].astype(F32)).astype(BF16)

            remote(pm.at[kept], rxh_ref.at[lp, r - 1, here], pm_s.at[kept], rx_r.at[lp * 6 + (r - 1) * 2 + lax.rem(u, 2)],
                   model(chip * 2 + core)).start()

        @pl.when(r == 0)
        def _():
            @pl.loop(0, CHUNKS)
            def _(d):
                cols = chunk_columns(d)
                rxo[here, cols] = (pm[kept, :, cols].astype(F32) + pb[slot, :, cols].astype(F32)).astype(BF16)

        @pl.when(order < 8 * LAYERS - 2)
        def _():
            signal(pbc, model(partner))

    def quarter(n):
        part = rows // 4
        return pl.ds(pl.multiple_of(n * part, part), part)

    def new_gradient_load(lp, n):
        @pl.when(lax.rem(n, 2) == 0)
        def _():
            for r in range(3):
                take(pm.at[0], rx_r.at[lp * 6 + r * 2 + n // 2])

        for r in range(3):
            pltpu.make_async_copy(rxh_ref.at[lp, r, quarter(n)], gr.at[quarter(r)], ld_rx.at[r]).start()

    def new_gradient(n):
        for r in range(3):
            take(gr.at[quarter(0)], ld_rx.at[r])

        @pl.loop(0, CHUNKS)
        def _(d):
            cols = chunk_columns(d)
            total = rxo[quarter(n), cols].astype(F32)
            for r in range(3):
                total += gr[quarter(r), cols].astype(F32)
            gown[quarter(n), cols] = (gown[quarter(n), cols].astype(F32) + total).astype(BF16)

    def piece_place(i):
        return LAYERS - 1 - i // PER_LAYER, lax.rem(i // PHASE, 2), lax.rem(i, PHASE) // PARTS, lax.rem(i, PARTS)

    def part_columns(n):
        return pl.ds(pl.multiple_of(n * fb, fb), fb)

    def piece(i):
        _, phase, _, n = piece_place(i)
        slot = lax.rem(i, SLOTS)

        @pl.when(jnp.logical_and(is_end, i >= SLOTS))
        def _():
            take(zp.at[slot], zs.at[slot])

        part = jnp.dot(lt[phase, part_columns(n), :], cbuf[lax.rem(i // PARTS, 2)], preferred_element_type=F32)

        @pl.when(phase == 0)
        def _():
            zp[slot] = part

        @pl.when(phase == 1)
        def _():
            zp[slot] = part.T

    def total_place(j):
        layer, _, c, n = piece_place(j)
        return down_ref.at[layer, part_columns(n), chunk_columns(c)], up_ref.at[layer, chunk_columns(c), part_columns(n)]

    def line_step(i):
        @pl.when(is_end)
        def _():
            @pl.when(i < PIECES)
            def _():
                slot, there = lax.rem(i, SLOTS), lax.rem(i, FIRST_SLOTS)

                @pl.when(i >= FIRST_SLOTS)
                def _():
                    pl.semaphore_wait(c1, 1)

                remote(zp.at[slot], z1.at[there], zs.at[slot], z_r1.at[there], data(line_mid)).start()

            j = i - LAG_LAST

            @pl.when(jnp.logical_and(j >= 0, j < FULL))
            def _():
                take(zp.at[0], z_rt.at[lax.rem(j, LAST_SLOTS)])

                @pl.when(j + LAST_SLOTS < FULL)
                def _():
                    signal(c3, data(line_mid))

        @pl.when(is_mid)
        def _():
            slot, there = lax.rem(i, SLOTS), lax.rem(i, FIRST_SLOTS)
            j = i - LAG_SUM
            old = lax.rem(j + SLOTS, SLOTS)

            @pl.when(jnp.logical_and(j >= 0, j < PIECES))
            def _():
                take(z2.at[old], z_r2.at[old])
                z2[old] = z2[old] + zp[old]
                take(zp.at[old], zs.at[old])

                @pl.when(jnp.logical_and(j >= LAST_SLOTS, j < FULL))
                def _():
                    pl.semaphore_wait(c3, 1)

            @pl.when(i < PIECES)
            def _():
                take(z1.at[there], z_r1.at[there])
                zp[slot] = zp[slot] + z1[there]

            @pl.when(jnp.logical_and(j >= FULL, j < PIECES))
            def _():
                pltpu.make_async_copy(z2.at[old], rest_ref.at[:, part_columns(j - FULL)], z_tl.at[old]).start()

            @pl.when(jnp.logical_and(j >= 0, j < FULL))
            def _():
                _, phase, _, _ = piece_place(j)
                for kind, place in enumerate(total_place(j)):
                    @pl.when(phase == kind)
                    def _():
                        remote(z2.at[old], place, z_ts.at[old], z_rt.at[lax.rem(j, LAST_SLOTS)], data(line_end)).start()
                        pltpu.make_async_copy(z2.at[old], place, z_tl.at[old]).start()

            @pl.when(i < PIECES)
            def _():
                @pl.when(i + FIRST_SLOTS < PIECES)
                def _():
                    signal(c1, data(line_end))

                @pl.when(i >= SLOTS)
                def _():
                    pl.semaphore_wait(c2, 1)

                remote(zp.at[slot], z2.at[slot], zs.at[slot], z_r2.at[slot], data(line_across)).start()

            k = i - LAG_FREE

            @pl.when(jnp.logical_and(k >= 0, k < PIECES))
            def _():
                free = lax.rem(k, SLOTS)
                @pl.when(k < FULL)
                def _():
                    take(z2.at[free], z_ts.at[free])

                take(z2.at[free], z_tl.at[free])

                @pl.when(k + SLOTS < PIECES)
                def _():
                    signal(c2, data(line_across))

    top = LAYERS - 1
    load_g = pltpu.make_async_copy(g_ref, gown, ld_o)
    load_g.start()
    held = ((ha, ld_a), (hr, ld_h))
    for n, (ref, sem) in enumerate(held):
        act_load(top, n, ref, sem).start()
    barrier = pltpu.get_barrier_semaphore()
    for peer in (near_x, near_y, far, partner):
        signal(barrier, model(peer))

    @pl.when(is_end)
    def _():
        signal(barrier, data(line_mid))
        pl.semaphore_wait(barrier, 5)

    @pl.when(is_mid)
    def _():
        signal(barrier, data(line_end))
        signal(barrier, data(line_across))
        pl.semaphore_wait(barrier, 6)

    load_g.wait()
    first_chunk = cbuf.at[0]
    gather_send(0, 0, gown, first_chunk)
    gather_keep(0, gown, 1)
    cbuf[0, row_block(me), :] = gown[:, :cw]
    load_x = pltpu.make_async_copy(x_ref.at[top], xown, ld_o)
    load_x.start()
    for load in weight_loads(top):
        load.start()

    @pl.loop(0, 4)
    def _(b):
        for n, (ref, sem) in enumerate(held):
            act_load(top, 0, ref, sem).wait()
            act_block(2 * b + n, ref)

            @pl.when(b < 3)
            def _():
                act_load(top, 2 * b + n + 2, ref, sem).start()

        @pl.when(b == 2)
        def _():
            gather_relay(0, 0, first_chunk, first_s)
            gather_send(0, 1, gown, gathered(0, 1))

    load_x.wait()
    gather_forward(0, 0, first_chunk, first_s)
    gather_send(0, 2, gown, gathered(0, 2))
    gather_wait(0, 0, first_chunk)
    take(gown.at[:, pl.ds(0, hidden - cw)], ag_l.at[0])
    pltpu.make_async_copy(first_chunk, gathered(0, 0), first_l).start()

    @pl.loop(0, PIECES + LAG_LAST)
    def _(i):
        lp = i // PER_LAYER
        layer = LAYERS - 1 - lp
        s = i // 2
        sl = lax.rem(s, PER_LAYER // 2)
        il = lax.rem(i, PER_LAYER)
        even = lax.rem(i, 2) == 0
        odd = jnp.logical_not(even)
        odd_pair = lax.rem(s, 2) == 1
        even_pair = jnp.logical_not(odd_pair)
        ggid, xgid = 2 * lp, 2 * lp + 1
        live = i < PIECES

        @pl.when(live)
        def _():
            @pl.when(jnp.logical_and(i > 0, lax.rem(i, PARTS) == 0))
            def _():
                take(cbuf.at[0], ld_c.at[lax.rem(i // PARTS, 2)])

            piece(i)

        line_step(i)

        def when(*conds):
            return pl.when(functools.reduce(jnp.logical_and, conds, live))

        @when(even, s < CHUNKS - 1)
        def _():
            gather_relay(0, s + 1, gathered(0, s + 1), ag_s.at[0])

        @when(even, s < CHUNKS - 3)
        def _():
            gather_send(0, s + 3, gown, gathered(0, s + 3))

        @when(even, s >= 1, s < CHUNKS)
        def _():
            gather_forward(0, s, gathered(0, s), ag_f.at[0])

        @when(odd, s >= 1, s < CHUNKS)
        def _():
            gather_wait(0, s, gathered(0, s))

        @when(i == 2 * PARTS - 2)
        def _():
            take(cbuf.at[0, pl.ds(0, 4 * rows)], first_s)
            take(cbuf.at[0], first_l)

        @when(even, sl == X_RUNS[0][2])
        def _():
            gather_keep(xgid, xown)

        for first, count, start, relay, forward in X_RUNS:
            @when(even, sl >= start, sl < start + count)
            def _():
                gather_send(xgid, sl - start + first, xown, gathered(xgid, sl - start + first))

            @when(even, sl >= start + relay, sl < start + relay + count)
            def _():
                gather_relay(xgid, sl - start - relay + first, gathered(xgid, sl - start - relay + first), ag_s.at[xgid])

            @when(even, sl >= start + forward, sl < start + forward + count)
            def _():
                gather_forward(xgid, sl - start - forward + first, gathered(xgid, sl - start - forward + first), ag_f.at[xgid])

        @when(odd, sl == 15)
        def _():
            take(xown, ag_l.at[xgid])

        @when(odd, odd_pair, sl >= 15, sl < 31)
        def _():
            gather_wait(xgid, (sl - 15) // 2, gathered(xgid, (sl - 15) // 2))

        @when(even, s == 25)
        def _():
            gather_keep(2, gown)

        @when(even, s >= 25, s < 25 + CHUNKS)
        def _():
            gather_send(2, s - 25, gown, gathered(2, s - 25))

        @when(even, s >= 27, s < 27 + CHUNKS)
        def _():
            gather_relay(2, s - 27, gathered(2, s - 27), ag_s.at[2])

        @when(even, s >= 29, s < 29 + CHUNKS)
        def _():
            gather_forward(2, s - 29, gathered(2, s - 29), ag_f.at[2])

        @when(odd, s == 30)
        def _():
            take(gown, ag_l.at[2])

        @when(odd, s >= 30, s < 30 + CHUNKS)
        def _():
            gather_wait(2, s - 30, gathered(2, s - 30))

        @when(lax.rem(i, PARTS) == PARTS - 1, i + 1 < PIECES)
        def _():
            nxt = i + 1
            chunk_load(nxt // PHASE, lax.rem(nxt, PHASE) // PARTS, lax.rem(nxt // PARTS, 2)).start()

        @when(even, sl == UNIT_STEP)
        def _():
            for load in weight_loads(0):
                load.wait()

        @when(even, sl >= UNIT_STEP, sl < UNIT_STEP + 8)
        def _():
            unit_first(sl - UNIT_STEP)

        @when(even, sl > UNIT_STEP, sl <= UNIT_STEP + 8)
        def _():
            unit_finish(lp, sl - UNIT_STEP - 1)

        @when(odd, sl >= UNIT_STEP - 1, sl < UNIT_STEP + 7)
        def _():
            unit_load(ggid, layer, sl - UNIT_STEP + 1)

        @when(odd, sl >= UNIT_STEP, sl < UNIT_STEP + 8)
        def _():
            unit_second(lp, sl - UNIT_STEP)

        @when(il == FINAL_STEP - 1)
        def _():
            take(gb_ref.at[ggid, 0, pl.ds(0, 7 * rows)], ag_s.at[ggid])
            take(gb_ref.at[ggid, pl.ds(0, 3)], ag_s.at[ggid])

            @pl.when(lp > 0)
            def _():
                take(gb_ref.at[ggid, 0, row_block(0)], ag_s.at[ggid])

            new_gradient_load(lp, 0)

        @when(il >= FINAL_STEP, il < FINAL_STEP + 4)
        def _():
            new_gradient(il - FINAL_STEP)

            @pl.when(il < FINAL_STEP + 3)
            def _():
                new_gradient_load(lp, il - FINAL_STEP + 1)

        @when(i == PER_LAYER + FINAL_STEP + 4)
        def _():
            pltpu.make_async_copy(gown, gx_ref, st_gx).start()

        @when(lp == 0, even, sl == 17)
        def _():
            for load in weight_loads(0):
                load.start()

        @when(lp == 0, even, even_pair, sl >= 16)
        def _():
            act_load(0, (sl - 16) // 2, ha, ld_a).start()

        @when(lp == 0, odd, odd_pair, sl >= 16)
        def _():
            act_load(0, 0, ha, ld_a).wait()
            act_block((sl - 16) // 2, ha)

        @when(even, sl == 31)
        def _():
            take(gb_ref.at[xgid, pl.ds(0, 4)], ag_s.at[xgid])

            @pl.when(lp == 0)
            def _():
                pltpu.make_async_copy(x_ref.at[0], xown, ld_o).start()

        @when(lp == 0, odd, sl == 31)
        def _():
            pltpu.make_async_copy(x_ref.at[0], xown, ld_o).wait()

    take(gb_ref.at[0, 0, pl.ds(0, 5 * rows)], ag_f.at[0])
    take(gb_ref.at[0, pl.ds(0, 2)], ag_f.at[0])
    for gid in range(1, 2 * LAYERS):
        take(gb_ref.at[gid, pl.ds(0, 3)], ag_f.at[gid])
    for slot in range(2):
        take(pp.at[slot], pp_s.at[slot])
    for kept in range(8 - SUMS, SUMS):
        take(pm.at[kept], pm_s.at[kept])
    take(gown, st_gx)

    @pl.when(is_end)
    def _():
        for slot in range(SLOTS):
            take(zp.at[slot], zs.at[slot])


def move_kernel(count, *refs):
    sources, targets = refs[:count], refs[count:2 * count]
    buffers, read, written = refs[2 * count:3 * count], refs[-2], refs[-1]
    copies, slot = [], 0
    for source, target, buffer in zip(sources, targets, buffers):
        size = buffer.shape[1]
        for n in range(buffer.shape[0]):
            rows = pl.ds(n * size, size)
            copies.append((pltpu.make_async_copy(source.at[rows], buffer.at[n], read.at[slot]),
                           pltpu.make_async_copy(buffer.at[n], target.at[rows], written.at[slot])))
            slot += 1
    for first, _ in copies:
        first.start()
    for first, _ in copies:
        first.wait()
    for _, second in copies:
        second.start()
    for _, second in copies:
        second.wait()


def move(*arrays):
    flat = [a.reshape(-1, a.shape[-1]) for a in arrays]
    parts = [max(1, a.size * a.dtype.itemsize // MOVE_BYTES) for a in flat]
    any_space = pl.BlockSpec(memory_space=pl.ANY)
    size = sum(a.size * a.dtype.itemsize for a in flat)
    moved = pl.pallas_call(
        functools.partial(move_kernel, len(flat)),
        name="move",
        out_shape=tuple(jax.ShapeDtypeStruct(a.shape, a.dtype) for a in flat),
        in_specs=[any_space] * len(flat),
        out_specs=(any_space,) * len(flat),
        scratch_shapes=[pltpu.VMEM((n, a.shape[0] // n, a.shape[1]), a.dtype) for a, n in zip(flat, parts)]
        + [pltpu.SemaphoreType.DMA((sum(parts),))] * 2,
        compiler_params=pltpu.CompilerParams(vmem_limit_bytes=67043328),
        cost_estimate=pl.CostEstimate(flops=int(size * MOVE_FLOPS), bytes_accessed=2 * size, transcendentals=0),
    )(*flat)
    return [m.reshape(a.shape) for m, a in zip(moved, arrays)]


def solution(mesh):
    def device_step(x_saved, h_saved, w_up, w_down, grad_out):
        layers, hidden, ffn = w_up.shape
        rows = grad_out.shape[1]
        tokens = h_saved.shape[2]
        cw, fb = hidden // CHUNKS, ffn // PARTS
        half_rows = rows // 2
        any_space = pl.BlockSpec(memory_space=pl.ANY)
        dma = pltpu.SemaphoreType.DMA
        vmem = pltpu.VMEM
        grad_x, grad_up, grad_down, rest, _, _ = pl.pallas_call(
            kernel,
            name="backward",
            out_shape=(
                jax.ShapeDtypeStruct((rows, hidden), BF16),
                jax.ShapeDtypeStruct(w_up.shape, F32),
                jax.ShapeDtypeStruct(w_down.shape, F32),
                jax.ShapeDtypeStruct((cw, REST * fb), F32),
                jax.ShapeDtypeStruct((2 * layers, CHUNKS, tokens, cw), BF16),
                jax.ShapeDtypeStruct((layers, 3, rows, hidden), BF16),
            ),
            in_specs=[any_space] * 5,
            out_specs=(any_space,) * 6,
            scratch_shapes=[
                vmem((2, ffn, tokens), BF16),
                vmem((ffn, hidden), BF16),
                vmem((hidden, ffn), BF16),
                vmem((2, tokens, cw), BF16),
                vmem((rows, hidden), BF16),
                vmem((rows, ffn), BF16),
                vmem((rows, ffn), BF16),
                vmem((rows, ffn), BF16),
                vmem((rows, hidden), BF16),
                vmem((rows, hidden), BF16),
                vmem((SUMS, half_rows, hidden), BF16),
                vmem((2, half_rows, hidden), BF16),
                vmem((2, half_rows, hidden), BF16),
                vmem((rows, hidden), BF16),
                vmem((SLOTS, fb, cw), F32),
                vmem((FIRST_SLOTS, fb, cw), F32),
                vmem((SLOTS, fb, cw), F32),
                dma((SLOTS,)), dma((FIRST_SLOTS,)), dma((SLOTS,)), dma((SLOTS,)), dma((SLOTS,)), dma((LAST_SLOTS,)),
                pltpu.SemaphoreType.REGULAR, pltpu.SemaphoreType.REGULAR, pltpu.SemaphoreType.REGULAR,
                dma((2 * layers, CHUNKS)), dma((2 * layers, CHUNKS)), dma((2 * layers, CHUNKS)), dma((2 * layers, CHUNKS)),
                dma((2 * layers,)), dma((2 * layers,)), dma((2 * layers,)),
                dma((2,)), dma((2,)), dma((SUMS,)), dma((6 * layers,)), pltpu.SemaphoreType.REGULAR,
                dma((2,)), dma(()), dma(()), dma(()), dma((2,)), dma(()), dma((3,)), dma(()), dma(()), dma(()),
            ],
            compiler_params=pltpu.CompilerParams(collective_id=0, has_side_effects=True, vmem_limit_bytes=67043328),
        )(x_saved[:, 0], h_saved[:, 0], w_up, w_down, grad_out[0])
        spot = lax.axis_index("data")
        is_end = (spot == 0) | (spot == 3)
        rest = jnp.where(is_end, lax.ppermute(rest, "data", [(1, 0), (2, 3)]), rest)
        grad_x, grad_up, grad_down = move(grad_x, grad_up, grad_down)
        grad_up = grad_up.at[0, hidden - cw:, ffn - REST * fb:].set(rest)
        return grad_x[None], grad_up, grad_down

    return jax.shard_map(
        device_step,
        mesh=mesh,
        in_specs=(P(None, "data", "model", None), P(None, "data", None, "model"), P(None, None, "model"), P(None, "model", None), P("data", "model", None)),
        out_specs=(P("data", "model", None), P(None, None, "model"), P(None, "model", None)),
        check_vma=False,
    )
```

```python
import functools

import jax
import jax.numpy as jnp
from jax import lax
from jax.experimental import pallas as pl
from jax.experimental.pallas import tpu as pltpu
from jax.sharding import PartitionSpec as P

MESH = pl.DeviceIdType.MESH
F32, BF16 = jnp.float32, jnp.bfloat16
NT = (((1,), (1,)), ((), ()))

LAYERS = 2
CHUNKS = 8
PARTS = 4
PHASE = CHUNKS * PARTS
PER_LAYER = 2 * PHASE
PIECES = LAYERS * PER_LAYER
REST = 2
FULL = PIECES - REST
SLOTS = 16
FIRST_SLOTS = 8
LAST_SLOTS = 32
LAG_SUM = 2
LAG_FREE = 6
LAG_LAST = 20
FORWARD_LAG, WAIT_LAG = 2, 3
UNIT_STEP = 12
X_RUNS = ((0, 5, 4, 3, 8), (5, 3, 19, 3, 5))
FINAL_STEP = 46
SUMS = 6

MOVE_BYTES = 1 << 21
MOVE_FLOPS = 10


def gelu_tanh(pre):
    return jnp.tanh(0.7978845608028654 * (pre + 0.044715 * pre * pre * pre))


def gelu(pre):
    return 0.5 * pre * (1.0 + gelu_tanh(pre))


def gelu_slope(pre):
    tanh_val = gelu_tanh(pre)
    return 0.5 * (1.0 + tanh_val) + 0.5 * pre * (1.0 - tanh_val * tanh_val) * 0.7978845608028654 * (1.0 + 0.134145 * pre * pre)


def kernel(x_ref, h_ref, wu_ref, wd_ref, g_ref, gx_ref, up_ref, down_ref, rest_ref, gb_ref, rxh_ref,
           lt, wd, wu, cbuf, gr, hr, dh, ha, gown, xown, pm, pp, pb, rxo, zp, z1, z2,
           zs, z_r1, z_r2, z_ts, z_tl, z_rt, c1, c2, c3,
           ag_x, ag_y, ag_d, ag_p, ag_s, ag_f, ag_l, pp_s, pb_r, pm_s, rx_r, pbc,
           ld_c, ld_g, ld_h, ld_a, ld_w, ld_o, ld_rx, st_gx, first_s, first_l):
    rows, hidden = gown.shape
    ffn = lt.shape[1]
    half_rows = rows // 2
    cw = hidden // CHUNKS
    fb = ffn // 4

    me = lax.axis_index("model")
    spot = lax.axis_index("data")
    core = lax.rem(me, 2)
    px = lax.rem(me // 2, 2)
    py = me // 4
    partner = me + 1 - 2 * core
    step_x, step_y = 2 * (1 - 2 * px), 4 * (1 - 2 * py)
    near_x, near_y, far = me + step_x, me + step_y, me + step_x + step_y
    is_end = jnp.logical_or(spot == 0, spot == 3)
    is_mid = jnp.logical_not(is_end)
    line_mid = jnp.where(spot < 2, 1, 2)
    line_end = jnp.where(spot < 2, 0, 3)
    line_across = 3 - spot

    def model(i):
        return {"model": i}

    def data(i):
        return {"data": i}

    def signal(sem, where):
        pl.semaphore_signal(sem, inc=1, device_id=where, device_id_type=MESH)

    def remote(src, dst, send, recv, where):
        return pltpu.make_async_remote_copy(src_ref=src, dst_ref=dst, send_sem=send, recv_sem=recv, device_id=where, device_id_type=MESH)

    def take(ref, sem):
        pltpu.make_async_copy(ref, ref, sem).wait()

    def chunk_columns(c):
        return pl.ds(pl.multiple_of(c * cw, cw), cw)

    def row_block(i):
        return pl.ds(pl.multiple_of(i * rows, rows), rows)

    def gather_keep(gid, own, first=0):
        for c in range(first, CHUNKS):
            pltpu.make_async_copy(own.at[:, pl.ds(c * cw, cw)], gb_ref.at[gid, c, row_block(me)], ag_l.at[gid]).start()

    def gather_send(gid, c, own, buf):
        src = own.at[:, chunk_columns(c)]
        dst = buf.at[row_block(me)]
        remote(src, dst, ag_s.at[gid], ag_x.at[gid, c], model(near_x)).start()
        remote(src, dst, ag_s.at[gid], ag_y.at[gid, c], model(near_y)).start()
        remote(src, dst, ag_s.at[gid], ag_p.at[gid, c], model(partner)).start()

    def gather_relay(gid, c, buf, sent):
        take(buf.at[row_block(0)], ag_x.at[gid, c])
        take(buf.at[row_block(0)], ag_y.at[gid, c])
        for n, (source, target) in enumerate(((near_x, near_y), (near_y, near_x))):
            @pl.when(core == n)
            def _():
                block = buf.at[row_block(source)]
                remote(block, block, sent, ag_d.at[gid, c], model(target)).start()

    def gather_forward(gid, c, buf, sent):
        take(buf.at[row_block(0)], ag_d.at[gid, c])
        for peer in (near_x, near_y, far):
            block = buf.at[row_block(peer)]
            remote(block, block, sent, ag_p.at[gid, c], model(partner)).start()

    def gather_wait(gid, c, buf):
        take(buf.at[pl.ds(0, 4 * rows)], ag_p.at[gid, c])

    def gathered(gid, c):
        return gb_ref.at[gid, c]

    def chunk_load(gid, c, slot):
        return pltpu.make_async_copy(gb_ref.at[gid, c], cbuf.at[slot], ld_c.at[slot])

    def act_load(layer, b, ref, sem):
        return pltpu.make_async_copy(h_ref.at[layer, row_block(b)], ref, sem)

    def act_block(b, ref):
        @pl.loop(0, 4)
        def _(f):
            cols = pl.ds(pl.multiple_of(f * fb, fb), fb)
            a = gelu(ref[:, cols].astype(F32)).astype(BF16).astype(F32)
            lt[0, cols, row_block(b)] = a.T.astype(BF16)

    def weight_loads(layer):
        return (pltpu.make_async_copy(wd_ref.at[layer], wd, ld_w.at[0]), pltpu.make_async_copy(wu_ref.at[layer], wu, ld_w.at[1]))

    def unit_place(u):
        r = lax.rem(u // 2 + 1, 4)
        chip = lax.rem(py + r // 2, 2) * 2 + lax.rem(px + lax.rem(r, 2), 2)
        return r, chip

    def unit_rows(u):
        _, chip = unit_place(u)
        start = (chip * 2 + core) * rows + lax.rem(u, 2) * half_rows
        other = (chip * 2 + 1 - core) * rows + lax.rem(u, 2) * half_rows
        return tuple(pl.ds(pl.multiple_of(s, half_rows), half_rows) for s in (start, other))

    def unit_load(gid, layer, u):
        for n, block in enumerate(unit_rows(u)):
            here = pl.ds(n * half_rows, half_rows)
            for c in range(CHUNKS):
                pltpu.make_async_copy(gb_ref.at[gid, c, block], gr.at[here, pl.ds(c * cw, cw)], ld_g).start()
            pltpu.make_async_copy(h_ref.at[layer, block], hr.at[here], ld_h).start()

    def unit_first(u):
        take(gr, ld_g)
        take(hr, ld_h)
        mine, other = unit_rows(u)

        @pl.loop(0, 4)
        def _(f):
            cols = pl.ds(pl.multiple_of(f * fb, fb), fb)
            d_act = lax.dot_general(gr[...], wd[cols, :], NT, preferred_element_type=F32)
            d_pre = (d_act * gelu_slope(hr[:, cols].astype(F32))).astype(BF16)
            dh[:, cols] = d_pre
            flipped = d_pre.astype(F32).T.astype(BF16)
            lt[1, cols, mine] = flipped[:, :half_rows]
            lt[1, cols, other] = flipped[:, half_rows:]

    def unit_second(lp, u):
        order = lp * 8 + u
        slot = lax.rem(order, 2)
        kept = lax.rem(u, SUMS)

        @pl.when(order >= 2)
        def _():
            take(pp.at[slot], pp_s.at[slot])

        @pl.when(jnp.logical_or(u >= SUMS, jnp.logical_and(lp > 0, u >= 8 - SUMS)))
        def _():
            take(pm.at[kept], pm_s.at[kept])

        @pl.loop(0, CHUNKS)
        def _(d):
            cols = chunk_columns(d)
            part = lax.dot_general(dh[...], wu[cols, :], NT, preferred_element_type=F32).astype(BF16)
            pm[kept, :, cols] = part[:half_rows]
            pp[slot, :, cols] = part[half_rows:]

        @pl.when(order >= 2)
        def _():
            pl.semaphore_wait(pbc, 1)

        remote(pp.at[slot], pb.at[slot], pp_s.at[slot], pb_r.at[slot], model(partner)).start()

    def unit_finish(lp, u):
        order = lp * 8 + u
        slot = lax.rem(order, 2)
        kept = lax.rem(u, SUMS)
        r, chip = unit_place(u)
        here = pl.ds(pl.multiple_of(lax.rem(u, 2) * half_rows, half_rows), half_rows)
        take(pb.at[slot], pb_r.at[slot])

        @pl.when(r != 0)
        def _():
            @pl.loop(0, CHUNKS)
            def _(d):
                cols = chunk_columns(d)
                pm[kept, :, cols] = (pm[kept, :, cols].astype(F32) + pb[slot, :, cols].astype(F32)).astype(BF16)

            remote(pm.at[kept], rxh_ref.at[lp, r - 1, here], pm_s.at[kept], rx_r.at[lp * 6 + (r - 1) * 2 + lax.rem(u, 2)],
                   model(chip * 2 + core)).start()

        @pl.when(r == 0)
        def _():
            @pl.loop(0, CHUNKS)
            def _(d):
                cols = chunk_columns(d)
                rxo[here, cols] = (pm[kept, :, cols].astype(F32) + pb[slot, :, cols].astype(F32)).astype(BF16)

        @pl.when(order < 8 * LAYERS - 2)
        def _():
            signal(pbc, model(partner))

    def quarter(n):
        part = rows // 4
        return pl.ds(pl.multiple_of(n * part, part), part)

    def new_gradient_load(lp, n):
        @pl.when(lax.rem(n, 2) == 0)
        def _():
            for r in range(3):
                take(pm.at[0], rx_r.at[lp * 6 + r * 2 + n // 2])

        for r in range(3):
            pltpu.make_async_copy(rxh_ref.at[lp, r, quarter(n)], gr.at[quarter(r)], ld_rx.at[r]).start()

    def new_gradient(n):
        for r in range(3):
            take(gr.at[quarter(0)], ld_rx.at[r])

        @pl.loop(0, CHUNKS)
        def _(d):
            cols = chunk_columns(d)
            total = rxo[quarter(n), cols].astype(F32)
            for r in range(3):
                total += gr[quarter(r), cols].astype(F32)
            gown[quarter(n), cols] = (gown[quarter(n), cols].astype(F32) + total).astype(BF16)

    def piece_place(i):
        return LAYERS - 1 - i // PER_LAYER, lax.rem(i // PHASE, 2), lax.rem(i, PHASE) // PARTS, lax.rem(i, PARTS)

    def part_columns(n):
        return pl.ds(pl.multiple_of(n * fb, fb), fb)

    def piece(i):
        _, phase, _, n = piece_place(i)
        slot = lax.rem(i, SLOTS)

        @pl.when(jnp.logical_and(is_end, i >= SLOTS))
        def _():
            take(zp.at[slot], zs.at[slot])

        part = jnp.dot(lt[phase, part_columns(n), :], cbuf[lax.rem(i // PARTS, 2)], preferred_element_type=F32)

        @pl.when(phase == 0)
        def _():
            zp[slot] = part

        @pl.when(phase == 1)
        def _():
            zp[slot] = part.T

    def total_place(j):
        layer, _, c, n = piece_place(j)
        return down_ref.at[layer, part_columns(n), chunk_columns(c)], up_ref.at[layer, chunk_columns(c), part_columns(n)]

    def line_step(i):
        @pl.when(is_end)
        def _():
            @pl.when(i < PIECES)
            def _():
                slot, there = lax.rem(i, SLOTS), lax.rem(i, FIRST_SLOTS)

                @pl.when(i >= FIRST_SLOTS)
                def _():
                    pl.semaphore_wait(c1, 1)

                remote(zp.at[slot], z1.at[there], zs.at[slot], z_r1.at[there], data(line_mid)).start()

            j = i - LAG_LAST

            @pl.when(jnp.logical_and(j >= 0, j < FULL))
            def _():
                take(zp.at[0], z_rt.at[lax.rem(j, LAST_SLOTS)])

                @pl.when(j + LAST_SLOTS < FULL)
                def _():
                    signal(c3, data(line_mid))

        @pl.when(is_mid)
        def _():
            slot, there = lax.rem(i, SLOTS), lax.rem(i, FIRST_SLOTS)
            j = i - LAG_SUM
            old = lax.rem(j + SLOTS, SLOTS)

            @pl.when(jnp.logical_and(j >= 0, j < PIECES))
            def _():
                take(z2.at[old], z_r2.at[old])
                z2[old] = z2[old] + zp[old]
                take(zp.at[old], zs.at[old])

                @pl.when(jnp.logical_and(j >= LAST_SLOTS, j < FULL))
                def _():
                    pl.semaphore_wait(c3, 1)

            @pl.when(i < PIECES)
            def _():
                take(z1.at[there], z_r1.at[there])
                zp[slot] = zp[slot] + z1[there]

            @pl.when(jnp.logical_and(j >= FULL, j < PIECES))
            def _():
                pltpu.make_async_copy(z2.at[old], rest_ref.at[:, part_columns(j - FULL)], z_tl.at[old]).start()

            @pl.when(jnp.logical_and(j >= 0, j < FULL))
            def _():
                _, phase, _, _ = piece_place(j)
                for kind, place in enumerate(total_place(j)):
                    @pl.when(phase == kind)
                    def _():
                        remote(z2.at[old], place, z_ts.at[old], z_rt.at[lax.rem(j, LAST_SLOTS)], data(line_end)).start()
                        pltpu.make_async_copy(z2.at[old], place, z_tl.at[old]).start()

            @pl.when(i < PIECES)
            def _():
                @pl.when(i + FIRST_SLOTS < PIECES)
                def _():
                    signal(c1, data(line_end))

                @pl.when(i >= SLOTS)
                def _():
                    pl.semaphore_wait(c2, 1)

                remote(zp.at[slot], z2.at[slot], zs.at[slot], z_r2.at[slot], data(line_across)).start()

            k = i - LAG_FREE

            @pl.when(jnp.logical_and(k >= 0, k < PIECES))
            def _():
                free = lax.rem(k, SLOTS)
                @pl.when(k < FULL)
                def _():
                    take(z2.at[free], z_ts.at[free])

                take(z2.at[free], z_tl.at[free])

                @pl.when(k + SLOTS < PIECES)
                def _():
                    signal(c2, data(line_across))

    top = LAYERS - 1
    load_g = pltpu.make_async_copy(g_ref, gown, ld_o)
    load_g.start()
    held = ((ha, ld_a), (hr, ld_h))
    for n, (ref, sem) in enumerate(held):
        act_load(top, n, ref, sem).start()
    barrier = pltpu.get_barrier_semaphore()
    for peer in (near_x, near_y, far, partner):
        signal(barrier, model(peer))

    @pl.when(is_end)
    def _():
        signal(barrier, data(line_mid))
        pl.semaphore_wait(barrier, 5)

    @pl.when(is_mid)
    def _():
        signal(barrier, data(line_end))
        signal(barrier, data(line_across))
        pl.semaphore_wait(barrier, 6)

    load_g.wait()
    first_chunk = cbuf.at[0]
    gather_send(0, 0, gown, first_chunk)
    gather_keep(0, gown, 1)
    cbuf[0, row_block(me), :] = gown[:, :cw]
    load_x = pltpu.make_async_copy(x_ref.at[top], xown, ld_o)
    load_x.start()
    for load in weight_loads(top):
        load.start()

    @pl.loop(0, 4)
    def _(b):
        for n, (ref, sem) in enumerate(held):
            act_load(top, 0, ref, sem).wait()
            act_block(2 * b + n, ref)

            @pl.when(b < 3)
            def _():
                act_load(top, 2 * b + n + 2, ref, sem).start()

        @pl.when(b == 2)
        def _():
            gather_relay(0, 0, first_chunk, first_s)
            gather_send(0, 1, gown, gathered(0, 1))

    load_x.wait()
    gather_forward(0, 0, first_chunk, first_s)
    gather_send(0, 2, gown, gathered(0, 2))
    gather_wait(0, 0, first_chunk)
    take(gown.at[:, pl.ds(0, hidden - cw)], ag_l.at[0])
    pltpu.make_async_copy(first_chunk, gathered(0, 0), first_l).start()

    @pl.loop(0, PIECES + LAG_LAST)
    def _(i):
        lp = i // PER_LAYER
        layer = LAYERS - 1 - lp
        s = i // 2
        sl = lax.rem(s, PER_LAYER // 2)
        il = lax.rem(i, PER_LAYER)
        even = lax.rem(i, 2) == 0
        odd = jnp.logical_not(even)
        odd_pair = lax.rem(s, 2) == 1
        even_pair = jnp.logical_not(odd_pair)
        ggid, xgid = 2 * lp, 2 * lp + 1
        live = i < PIECES

        @pl.when(live)
        def _():
            @pl.when(jnp.logical_and(i > 0, lax.rem(i, PARTS) == 0))
            def _():
                take(cbuf.at[0], ld_c.at[lax.rem(i // PARTS, 2)])

            piece(i)

        line_step(i)

        def when(*conds):
            return pl.when(functools.reduce(jnp.logical_and, conds, live))

        def first_gather(j):
            c = 2 * (j // 3) + lax.rem(j, 3) + 1
            return c, functools.reduce(jnp.logical_and, (j >= 0, lax.rem(j + 3, 3) < 2, c < CHUNKS))

        c, there = first_gather(i)

        @when(there)
        def _():
            gather_relay(0, c, gathered(0, c), ag_s.at[0])

        @when(there, c + 2 < CHUNKS)
        def _():
            gather_send(0, c + 2, gown, gathered(0, c + 2))

        c_forward, there_forward = first_gather(i - FORWARD_LAG)

        @when(there_forward)
        def _():
            gather_forward(0, c_forward, gathered(0, c_forward), ag_f.at[0])

        c_wait, there_wait = first_gather(i - WAIT_LAG)

        @when(there_wait)
        def _():
            gather_wait(0, c_wait, gathered(0, c_wait))

        @when(i == 2 * PARTS - 2)
        def _():
            take(cbuf.at[0, pl.ds(0, 4 * rows)], first_s)
            take(cbuf.at[0], first_l)

        @when(even, sl == X_RUNS[0][2])
        def _():
            gather_keep(xgid, xown)

        for first, count, start, relay, forward in X_RUNS:
            @when(even, sl >= start, sl < start + count)
            def _():
                gather_send(xgid, sl - start + first, xown, gathered(xgid, sl - start + first))

            @when(even, sl >= start + relay, sl < start + relay + count)
            def _():
                gather_relay(xgid, sl - start - relay + first, gathered(xgid, sl - start - relay + first), ag_s.at[xgid])

            @when(even, sl >= start + forward, sl < start + forward + count)
            def _():
                gather_forward(xgid, sl - start - forward + first, gathered(xgid, sl - start - forward + first), ag_f.at[xgid])

        @when(even, sl == 15)
        def _():
            take(xown, ag_l.at[xgid])

        @when(even, odd_pair, sl >= 15, sl < 31)
        def _():
            gather_wait(xgid, (sl - 15) // 2, gathered(xgid, (sl - 15) // 2))

        @when(even, s == 25)
        def _():
            gather_keep(2, gown)

        @when(even, s >= 25, s < 25 + CHUNKS)
        def _():
            gather_send(2, s - 25, gown, gathered(2, s - 25))

        @when(even, s >= 27, s < 27 + CHUNKS)
        def _():
            gather_relay(2, s - 27, gathered(2, s - 27), ag_s.at[2])

        @when(even, s >= 29, s < 29 + CHUNKS)
        def _():
            gather_forward(2, s - 29, gathered(2, s - 29), ag_f.at[2])

        @when(odd, s == 30)
        def _():
            take(gown, ag_l.at[2])

        @when(odd, s >= 30, s < 30 + CHUNKS)
        def _():
            gather_wait(2, s - 30, gathered(2, s - 30))

        @when(jnp.logical_or(i == PARTS - 1, jnp.logical_and(i >= PARTS, lax.rem(i, PARTS) == PARTS - 2)), i + 2 < PIECES)
        def _():
            nxt = i // PARTS * PARTS + PARTS
            chunk_load(nxt // PHASE, lax.rem(nxt, PHASE) // PARTS, lax.rem(nxt // PARTS, 2)).start()

        k = il - UNIT_STEP
        half = 4 * (k // 5) + lax.rem(k + 5, 5)
        u = half // 2
        on = functools.reduce(jnp.logical_and, (k >= 0, k < 20, lax.rem(k + 5, 5) < 4))
        first_half = lax.rem(half, 2) == 0

        @when(k == 0)
        def _():
            unit_load(ggid, layer, 0)
            for load in weight_loads(0):
                load.wait()

        @when(on, first_half)
        def _():
            unit_first(u)

        @when(jnp.logical_or(jnp.logical_and(jnp.logical_and(on, first_half), u > 0), k == 19))
        def _():
            unit_finish(lp, jnp.where(k == 19, 7, u - 1))

        @when(on, jnp.logical_not(first_half), u < 7)
        def _():
            unit_load(ggid, layer, u + 1)

        @when(on, jnp.logical_not(first_half))
        def _():
            unit_second(lp, u)

        @when(il == FINAL_STEP - 1)
        def _():
            take(gb_ref.at[ggid, 0, pl.ds(0, 7 * rows)], ag_s.at[ggid])
            take(gb_ref.at[ggid, pl.ds(0, 3)], ag_s.at[ggid])

            @pl.when(lp > 0)
            def _():
                take(gb_ref.at[ggid, 0, row_block(0)], ag_s.at[ggid])

            new_gradient_load(lp, 0)

        @when(il >= FINAL_STEP, il < FINAL_STEP + 4)
        def _():
            new_gradient(il - FINAL_STEP)

            @pl.when(il < FINAL_STEP + 3)
            def _():
                new_gradient_load(lp, il - FINAL_STEP + 1)

        @when(i == PER_LAYER + FINAL_STEP + 4)
        def _():
            pltpu.make_async_copy(gown, gx_ref, st_gx).start()

        @when(lp == 0, even, sl == 17)
        def _():
            for load in weight_loads(0):
                load.start()

        @when(lp == 0, even, even_pair, sl >= 16)
        def _():
            act_load(0, (sl - 16) // 2, ha, ld_a).start()

        @when(lp == 0, odd, odd_pair, sl >= 16)
        def _():
            act_load(0, 0, ha, ld_a).wait()
            act_block((sl - 16) // 2, ha)

        @when(even, sl == 31)
        def _():
            take(gb_ref.at[xgid, pl.ds(0, 4)], ag_s.at[xgid])

            @pl.when(lp == 0)
            def _():
                pltpu.make_async_copy(x_ref.at[0], xown, ld_o).start()

        @when(lp == 0, odd, sl == 31)
        def _():
            pltpu.make_async_copy(x_ref.at[0], xown, ld_o).wait()

    take(gb_ref.at[0, 0, pl.ds(0, 5 * rows)], ag_f.at[0])
    take(gb_ref.at[0, pl.ds(0, 2)], ag_f.at[0])
    for gid in range(1, 2 * LAYERS):
        take(gb_ref.at[gid, pl.ds(0, 3)], ag_f.at[gid])
    for slot in range(2):
        take(pp.at[slot], pp_s.at[slot])
    for kept in range(8 - SUMS, SUMS):
        take(pm.at[kept], pm_s.at[kept])
    take(gown, st_gx)

    @pl.when(is_end)
    def _():
        for slot in range(SLOTS):
            take(zp.at[slot], zs.at[slot])


def move_kernel(count, *refs):
    sources, targets = refs[:count], refs[count:2 * count]
    buffers, read, written = refs[2 * count:3 * count], refs[-2], refs[-1]
    copies, slot = [], 0
    for source, target, buffer in zip(sources, targets, buffers):
        size = buffer.shape[1]
        for n in range(buffer.shape[0]):
            rows = pl.ds(n * size, size)
            copies.append((pltpu.make_async_copy(source.at[rows], buffer.at[n], read.at[slot]),
                           pltpu.make_async_copy(buffer.at[n], target.at[rows], written.at[slot])))
            slot += 1
    for first, _ in copies:
        first.start()
    for first, _ in copies:
        first.wait()
    for _, second in copies:
        second.start()
    for _, second in copies:
        second.wait()


def move(*arrays):
    flat = [a.reshape(-1, a.shape[-1]) for a in arrays]
    parts = [max(1, a.size * a.dtype.itemsize // MOVE_BYTES) for a in flat]
    any_space = pl.BlockSpec(memory_space=pl.ANY)
    size = sum(a.size * a.dtype.itemsize for a in flat)
    moved = pl.pallas_call(
        functools.partial(move_kernel, len(flat)),
        name="move",
        out_shape=tuple(jax.ShapeDtypeStruct(a.shape, a.dtype) for a in flat),
        in_specs=[any_space] * len(flat),
        out_specs=(any_space,) * len(flat),
        scratch_shapes=[pltpu.VMEM((n, a.shape[0] // n, a.shape[1]), a.dtype) for a, n in zip(flat, parts)]
        + [pltpu.SemaphoreType.DMA((sum(parts),))] * 2,
        compiler_params=pltpu.CompilerParams(vmem_limit_bytes=67043328),
        cost_estimate=pl.CostEstimate(flops=int(size * MOVE_FLOPS), bytes_accessed=2 * size, transcendentals=0),
    )(*flat)
    return [m.reshape(a.shape) for m, a in zip(moved, arrays)]


def solution(mesh):
    def device_step(x_saved, h_saved, w_up, w_down, grad_out):
        layers, hidden, ffn = w_up.shape
        rows = grad_out.shape[1]
        tokens = h_saved.shape[2]
        cw, fb = hidden // CHUNKS, ffn // PARTS
        half_rows = rows // 2
        any_space = pl.BlockSpec(memory_space=pl.ANY)
        dma = pltpu.SemaphoreType.DMA
        vmem = pltpu.VMEM
        grad_x, grad_up, grad_down, rest, _, _ = pl.pallas_call(
            kernel,
            name="backward",
            out_shape=(
                jax.ShapeDtypeStruct((rows, hidden), BF16),
                jax.ShapeDtypeStruct(w_up.shape, F32),
                jax.ShapeDtypeStruct(w_down.shape, F32),
                jax.ShapeDtypeStruct((cw, REST * fb), F32),
                jax.ShapeDtypeStruct((2 * layers, CHUNKS, tokens, cw), BF16),
                jax.ShapeDtypeStruct((layers, 3, rows, hidden), BF16),
            ),
            in_specs=[any_space] * 5,
            out_specs=(any_space,) * 6,
            scratch_shapes=[
                vmem((2, ffn, tokens), BF16),
                vmem((ffn, hidden), BF16),
                vmem((hidden, ffn), BF16),
                vmem((2, tokens, cw), BF16),
                vmem((rows, hidden), BF16),
                vmem((rows, ffn), BF16),
                vmem((rows, ffn), BF16),
                vmem((rows, ffn), BF16),
                vmem((rows, hidden), BF16),
                vmem((rows, hidden), BF16),
                vmem((SUMS, half_rows, hidden), BF16),
                vmem((2, half_rows, hidden), BF16),
                vmem((2, half_rows, hidden), BF16),
                vmem((rows, hidden), BF16),
                vmem((SLOTS, fb, cw), F32),
                vmem((FIRST_SLOTS, fb, cw), F32),
                vmem((SLOTS, fb, cw), F32),
                dma((SLOTS,)), dma((FIRST_SLOTS,)), dma((SLOTS,)), dma((SLOTS,)), dma((SLOTS,)), dma((LAST_SLOTS,)),
                pltpu.SemaphoreType.REGULAR, pltpu.SemaphoreType.REGULAR, pltpu.SemaphoreType.REGULAR,
                dma((2 * layers, CHUNKS)), dma((2 * layers, CHUNKS)), dma((2 * layers, CHUNKS)), dma((2 * layers, CHUNKS)),
                dma((2 * layers,)), dma((2 * layers,)), dma((2 * layers,)),
                dma((2,)), dma((2,)), dma((SUMS,)), dma((6 * layers,)), pltpu.SemaphoreType.REGULAR,
                dma((2,)), dma(()), dma(()), dma(()), dma((2,)), dma(()), dma((3,)), dma(()), dma(()), dma(()),
            ],
            compiler_params=pltpu.CompilerParams(collective_id=0, has_side_effects=True, vmem_limit_bytes=67043328),
        )(x_saved[:, 0], h_saved[:, 0], w_up, w_down, grad_out[0])
        spot = lax.axis_index("data")
        is_end = (spot == 0) | (spot == 3)
        rest = jnp.where(is_end, lax.ppermute(rest, "data", [(1, 0), (2, 3)]), rest)
        grad_x, grad_up, grad_down = move(grad_x, grad_up, grad_down)
        grad_up = grad_up.at[0, hidden - cw:, ffn - REST * fb:].set(rest)
        return grad_x[None], grad_up, grad_down

    return jax.shard_map(
        device_step,
        mesh=mesh,
        in_specs=(P(None, "data", "model", None), P(None, "data", None, "model"), P(None, None, "model"), P(None, "model", None), P("data", "model", None)),
        out_specs=(P("data", "model", None), P(None, None, "model"), P(None, "model", None)),
        check_vma=False,
    )
```

```python
import functools

import jax
import jax.numpy as jnp
from jax import lax
from jax.experimental import pallas as pl
from jax.experimental.pallas import tpu as pltpu
from jax.sharding import PartitionSpec as P

MESH = pl.DeviceIdType.MESH
F32, BF16 = jnp.float32, jnp.bfloat16
NT = (((1,), (1,)), ((), ()))

LAYERS = 2
CHUNKS = 8
PARTS = 4
PHASE = CHUNKS * PARTS
PER_LAYER = 2 * PHASE
PIECES = LAYERS * PER_LAYER
REST = 4
FULL = PIECES - REST
SLOTS = 16
FIRST_SLOTS = 8
LAST_SLOTS = 32
LAG_SUM = 3
LAG_FREE = 7
LAG_LAST = 20
UNIT_STEP = 8
X_RUNS = ((0, 5, 4, 2, 8), (5, 3, 20, 3, 5))
FINAL_STEP = 46
SUMS = 6

MOVE_BYTES = 1 << 21
MOVE_FLOPS = 10


def gelu_tanh(pre):
    return jnp.tanh(0.7978845608028654 * (pre + 0.044715 * pre * pre * pre))


def gelu(pre):
    return 0.5 * pre * (1.0 + gelu_tanh(pre))


def gelu_slope(pre):
    tanh_val = gelu_tanh(pre)
    return 0.5 * (1.0 + tanh_val) + 0.5 * pre * (1.0 - tanh_val * tanh_val) * 0.7978845608028654 * (1.0 + 0.134145 * pre * pre)


def kernel(x_ref, h_ref, wu_ref, wd_ref, g_ref, gx_ref, up_ref, down_ref, rest_ref, gb_ref, rxh_ref,
           lt, wd, wu, cbuf, gr, hr, dh, ha, gown, xown, pm, pp, pb, rxo, zp, z1, z2,
           zs, z_r1, z_r2, z_ts, z_tl, z_rt, c1, c2, c3,
           ag_x, ag_y, ag_d, ag_p, ag_s, ag_f, ag_l, pp_s, pb_r, pm_s, rx_r, pbc,
           ld_c, ld_g, ld_h, ld_a, ld_w, ld_o, ld_rx, st_gx, first_s, first_l):
    rows, hidden = gown.shape
    ffn = lt.shape[1]
    half_rows = rows // 2
    cw = hidden // CHUNKS
    fb = ffn // 4

    me = lax.axis_index("model")
    spot = lax.axis_index("data")
    core = lax.rem(me, 2)
    px = lax.rem(me // 2, 2)
    py = me // 4
    partner = me + 1 - 2 * core
    step_x, step_y = 2 * (1 - 2 * px), 4 * (1 - 2 * py)
    near_x, near_y, far = me + step_x, me + step_y, me + step_x + step_y
    is_end = jnp.logical_or(spot == 0, spot == 3)
    is_mid = jnp.logical_not(is_end)
    line_mid = jnp.where(spot < 2, 1, 2)
    line_end = jnp.where(spot < 2, 0, 3)
    line_across = 3 - spot

    def model(i):
        return {"model": i}

    def data(i):
        return {"data": i}

    def signal(sem, where):
        pl.semaphore_signal(sem, inc=1, device_id=where, device_id_type=MESH)

    def remote(src, dst, send, recv, where):
        return pltpu.make_async_remote_copy(src_ref=src, dst_ref=dst, send_sem=send, recv_sem=recv, device_id=where, device_id_type=MESH)

    def take(ref, sem):
        pltpu.make_async_copy(ref, ref, sem).wait()

    def chunk_columns(c):
        return pl.ds(pl.multiple_of(c * cw, cw), cw)

    def row_block(i):
        return pl.ds(pl.multiple_of(i * rows, rows), rows)

    def gather_keep(gid, own, first=0):
        for c in range(first, CHUNKS):
            pltpu.make_async_copy(own.at[:, pl.ds(c * cw, cw)], gb_ref.at[gid, c, row_block(me)], ag_l.at[gid]).start()

    def gather_send(gid, c, own, buf):
        src = own.at[:, chunk_columns(c)]
        dst = buf.at[row_block(me)]
        remote(src, dst, ag_s.at[gid], ag_x.at[gid, c], model(near_x)).start()
        remote(src, dst, ag_s.at[gid], ag_y.at[gid, c], model(near_y)).start()
        remote(src, dst, ag_s.at[gid], ag_p.at[gid, c], model(partner)).start()

    def gather_relay(gid, c, buf, sent, forwarded):
        take(buf.at[row_block(0)], ag_x.at[gid, c])
        take(buf.at[row_block(0)], ag_y.at[gid, c])
        for n, (source, target) in enumerate(((near_x, near_y), (near_y, near_x))):
            @pl.when(core == n)
            def _():
                block = buf.at[row_block(source)]
                remote(block, block, sent, ag_d.at[gid, c], model(target)).start()
        for peer in (near_x, near_y):
            block = buf.at[row_block(peer)]
            remote(block, block, forwarded, ag_p.at[gid, c], model(partner)).start()

    def gather_forward(gid, c, buf, forwarded):
        take(buf.at[row_block(0)], ag_d.at[gid, c])
        block = buf.at[row_block(far)]
        remote(block, block, forwarded, ag_p.at[gid, c], model(partner)).start()

    def gather_wait(gid, c, buf):
        take(buf.at[pl.ds(0, 4 * rows)], ag_p.at[gid, c])

    def gathered(gid, c):
        return gb_ref.at[gid, c]

    def chunk_load(gid, c, slot):
        return pltpu.make_async_copy(gb_ref.at[gid, c], cbuf.at[slot], ld_c.at[slot])

    def act_load(layer, b, ref, sem):
        return pltpu.make_async_copy(h_ref.at[layer, row_block(b)], ref, sem)

    def act_block(b, ref):
        @pl.loop(0, 4)
        def _(f):
            cols = pl.ds(pl.multiple_of(f * fb, fb), fb)
            a = gelu(ref[:, cols].astype(F32)).astype(BF16).astype(F32)
            lt[0, cols, row_block(b)] = a.T.astype(BF16)

    def weight_loads(layer):
        return (pltpu.make_async_copy(wd_ref.at[layer], wd, ld_w.at[0]), pltpu.make_async_copy(wu_ref.at[layer], wu, ld_w.at[1]))

    def unit_place(u):
        r = lax.rem(u // 2 + 1, 4)
        chip = lax.rem(py + r // 2, 2) * 2 + lax.rem(px + lax.rem(r, 2), 2)
        return r, chip

    def unit_rows(u):
        _, chip = unit_place(u)
        start = (chip * 2 + core) * rows + lax.rem(u, 2) * half_rows
        other = (chip * 2 + 1 - core) * rows + lax.rem(u, 2) * half_rows
        return tuple(pl.ds(pl.multiple_of(s, half_rows), half_rows) for s in (start, other))

    def unit_load(gid, layer, u):
        for n, block in enumerate(unit_rows(u)):
            here = pl.ds(n * half_rows, half_rows)
            for c in range(CHUNKS):
                pltpu.make_async_copy(gb_ref.at[gid, c, block], gr.at[here, pl.ds(c * cw, cw)], ld_g).start()
            pltpu.make_async_copy(h_ref.at[layer, block], hr.at[here], ld_h).start()

    def unit_first(u):
        take(gr, ld_g)
        take(hr, ld_h)
        mine, other = unit_rows(u)

        @pl.loop(0, 4)
        def _(f):
            cols = pl.ds(pl.multiple_of(f * fb, fb), fb)
            d_act = lax.dot_general(gr[...], wd[cols, :], NT, preferred_element_type=F32)
            d_pre = (d_act * gelu_slope(hr[:, cols].astype(F32))).astype(BF16)
            dh[:, cols] = d_pre
            flipped = d_pre.astype(F32).T.astype(BF16)
            lt[1, cols, mine] = flipped[:, :half_rows]
            lt[1, cols, other] = flipped[:, half_rows:]

    def unit_second(lp, u):
        order = lp * 8 + u
        slot = lax.rem(order, 2)
        kept = lax.rem(u, SUMS)

        @pl.when(order >= 2)
        def _():
            take(pp.at[slot], pp_s.at[slot])

        @pl.when(jnp.logical_or(u >= SUMS, jnp.logical_and(lp > 0, u >= 8 - SUMS)))
        def _():
            take(pm.at[kept], pm_s.at[kept])

        @pl.loop(0, CHUNKS)
        def _(d):
            cols = chunk_columns(d)
            part = lax.dot_general(dh[...], wu[cols, :], NT, preferred_element_type=F32).astype(BF16)
            pm[kept, :, cols] = part[:half_rows]
            pp[slot, :, cols] = part[half_rows:]

        @pl.when(order >= 2)
        def _():
            pl.semaphore_wait(pbc, 1)

        remote(pp.at[slot], pb.at[slot], pp_s.at[slot], pb_r.at[slot], model(partner)).start()

    def unit_finish(lp, u):
        order = lp * 8 + u
        slot = lax.rem(order, 2)
        kept = lax.rem(u, SUMS)
        r, chip = unit_place(u)
        here = pl.ds(pl.multiple_of(lax.rem(u, 2) * half_rows, half_rows), half_rows)
        take(pb.at[slot], pb_r.at[slot])

        @pl.when(r != 0)
        def _():
            @pl.loop(0, CHUNKS)
            def _(d):
                cols = chunk_columns(d)
                pm[kept, :, cols] = (pm[kept, :, cols].astype(F32) + pb[slot, :, cols].astype(F32)).astype(BF16)

            remote(pm.at[kept], rxh_ref.at[lp, r - 1, here], pm_s.at[kept], rx_r.at[lp * 6 + (r - 1) * 2 + lax.rem(u, 2)],
                   model(chip * 2 + core)).start()

        @pl.when(r == 0)
        def _():
            @pl.loop(0, CHUNKS)
            def _(d):
                cols = chunk_columns(d)
                rxo[here, cols] = (pm[kept, :, cols].astype(F32) + pb[slot, :, cols].astype(F32)).astype(BF16)

        @pl.when(order < 8 * LAYERS - 2)
        def _():
            signal(pbc, model(partner))

    def quarter(n):
        part = rows // 4
        return pl.ds(pl.multiple_of(n * part, part), part)

    def new_gradient_load(lp, n):
        @pl.when(lax.rem(n, 2) == 0)
        def _():
            for r in range(3):
                take(pm.at[0], rx_r.at[lp * 6 + r * 2 + n // 2])

        for r in range(3):
            pltpu.make_async_copy(rxh_ref.at[lp, r, quarter(n)], gr.at[quarter(r)], ld_rx.at[r]).start()

    def new_gradient(n):
        for r in range(3):
            take(gr.at[quarter(0)], ld_rx.at[r])

        @pl.loop(0, CHUNKS)
        def _(d):
            cols = chunk_columns(d)
            total = rxo[quarter(n), cols].astype(F32)
            for r in range(3):
                total += gr[quarter(r), cols].astype(F32)
            gown[quarter(n), cols] = (gown[quarter(n), cols].astype(F32) + total).astype(BF16)

    def piece_place(i):
        return LAYERS - 1 - i // PER_LAYER, lax.rem(i // PHASE, 2), lax.rem(i, PHASE) // PARTS, lax.rem(i, PARTS)

    def part_columns(n):
        return pl.ds(pl.multiple_of(n * fb, fb), fb)

    def piece(i):
        _, phase, _, n = piece_place(i)
        slot = lax.rem(i, SLOTS)

        @pl.when(jnp.logical_and(is_end, i >= SLOTS))
        def _():
            take(zp.at[slot], zs.at[slot])

        part = jnp.dot(lt[phase, part_columns(n), :], cbuf[lax.rem(i // PARTS, 2)], preferred_element_type=F32)

        @pl.when(phase == 0)
        def _():
            zp[slot] = part

        @pl.when(phase == 1)
        def _():
            zp[slot] = part.T

    def total_place(j):
        layer, _, c, n = piece_place(j)
        return down_ref.at[layer, part_columns(n), chunk_columns(c)], up_ref.at[layer, chunk_columns(c), part_columns(n)]

    def line_step(i):
        @pl.when(is_end)
        def _():
            @pl.when(i < PIECES)
            def _():
                slot, there = lax.rem(i, SLOTS), lax.rem(i, FIRST_SLOTS)

                @pl.when(i >= FIRST_SLOTS)
                def _():
                    pl.semaphore_wait(c1, 1)

                remote(zp.at[slot], z1.at[there], zs.at[slot], z_r1.at[there], data(line_mid)).start()

            j = i - LAG_LAST

            @pl.when(jnp.logical_and(j >= 0, j < FULL))
            def _():
                take(zp.at[0], z_rt.at[lax.rem(j, LAST_SLOTS)])

                @pl.when(j + LAST_SLOTS < FULL)
                def _():
                    signal(c3, data(line_mid))

        @pl.when(is_mid)
        def _():
            slot, there = lax.rem(i, SLOTS), lax.rem(i, FIRST_SLOTS)
            j = i - LAG_SUM
            old = lax.rem(j + SLOTS, SLOTS)

            @pl.when(jnp.logical_and(j >= 0, j < PIECES))
            def _():
                take(z2.at[old], z_r2.at[old])
                z2[old] = z2[old] + zp[old]
                take(zp.at[old], zs.at[old])

                @pl.when(jnp.logical_and(j >= LAST_SLOTS, j < FULL))
                def _():
                    pl.semaphore_wait(c3, 1)

            @pl.when(i < PIECES)
            def _():
                take(z1.at[there], z_r1.at[there])
                zp[slot] = zp[slot] + z1[there]

            @pl.when(jnp.logical_and(j >= FULL, j < PIECES))
            def _():
                pltpu.make_async_copy(z2.at[old], rest_ref.at[:, part_columns(j - FULL)], z_tl.at[old]).start()

            @pl.when(jnp.logical_and(j >= 0, j < FULL))
            def _():
                _, phase, _, _ = piece_place(j)
                for kind, place in enumerate(total_place(j)):
                    @pl.when(phase == kind)
                    def _():
                        remote(z2.at[old], place, z_ts.at[old], z_rt.at[lax.rem(j, LAST_SLOTS)], data(line_end)).start()
                        pltpu.make_async_copy(z2.at[old], place, z_tl.at[old]).start()

            @pl.when(i < PIECES)
            def _():
                @pl.when(i + FIRST_SLOTS < PIECES)
                def _():
                    signal(c1, data(line_end))

                @pl.when(i >= SLOTS)
                def _():
                    pl.semaphore_wait(c2, 1)

                remote(zp.at[slot], z2.at[slot], zs.at[slot], z_r2.at[slot], data(line_across)).start()

            k = i - LAG_FREE

            @pl.when(jnp.logical_and(k >= 0, k < PIECES))
            def _():
                free = lax.rem(k, SLOTS)
                @pl.when(k < FULL)
                def _():
                    take(z2.at[free], z_ts.at[free])

                take(z2.at[free], z_tl.at[free])

                @pl.when(k + SLOTS < PIECES)
                def _():
                    signal(c2, data(line_across))

    top = LAYERS - 1
    loads_g = [pltpu.make_async_copy(g_ref.at[:, part], gown.at[:, part], sem)
               for part, sem in ((pl.ds(0, cw), ld_rx.at[0]), (pl.ds(cw, hidden - cw), ld_o))]
    for load in loads_g:
        load.start()
    held = ((ha, ld_a), (hr, ld_h))
    for n, (ref, sem) in enumerate(held):
        act_load(top, n, ref, sem).start()
    barrier = pltpu.get_barrier_semaphore()
    for peer in (near_x, near_y, far, partner):
        signal(barrier, model(peer))

    @pl.when(is_end)
    def _():
        signal(barrier, data(line_mid))
        pl.semaphore_wait(barrier, 5)

    @pl.when(is_mid)
    def _():
        signal(barrier, data(line_end))
        signal(barrier, data(line_across))
        pl.semaphore_wait(barrier, 6)

    loads_g[0].wait()
    first_chunk = cbuf.at[0]
    gather_send(0, 0, gown, first_chunk)
    cbuf[0, row_block(me), :] = gown[:, :cw]
    loads_g[1].wait()
    gather_keep(0, gown, 1)
    load_x = pltpu.make_async_copy(x_ref.at[top], xown, ld_o)
    load_x.start()
    for load in weight_loads(top):
        load.start()

    @pl.loop(0, 4)
    def _(b):
        for n, (ref, sem) in enumerate(held):
            act_load(top, 0, ref, sem).wait()
            act_block(2 * b + n, ref)

            @pl.when(b < 3)
            def _():
                act_load(top, 2 * b + n + 2, ref, sem).start()

        @pl.when(b == 2)
        def _():
            gather_relay(0, 0, first_chunk, first_s, first_s)
            gather_send(0, 1, gown, gathered(0, 1))

    load_x.wait()
    gather_forward(0, 0, first_chunk, first_s)
    gather_send(0, 2, gown, gathered(0, 2))
    gather_wait(0, 0, first_chunk)
    take(gown.at[:, pl.ds(0, hidden - cw)], ag_l.at[0])
    pltpu.make_async_copy(first_chunk, gathered(0, 0), first_l).start()

    @pl.loop(0, PIECES + LAG_LAST)
    def _(i):
        lp = i // PER_LAYER
        layer = LAYERS - 1 - lp
        s = i // 2
        sl = lax.rem(s, PER_LAYER // 2)
        il = lax.rem(i, PER_LAYER)
        even = lax.rem(i, 2) == 0
        odd = jnp.logical_not(even)
        odd_pair = lax.rem(s, 2) == 1
        even_pair = jnp.logical_not(odd_pair)
        ggid, xgid = 2 * lp, 2 * lp + 1
        live = i < PIECES

        @pl.when(live)
        def _():
            @pl.when(jnp.logical_and(i > 0, lax.rem(i, PARTS) == 0))
            def _():
                take(cbuf.at[0], ld_c.at[lax.rem(i // PARTS, 2)])

            piece(i)

        line_step(i)

        def when(*conds):
            return pl.when(functools.reduce(jnp.logical_and, conds, live))

        @when(even, s < CHUNKS - 1)
        def _():
            gather_relay(0, s + 1, gathered(0, s + 1), ag_s.at[0], ag_f.at[0])

        @when(even, s < CHUNKS - 3)
        def _():
            gather_send(0, s + 3, gown, gathered(0, s + 3))

        @when(even, s >= 1, s < CHUNKS)
        def _():
            gather_forward(0, s, gathered(0, s), ag_f.at[0])

        @when(odd, s >= 1, s < CHUNKS)
        def _():
            gather_wait(0, s, gathered(0, s))

        @when(i == 2 * PARTS - 2)
        def _():
            take(cbuf.at[0, pl.ds(0, 4 * rows)], first_s)
            take(cbuf.at[0], first_l)

        @when(even, sl == X_RUNS[0][2])
        def _():
            gather_keep(xgid, xown)

        for first, count, start, relay, forward in X_RUNS:
            @when(even, sl >= start, sl < start + count)
            def _():
                gather_send(xgid, sl - start + first, xown, gathered(xgid, sl - start + first))

            @when(even, sl >= start + relay, sl < start + relay + count)
            def _():
                gather_relay(xgid, sl - start - relay + first, gathered(xgid, sl - start - relay + first), ag_s.at[xgid], ag_f.at[xgid])

            @when(even, sl >= start + forward, sl < start + forward + count)
            def _():
                gather_forward(xgid, sl - start - forward + first, gathered(xgid, sl - start - forward + first), ag_f.at[xgid])

        @when(odd, sl == 15)
        def _():
            take(xown, ag_l.at[xgid])

        @when(odd, odd_pair, sl >= 15, sl < 31)
        def _():
            gather_wait(xgid, (sl - 15) // 2, gathered(xgid, (sl - 15) // 2))

        @when(even, s == 25)
        def _():
            gather_keep(2, gown)

        @when(even, s >= 25, s < 25 + CHUNKS)
        def _():
            gather_send(2, s - 25, gown, gathered(2, s - 25))

        @when(even, s >= 27, s < 27 + CHUNKS)
        def _():
            gather_relay(2, s - 27, gathered(2, s - 27), ag_s.at[2], ag_f.at[2])

        @when(even, s >= 29, s < 29 + CHUNKS)
        def _():
            gather_forward(2, s - 29, gathered(2, s - 29), ag_f.at[2])

        @when(odd, s == 30)
        def _():
            take(gown, ag_l.at[2])

        @when(odd, s >= 30, s < 30 + CHUNKS)
        def _():
            gather_wait(2, s - 30, gathered(2, s - 30))

        @when(lax.rem(i, PARTS) == PARTS - 1, i + 1 < PIECES)
        def _():
            nxt = i + 1
            chunk_load(nxt // PHASE, lax.rem(nxt, PHASE) // PARTS, lax.rem(nxt // PARTS, 2)).start()

        @when(even, sl == UNIT_STEP)
        def _():
            for load in weight_loads(0):
                load.wait()

        @when(even, sl >= UNIT_STEP, sl < UNIT_STEP + 8)
        def _():
            unit_first(sl - UNIT_STEP)

        @when(even, sl > UNIT_STEP, sl <= UNIT_STEP + 8)
        def _():
            unit_finish(lp, sl - UNIT_STEP - 1)

        @when(odd, sl >= UNIT_STEP - 1, sl < UNIT_STEP + 7)
        def _():
            unit_load(ggid, layer, sl - UNIT_STEP + 1)

        @when(odd, sl >= UNIT_STEP, sl < UNIT_STEP + 8)
        def _():
            unit_second(lp, sl - UNIT_STEP)

        @when(il == FINAL_STEP - 1)
        def _():
            take(gb_ref.at[ggid, 0, pl.ds(0, 7 * rows)], ag_s.at[ggid])
            take(gb_ref.at[ggid, pl.ds(0, 3)], ag_s.at[ggid])

            @pl.when(lp > 0)
            def _():
                take(gb_ref.at[ggid, 0, row_block(0)], ag_s.at[ggid])

            new_gradient_load(lp, 0)

        @when(il >= FINAL_STEP, il < FINAL_STEP + 4)
        def _():
            new_gradient(il - FINAL_STEP)

            @pl.when(il < FINAL_STEP + 3)
            def _():
                new_gradient_load(lp, il - FINAL_STEP + 1)

        @when(i == PER_LAYER + FINAL_STEP + 4)
        def _():
            pltpu.make_async_copy(gown, gx_ref, st_gx).start()

        @when(lp == 0, even, sl == 17)
        def _():
            for load in weight_loads(0):
                load.start()

        @when(lp == 0, even, even_pair, sl >= 16)
        def _():
            act_load(0, (sl - 16) // 2, ha, ld_a).start()

        @when(lp == 0, odd, odd_pair, sl >= 16)
        def _():
            act_load(0, 0, ha, ld_a).wait()
            act_block((sl - 16) // 2, ha)

        @when(even, sl == 31)
        def _():
            take(gb_ref.at[xgid, pl.ds(0, 4)], ag_s.at[xgid])

            @pl.when(lp == 0)
            def _():
                pltpu.make_async_copy(x_ref.at[0], xown, ld_o).start()

        @when(lp == 0, odd, sl == 31)
        def _():
            pltpu.make_async_copy(x_ref.at[0], xown, ld_o).wait()

    take(gb_ref.at[0, 0, pl.ds(0, 5 * rows)], ag_f.at[0])
    take(gb_ref.at[0, pl.ds(0, 2)], ag_f.at[0])
    for gid in range(1, 2 * LAYERS):
        take(gb_ref.at[gid, pl.ds(0, 3)], ag_f.at[gid])
    for slot in range(2):
        take(pp.at[slot], pp_s.at[slot])
    for kept in range(8 - SUMS, SUMS):
        take(pm.at[kept], pm_s.at[kept])
    take(gown, st_gx)

    @pl.when(is_end)
    def _():
        for slot in range(SLOTS):
            take(zp.at[slot], zs.at[slot])


def move_kernel(count, *refs):
    sources, targets = refs[:count], refs[count:2 * count]
    buffers, read, written = refs[2 * count:3 * count], refs[-2], refs[-1]
    copies, slot = [], 0
    for source, target, buffer in zip(sources, targets, buffers):
        size = buffer.shape[1]
        for n in range(buffer.shape[0]):
            rows = pl.ds(n * size, size)
            copies.append((pltpu.make_async_copy(source.at[rows], buffer.at[n], read.at[slot]),
                           pltpu.make_async_copy(buffer.at[n], target.at[rows], written.at[slot])))
            slot += 1
    for first, _ in copies:
        first.start()
    for first, _ in copies:
        first.wait()
    for _, second in copies:
        second.start()
    for _, second in copies:
        second.wait()


def move(*arrays):
    flat = [a.reshape(-1, a.shape[-1]) for a in arrays]
    parts = [max(1, a.size * a.dtype.itemsize // MOVE_BYTES) for a in flat]
    any_space = pl.BlockSpec(memory_space=pl.ANY)
    size = sum(a.size * a.dtype.itemsize for a in flat)
    moved = pl.pallas_call(
        functools.partial(move_kernel, len(flat)),
        name="move",
        out_shape=tuple(jax.ShapeDtypeStruct(a.shape, a.dtype) for a in flat),
        in_specs=[any_space] * len(flat),
        out_specs=(any_space,) * len(flat),
        scratch_shapes=[pltpu.VMEM((n, a.shape[0] // n, a.shape[1]), a.dtype) for a, n in zip(flat, parts)]
        + [pltpu.SemaphoreType.DMA((sum(parts),))] * 2,
        compiler_params=pltpu.CompilerParams(vmem_limit_bytes=67043328),
        cost_estimate=pl.CostEstimate(flops=int(size * MOVE_FLOPS), bytes_accessed=2 * size, transcendentals=0),
    )(*flat)
    return [m.reshape(a.shape) for m, a in zip(moved, arrays)]


def solution(mesh):
    def device_step(x_saved, h_saved, w_up, w_down, grad_out):
        layers, hidden, ffn = w_up.shape
        rows = grad_out.shape[1]
        tokens = h_saved.shape[2]
        cw, fb = hidden // CHUNKS, ffn // PARTS
        half_rows = rows // 2
        any_space = pl.BlockSpec(memory_space=pl.ANY)
        dma = pltpu.SemaphoreType.DMA
        vmem = pltpu.VMEM
        grad_x, grad_up, grad_down, rest, _, _ = pl.pallas_call(
            kernel,
            name="backward",
            out_shape=(
                jax.ShapeDtypeStruct((rows, hidden), BF16),
                jax.ShapeDtypeStruct(w_up.shape, F32),
                jax.ShapeDtypeStruct(w_down.shape, F32),
                jax.ShapeDtypeStruct((cw, REST * fb), F32),
                jax.ShapeDtypeStruct((2 * layers, CHUNKS, tokens, cw), BF16),
                jax.ShapeDtypeStruct((layers, 3, rows, hidden), BF16),
            ),
            in_specs=[any_space] * 5,
            out_specs=(any_space,) * 6,
            scratch_shapes=[
                vmem((2, ffn, tokens), BF16),
                vmem((ffn, hidden), BF16),
                vmem((hidden, ffn), BF16),
                vmem((2, tokens, cw), BF16),
                vmem((rows, hidden), BF16),
                vmem((rows, ffn), BF16),
                vmem((rows, ffn), BF16),
                vmem((rows, ffn), BF16),
                vmem((rows, hidden), BF16),
                vmem((rows, hidden), BF16),
                vmem((SUMS, half_rows, hidden), BF16),
                vmem((2, half_rows, hidden), BF16),
                vmem((2, half_rows, hidden), BF16),
                vmem((rows, hidden), BF16),
                vmem((SLOTS, fb, cw), F32),
                vmem((FIRST_SLOTS, fb, cw), F32),
                vmem((SLOTS, fb, cw), F32),
                dma((SLOTS,)), dma((FIRST_SLOTS,)), dma((SLOTS,)), dma((SLOTS,)), dma((SLOTS,)), dma((LAST_SLOTS,)),
                pltpu.SemaphoreType.REGULAR, pltpu.SemaphoreType.REGULAR, pltpu.SemaphoreType.REGULAR,
                dma((2 * layers, CHUNKS)), dma((2 * layers, CHUNKS)), dma((2 * layers, CHUNKS)), dma((2 * layers, CHUNKS)),
                dma((2 * layers,)), dma((2 * layers,)), dma((2 * layers,)),
                dma((2,)), dma((2,)), dma((SUMS,)), dma((6 * layers,)), pltpu.SemaphoreType.REGULAR,
                dma((2,)), dma(()), dma(()), dma(()), dma((2,)), dma(()), dma((3,)), dma(()), dma(()), dma(()),
            ],
            compiler_params=pltpu.CompilerParams(collective_id=0, has_side_effects=True, vmem_limit_bytes=67043328),
        )(x_saved[:, 0], h_saved[:, 0], w_up, w_down, grad_out[0])
        spot = lax.axis_index("data")
        is_end = (spot == 0) | (spot == 3)
        rest = jnp.where(is_end, lax.ppermute(rest, "data", [(1, 0), (2, 3)]), rest)
        grad_x, grad_up, grad_down = move(grad_x, grad_up, grad_down)
        grad_up = grad_up.at[0, hidden - cw:, ffn - REST * fb:].set(rest)
        return grad_x[None], grad_up, grad_down

    return jax.shard_map(
        device_step,
        mesh=mesh,
        in_specs=(P(None, "data", "model", None), P(None, "data", None, "model"), P(None, None, "model"), P(None, "model", None), P("data", "model", None)),
        out_specs=(P("data", "model", None), P(None, None, "model"), P(None, "model", None)),
        check_vma=False,
    )
```

```python
import functools

import jax
import jax.numpy as jnp
from jax import lax
from jax.experimental import pallas as pl
from jax.experimental.pallas import tpu as pltpu
from jax.sharding import PartitionSpec as P

MESH = pl.DeviceIdType.MESH
F32, BF16 = jnp.float32, jnp.bfloat16
NT = (((1,), (1,)), ((), ()))

LAYERS = 2
CHUNKS = 8
PARTS = 4
PHASE = CHUNKS * PARTS
PER_LAYER = 2 * PHASE
PIECES = LAYERS * PER_LAYER
REST = 2
FULL = PIECES - REST
SLOTS = 16
FIRST_SLOTS = 8
SPLIT = 4
LAST_SLOTS = 32
LAG_SUM = 2
LAG_FREE = 6
LAG_LAST = 20
UNIT_STEP = 8
X_RUNS = ((0, 5, 4, 2, 8), (5, 3, 20, 3, 5))
FINAL_STEP = 46
SUMS = 6

MOVE_BYTES = 1 << 21
MOVE_FLOPS = 10


def gelu_tanh(pre):
    return jnp.tanh(0.7978845608028654 * (pre + 0.044715 * pre * pre * pre))


def gelu(pre):
    return 0.5 * pre * (1.0 + gelu_tanh(pre))


def gelu_slope(pre):
    tanh_val = gelu_tanh(pre)
    return 0.5 * (1.0 + tanh_val) + 0.5 * pre * (1.0 - tanh_val * tanh_val) * 0.7978845608028654 * (1.0 + 0.134145 * pre * pre)


def kernel(x_ref, h_ref, wu_ref, wd_ref, g_ref, gx_ref, up_ref, down_ref, rest_ref, gb_ref, rxh_ref,
           lt, wd, wu, cbuf, gr, hr, dh, ha, gown, xown, pm, pp, pb, rxo, zp, z1, z2,
           zs, z_r1, z_r2, z_ts, z_tl, z_rt, c1, c2, c3,
           ag_x, ag_y, ag_d, ag_p, ag_s, ag_f, ag_l, pp_s, pb_r, pm_s, rx_r, pbc,
           ld_c, ld_g, ld_h, ld_a, ld_w, ld_o, ld_rx, st_gx, first_s, first_l):
    rows, hidden = gown.shape
    ffn = lt.shape[1]
    half_rows = rows // 2
    cw = hidden // CHUNKS
    fb = ffn // 4

    me = lax.axis_index("model")
    spot = lax.axis_index("data")
    core = lax.rem(me, 2)
    px = lax.rem(me // 2, 2)
    py = me // 4
    partner = me + 1 - 2 * core
    step_x, step_y = 2 * (1 - 2 * px), 4 * (1 - 2 * py)
    near_x, near_y, far = me + step_x, me + step_y, me + step_x + step_y
    is_end = jnp.logical_or(spot == 0, spot == 3)
    is_mid = jnp.logical_not(is_end)
    line_mid = jnp.where(spot < 2, 1, 2)
    line_end = jnp.where(spot < 2, 0, 3)
    line_across = 3 - spot

    def model(i):
        return {"model": i}

    def data(i):
        return {"data": i}

    def signal(sem, where):
        pl.semaphore_signal(sem, inc=1, device_id=where, device_id_type=MESH)

    def remote(src, dst, send, recv, where):
        return pltpu.make_async_remote_copy(src_ref=src, dst_ref=dst, send_sem=send, recv_sem=recv, device_id=where, device_id_type=MESH)

    def take(ref, sem):
        pltpu.make_async_copy(ref, ref, sem).wait()

    def chunk_columns(c):
        return pl.ds(pl.multiple_of(c * cw, cw), cw)

    def row_block(i):
        return pl.ds(pl.multiple_of(i * rows, rows), rows)

    def gather_keep(gid, own, first=0):
        for c in range(first, CHUNKS):
            pltpu.make_async_copy(own.at[:, pl.ds(c * cw, cw)], gb_ref.at[gid, c, row_block(me)], ag_l.at[gid]).start()

    def gather_send(gid, c, own, buf):
        src = own.at[:, chunk_columns(c)]
        dst = buf.at[row_block(me)]
        remote(src, dst, ag_s.at[gid], ag_x.at[gid, c], model(near_x)).start()
        remote(src, dst, ag_s.at[gid], ag_y.at[gid, c], model(near_y)).start()
        remote(src, dst, ag_s.at[gid], ag_p.at[gid, c], model(partner)).start()

    def gather_relay(gid, c, buf, sent, forwarded):
        take(buf.at[row_block(0)], ag_x.at[gid, c])
        take(buf.at[row_block(0)], ag_y.at[gid, c])
        for n, (source, target) in enumerate(((near_x, near_y), (near_y, near_x))):
            @pl.when(core == n)
            def _():
                block = buf.at[row_block(source)]
                remote(block, block, sent, ag_d.at[gid, c], model(target)).start()
        for peer in (near_x, near_y):
            block = buf.at[row_block(peer)]
            remote(block, block, forwarded, ag_p.at[gid, c], model(partner)).start()

    def gather_forward(gid, c, buf, forwarded):
        take(buf.at[row_block(0)], ag_d.at[gid, c])
        block = buf.at[row_block(far)]
        remote(block, block, forwarded, ag_p.at[gid, c], model(partner)).start()

    def gather_wait(gid, c, buf):
        take(buf.at[pl.ds(0, 4 * rows)], ag_p.at[gid, c])

    def gathered(gid, c):
        return gb_ref.at[gid, c]

    def chunk_load(gid, c, slot):
        return pltpu.make_async_copy(gb_ref.at[gid, c], cbuf.at[slot], ld_c.at[slot])

    def act_load(layer, b, ref, sem):
        return pltpu.make_async_copy(h_ref.at[layer, row_block(b)], ref, sem)

    def act_block(b, ref):
        @pl.loop(0, 4)
        def _(f):
            cols = pl.ds(pl.multiple_of(f * fb, fb), fb)
            a = gelu(ref[:, cols].astype(F32)).astype(BF16).astype(F32)
            lt[0, cols, row_block(b)] = a.T.astype(BF16)

    def weight_loads(layer):
        return (pltpu.make_async_copy(wd_ref.at[layer], wd, ld_w.at[0]), pltpu.make_async_copy(wu_ref.at[layer], wu, ld_w.at[1]))

    def unit_place(u):
        r = lax.rem(u // 2 + 1, 4)
        chip = lax.rem(py + r // 2, 2) * 2 + lax.rem(px + lax.rem(r, 2), 2)
        return r, chip

    def unit_rows(u):
        _, chip = unit_place(u)
        start = (chip * 2 + core) * rows + lax.rem(u, 2) * half_rows
        other = (chip * 2 + 1 - core) * rows + lax.rem(u, 2) * half_rows
        return tuple(pl.ds(pl.multiple_of(s, half_rows), half_rows) for s in (start, other))

    def unit_load(gid, layer, u):
        for n, block in enumerate(unit_rows(u)):
            here = pl.ds(n * half_rows, half_rows)
            for c in range(CHUNKS):
                pltpu.make_async_copy(gb_ref.at[gid, c, block], gr.at[here, pl.ds(c * cw, cw)], ld_g).start()
            pltpu.make_async_copy(h_ref.at[layer, block], hr.at[here], ld_h).start()

    def unit_first(u):
        take(gr, ld_g)
        take(hr, ld_h)
        mine, other = unit_rows(u)

        @pl.loop(0, 4)
        def _(f):
            cols = pl.ds(pl.multiple_of(f * fb, fb), fb)
            d_act = lax.dot_general(gr[...], wd[cols, :], NT, preferred_element_type=F32)
            d_pre = (d_act * gelu_slope(hr[:, cols].astype(F32))).astype(BF16)
            dh[:, cols] = d_pre
            flipped = d_pre.astype(F32).T.astype(BF16)
            lt[1, cols, mine] = flipped[:, :half_rows]
            lt[1, cols, other] = flipped[:, half_rows:]

    def unit_second(lp, u):
        order = lp * 8 + u
        slot = lax.rem(order, 2)
        kept = lax.rem(u, SUMS)

        @pl.when(order >= 2)
        def _():
            take(pp.at[slot], pp_s.at[slot])

        @pl.when(jnp.logical_or(u >= SUMS, jnp.logical_and(lp > 0, u >= 8 - SUMS)))
        def _():
            take(pm.at[kept], pm_s.at[kept])

        @pl.loop(0, CHUNKS)
        def _(d):
            cols = chunk_columns(d)
            part = lax.dot_general(dh[...], wu[cols, :], NT, preferred_element_type=F32).astype(BF16)
            pm[kept, :, cols] = part[:half_rows]
            pp[slot, :, cols] = part[half_rows:]

        @pl.when(order >= 2)
        def _():
            pl.semaphore_wait(pbc, 1)

        remote(pp.at[slot], pb.at[slot], pp_s.at[slot], pb_r.at[slot], model(partner)).start()

    def unit_finish(lp, u):
        order = lp * 8 + u
        slot = lax.rem(order, 2)
        kept = lax.rem(u, SUMS)
        r, chip = unit_place(u)
        here = pl.ds(pl.multiple_of(lax.rem(u, 2) * half_rows, half_rows), half_rows)
        take(pb.at[slot], pb_r.at[slot])

        @pl.when(r != 0)
        def _():
            @pl.loop(0, CHUNKS)
            def _(d):
                cols = chunk_columns(d)
                pm[kept, :, cols] = (pm[kept, :, cols].astype(F32) + pb[slot, :, cols].astype(F32)).astype(BF16)

            remote(pm.at[kept], rxh_ref.at[lp, r - 1, here], pm_s.at[kept], rx_r.at[lp * 6 + (r - 1) * 2 + lax.rem(u, 2)],
                   model(chip * 2 + core)).start()

        @pl.when(r == 0)
        def _():
            @pl.loop(0, CHUNKS)
            def _(d):
                cols = chunk_columns(d)
                rxo[here, cols] = (pm[kept, :, cols].astype(F32) + pb[slot, :, cols].astype(F32)).astype(BF16)

        @pl.when(order < 8 * LAYERS - 2)
        def _():
            signal(pbc, model(partner))

    def quarter(n):
        part = rows // 4
        return pl.ds(pl.multiple_of(n * part, part), part)

    def new_gradient_load(lp, n):
        @pl.when(lax.rem(n, 2) == 0)
        def _():
            for r in range(3):
                take(pm.at[0], rx_r.at[lp * 6 + r * 2 + n // 2])

        for r in range(3):
            pltpu.make_async_copy(rxh_ref.at[lp, r, quarter(n)], gr.at[quarter(r)], ld_rx.at[r]).start()

    def new_gradient(n):
        for r in range(3):
            take(gr.at[quarter(0)], ld_rx.at[r])

        @pl.loop(0, CHUNKS)
        def _(d):
            cols = chunk_columns(d)
            total = rxo[quarter(n), cols].astype(F32)
            for r in range(3):
                total += gr[quarter(r), cols].astype(F32)
            gown[quarter(n), cols] = (gown[quarter(n), cols].astype(F32) + total).astype(BF16)

    def split(q):
        return pl.ds(q * (fb // SPLIT), fb // SPLIT)

    def piece_place(i):
        return LAYERS - 1 - i // PER_LAYER, lax.rem(i // PHASE, 2), lax.rem(i, PHASE) // PARTS, lax.rem(i, PARTS)

    def part_columns(n):
        return pl.ds(pl.multiple_of(n * fb, fb), fb)

    def piece(i):
        _, phase, _, n = piece_place(i)
        slot = lax.rem(i, SLOTS)

        @pl.when(jnp.logical_and(is_end, i >= SLOTS))
        def _():
            take(zp.at[slot], zs.at[slot])

        part = jnp.dot(lt[phase, part_columns(n), :], cbuf[lax.rem(i // PARTS, 2)], preferred_element_type=F32)

        @pl.when(phase == 0)
        def _():
            zp[slot] = part

        @pl.when(phase == 1)
        def _():
            zp[slot] = part.T

    def total_place(j):
        layer, _, c, n = piece_place(j)
        return down_ref.at[layer, part_columns(n), chunk_columns(c)], up_ref.at[layer, chunk_columns(c), part_columns(n)]

    def total_send(j, slot):
        @pl.when(jnp.logical_and(j >= 0, j < FULL))
        def _():
            _, phase, _, _ = piece_place(j)
            for kind, place in enumerate(total_place(j)):
                @pl.when(phase == kind)
                def _():
                    remote(z2.at[slot], place, z_ts.at[slot], z_rt.at[lax.rem(j, LAST_SLOTS)], data(line_end)).start()
                    pltpu.make_async_copy(z2.at[slot], place, z_tl.at[slot]).start()

    def sum_send(slot, q):
        remote(zp.at[slot, split(q)], z2.at[slot, split(q)], zs.at[slot], z_r2.at[slot], data(line_across)).start()

    def line_step(i):
        @pl.when(is_end)
        def _():
            @pl.when(i < PIECES)
            def _():
                slot, there = lax.rem(i, SLOTS), lax.rem(i, FIRST_SLOTS)

                @pl.when(i >= FIRST_SLOTS)
                def _():
                    pl.semaphore_wait(c1, 1)

                for q in range(SPLIT):
                    remote(zp.at[slot, split(q)], z1.at[there, split(q)], zs.at[slot], z_r1.at[there, q], data(line_mid)).start()

            j = i - LAG_LAST

            @pl.when(jnp.logical_and(j >= 0, j < FULL))
            def _():
                take(zp.at[0], z_rt.at[lax.rem(j, LAST_SLOTS)])

                @pl.when(j + LAST_SLOTS < FULL)
                def _():
                    signal(c3, data(line_mid))

        @pl.when(is_mid)
        def _():
            slot, there = lax.rem(i, SLOTS), lax.rem(i, FIRST_SLOTS)
            j = i - LAG_SUM
            old = lax.rem(j + SLOTS, SLOTS)

            @pl.when(jnp.logical_and(j >= 0, j < PIECES))
            def _():
                take(z2.at[old], z_r2.at[old])
                z2[old] = z2[old] + zp[old]
                take(zp.at[old], zs.at[old])

                @pl.when(jnp.logical_and(j >= LAST_SLOTS, j < FULL))
                def _():
                    pl.semaphore_wait(c3, 1)

            @pl.when(jnp.logical_and(j >= FULL, j < PIECES))
            def _():
                pltpu.make_async_copy(z2.at[old], rest_ref.at[:, part_columns(j - FULL)], z_tl.at[old]).start()

            @pl.when(i < PIECES)
            def _():
                @pl.when(i >= SLOTS)
                def _():
                    pl.semaphore_wait(c2, 1)

                for q in range(SPLIT):
                    take(z1.at[there, split(q)], z_r1.at[there, q])
                    zp[slot, split(q), :] = zp[slot, split(q), :] + z1[there, split(q), :]

                    if q == 0:
                        total_send(j, old)
                    else:
                        sum_send(slot, q - 1)
                sum_send(slot, SPLIT - 1)

                @pl.when(i + FIRST_SLOTS < PIECES)
                def _():
                    signal(c1, data(line_end))

            @pl.when(i >= PIECES)
            def _():
                total_send(j, old)

            k = i - LAG_FREE

            @pl.when(jnp.logical_and(k >= 0, k < PIECES))
            def _():
                free = lax.rem(k, SLOTS)
                @pl.when(k < FULL)
                def _():
                    take(z2.at[free], z_ts.at[free])

                take(z2.at[free], z_tl.at[free])

                @pl.when(k + SLOTS < PIECES)
                def _():
                    signal(c2, data(line_across))

    top = LAYERS - 1
    loads_g = [pltpu.make_async_copy(g_ref.at[:, part], gown.at[:, part], sem)
               for part, sem in ((pl.ds(0, cw), ld_rx.at[0]), (pl.ds(cw, hidden - cw), ld_o))]
    for load in loads_g:
        load.start()
    held = ((ha, ld_a), (hr, ld_h))
    for n, (ref, sem) in enumerate(held):
        act_load(top, n, ref, sem).start()
    barrier = pltpu.get_barrier_semaphore()
    for peer in (near_x, near_y, far, partner):
        signal(barrier, model(peer))

    @pl.when(is_end)
    def _():
        signal(barrier, data(line_mid))
        pl.semaphore_wait(barrier, 5)

    @pl.when(is_mid)
    def _():
        signal(barrier, data(line_end))
        signal(barrier, data(line_across))
        pl.semaphore_wait(barrier, 6)

    loads_g[0].wait()
    first_chunk = cbuf.at[0]
    gather_send(0, 0, gown, first_chunk)
    cbuf[0, row_block(me), :] = gown[:, :cw]
    loads_g[1].wait()
    gather_keep(0, gown, 1)
    load_x = pltpu.make_async_copy(x_ref.at[top], xown, ld_o)
    load_x.start()
    for load in weight_loads(top):
        load.start()

    @pl.loop(0, 4)
    def _(b):
        for n, (ref, sem) in enumerate(held):
            act_load(top, 0, ref, sem).wait()
            act_block(2 * b + n, ref)

            @pl.when(b < 3)
            def _():
                act_load(top, 2 * b + n + 2, ref, sem).start()

        @pl.when(b == 2)
        def _():
            gather_relay(0, 0, first_chunk, first_s, first_s)
            gather_send(0, 1, gown, gathered(0, 1))

    load_x.wait()
    gather_forward(0, 0, first_chunk, first_s)
    gather_send(0, 2, gown, gathered(0, 2))
    gather_wait(0, 0, first_chunk)
    take(gown.at[:, pl.ds(0, hidden - cw)], ag_l.at[0])
    pltpu.make_async_copy(first_chunk, gathered(0, 0), first_l).start()

    @pl.loop(0, PIECES + LAG_LAST)
    def _(i):
        lp = i // PER_LAYER
        layer = LAYERS - 1 - lp
        s = i // 2
        sl = lax.rem(s, PER_LAYER // 2)
        il = lax.rem(i, PER_LAYER)
        even = lax.rem(i, 2) == 0
        odd = jnp.logical_not(even)
        odd_pair = lax.rem(s, 2) == 1
        even_pair = jnp.logical_not(odd_pair)
        ggid, xgid = 2 * lp, 2 * lp + 1
        live = i < PIECES

        @pl.when(live)
        def _():
            @pl.when(jnp.logical_and(i > 0, lax.rem(i, PARTS) == 0))
            def _():
                take(cbuf.at[0], ld_c.at[lax.rem(i // PARTS, 2)])

            piece(i)

        line_step(i)

        def when(*conds):
            return pl.when(functools.reduce(jnp.logical_and, conds, live))

        @when(even, s < CHUNKS - 1)
        def _():
            gather_relay(0, s + 1, gathered(0, s + 1), ag_s.at[0], ag_f.at[0])

        @when(even, s < CHUNKS - 3)
        def _():
            gather_send(0, s + 3, gown, gathered(0, s + 3))

        @when(even, s >= 1, s < CHUNKS)
        def _():
            gather_forward(0, s, gathered(0, s), ag_f.at[0])

        @when(odd, s >= 1, s < CHUNKS)
        def _():
            gather_wait(0, s, gathered(0, s))

        @when(i == 2 * PARTS - 2)
        def _():
            take(cbuf.at[0, pl.ds(0, 4 * rows)], first_s)
            take(cbuf.at[0], first_l)

        @when(even, sl == X_RUNS[0][2])
        def _():
            gather_keep(xgid, xown)

        for first, count, start, relay, forward in X_RUNS:
            @when(even, sl >= start, sl < start + count)
            def _():
                gather_send(xgid, sl - start + first, xown, gathered(xgid, sl - start + first))

            @when(even, sl >= start + relay, sl < start + relay + count)
            def _():
                gather_relay(xgid, sl - start - relay + first, gathered(xgid, sl - start - relay + first), ag_s.at[xgid], ag_f.at[xgid])

            @when(even, sl >= start + forward, sl < start + forward + count)
            def _():
                gather_forward(xgid, sl - start - forward + first, gathered(xgid, sl - start - forward + first), ag_f.at[xgid])

        @when(odd, sl == 15)
        def _():
            take(xown, ag_l.at[xgid])

        @when(odd, odd_pair, sl >= 15, sl < 31)
        def _():
            gather_wait(xgid, (sl - 15) // 2, gathered(xgid, (sl - 15) // 2))

        @when(even, s == 25)
        def _():
            gather_keep(2, gown)

        @when(even, s >= 25, s < 25 + CHUNKS)
        def _():
            gather_send(2, s - 25, gown, gathered(2, s - 25))

        @when(even, s >= 27, s < 27 + CHUNKS)
        def _():
            gather_relay(2, s - 27, gathered(2, s - 27), ag_s.at[2], ag_f.at[2])

        @when(even, s >= 29, s < 29 + CHUNKS)
        def _():
            gather_forward(2, s - 29, gathered(2, s - 29), ag_f.at[2])

        @when(odd, s == 30)
        def _():
            take(gown, ag_l.at[2])

        @when(odd, s >= 30, s < 30 + CHUNKS)
        def _():
            gather_wait(2, s - 30, gathered(2, s - 30))

        @when(lax.rem(i, PARTS) == PARTS - 1, i + 1 < PIECES)
        def _():
            nxt = i + 1
            chunk_load(nxt // PHASE, lax.rem(nxt, PHASE) // PARTS, lax.rem(nxt // PARTS, 2)).start()

        @when(even, sl == UNIT_STEP)
        def _():
            for load in weight_loads(0):
                load.wait()

        @when(even, sl >= UNIT_STEP, sl < UNIT_STEP + 8)
        def _():
            unit_first(sl - UNIT_STEP)

        @when(even, sl > UNIT_STEP, sl <= UNIT_STEP + 8)
        def _():
            unit_finish(lp, sl - UNIT_STEP - 1)

        @when(odd, sl >= UNIT_STEP - 1, sl < UNIT_STEP + 7)
        def _():
            unit_load(ggid, layer, sl - UNIT_STEP + 1)

        @when(odd, sl >= UNIT_STEP, sl < UNIT_STEP + 8)
        def _():
            unit_second(lp, sl - UNIT_STEP)

        @when(il == FINAL_STEP - 1)
        def _():
            take(gb_ref.at[ggid, 0, pl.ds(0, 7 * rows)], ag_s.at[ggid])
            take(gb_ref.at[ggid, pl.ds(0, 3)], ag_s.at[ggid])

            @pl.when(lp > 0)
            def _():
                take(gb_ref.at[ggid, 0, row_block(0)], ag_s.at[ggid])

            new_gradient_load(lp, 0)

        @when(il >= FINAL_STEP, il < FINAL_STEP + 4)
        def _():
            new_gradient(il - FINAL_STEP)

            @pl.when(il < FINAL_STEP + 3)
            def _():
                new_gradient_load(lp, il - FINAL_STEP + 1)

        @when(i == PER_LAYER + FINAL_STEP + 4)
        def _():
            pltpu.make_async_copy(gown, gx_ref, st_gx).start()

        @when(lp == 0, even, sl == 17)
        def _():
            for load in weight_loads(0):
                load.start()

        @when(lp == 0, even, even_pair, sl >= 16)
        def _():
            act_load(0, (sl - 16) // 2, ha, ld_a).start()

        @when(lp == 0, odd, odd_pair, sl >= 16)
        def _():
            act_load(0, 0, ha, ld_a).wait()
            act_block((sl - 16) // 2, ha)

        @when(even, sl == 31)
        def _():
            take(gb_ref.at[xgid, pl.ds(0, 4)], ag_s.at[xgid])

            @pl.when(lp == 0)
            def _():
                pltpu.make_async_copy(x_ref.at[0], xown, ld_o).start()

        @when(lp == 0, odd, sl == 31)
        def _():
            pltpu.make_async_copy(x_ref.at[0], xown, ld_o).wait()

    take(gb_ref.at[0, 0, pl.ds(0, 5 * rows)], ag_f.at[0])
    take(gb_ref.at[0, pl.ds(0, 2)], ag_f.at[0])
    for gid in range(1, 2 * LAYERS):
        take(gb_ref.at[gid, pl.ds(0, 3)], ag_f.at[gid])
    for slot in range(2):
        take(pp.at[slot], pp_s.at[slot])
    for kept in range(8 - SUMS, SUMS):
        take(pm.at[kept], pm_s.at[kept])
    take(gown, st_gx)

    @pl.when(is_end)
    def _():
        for slot in range(SLOTS):
            take(zp.at[slot], zs.at[slot])


def move_kernel(count, *refs):
    sources, targets = refs[:count], refs[count:2 * count]
    buffers, read, written = refs[2 * count:3 * count], refs[-2], refs[-1]
    copies, slot = [], 0
    for source, target, buffer in zip(sources, targets, buffers):
        size = buffer.shape[1]
        for n in range(buffer.shape[0]):
            rows = pl.ds(n * size, size)
            copies.append((pltpu.make_async_copy(source.at[rows], buffer.at[n], read.at[slot]),
                           pltpu.make_async_copy(buffer.at[n], target.at[rows], written.at[slot])))
            slot += 1
    for first, _ in copies:
        first.start()
    for first, _ in copies:
        first.wait()
    for _, second in copies:
        second.start()
    for _, second in copies:
        second.wait()


def move(*arrays):
    flat = [a.reshape(-1, a.shape[-1]) for a in arrays]
    parts = [max(1, a.size * a.dtype.itemsize // MOVE_BYTES) for a in flat]
    any_space = pl.BlockSpec(memory_space=pl.ANY)
    size = sum(a.size * a.dtype.itemsize for a in flat)
    moved = pl.pallas_call(
        functools.partial(move_kernel, len(flat)),
        name="move",
        out_shape=tuple(jax.ShapeDtypeStruct(a.shape, a.dtype) for a in flat),
        in_specs=[any_space] * len(flat),
        out_specs=(any_space,) * len(flat),
        scratch_shapes=[pltpu.VMEM((n, a.shape[0] // n, a.shape[1]), a.dtype) for a, n in zip(flat, parts)]
        + [pltpu.SemaphoreType.DMA((sum(parts),))] * 2,
        compiler_params=pltpu.CompilerParams(vmem_limit_bytes=67043328),
        cost_estimate=pl.CostEstimate(flops=int(size * MOVE_FLOPS), bytes_accessed=2 * size, transcendentals=0),
    )(*flat)
    return [m.reshape(a.shape) for m, a in zip(moved, arrays)]


def solution(mesh):
    def device_step(x_saved, h_saved, w_up, w_down, grad_out):
        layers, hidden, ffn = w_up.shape
        rows = grad_out.shape[1]
        tokens = h_saved.shape[2]
        cw, fb = hidden // CHUNKS, ffn // PARTS
        half_rows = rows // 2
        any_space = pl.BlockSpec(memory_space=pl.ANY)
        dma = pltpu.SemaphoreType.DMA
        vmem = pltpu.VMEM
        grad_x, grad_up, grad_down, rest, _, _ = pl.pallas_call(
            kernel,
            name="backward",
            out_shape=(
                jax.ShapeDtypeStruct((rows, hidden), BF16),
                jax.ShapeDtypeStruct(w_up.shape, F32),
                jax.ShapeDtypeStruct(w_down.shape, F32),
                jax.ShapeDtypeStruct((cw, REST * fb), F32),
                jax.ShapeDtypeStruct((2 * layers, CHUNKS, tokens, cw), BF16),
                jax.ShapeDtypeStruct((layers, 3, rows, hidden), BF16),
            ),
            in_specs=[any_space] * 5,
            out_specs=(any_space,) * 6,
            scratch_shapes=[
                vmem((2, ffn, tokens), BF16),
                vmem((ffn, hidden), BF16),
                vmem((hidden, ffn), BF16),
                vmem((2, tokens, cw), BF16),
                vmem((rows, hidden), BF16),
                vmem((rows, ffn), BF16),
                vmem((rows, ffn), BF16),
                vmem((rows, ffn), BF16),
                vmem((rows, hidden), BF16),
                vmem((rows, hidden), BF16),
                vmem((SUMS, half_rows, hidden), BF16),
                vmem((2, half_rows, hidden), BF16),
                vmem((2, half_rows, hidden), BF16),
                vmem((rows, hidden), BF16),
                vmem((SLOTS, fb, cw), F32),
                vmem((FIRST_SLOTS, fb, cw), F32),
                vmem((SLOTS, fb, cw), F32),
                dma((SLOTS,)), dma((FIRST_SLOTS, SPLIT)), dma((SLOTS,)), dma((SLOTS,)), dma((SLOTS,)), dma((LAST_SLOTS,)),
                pltpu.SemaphoreType.REGULAR, pltpu.SemaphoreType.REGULAR, pltpu.SemaphoreType.REGULAR,
                dma((2 * layers, CHUNKS)), dma((2 * layers, CHUNKS)), dma((2 * layers, CHUNKS)), dma((2 * layers, CHUNKS)),
                dma((2 * layers,)), dma((2 * layers,)), dma((2 * layers,)),
                dma((2,)), dma((2,)), dma((SUMS,)), dma((6 * layers,)), pltpu.SemaphoreType.REGULAR,
                dma((2,)), dma(()), dma(()), dma(()), dma((2,)), dma(()), dma((3,)), dma(()), dma(()), dma(()),
            ],
            compiler_params=pltpu.CompilerParams(collective_id=0, has_side_effects=True, vmem_limit_bytes=67043328),
        )(x_saved[:, 0], h_saved[:, 0], w_up, w_down, grad_out[0])
        spot = lax.axis_index("data")
        is_end = (spot == 0) | (spot == 3)
        rest = jnp.where(is_end, lax.ppermute(rest, "data", [(1, 0), (2, 3)]), rest)
        grad_x, grad_up, grad_down = move(grad_x, grad_up, grad_down)
        grad_up = grad_up.at[0, hidden - cw:, ffn - REST * fb:].set(rest)
        return grad_x[None], grad_up, grad_down

    return jax.shard_map(
        device_step,
        mesh=mesh,
        in_specs=(P(None, "data", "model", None), P(None, "data", None, "model"), P(None, None, "model"), P(None, "model", None), P("data", "model", None)),
        out_specs=(P("data", "model", None), P(None, None, "model"), P(None, "model", None)),
        check_vma=False,
    )
```

```python
import functools

import jax
import jax.numpy as jnp
from jax import lax
from jax.experimental import pallas as pl
from jax.experimental.pallas import tpu as pltpu
from jax.sharding import PartitionSpec as P

MESH = pl.DeviceIdType.MESH
F32, BF16 = jnp.float32, jnp.bfloat16
NT = (((1,), (1,)), ((), ()))

LAYERS = 2
CHUNKS = 8
PARTS = 4
PHASE = CHUNKS * PARTS
PER_LAYER = 2 * PHASE
PIECES = LAYERS * PER_LAYER
REST = 2
FULL = PIECES - REST
SLOTS = 16
FIRST_SLOTS = 8
SPLIT = 4
LAST_SLOTS = 32
LAG_SUM = 2
LAG_FREE = 6
LAG_LAST = 20
UNIT_STEP = 8
X_RUNS = ((0, 5, 4, 2, 8), (5, 3, 20, 3, 4))
FINAL_STEP = 46
HELD = 3
SUMS = 6

MOVE_BYTES = 1 << 22
MOVE_FLOPS = 10


def gelu_tanh(pre):
    return jnp.tanh(0.7978845608028654 * (pre + 0.044715 * pre * pre * pre))


def gelu(pre):
    return 0.5 * pre * (1.0 + gelu_tanh(pre))


def gelu_slope(pre):
    tanh_val = gelu_tanh(pre)
    return 0.5 * (1.0 + tanh_val) + 0.5 * pre * (1.0 - tanh_val * tanh_val) * 0.7978845608028654 * (1.0 + 0.134145 * pre * pre)


def kernel(x_ref, h_ref, wu_ref, wd_ref, g_ref, gx_ref, up_ref, down_ref, rest_ref, gb_ref, rxh_ref,
           lt, wd, wu, cbuf, gr, hr, dh, ha, gown, xown, pm, pp, pb, rxo, zp, z1, z2,
           zs, z_r1, z_r2, z_ts, z_tl, z_rt, c1, c2, c3,
           ag_x, ag_y, ag_d, ag_p, ag_s, ag_f, ag_l, pp_s, pb_r, pm_s, rx_r, pbc,
           ld_c, ld_g, ld_h, ld_a, ld_w, ld_o, ld_rx, st_gx, first_s, first_l):
    rows, hidden = gown.shape
    ffn = lt.shape[1]
    half_rows = rows // 2
    cw = hidden // CHUNKS
    fb = ffn // 4

    me = lax.axis_index("model")
    spot = lax.axis_index("data")
    core = lax.rem(me, 2)
    px = lax.rem(me // 2, 2)
    py = me // 4
    partner = me + 1 - 2 * core
    step_x, step_y = 2 * (1 - 2 * px), 4 * (1 - 2 * py)
    near_x, near_y, far = me + step_x, me + step_y, me + step_x + step_y
    is_end = jnp.logical_or(spot == 0, spot == 3)
    is_mid = jnp.logical_not(is_end)
    line_mid = jnp.where(spot < 2, 1, 2)
    line_end = jnp.where(spot < 2, 0, 3)
    line_across = 3 - spot

    def model(i):
        return {"model": i}

    def data(i):
        return {"data": i}

    def signal(sem, where):
        pl.semaphore_signal(sem, inc=1, device_id=where, device_id_type=MESH)

    def remote(src, dst, send, recv, where):
        return pltpu.make_async_remote_copy(src_ref=src, dst_ref=dst, send_sem=send, recv_sem=recv, device_id=where, device_id_type=MESH)

    def take(ref, sem):
        pltpu.make_async_copy(ref, ref, sem).wait()

    def chunk_columns(c):
        return pl.ds(pl.multiple_of(c * cw, cw), cw)

    def row_block(i):
        return pl.ds(pl.multiple_of(i * rows, rows), rows)

    def gather_keep(gid, own, first=0):
        for c in range(first, CHUNKS):
            pltpu.make_async_copy(own.at[:, pl.ds(c * cw, cw)], gb_ref.at[gid, c, row_block(me)], ag_l.at[gid]).start()

    def gather_send(gid, c, own, buf):
        src = own.at[:, chunk_columns(c)]
        dst = buf.at[row_block(me)]
        remote(src, dst, ag_s.at[gid], ag_x.at[gid, c], model(near_x)).start()
        remote(src, dst, ag_s.at[gid], ag_y.at[gid, c], model(near_y)).start()
        remote(src, dst, ag_s.at[gid], ag_p.at[gid, c], model(partner)).start()

    def gather_relay(gid, c, buf, sent, forwarded):
        take(buf.at[row_block(0)], ag_x.at[gid, c])
        take(buf.at[row_block(0)], ag_y.at[gid, c])
        for n, (source, target) in enumerate(((near_x, near_y), (near_y, near_x))):
            @pl.when(core == n)
            def _():
                block = buf.at[row_block(source)]
                remote(block, block, sent, ag_d.at[gid, c], model(target)).start()
        for peer in (near_x, near_y):
            block = buf.at[row_block(peer)]
            remote(block, block, forwarded, ag_p.at[gid, c], model(partner)).start()

    def gather_forward(gid, c, buf, forwarded):
        take(buf.at[row_block(0)], ag_d.at[gid, c])
        block = buf.at[row_block(far)]
        remote(block, block, forwarded, ag_p.at[gid, c], model(partner)).start()

    def gather_wait(gid, c, buf):
        take(buf.at[pl.ds(0, 4 * rows)], ag_p.at[gid, c])

    def gathered(gid, c):
        return gb_ref.at[gid, c]

    def chunk_load(gid, c, slot):
        return pltpu.make_async_copy(gb_ref.at[gid, c], cbuf.at[slot], ld_c.at[slot])

    def act_load(layer, b, ref, sem):
        return pltpu.make_async_copy(h_ref.at[layer, row_block(b)], ref, sem)

    def act_block(b, ref):
        @pl.loop(0, 4)
        def _(f):
            cols = pl.ds(pl.multiple_of(f * fb, fb), fb)
            a = gelu(ref[:, cols].astype(F32)).astype(BF16).astype(F32)
            lt[0, cols, row_block(b)] = a.T.astype(BF16)

    def weight_loads(layer):
        return (pltpu.make_async_copy(wd_ref.at[layer], wd, ld_w.at[0]), pltpu.make_async_copy(wu_ref.at[layer], wu, ld_w.at[1]))

    def unit_place(u):
        r = lax.rem(u // 2 + 1, 4)
        chip = lax.rem(py + r // 2, 2) * 2 + lax.rem(px + lax.rem(r, 2), 2)
        return r, chip

    def unit_rows(u):
        _, chip = unit_place(u)
        start = (chip * 2 + core) * rows + lax.rem(u, 2) * half_rows
        other = (chip * 2 + 1 - core) * rows + lax.rem(u, 2) * half_rows
        return tuple(pl.ds(pl.multiple_of(s, half_rows), half_rows) for s in (start, other))

    def unit_load(gid, layer, u):
        for n, block in enumerate(unit_rows(u)):
            here = pl.ds(n * half_rows, half_rows)
            for c in range(CHUNKS):
                pltpu.make_async_copy(gb_ref.at[gid, c, block], gr.at[here, pl.ds(c * cw, cw)], ld_g).start()
            pltpu.make_async_copy(h_ref.at[layer, block], hr.at[here], ld_h).start()

    def unit_first(u):
        take(gr, ld_g)
        take(hr, ld_h)
        mine, other = unit_rows(u)

        @pl.loop(0, 4)
        def _(f):
            cols = pl.ds(pl.multiple_of(f * fb, fb), fb)
            d_act = lax.dot_general(gr[...], wd[cols, :], NT, preferred_element_type=F32)
            d_pre = (d_act * gelu_slope(hr[:, cols].astype(F32))).astype(BF16)
            dh[:, cols] = d_pre
            flipped = d_pre.astype(F32).T.astype(BF16)
            lt[1, cols, mine] = flipped[:, :half_rows]
            lt[1, cols, other] = flipped[:, half_rows:]

    def unit_second(lp, u):
        order = lp * 8 + u
        slot = lax.rem(order, 2)
        kept = lax.rem(u, SUMS)

        @pl.when(order >= 2)
        def _():
            take(pp.at[slot], pp_s.at[slot])

        @pl.when(jnp.logical_or(u >= SUMS, jnp.logical_and(lp > 0, u >= 8 - SUMS)))
        def _():
            take(pm.at[kept], pm_s.at[kept])

        @pl.loop(0, CHUNKS)
        def _(d):
            cols = chunk_columns(d)
            part = lax.dot_general(dh[...], wu[cols, :], NT, preferred_element_type=F32).astype(BF16)
            pm[kept, :, cols] = part[:half_rows]
            pp[slot, :, cols] = part[half_rows:]

        @pl.when(order >= HELD)
        def _():
            pl.semaphore_wait(pbc, 1)

        there = lax.rem(order, HELD)
        remote(pp.at[slot], pb.at[there], pp_s.at[slot], pb_r.at[there], model(partner)).start()

    def unit_finish(lp, u):
        order = lp * 8 + u
        slot = lax.rem(order, HELD)
        kept = lax.rem(u, SUMS)
        r, chip = unit_place(u)
        here = pl.ds(pl.multiple_of(lax.rem(u, 2) * half_rows, half_rows), half_rows)
        take(pb.at[slot], pb_r.at[slot])

        @pl.when(r != 0)
        def _():
            @pl.loop(0, CHUNKS)
            def _(d):
                cols = chunk_columns(d)
                pm[kept, :, cols] = (pm[kept, :, cols].astype(F32) + pb[slot, :, cols].astype(F32)).astype(BF16)

            remote(pm.at[kept], rxh_ref.at[lp, r - 1, here], pm_s.at[kept], rx_r.at[lp * 6 + (r - 1) * 2 + lax.rem(u, 2)],
                   model(chip * 2 + core)).start()

        @pl.when(r == 0)
        def _():
            @pl.loop(0, CHUNKS)
            def _(d):
                cols = chunk_columns(d)
                rxo[here, cols] = (pm[kept, :, cols].astype(F32) + pb[slot, :, cols].astype(F32)).astype(BF16)

        @pl.when(order < 8 * LAYERS - HELD)
        def _():
            signal(pbc, model(partner))

    def quarter(n):
        part = rows // 4
        return pl.ds(pl.multiple_of(n * part, part), part)

    def new_gradient_load(lp, n):
        @pl.when(lax.rem(n, 2) == 0)
        def _():
            for r in range(3):
                take(pm.at[0], rx_r.at[lp * 6 + r * 2 + n // 2])

        for r in range(3):
            pltpu.make_async_copy(rxh_ref.at[lp, r, quarter(n)], gr.at[quarter(r)], ld_rx.at[r]).start()

    def new_gradient(n):
        for r in range(3):
            take(gr.at[quarter(0)], ld_rx.at[r])

        @pl.loop(0, CHUNKS)
        def _(d):
            cols = chunk_columns(d)
            total = rxo[quarter(n), cols].astype(F32)
            for r in range(3):
                total += gr[quarter(r), cols].astype(F32)
            gown[quarter(n), cols] = (gown[quarter(n), cols].astype(F32) + total).astype(BF16)

    def split(q):
        return pl.ds(q * (fb // SPLIT), fb // SPLIT)

    def piece_place(i):
        return LAYERS - 1 - i // PER_LAYER, lax.rem(i // PHASE, 2), lax.rem(i, PHASE) // PARTS, lax.rem(i, PARTS)

    def part_columns(n):
        return pl.ds(pl.multiple_of(n * fb, fb), fb)

    def piece(i):
        _, phase, _, n = piece_place(i)
        slot = lax.rem(i, SLOTS)

        @pl.when(jnp.logical_and(is_end, i >= SLOTS))
        def _():
            take(zp.at[slot], zs.at[slot])

        part = jnp.dot(lt[phase, part_columns(n), :], cbuf[lax.rem(i // PARTS, 2)], preferred_element_type=F32)

        @pl.when(phase == 0)
        def _():
            zp[slot] = part

        @pl.when(phase == 1)
        def _():
            zp[slot] = part.T

    def total_place(j):
        layer, _, c, n = piece_place(j)
        return down_ref.at[layer, part_columns(n), chunk_columns(c)], up_ref.at[layer, chunk_columns(c), part_columns(n)]

    def total_send(j, slot):
        @pl.when(jnp.logical_and(j >= 0, j < FULL))
        def _():
            _, phase, _, _ = piece_place(j)
            for kind, place in enumerate(total_place(j)):
                @pl.when(phase == kind)
                def _():
                    remote(z2.at[slot], place, z_ts.at[slot], z_rt.at[lax.rem(j, LAST_SLOTS)], data(line_end)).start()
                    pltpu.make_async_copy(z2.at[slot], place, z_tl.at[slot]).start()

    def sum_send(slot, q):
        remote(zp.at[slot, split(q)], z2.at[slot, split(q)], zs.at[slot], z_r2.at[slot], data(line_across)).start()

    def line_step(i):
        @pl.when(is_end)
        def _():
            @pl.when(i < PIECES)
            def _():
                slot, there = lax.rem(i, SLOTS), lax.rem(i, FIRST_SLOTS)

                @pl.when(i >= FIRST_SLOTS)
                def _():
                    pl.semaphore_wait(c1, 1)

                for q in range(SPLIT):
                    remote(zp.at[slot, split(q)], z1.at[there, split(q)], zs.at[slot], z_r1.at[there, q], data(line_mid)).start()

            j = i - LAG_LAST

            @pl.when(jnp.logical_and(j >= 0, j < FULL))
            def _():
                take(zp.at[0], z_rt.at[lax.rem(j, LAST_SLOTS)])

                @pl.when(j + LAST_SLOTS < FULL)
                def _():
                    signal(c3, data(line_mid))

        @pl.when(is_mid)
        def _():
            slot, there = lax.rem(i, SLOTS), lax.rem(i, FIRST_SLOTS)
            j = i - LAG_SUM
            old = lax.rem(j + SLOTS, SLOTS)

            @pl.when(jnp.logical_and(j >= 0, j < PIECES))
            def _():
                take(z2.at[old], z_r2.at[old])
                z2[old] = z2[old] + zp[old]
                take(zp.at[old], zs.at[old])

                @pl.when(jnp.logical_and(j >= LAST_SLOTS, j < FULL))
                def _():
                    pl.semaphore_wait(c3, 1)

            @pl.when(jnp.logical_and(j >= FULL, j < PIECES))
            def _():
                pltpu.make_async_copy(z2.at[old], rest_ref.at[:, part_columns(j - FULL)], z_tl.at[old]).start()

            @pl.when(i < PIECES)
            def _():
                @pl.when(i >= SLOTS)
                def _():
                    pl.semaphore_wait(c2, 1)

                for q in range(SPLIT):
                    take(z1.at[there, split(q)], z_r1.at[there, q])
                    zp[slot, split(q), :] = zp[slot, split(q), :] + z1[there, split(q), :]

                    if q == 0:
                        total_send(j, old)
                    else:
                        sum_send(slot, q - 1)
                sum_send(slot, SPLIT - 1)

                @pl.when(i + FIRST_SLOTS < PIECES)
                def _():
                    signal(c1, data(line_end))

            @pl.when(i >= PIECES)
            def _():
                total_send(j, old)

            k = i - LAG_FREE

            @pl.when(jnp.logical_and(k >= 0, k < PIECES))
            def _():
                free = lax.rem(k, SLOTS)
                @pl.when(k < FULL)
                def _():
                    take(z2.at[free], z_ts.at[free])

                take(z2.at[free], z_tl.at[free])

                @pl.when(k + SLOTS < PIECES)
                def _():
                    signal(c2, data(line_across))

    top = LAYERS - 1
    loads_g = [pltpu.make_async_copy(g_ref.at[:, part], gown.at[:, part], sem)
               for part, sem in ((pl.ds(0, cw), ld_rx.at[0]), (pl.ds(cw, hidden - cw), ld_o))]
    for load in loads_g:
        load.start()
    held = ((ha, ld_a), (hr, ld_h))
    for n, (ref, sem) in enumerate(held):
        act_load(top, n, ref, sem).start()
    barrier = pltpu.get_barrier_semaphore()
    for peer in (near_x, near_y, far, partner):
        signal(barrier, model(peer))

    @pl.when(is_end)
    def _():
        signal(barrier, data(line_mid))
        pl.semaphore_wait(barrier, 5)

    @pl.when(is_mid)
    def _():
        signal(barrier, data(line_end))
        signal(barrier, data(line_across))
        pl.semaphore_wait(barrier, 6)

    loads_g[0].wait()
    first_chunk = cbuf.at[0]
    gather_send(0, 0, gown, first_chunk)
    cbuf[0, row_block(me), :] = gown[:, :cw]
    loads_g[1].wait()
    gather_keep(0, gown, 1)
    load_x = pltpu.make_async_copy(x_ref.at[top], xown, ld_o)
    load_x.start()
    for load in weight_loads(top):
        load.start()

    @pl.loop(0, 4)
    def _(b):
        for n, (ref, sem) in enumerate(held):
            act_load(top, 0, ref, sem).wait()
            act_block(2 * b + n, ref)

            @pl.when(b < 3)
            def _():
                act_load(top, 2 * b + n + 2, ref, sem).start()

        @pl.when(b == 2)
        def _():
            gather_relay(0, 0, first_chunk, first_s, first_s)
            gather_send(0, 1, gown, gathered(0, 1))

    load_x.wait()
    gather_forward(0, 0, first_chunk, first_s)
    gather_send(0, 2, gown, gathered(0, 2))
    gather_wait(0, 0, first_chunk)
    take(gown.at[:, pl.ds(0, hidden - cw)], ag_l.at[0])
    pltpu.make_async_copy(first_chunk, gathered(0, 0), first_l).start()

    @pl.loop(0, PIECES + LAG_LAST)
    def _(i):
        lp = i // PER_LAYER
        layer = LAYERS - 1 - lp
        s = i // 2
        sl = lax.rem(s, PER_LAYER // 2)
        il = lax.rem(i, PER_LAYER)
        even = lax.rem(i, 2) == 0
        odd = jnp.logical_not(even)
        odd_pair = lax.rem(s, 2) == 1
        even_pair = jnp.logical_not(odd_pair)
        ggid, xgid = 2 * lp, 2 * lp + 1
        live = i < PIECES

        @pl.when(live)
        def _():
            @pl.when(jnp.logical_and(i > 0, lax.rem(i, PARTS) == 0))
            def _():
                take(cbuf.at[0], ld_c.at[lax.rem(i // PARTS, 2)])

            piece(i)

        line_step(i)

        def when(*conds):
            return pl.when(functools.reduce(jnp.logical_and, conds, live))

        @when(even, s < CHUNKS - 1)
        def _():
            gather_relay(0, s + 1, gathered(0, s + 1), ag_s.at[0], ag_f.at[0])

        @when(even, s < CHUNKS - 3)
        def _():
            gather_send(0, s + 3, gown, gathered(0, s + 3))

        @when(even, s >= 1, s < CHUNKS)
        def _():
            gather_forward(0, s, gathered(0, s), ag_f.at[0])

        @when(odd, s >= 1, s < CHUNKS)
        def _():
            gather_wait(0, s, gathered(0, s))

        @when(i == 2 * PARTS - 2)
        def _():
            take(cbuf.at[0, pl.ds(0, 4 * rows)], first_s)
            take(cbuf.at[0], first_l)

        @when(even, sl == X_RUNS[0][2])
        def _():
            gather_keep(xgid, xown)

        for first, count, start, relay, forward in X_RUNS:
            @when(even, sl >= start, sl < start + count)
            def _():
                gather_send(xgid, sl - start + first, xown, gathered(xgid, sl - start + first))

            @when(even, sl >= start + relay, sl < start + relay + count)
            def _():
                gather_relay(xgid, sl - start - relay + first, gathered(xgid, sl - start - relay + first), ag_s.at[xgid], ag_f.at[xgid])

            @when(even, sl >= start + forward, sl < start + forward + count)
            def _():
                gather_forward(xgid, sl - start - forward + first, gathered(xgid, sl - start - forward + first), ag_f.at[xgid])

        @when(even, sl == 15)
        def _():
            take(xown, ag_l.at[xgid])

        @when(even, odd_pair, sl >= 15, sl < 31)
        def _():
            gather_wait(xgid, (sl - 15) // 2, gathered(xgid, (sl - 15) // 2))

        @when(even, s == 25)
        def _():
            gather_keep(2, gown)

        @when(even, s >= 25, s < 25 + CHUNKS)
        def _():
            gather_send(2, s - 25, gown, gathered(2, s - 25))

        @when(even, s >= 27, s < 27 + CHUNKS)
        def _():
            gather_relay(2, s - 27, gathered(2, s - 27), ag_s.at[2], ag_f.at[2])

        @when(even, s >= 29, s < 29 + CHUNKS)
        def _():
            gather_forward(2, s - 29, gathered(2, s - 29), ag_f.at[2])

        @when(odd, s == 30)
        def _():
            take(gown, ag_l.at[2])

        @when(odd, s >= 30, s < 30 + CHUNKS)
        def _():
            gather_wait(2, s - 30, gathered(2, s - 30))

        @when(jnp.logical_or(i == PARTS - 1, jnp.logical_and(i >= PARTS, lax.rem(i, PARTS) == PARTS - 2)), i + 2 < PIECES)
        def _():
            nxt = i // PARTS * PARTS + PARTS
            chunk_load(nxt // PHASE, lax.rem(nxt, PHASE) // PARTS, lax.rem(nxt // PARTS, 2)).start()

        @when(even, sl == UNIT_STEP)
        def _():
            for load in weight_loads(0):
                load.wait()

        @when(even, sl >= UNIT_STEP, sl < UNIT_STEP + 8)
        def _():
            unit_first(sl - UNIT_STEP)

        @when(even, sl > UNIT_STEP + 1, sl <= UNIT_STEP + 9)
        def _():
            unit_finish(lp, sl - UNIT_STEP - 2)

        @when(odd, sl >= UNIT_STEP - 1, sl < UNIT_STEP + 7)
        def _():
            unit_load(ggid, layer, sl - UNIT_STEP + 1)

        @when(odd, sl >= UNIT_STEP, sl < UNIT_STEP + 8)
        def _():
            unit_second(lp, sl - UNIT_STEP)

        @when(il == FINAL_STEP - 1)
        def _():
            take(gb_ref.at[ggid, 0, pl.ds(0, 7 * rows)], ag_s.at[ggid])
            take(gb_ref.at[ggid, pl.ds(0, 3)], ag_s.at[ggid])

            @pl.when(lp > 0)
            def _():
                take(gb_ref.at[ggid, 0, row_block(0)], ag_s.at[ggid])

            new_gradient_load(lp, 0)

        @when(il >= FINAL_STEP, il < FINAL_STEP + 4)
        def _():
            new_gradient(il - FINAL_STEP)

            @pl.when(il < FINAL_STEP + 3)
            def _():
                new_gradient_load(lp, il - FINAL_STEP + 1)

        @when(i == PER_LAYER + FINAL_STEP + 4)
        def _():
            pltpu.make_async_copy(gown, gx_ref, st_gx).start()

        @when(lp == 0, even, sl == 17)
        def _():
            for load in weight_loads(0):
                load.start()

        @when(lp == 0, even, even_pair, sl >= 16)
        def _():
            act_load(0, (sl - 16) // 2, ha, ld_a).start()

        @when(lp == 0, odd, odd_pair, sl >= 16)
        def _():
            act_load(0, 0, ha, ld_a).wait()
            act_block((sl - 16) // 2, ha)

        @when(even, sl == 31)
        def _():
            take(gb_ref.at[xgid, pl.ds(0, 4)], ag_s.at[xgid])

            @pl.when(lp == 0)
            def _():
                pltpu.make_async_copy(x_ref.at[0], xown, ld_o).start()

        @when(lp == 0, odd, sl == 31)
        def _():
            pltpu.make_async_copy(x_ref.at[0], xown, ld_o).wait()

    take(gb_ref.at[0, 0, pl.ds(0, 5 * rows)], ag_f.at[0])
    take(gb_ref.at[0, pl.ds(0, 2)], ag_f.at[0])
    for gid in range(1, 2 * LAYERS):
        take(gb_ref.at[gid, pl.ds(0, 3)], ag_f.at[gid])
    for slot in range(2):
        take(pp.at[slot], pp_s.at[slot])
    for kept in range(8 - SUMS, SUMS):
        take(pm.at[kept], pm_s.at[kept])
    take(gown, st_gx)

    @pl.when(is_end)
    def _():
        for slot in range(SLOTS):
            take(zp.at[slot], zs.at[slot])


def move_kernel(count, *refs):
    sources, targets = refs[:count], refs[count:2 * count]
    buffers, read, written = refs[2 * count:3 * count], refs[-2], refs[-1]
    copies, slot = [], 0
    for source, target, buffer in zip(sources, targets, buffers):
        size = buffer.shape[1]
        for n in range(buffer.shape[0]):
            rows = pl.ds(n * size, size)
            copies.append((pltpu.make_async_copy(source.at[rows], buffer.at[n], read.at[slot]),
                           pltpu.make_async_copy(buffer.at[n], target.at[rows], written.at[slot])))
            slot += 1
    for first, _ in copies:
        first.start()
    for first, _ in copies:
        first.wait()
    for _, second in copies:
        second.start()
    for _, second in copies:
        second.wait()


def move(*arrays):
    flat = [a.reshape(-1, a.shape[-1]) for a in arrays]
    parts = [max(1, a.size * a.dtype.itemsize // MOVE_BYTES) for a in flat]
    any_space = pl.BlockSpec(memory_space=pl.ANY)
    size = sum(a.size * a.dtype.itemsize for a in flat)
    moved = pl.pallas_call(
        functools.partial(move_kernel, len(flat)),
        name="move",
        out_shape=tuple(jax.ShapeDtypeStruct(a.shape, a.dtype) for a in flat),
        in_specs=[any_space] * len(flat),
        out_specs=(any_space,) * len(flat),
        scratch_shapes=[pltpu.VMEM((n, a.shape[0] // n, a.shape[1]), a.dtype) for a, n in zip(flat, parts)]
        + [pltpu.SemaphoreType.DMA((sum(parts),))] * 2,
        compiler_params=pltpu.CompilerParams(vmem_limit_bytes=67043328),
        cost_estimate=pl.CostEstimate(flops=int(size * MOVE_FLOPS), bytes_accessed=2 * size, transcendentals=0),
    )(*flat)
    return [m.reshape(a.shape) for m, a in zip(moved, arrays)]


def solution(mesh):
    def device_step(x_saved, h_saved, w_up, w_down, grad_out):
        layers, hidden, ffn = w_up.shape
        rows = grad_out.shape[1]
        tokens = h_saved.shape[2]
        cw, fb = hidden // CHUNKS, ffn // PARTS
        half_rows = rows // 2
        any_space = pl.BlockSpec(memory_space=pl.ANY)
        dma = pltpu.SemaphoreType.DMA
        vmem = pltpu.VMEM
        grad_x, grad_up, grad_down, rest, _, _ = pl.pallas_call(
            kernel,
            name="backward",
            out_shape=(
                jax.ShapeDtypeStruct((rows, hidden), BF16),
                jax.ShapeDtypeStruct(w_up.shape, F32),
                jax.ShapeDtypeStruct(w_down.shape, F32),
                jax.ShapeDtypeStruct((cw, REST * fb), F32),
                jax.ShapeDtypeStruct((2 * layers, CHUNKS, tokens, cw), BF16),
                jax.ShapeDtypeStruct((layers, 3, rows, hidden), BF16),
            ),
            in_specs=[any_space] * 5,
            out_specs=(any_space,) * 6,
            scratch_shapes=[
                vmem((2, ffn, tokens), BF16),
                vmem((ffn, hidden), BF16),
                vmem((hidden, ffn), BF16),
                vmem((2, tokens, cw), BF16),
                vmem((rows, hidden), BF16),
                vmem((rows, ffn), BF16),
                vmem((rows, ffn), BF16),
                vmem((rows, ffn), BF16),
                vmem((rows, hidden), BF16),
                vmem((rows, hidden), BF16),
                vmem((SUMS, half_rows, hidden), BF16),
                vmem((2, half_rows, hidden), BF16),
                vmem((HELD, half_rows, hidden), BF16),
                vmem((rows, hidden), BF16),
                vmem((SLOTS, fb, cw), F32),
                vmem((FIRST_SLOTS, fb, cw), F32),
                vmem((SLOTS, fb, cw), F32),
                dma((SLOTS,)), dma((FIRST_SLOTS, SPLIT)), dma((SLOTS,)), dma((SLOTS,)), dma((SLOTS,)), dma((LAST_SLOTS,)),
                pltpu.SemaphoreType.REGULAR, pltpu.SemaphoreType.REGULAR, pltpu.SemaphoreType.REGULAR,
                dma((2 * layers, CHUNKS)), dma((2 * layers, CHUNKS)), dma((2 * layers, CHUNKS)), dma((2 * layers, CHUNKS)),
                dma((2 * layers,)), dma((2 * layers,)), dma((2 * layers,)),
                dma((2,)), dma((HELD,)), dma((SUMS,)), dma((6 * layers,)), pltpu.SemaphoreType.REGULAR,
                dma((2,)), dma(()), dma(()), dma(()), dma((2,)), dma(()), dma((3,)), dma(()), dma(()), dma(()),
            ],
            compiler_params=pltpu.CompilerParams(collective_id=0, has_side_effects=True, vmem_limit_bytes=67043328),
        )(x_saved[:, 0], h_saved[:, 0], w_up, w_down, grad_out[0])
        spot = lax.axis_index("data")
        is_end = (spot == 0) | (spot == 3)
        rest = jnp.where(is_end, lax.ppermute(rest, "data", [(1, 0), (2, 3)]), rest)
        grad_x, grad_up, grad_down = move(grad_x, grad_up, grad_down)
        grad_up = grad_up.at[0, hidden - cw:, ffn - REST * fb:].set(rest)
        return grad_x[None], grad_up, grad_down

    return jax.shard_map(
        device_step,
        mesh=mesh,
        in_specs=(P(None, "data", "model", None), P(None, "data", None, "model"), P(None, None, "model"), P(None, "model", None), P("data", "model", None)),
        out_specs=(P("data", "model", None), P(None, None, "model"), P(None, "model", None)),
        check_vma=False,
    )
```

```python
import functools

import jax
import jax.numpy as jnp
from jax import lax
from jax.experimental import pallas as pl
from jax.experimental.pallas import tpu as pltpu
from jax.sharding import PartitionSpec as P

MESH = pl.DeviceIdType.MESH
F32, BF16 = jnp.float32, jnp.bfloat16
NT = (((1,), (1,)), ((), ()))

LAYERS = 2
CHUNKS = 8
PARTS = 4
PHASE = CHUNKS * PARTS
PER_LAYER = 2 * PHASE
PIECES = LAYERS * PER_LAYER
REST = 2
FULL = PIECES - REST
SLOTS = 16
FIRST_SLOTS = 8
SPLIT = 4
LAST_SLOTS = 32
LAG_SUM = 2
LAG_FREE = 6
LAG_LAST = 20
UNIT_STEP = 8
X_RUNS = ((0, 5, 4, 2, 8), (5, 3, 20, 3, 4))
FINAL_STEP = 46
HELD = 3
SUMS = 6

MOVE_BYTES = 1 << 22
MOVE_FLOPS = 10


def gelu_tanh(pre):
    return jnp.tanh(0.7978845608028654 * (pre + 0.044715 * pre * pre * pre))


def gelu(pre):
    return 0.5 * pre * (1.0 + gelu_tanh(pre))


def gelu_slope(pre):
    tanh_val = gelu_tanh(pre)
    return 0.5 * (1.0 + tanh_val) + 0.5 * pre * (1.0 - tanh_val * tanh_val) * 0.7978845608028654 * (1.0 + 0.134145 * pre * pre)


def kernel(x_ref, h_ref, wu_ref, wd_ref, g_ref, gx_ref, up_ref, down_ref, rest_ref, gb_ref, rxh_ref,
           lt, wd, wu, cbuf, gr, hr, dh, ha, gown, xown, pm, pp, pb, rxo, zp, z1, z2,
           zs, z_r1, z_r2, z_ts, z_tl, z_rt, c1, c2, c3,
           ag_x, ag_y, ag_d, ag_p, ag_s, ag_f, ag_l, pp_s, pb_r, pm_s, rx_r, pbc,
           ld_c, ld_g, ld_h, ld_a, ld_w, ld_o, ld_rx, st_gx, first_s, first_l):
    rows, hidden = gown.shape
    ffn = lt.shape[1]
    half_rows = rows // 2
    cw = hidden // CHUNKS
    fb = ffn // 4

    me = lax.axis_index("model")
    spot = lax.axis_index("data")
    core = lax.rem(me, 2)
    px = lax.rem(me // 2, 2)
    py = me // 4
    partner = me + 1 - 2 * core
    step_x, step_y = 2 * (1 - 2 * px), 4 * (1 - 2 * py)
    near_x, near_y, far = me + step_x, me + step_y, me + step_x + step_y
    is_end = jnp.logical_or(spot == 0, spot == 3)
    is_mid = jnp.logical_not(is_end)
    line_mid = jnp.where(spot < 2, 1, 2)
    line_end = jnp.where(spot < 2, 0, 3)
    line_across = 3 - spot

    def model(i):
        return {"model": i}

    def data(i):
        return {"data": i}

    def signal(sem, where):
        pl.semaphore_signal(sem, inc=1, device_id=where, device_id_type=MESH)

    def remote(src, dst, send, recv, where):
        return pltpu.make_async_remote_copy(src_ref=src, dst_ref=dst, send_sem=send, recv_sem=recv, device_id=where, device_id_type=MESH)

    def take(ref, sem):
        pltpu.make_async_copy(ref, ref, sem).wait()

    def chunk_columns(c):
        return pl.ds(pl.multiple_of(c * cw, cw), cw)

    def row_block(i):
        return pl.ds(pl.multiple_of(i * rows, rows), rows)

    def gather_keep(gid, own, first=0):
        for c in range(first, CHUNKS):
            pltpu.make_async_copy(own.at[:, pl.ds(c * cw, cw)], gb_ref.at[gid, c, row_block(me)], ag_l.at[gid]).start()

    def gather_send(gid, c, own, buf):
        src = own.at[:, chunk_columns(c)]
        dst = buf.at[row_block(me)]
        remote(src, dst, ag_s.at[gid], ag_x.at[gid, c], model(near_x)).start()
        remote(src, dst, ag_s.at[gid], ag_y.at[gid, c], model(near_y)).start()
        remote(src, dst, ag_s.at[gid], ag_p.at[gid, c], model(partner)).start()

    def gather_relay(gid, c, buf, sent, forwarded):
        take(buf.at[row_block(0)], ag_x.at[gid, c])
        take(buf.at[row_block(0)], ag_y.at[gid, c])
        for n, (source, target) in enumerate(((near_x, near_y), (near_y, near_x))):
            @pl.when(core == n)
            def _():
                block = buf.at[row_block(source)]
                remote(block, block, sent, ag_d.at[gid, c], model(target)).start()
        for peer in (near_x, near_y):
            block = buf.at[row_block(peer)]
            remote(block, block, forwarded, ag_p.at[gid, c], model(partner)).start()

    def gather_forward(gid, c, buf, forwarded):
        take(buf.at[row_block(0)], ag_d.at[gid, c])
        block = buf.at[row_block(far)]
        remote(block, block, forwarded, ag_p.at[gid, c], model(partner)).start()

    def gather_wait(gid, c, buf):
        take(buf.at[pl.ds(0, 4 * rows)], ag_p.at[gid, c])

    def gathered(gid, c):
        return gb_ref.at[gid, c]

    def chunk_load(gid, c, slot):
        return pltpu.make_async_copy(gb_ref.at[gid, c], cbuf.at[slot], ld_c.at[slot])

    def act_load(layer, b, ref, sem):
        return pltpu.make_async_copy(h_ref.at[layer, row_block(b)], ref, sem)

    def act_block(b, ref):
        @pl.loop(0, 4)
        def _(f):
            cols = pl.ds(pl.multiple_of(f * fb, fb), fb)
            a = gelu(ref[:, cols].astype(F32)).astype(BF16).astype(F32)
            lt[0, cols, row_block(b)] = a.T.astype(BF16)

    def weight_loads(layer):
        return (pltpu.make_async_copy(wd_ref.at[layer], wd, ld_w.at[0]), pltpu.make_async_copy(wu_ref.at[layer], wu, ld_w.at[1]))

    def unit_place(u):
        r = lax.rem(u // 2 + 1, 4)
        chip = lax.rem(py + r // 2, 2) * 2 + lax.rem(px + lax.rem(r, 2), 2)
        return r, chip

    def unit_rows(u):
        _, chip = unit_place(u)
        start = (chip * 2 + core) * rows + lax.rem(u, 2) * half_rows
        other = (chip * 2 + 1 - core) * rows + lax.rem(u, 2) * half_rows
        return tuple(pl.ds(pl.multiple_of(s, half_rows), half_rows) for s in (start, other))

    def unit_load(gid, layer, u):
        for n, block in enumerate(unit_rows(u)):
            here = pl.ds(n * half_rows, half_rows)
            for c in range(CHUNKS):
                pltpu.make_async_copy(gb_ref.at[gid, c, block], gr.at[here, pl.ds(c * cw, cw)], ld_g).start()
            pltpu.make_async_copy(h_ref.at[layer, block], hr.at[here], ld_h).start()

    def unit_first(u):
        take(gr, ld_g)
        take(hr, ld_h)
        mine, other = unit_rows(u)

        @pl.loop(0, 4)
        def _(f):
            cols = pl.ds(pl.multiple_of(f * fb, fb), fb)
            d_act = lax.dot_general(gr[...], wd[cols, :], NT, preferred_element_type=F32)
            d_pre = (d_act * gelu_slope(hr[:, cols].astype(F32))).astype(BF16)
            dh[:, cols] = d_pre
            flipped = d_pre.astype(F32).T.astype(BF16)
            lt[1, cols, mine] = flipped[:, :half_rows]
            lt[1, cols, other] = flipped[:, half_rows:]

    def unit_second(lp, u):
        order = lp * 8 + u
        slot = lax.rem(order, 2)
        kept = lax.rem(u, SUMS)

        @pl.when(order >= 2)
        def _():
            take(pp.at[slot], pp_s.at[slot])

        @pl.when(jnp.logical_or(u >= SUMS, jnp.logical_and(lp > 0, u >= 8 - SUMS)))
        def _():
            take(pm.at[kept], pm_s.at[kept])

        @pl.loop(0, CHUNKS)
        def _(d):
            cols = chunk_columns(d)
            part = lax.dot_general(dh[...], wu[cols, :], NT, preferred_element_type=F32).astype(BF16)
            pm[kept, :, cols] = part[:half_rows]
            pp[slot, :, cols] = part[half_rows:]

        @pl.when(order >= HELD)
        def _():
            pl.semaphore_wait(pbc, 1)

        there = lax.rem(order, HELD)
        remote(pp.at[slot], pb.at[there], pp_s.at[slot], pb_r.at[there], model(partner)).start()

    def unit_finish(lp, u):
        order = lp * 8 + u
        slot = lax.rem(order, HELD)
        kept = lax.rem(u, SUMS)
        r, chip = unit_place(u)
        here = pl.ds(pl.multiple_of(lax.rem(u, 2) * half_rows, half_rows), half_rows)
        take(pb.at[slot], pb_r.at[slot])

        @pl.when(r != 0)
        def _():
            @pl.loop(0, CHUNKS)
            def _(d):
                cols = chunk_columns(d)
                pm[kept, :, cols] = (pm[kept, :, cols].astype(F32) + pb[slot, :, cols].astype(F32)).astype(BF16)

            remote(pm.at[kept], rxh_ref.at[lp, r - 1, here], pm_s.at[kept], rx_r.at[lp * 6 + (r - 1) * 2 + lax.rem(u, 2)],
                   model(chip * 2 + core)).start()

        @pl.when(r == 0)
        def _():
            @pl.loop(0, CHUNKS)
            def _(d):
                cols = chunk_columns(d)
                rxo[here, cols] = (pm[kept, :, cols].astype(F32) + pb[slot, :, cols].astype(F32)).astype(BF16)

        @pl.when(order < 8 * LAYERS - HELD)
        def _():
            signal(pbc, model(partner))

    def quarter(n):
        part = rows // 4
        return pl.ds(pl.multiple_of(n * part, part), part)

    def new_gradient_load(lp, n):
        @pl.when(lax.rem(n, 2) == 0)
        def _():
            for r in range(3):
                take(pm.at[0], rx_r.at[lp * 6 + r * 2 + n // 2])

        for r in range(3):
            pltpu.make_async_copy(rxh_ref.at[lp, r, quarter(n)], gr.at[quarter(r)], ld_rx.at[r]).start()

    def new_gradient(n):
        for r in range(3):
            take(gr.at[quarter(0)], ld_rx.at[r])

        @pl.loop(0, CHUNKS)
        def _(d):
            cols = chunk_columns(d)
            total = rxo[quarter(n), cols].astype(F32)
            for r in range(3):
                total += gr[quarter(r), cols].astype(F32)
            gown[quarter(n), cols] = (gown[quarter(n), cols].astype(F32) + total).astype(BF16)

    def split(q):
        return pl.ds(q * (fb // SPLIT), fb // SPLIT)

    def piece_place(i):
        return LAYERS - 1 - i // PER_LAYER, lax.rem(i // PHASE, 2), lax.rem(i, PHASE) // PARTS, lax.rem(i, PARTS)

    def part_columns(n):
        return pl.ds(pl.multiple_of(n * fb, fb), fb)

    def piece(i):
        _, phase, _, n = piece_place(i)
        slot = lax.rem(i, SLOTS)

        @pl.when(jnp.logical_and(is_end, i >= SLOTS))
        def _():
            take(zp.at[slot], zs.at[slot])

        part = jnp.dot(lt[phase, part_columns(n), :], cbuf[lax.rem(i // PARTS, 2)], preferred_element_type=F32)

        @pl.when(phase == 0)
        def _():
            zp[slot] = part

        @pl.when(phase == 1)
        def _():
            zp[slot] = part.T

    def total_place(j):
        layer, _, c, n = piece_place(j)
        return down_ref.at[layer, part_columns(n), chunk_columns(c)], up_ref.at[layer, chunk_columns(c), part_columns(n)]

    def total_send(j, slot):
        @pl.when(jnp.logical_and(j >= 0, j < FULL))
        def _():
            _, phase, _, _ = piece_place(j)
            for kind, place in enumerate(total_place(j)):
                @pl.when(phase == kind)
                def _():
                    remote(z2.at[slot], place, z_ts.at[slot], z_rt.at[lax.rem(j, LAST_SLOTS)], data(line_end)).start()
                    pltpu.make_async_copy(z2.at[slot], place, z_tl.at[slot]).start()

    def sum_send(slot, q):
        remote(zp.at[slot, split(q)], z2.at[slot, split(q)], zs.at[slot], z_r2.at[slot], data(line_across)).start()

    def line_step(i):
        @pl.when(is_end)
        def _():
            @pl.when(i < PIECES)
            def _():
                slot, there = lax.rem(i, SLOTS), lax.rem(i, FIRST_SLOTS)

                @pl.when(i >= FIRST_SLOTS)
                def _():
                    pl.semaphore_wait(c1, 1)

                for q in range(SPLIT):
                    remote(zp.at[slot, split(q)], z1.at[there, split(q)], zs.at[slot], z_r1.at[there, q], data(line_mid)).start()

            j = i - LAG_LAST

            @pl.when(jnp.logical_and(j >= 0, j < FULL))
            def _():
                take(zp.at[0], z_rt.at[lax.rem(j, LAST_SLOTS)])

                @pl.when(j + LAST_SLOTS < FULL)
                def _():
                    signal(c3, data(line_mid))

        @pl.when(is_mid)
        def _():
            slot, there = lax.rem(i, SLOTS), lax.rem(i, FIRST_SLOTS)
            j = i - LAG_SUM
            old = lax.rem(j + SLOTS, SLOTS)

            @pl.when(jnp.logical_and(j >= 0, j < PIECES))
            def _():
                take(z2.at[old], z_r2.at[old])
                z2[old] = z2[old] + zp[old]
                take(zp.at[old], zs.at[old])

                @pl.when(jnp.logical_and(j >= LAST_SLOTS, j < FULL))
                def _():
                    pl.semaphore_wait(c3, 1)

            @pl.when(jnp.logical_and(j >= FULL, j < PIECES))
            def _():
                pltpu.make_async_copy(z2.at[old], rest_ref.at[:, part_columns(j - FULL)], z_tl.at[old]).start()

            @pl.when(i < PIECES)
            def _():
                @pl.when(i >= SLOTS)
                def _():
                    pl.semaphore_wait(c2, 1)

                for q in range(SPLIT):
                    take(z1.at[there, split(q)], z_r1.at[there, q])
                    zp[slot, split(q), :] = zp[slot, split(q), :] + z1[there, split(q), :]

                    if q == 0:
                        total_send(j, old)
                    else:
                        sum_send(slot, q - 1)
                sum_send(slot, SPLIT - 1)

                @pl.when(i + FIRST_SLOTS < PIECES)
                def _():
                    signal(c1, data(line_end))

            @pl.when(i >= PIECES)
            def _():
                total_send(j, old)

            k = i - LAG_FREE

            @pl.when(jnp.logical_and(k >= 0, k < PIECES))
            def _():
                free = lax.rem(k, SLOTS)
                @pl.when(k < FULL)
                def _():
                    take(z2.at[free], z_ts.at[free])

                take(z2.at[free], z_tl.at[free])

                @pl.when(k + SLOTS < PIECES)
                def _():
                    signal(c2, data(line_across))

    top = LAYERS - 1
    loads_g = [pltpu.make_async_copy(g_ref.at[:, part], gown.at[:, part], sem)
               for part, sem in ((pl.ds(0, cw), ld_rx.at[0]), (pl.ds(cw, hidden - cw), ld_o))]
    for load in loads_g:
        load.start()
    held = ((ha, ld_a), (hr, ld_h))
    for n, (ref, sem) in enumerate(held):
        act_load(top, n, ref, sem).start()
    barrier = pltpu.get_barrier_semaphore()
    for peer in (near_x, near_y, far, partner):
        signal(barrier, model(peer))

    @pl.when(is_end)
    def _():
        signal(barrier, data(line_mid))
        pl.semaphore_wait(barrier, 5)

    @pl.when(is_mid)
    def _():
        signal(barrier, data(line_end))
        signal(barrier, data(line_across))
        pl.semaphore_wait(barrier, 6)

    loads_g[0].wait()
    first_chunk = cbuf.at[0]
    gather_send(0, 0, gown, first_chunk)
    cbuf[0, row_block(me), :] = gown[:, :cw]
    loads_g[1].wait()
    gather_keep(0, gown, 1)
    load_x = pltpu.make_async_copy(x_ref.at[top], xown, ld_o)
    load_x.start()
    for load in weight_loads(top):
        load.start()

    @pl.loop(0, 4)
    def _(b):
        for n, (ref, sem) in enumerate(held):
            act_load(top, 0, ref, sem).wait()
            act_block(2 * b + n, ref)

            @pl.when(b < 3)
            def _():
                act_load(top, 2 * b + n + 2, ref, sem).start()

        @pl.when(b == 2)
        def _():
            gather_relay(0, 0, first_chunk, first_s, first_s)
            gather_send(0, 1, gown, gathered(0, 1))

    load_x.wait()
    gather_forward(0, 0, first_chunk, first_s)
    gather_send(0, 2, gown, gathered(0, 2))
    gather_wait(0, 0, first_chunk)
    take(gown.at[:, pl.ds(0, hidden - cw)], ag_l.at[0])
    pltpu.make_async_copy(first_chunk, gathered(0, 0), first_l).start()

    @pl.loop(0, PIECES)
    def _(i):
        lp = i // PER_LAYER
        layer = LAYERS - 1 - lp
        s = i // 2
        sl = lax.rem(s, PER_LAYER // 2)
        il = lax.rem(i, PER_LAYER)
        even = lax.rem(i, 2) == 0
        odd = jnp.logical_not(even)
        odd_pair = lax.rem(s, 2) == 1
        even_pair = jnp.logical_not(odd_pair)
        ggid, xgid = 2 * lp, 2 * lp + 1

        @pl.when(jnp.logical_and(i > 0, lax.rem(i, PARTS) == 0))
        def _():
            take(cbuf.at[0], ld_c.at[lax.rem(i // PARTS, 2)])

        piece(i)

        line_step(i)

        def when(*conds):
            return pl.when(functools.reduce(jnp.logical_and, conds))

        @when(even, s < CHUNKS - 1)
        def _():
            gather_relay(0, s + 1, gathered(0, s + 1), ag_s.at[0], ag_f.at[0])

        @when(even, s < CHUNKS - 3)
        def _():
            gather_send(0, s + 3, gown, gathered(0, s + 3))

        @when(even, s >= 1, s < CHUNKS)
        def _():
            gather_forward(0, s, gathered(0, s), ag_f.at[0])

        @when(odd, s >= 1, s < CHUNKS)
        def _():
            gather_wait(0, s, gathered(0, s))

        @when(i == 2 * PARTS - 2)
        def _():
            take(cbuf.at[0, pl.ds(0, 4 * rows)], first_s)
            take(cbuf.at[0], first_l)

        @when(even, sl == X_RUNS[0][2])
        def _():
            gather_keep(xgid, xown)

        for first, count, start, relay, forward in X_RUNS:
            @when(even, sl >= start, sl < start + count)
            def _():
                gather_send(xgid, sl - start + first, xown, gathered(xgid, sl - start + first))

            @when(even, sl >= start + relay, sl < start + relay + count)
            def _():
                gather_relay(xgid, sl - start - relay + first, gathered(xgid, sl - start - relay + first), ag_s.at[xgid], ag_f.at[xgid])

            @when(even, sl >= start + forward, sl < start + forward + count)
            def _():
                gather_forward(xgid, sl - start - forward + first, gathered(xgid, sl - start - forward + first), ag_f.at[xgid])

        @when(even, sl == 15)
        def _():
            take(xown, ag_l.at[xgid])

        @when(even, odd_pair, sl >= 15, sl < 31)
        def _():
            gather_wait(xgid, (sl - 15) // 2, gathered(xgid, (sl - 15) // 2))

        @when(even, s == 25)
        def _():
            gather_keep(2, gown)

        @when(even, s >= 25, s < 25 + CHUNKS)
        def _():
            gather_send(2, s - 25, gown, gathered(2, s - 25))

        @when(even, s >= 27, s < 27 + CHUNKS)
        def _():
            gather_relay(2, s - 27, gathered(2, s - 27), ag_s.at[2], ag_f.at[2])

        @when(even, s >= 29, s < 29 + CHUNKS)
        def _():
            gather_forward(2, s - 29, gathered(2, s - 29), ag_f.at[2])

        @when(odd, s == 30)
        def _():
            take(gown, ag_l.at[2])

        @when(odd, s >= 30, s < 30 + CHUNKS)
        def _():
            gather_wait(2, s - 30, gathered(2, s - 30))

        @when(jnp.logical_or(i == PARTS - 1, jnp.logical_and(i >= PARTS, lax.rem(i, PARTS) == PARTS - 2)), i + 2 < PIECES)
        def _():
            nxt = i // PARTS * PARTS + PARTS
            chunk_load(nxt // PHASE, lax.rem(nxt, PHASE) // PARTS, lax.rem(nxt // PARTS, 2)).start()

        @when(even, sl == UNIT_STEP)
        def _():
            for load in weight_loads(0):
                load.wait()

        @when(even, sl >= UNIT_STEP, sl < UNIT_STEP + 8)
        def _():
            unit_first(sl - UNIT_STEP)

        @when(even, sl > UNIT_STEP + 1, sl <= UNIT_STEP + 9)
        def _():
            unit_finish(lp, sl - UNIT_STEP - 2)

        @when(odd, sl >= UNIT_STEP - 1, sl < UNIT_STEP + 7)
        def _():
            unit_load(ggid, layer, sl - UNIT_STEP + 1)

        @when(odd, sl >= UNIT_STEP, sl < UNIT_STEP + 8)
        def _():
            unit_second(lp, sl - UNIT_STEP)

        @when(il == FINAL_STEP - 1)
        def _():
            take(gb_ref.at[ggid, 0, pl.ds(0, 7 * rows)], ag_s.at[ggid])
            take(gb_ref.at[ggid, pl.ds(0, 3)], ag_s.at[ggid])

            @pl.when(lp > 0)
            def _():
                take(gb_ref.at[ggid, 0, row_block(0)], ag_s.at[ggid])

            new_gradient_load(lp, 0)

        @when(il >= FINAL_STEP, il < FINAL_STEP + 4)
        def _():
            new_gradient(il - FINAL_STEP)

            @pl.when(il < FINAL_STEP + 3)
            def _():
                new_gradient_load(lp, il - FINAL_STEP + 1)

        @when(i == PER_LAYER + FINAL_STEP + 4)
        def _():
            pltpu.make_async_copy(gown, gx_ref, st_gx).start()

        @when(lp == 0, even, sl == 17)
        def _():
            for load in weight_loads(0):
                load.start()

        @when(lp == 0, even, even_pair, sl >= 16)
        def _():
            act_load(0, (sl - 16) // 2, ha, ld_a).start()

        @when(lp == 0, odd, odd_pair, sl >= 16)
        def _():
            act_load(0, 0, ha, ld_a).wait()
            act_block((sl - 16) // 2, ha)

        @when(even, sl == 31)
        def _():
            take(gb_ref.at[xgid, pl.ds(0, 4)], ag_s.at[xgid])

            @pl.when(lp == 0)
            def _():
                pltpu.make_async_copy(x_ref.at[0], xown, ld_o).start()

        @when(lp == 0, odd, sl == 31)
        def _():
            pltpu.make_async_copy(x_ref.at[0], xown, ld_o).wait()

    @pl.loop(PIECES, PIECES + LAG_LAST)
    def _(i):
        line_step(i)

    take(gb_ref.at[0, 0, pl.ds(0, 5 * rows)], ag_f.at[0])
    take(gb_ref.at[0, pl.ds(0, 2)], ag_f.at[0])
    for gid in range(1, 2 * LAYERS):
        take(gb_ref.at[gid, pl.ds(0, 3)], ag_f.at[gid])
    for slot in range(2):
        take(pp.at[slot], pp_s.at[slot])
    for kept in range(8 - SUMS, SUMS):
        take(pm.at[kept], pm_s.at[kept])
    take(gown, st_gx)

    @pl.when(is_end)
    def _():
        for slot in range(SLOTS):
            take(zp.at[slot], zs.at[slot])


def move_kernel(count, *refs):
    sources, targets = refs[:count], refs[count:2 * count]
    buffers, read, written = refs[2 * count:3 * count], refs[-2], refs[-1]
    copies, slot = [], 0
    for source, target, buffer in zip(sources, targets, buffers):
        size = buffer.shape[1]
        for n in range(buffer.shape[0]):
            rows = pl.ds(n * size, size)
            copies.append((pltpu.make_async_copy(source.at[rows], buffer.at[n], read.at[slot]),
                           pltpu.make_async_copy(buffer.at[n], target.at[rows], written.at[slot])))
            slot += 1
    for first, _ in copies:
        first.start()
    for first, _ in copies:
        first.wait()
    for _, second in copies:
        second.start()
    for _, second in copies:
        second.wait()


def move(*arrays):
    flat = [a.reshape(-1, a.shape[-1]) for a in arrays]
    parts = [max(1, a.size * a.dtype.itemsize // MOVE_BYTES) for a in flat]
    any_space = pl.BlockSpec(memory_space=pl.ANY)
    size = sum(a.size * a.dtype.itemsize for a in flat)
    moved = pl.pallas_call(
        functools.partial(move_kernel, len(flat)),
        name="move",
        out_shape=tuple(jax.ShapeDtypeStruct(a.shape, a.dtype) for a in flat),
        in_specs=[any_space] * len(flat),
        out_specs=(any_space,) * len(flat),
        scratch_shapes=[pltpu.VMEM((n, a.shape[0] // n, a.shape[1]), a.dtype) for a, n in zip(flat, parts)]
        + [pltpu.SemaphoreType.DMA((sum(parts),))] * 2,
        compiler_params=pltpu.CompilerParams(vmem_limit_bytes=67043328),
        cost_estimate=pl.CostEstimate(flops=int(size * MOVE_FLOPS), bytes_accessed=2 * size, transcendentals=0),
    )(*flat)
    return [m.reshape(a.shape) for m, a in zip(moved, arrays)]


def solution(mesh):
    def device_step(x_saved, h_saved, w_up, w_down, grad_out):
        layers, hidden, ffn = w_up.shape
        rows = grad_out.shape[1]
        tokens = h_saved.shape[2]
        cw, fb = hidden // CHUNKS, ffn // PARTS
        half_rows = rows // 2
        any_space = pl.BlockSpec(memory_space=pl.ANY)
        dma = pltpu.SemaphoreType.DMA
        vmem = pltpu.VMEM
        grad_x, grad_up, grad_down, rest, _, _ = pl.pallas_call(
            kernel,
            name="backward",
            out_shape=(
                jax.ShapeDtypeStruct((rows, hidden), BF16),
                jax.ShapeDtypeStruct(w_up.shape, F32),
                jax.ShapeDtypeStruct(w_down.shape, F32),
                jax.ShapeDtypeStruct((cw, REST * fb), F32),
                jax.ShapeDtypeStruct((2 * layers, CHUNKS, tokens, cw), BF16),
                jax.ShapeDtypeStruct((layers, 3, rows, hidden), BF16),
            ),
            in_specs=[any_space] * 5,
            out_specs=(any_space,) * 6,
            scratch_shapes=[
                vmem((2, ffn, tokens), BF16),
                vmem((ffn, hidden), BF16),
                vmem((hidden, ffn), BF16),
                vmem((2, tokens, cw), BF16),
                vmem((rows, hidden), BF16),
                vmem((rows, ffn), BF16),
                vmem((rows, ffn), BF16),
                vmem((rows, ffn), BF16),
                vmem((rows, hidden), BF16),
                vmem((rows, hidden), BF16),
                vmem((SUMS, half_rows, hidden), BF16),
                vmem((2, half_rows, hidden), BF16),
                vmem((HELD, half_rows, hidden), BF16),
                vmem((rows, hidden), BF16),
                vmem((SLOTS, fb, cw), F32),
                vmem((FIRST_SLOTS, fb, cw), F32),
                vmem((SLOTS, fb, cw), F32),
                dma((SLOTS,)), dma((FIRST_SLOTS, SPLIT)), dma((SLOTS,)), dma((SLOTS,)), dma((SLOTS,)), dma((LAST_SLOTS,)),
                pltpu.SemaphoreType.REGULAR, pltpu.SemaphoreType.REGULAR, pltpu.SemaphoreType.REGULAR,
                dma((2 * layers, CHUNKS)), dma((2 * layers, CHUNKS)), dma((2 * layers, CHUNKS)), dma((2 * layers, CHUNKS)),
                dma((2 * layers,)), dma((2 * layers,)), dma((2 * layers,)),
                dma((2,)), dma((HELD,)), dma((SUMS,)), dma((6 * layers,)), pltpu.SemaphoreType.REGULAR,
                dma((2,)), dma(()), dma(()), dma(()), dma((2,)), dma(()), dma((3,)), dma(()), dma(()), dma(()),
            ],
            compiler_params=pltpu.CompilerParams(collective_id=0, has_side_effects=True, vmem_limit_bytes=67043328),
        )(x_saved[:, 0], h_saved[:, 0], w_up, w_down, grad_out[0])
        spot = lax.axis_index("data")
        is_end = (spot == 0) | (spot == 3)
        rest = jnp.where(is_end, lax.ppermute(rest, "data", [(1, 0), (2, 3)]), rest)
        grad_x, grad_up, grad_down = move(grad_x, grad_up, grad_down)
        grad_up = grad_up.at[0, hidden - cw:, ffn - REST * fb:].set(rest)
        return grad_x[None], grad_up, grad_down

    return jax.shard_map(
        device_step,
        mesh=mesh,
        in_specs=(P(None, "data", "model", None), P(None, "data", None, "model"), P(None, None, "model"), P(None, "model", None), P("data", "model", None)),
        out_specs=(P("data", "model", None), P(None, None, "model"), P(None, "model", None)),
        check_vma=False,
    )
```

```python
import functools

import jax
import jax.numpy as jnp
from jax import lax
from jax.experimental import pallas as pl
from jax.experimental.pallas import tpu as pltpu
from jax.sharding import PartitionSpec as P

MESH = pl.DeviceIdType.MESH
F32, BF16 = jnp.float32, jnp.bfloat16
NT = (((1,), (1,)), ((), ()))

LAYERS = 2
CHUNKS = 8
PARTS = 4
PHASE = CHUNKS * PARTS
PER_LAYER = 2 * PHASE
PIECES = LAYERS * PER_LAYER
REST = 2
FULL = PIECES - REST
SLOTS = 16
FIRST_SLOTS = 8
SPLIT = 4
LAST_SLOTS = 32
LAG_SUM = 2
LAG_FREE = 6
LAG_LAST = 20
UNIT_STEP = 8
X_RUNS = ((0, 5, 6, 2, 8), (5, 3, 20, 3, 4))
FIRST_RELAY = 1
FINAL_STEP = 46
HELD = 3
SUMS = 6

MOVE_BYTES = 1 << 22
MOVE_FLOPS = 10


def gelu_tanh(pre):
    return jnp.tanh(0.7978845608028654 * (pre + 0.044715 * pre * pre * pre))


def gelu(pre):
    return 0.5 * pre * (1.0 + gelu_tanh(pre))


def gelu_slope(pre):
    tanh_val = gelu_tanh(pre)
    return 0.5 * (1.0 + tanh_val) + 0.5 * pre * (1.0 - tanh_val * tanh_val) * 0.7978845608028654 * (1.0 + 0.134145 * pre * pre)


def kernel(x_ref, h_ref, wu_ref, wd_ref, g_ref, gx_ref, up_ref, down_ref, rest_ref, gb_ref, rxh_ref,
           lt, wd, wu, cbuf, gr, hr, dh, ha, gown, xown, pm, pp, pb, rxo, zp, z1, z2,
           zs, z_r1, z_r2, z_ts, z_tl, z_rt, c1, c2, c3,
           ag_x, ag_y, ag_d, ag_p, ag_s, ag_f, ag_l, pp_s, pb_r, pm_s, rx_r, pbc,
           ld_c, ld_g, ld_h, ld_a, ld_w, ld_o, ld_rx, st_gx, first_s, first_l, first_x, first_y, first_d, first_p):
    rows, hidden = gown.shape
    ffn = lt.shape[1]
    half_rows = rows // 2
    cw = hidden // CHUNKS
    fb = ffn // 4

    me = lax.axis_index("model")
    spot = lax.axis_index("data")
    core = lax.rem(me, 2)
    px = lax.rem(me // 2, 2)
    py = me // 4
    partner = me + 1 - 2 * core
    step_x, step_y = 2 * (1 - 2 * px), 4 * (1 - 2 * py)
    near_x, near_y, far = me + step_x, me + step_y, me + step_x + step_y
    is_end = jnp.logical_or(spot == 0, spot == 3)
    is_mid = jnp.logical_not(is_end)
    line_mid = jnp.where(spot < 2, 1, 2)
    line_end = jnp.where(spot < 2, 0, 3)
    line_across = 3 - spot

    def model(i):
        return {"model": i}

    def data(i):
        return {"data": i}

    def signal(sem, where):
        pl.semaphore_signal(sem, inc=1, device_id=where, device_id_type=MESH)

    def remote(src, dst, send, recv, where):
        return pltpu.make_async_remote_copy(src_ref=src, dst_ref=dst, send_sem=send, recv_sem=recv, device_id=where, device_id_type=MESH)

    def take(ref, sem):
        pltpu.make_async_copy(ref, ref, sem).wait()

    def chunk_columns(c):
        return pl.ds(pl.multiple_of(c * cw, cw), cw)

    def row_block(i):
        return pl.ds(pl.multiple_of(i * rows, rows), rows)

    def gather_keep(gid, own, first=0):
        for c in range(first, CHUNKS):
            pltpu.make_async_copy(own.at[:, pl.ds(c * cw, cw)], gb_ref.at[gid, c, row_block(me)], ag_l.at[gid]).start()

    def gather_send(gid, c, own, buf):
        src = own.at[:, chunk_columns(c)]
        dst = buf.at[row_block(me)]
        remote(src, dst, ag_s.at[gid], ag_x.at[gid, c], model(near_x)).start()
        remote(src, dst, ag_s.at[gid], ag_y.at[gid, c], model(near_y)).start()
        remote(src, dst, ag_s.at[gid], ag_p.at[gid, c], model(partner)).start()

    def gather_relay(gid, c, buf, sent, forwarded):
        take(buf.at[row_block(0)], ag_x.at[gid, c])
        take(buf.at[row_block(0)], ag_y.at[gid, c])
        for n, (source, target) in enumerate(((near_x, near_y), (near_y, near_x))):
            @pl.when(core == n)
            def _():
                block = buf.at[row_block(source)]
                remote(block, block, sent, ag_d.at[gid, c], model(target)).start()
        for peer in (near_x, near_y):
            block = buf.at[row_block(peer)]
            remote(block, block, forwarded, ag_p.at[gid, c], model(partner)).start()

    def gather_forward(gid, c, buf, forwarded):
        take(buf.at[row_block(0)], ag_d.at[gid, c])
        block = buf.at[row_block(far)]
        remote(block, block, forwarded, ag_p.at[gid, c], model(partner)).start()

    def gather_wait(gid, c, buf):
        take(buf.at[pl.ds(0, 4 * rows)], ag_p.at[gid, c])

    def gathered(gid, c):
        return gb_ref.at[gid, c]

    def half_block(i, h):
        return cbuf.at[0, row_block(i), pl.ds(h * (cw // 2), cw // 2)]

    def half_send(h):
        src = gown.at[:, pl.ds(h * (cw // 2), cw // 2)]
        for peer, sem in ((near_x, first_x), (near_y, first_y), (partner, first_p)):
            remote(src, half_block(me, h), ag_s.at[0], sem.at[h], model(peer)).start()

    def half_relay(h):
        take(half_block(0, h), first_x.at[h])
        take(half_block(0, h), first_y.at[h])
        for n, (source, target) in enumerate(((near_x, near_y), (near_y, near_x))):
            @pl.when(core == n)
            def _():
                remote(half_block(source, h), half_block(source, h), first_s, first_d.at[h], model(target)).start()
        for peer in (near_x, near_y):
            remote(half_block(peer, h), half_block(peer, h), first_s, first_p.at[h], model(partner)).start()

    def half_forward(h):
        take(half_block(0, h), first_d.at[h])
        remote(half_block(far, h), half_block(far, h), first_s, first_p.at[h], model(partner)).start()

    def half_wait(h):
        take(cbuf.at[0, pl.ds(0, 4 * rows), pl.ds(h * (cw // 2), cw // 2)], first_p.at[h])

    def chunk_load(gid, c, slot):
        return pltpu.make_async_copy(gb_ref.at[gid, c], cbuf.at[slot], ld_c.at[slot])

    def act_load(layer, b, ref, sem):
        return pltpu.make_async_copy(h_ref.at[layer, row_block(b)], ref, sem)

    def act_block(b, ref):
        @pl.loop(0, 4)
        def _(f):
            cols = pl.ds(pl.multiple_of(f * fb, fb), fb)
            a = gelu(ref[:, cols].astype(F32)).astype(BF16).astype(F32)
            lt[0, cols, row_block(b)] = a.T.astype(BF16)

    def weight_loads(layer):
        return (pltpu.make_async_copy(wd_ref.at[layer], wd, ld_w.at[0]), pltpu.make_async_copy(wu_ref.at[layer], wu, ld_w.at[1]))

    def unit_place(u):
        r = lax.rem(u // 2 + 1, 4)
        chip = lax.rem(py + r // 2, 2) * 2 + lax.rem(px + lax.rem(r, 2), 2)
        return r, chip

    def unit_rows(u):
        _, chip = unit_place(u)
        start = (chip * 2 + core) * rows + lax.rem(u, 2) * half_rows
        other = (chip * 2 + 1 - core) * rows + lax.rem(u, 2) * half_rows
        return tuple(pl.ds(pl.multiple_of(s, half_rows), half_rows) for s in (start, other))

    def unit_load(gid, layer, u):
        for n, block in enumerate(unit_rows(u)):
            here = pl.ds(n * half_rows, half_rows)
            for c in range(CHUNKS):
                pltpu.make_async_copy(gb_ref.at[gid, c, block], gr.at[here, pl.ds(c * cw, cw)], ld_g).start()
            pltpu.make_async_copy(h_ref.at[layer, block], hr.at[here], ld_h).start()

    def unit_first(u):
        take(gr, ld_g)
        take(hr, ld_h)
        mine, other = unit_rows(u)

        @pl.loop(0, 4)
        def _(f):
            cols = pl.ds(pl.multiple_of(f * fb, fb), fb)
            d_act = lax.dot_general(gr[...], wd[cols, :], NT, preferred_element_type=F32)
            d_pre = (d_act * gelu_slope(hr[:, cols].astype(F32))).astype(BF16)
            dh[:, cols] = d_pre
            flipped = d_pre.astype(F32).T.astype(BF16)
            lt[1, cols, mine] = flipped[:, :half_rows]
            lt[1, cols, other] = flipped[:, half_rows:]

    def unit_second(lp, u):
        order = lp * 8 + u
        slot = lax.rem(order, 2)
        kept = lax.rem(u, SUMS)

        @pl.when(order >= 2)
        def _():
            take(pp.at[slot], pp_s.at[slot])

        @pl.when(jnp.logical_or(u >= SUMS, jnp.logical_and(lp > 0, u >= 8 - SUMS)))
        def _():
            take(pm.at[kept], pm_s.at[kept])

        @pl.loop(0, CHUNKS)
        def _(d):
            cols = chunk_columns(d)
            part = lax.dot_general(dh[...], wu[cols, :], NT, preferred_element_type=F32).astype(BF16)
            pm[kept, :, cols] = part[:half_rows]
            pp[slot, :, cols] = part[half_rows:]

        @pl.when(order >= HELD)
        def _():
            pl.semaphore_wait(pbc, 1)

        there = lax.rem(order, HELD)
        remote(pp.at[slot], pb.at[there], pp_s.at[slot], pb_r.at[there], model(partner)).start()

    def unit_finish(lp, u):
        order = lp * 8 + u
        slot = lax.rem(order, HELD)
        kept = lax.rem(u, SUMS)
        r, chip = unit_place(u)
        here = pl.ds(pl.multiple_of(lax.rem(u, 2) * half_rows, half_rows), half_rows)
        take(pb.at[slot], pb_r.at[slot])

        @pl.when(r != 0)
        def _():
            @pl.loop(0, CHUNKS)
            def _(d):
                cols = chunk_columns(d)
                pm[kept, :, cols] = (pm[kept, :, cols].astype(F32) + pb[slot, :, cols].astype(F32)).astype(BF16)

            remote(pm.at[kept], rxh_ref.at[lp, r - 1, here], pm_s.at[kept], rx_r.at[lp * 6 + (r - 1) * 2 + lax.rem(u, 2)],
                   model(chip * 2 + core)).start()

        @pl.when(r == 0)
        def _():
            @pl.loop(0, CHUNKS)
            def _(d):
                cols = chunk_columns(d)
                rxo[here, cols] = (pm[kept, :, cols].astype(F32) + pb[slot, :, cols].astype(F32)).astype(BF16)

        @pl.when(order < 8 * LAYERS - HELD)
        def _():
            signal(pbc, model(partner))

    def quarter(n):
        part = rows // 4
        return pl.ds(pl.multiple_of(n * part, part), part)

    def new_gradient_load(lp, n):
        @pl.when(lax.rem(n, 2) == 0)
        def _():
            for r in range(3):
                take(pm.at[0], rx_r.at[lp * 6 + r * 2 + n // 2])

        for r in range(3):
            pltpu.make_async_copy(rxh_ref.at[lp, r, quarter(n)], gr.at[quarter(r)], ld_rx.at[r]).start()

    def new_gradient(n):
        for r in range(3):
            take(gr.at[quarter(0)], ld_rx.at[r])

        @pl.loop(0, CHUNKS)
        def _(d):
            cols = chunk_columns(d)
            total = rxo[quarter(n), cols].astype(F32)
            for r in range(3):
                total += gr[quarter(r), cols].astype(F32)
            gown[quarter(n), cols] = (gown[quarter(n), cols].astype(F32) + total).astype(BF16)

    def split(q):
        return pl.ds(q * (fb // SPLIT), fb // SPLIT)

    def piece_place(i):
        return LAYERS - 1 - i // PER_LAYER, lax.rem(i // PHASE, 2), lax.rem(i, PHASE) // PARTS, lax.rem(i, PARTS)

    def part_columns(n):
        return pl.ds(pl.multiple_of(n * fb, fb), fb)

    def piece(i):
        _, phase, _, n = piece_place(i)
        slot = lax.rem(i, SLOTS)

        @pl.when(jnp.logical_and(is_end, i >= SLOTS))
        def _():
            take(zp.at[slot], zs.at[slot])

        @pl.when(i < PARTS)
        def _():
            wide = pl.ds(pl.multiple_of(lax.rem(i, 2) * 2 * fb, 2 * fb), 2 * fb)

            for h in range(2):
                @pl.when(i // 2 == h)
                def _():
                    part = jnp.dot(lt[0, wide, :], cbuf[0, :, pl.ds(h * (cw // 2), cw // 2)], preferred_element_type=F32)
                    for b in range(2):
                        zp[slot, :, pl.ds(b * (cw // 2), cw // 2)] = part[b * fb:(b + 1) * fb]

        @pl.when(i >= PARTS)
        def _():
            part = jnp.dot(lt[phase, part_columns(n), :], cbuf[lax.rem(i // PARTS, 2)], preferred_element_type=F32)

            @pl.when(phase == 0)
            def _():
                zp[slot] = part

            @pl.when(phase == 1)
            def _():
                zp[slot] = part.T

    def total_place(j):
        layer, _, c, n = piece_place(j)
        return down_ref.at[layer, part_columns(n), chunk_columns(c)], up_ref.at[layer, chunk_columns(c), part_columns(n)]

    def total_copies(j, slot):
        _, phase, _, _ = piece_place(j)
        down, up = total_place(j)
        first = []
        for b in range(2):
            f0 = (lax.rem(j, 2) * 2 + b) * fb
            d0 = j // 2 * (cw // 2)
            first.append((z2.at[slot, :, pl.ds(b * (cw // 2), cw // 2)],
                          down_ref.at[LAYERS - 1, pl.ds(pl.multiple_of(f0, fb), fb), pl.ds(pl.multiple_of(d0, cw // 2), cw // 2)]))
        return ((j < PARTS, first), (jnp.logical_and(j >= PARTS, phase == 0), [(z2.at[slot], down)]), (phase == 1, [(z2.at[slot], up)]))

    def total_send(j, slot):
        @pl.when(jnp.logical_and(j >= 0, j < FULL))
        def _():
            for cond, copies in total_copies(j, slot):
                @pl.when(cond)
                def _():
                    for source, place in copies:
                        remote(source, place, z_ts.at[slot], z_rt.at[lax.rem(j, LAST_SLOTS)], data(line_end)).start()
                        pltpu.make_async_copy(source, place, z_tl.at[slot]).start()

    def sum_send(slot, q):
        remote(zp.at[slot, split(q)], z2.at[slot, split(q)], zs.at[slot], z_r2.at[slot], data(line_across)).start()

    def line_step(i):
        @pl.when(is_end)
        def _():
            @pl.when(i < PIECES)
            def _():
                slot, there = lax.rem(i, SLOTS), lax.rem(i, FIRST_SLOTS)

                @pl.when(i >= FIRST_SLOTS)
                def _():
                    pl.semaphore_wait(c1, 1)

                for q in range(SPLIT):
                    remote(zp.at[slot, split(q)], z1.at[there, split(q)], zs.at[slot], z_r1.at[there, q], data(line_mid)).start()

            j = i - LAG_LAST

            @pl.when(jnp.logical_and(j >= 0, j < FULL))
            def _():
                take(zp.at[0], z_rt.at[lax.rem(j, LAST_SLOTS)])

                @pl.when(j + LAST_SLOTS < FULL)
                def _():
                    signal(c3, data(line_mid))

        @pl.when(is_mid)
        def _():
            slot, there = lax.rem(i, SLOTS), lax.rem(i, FIRST_SLOTS)
            j = i - LAG_SUM
            old = lax.rem(j + SLOTS, SLOTS)

            @pl.when(jnp.logical_and(j >= 0, j < PIECES))
            def _():
                take(z2.at[old], z_r2.at[old])
                z2[old] = z2[old] + zp[old]
                take(zp.at[old], zs.at[old])

                @pl.when(jnp.logical_and(j >= LAST_SLOTS, j < FULL))
                def _():
                    pl.semaphore_wait(c3, 1)

            @pl.when(jnp.logical_and(j >= FULL, j < PIECES))
            def _():
                pltpu.make_async_copy(z2.at[old], rest_ref.at[:, part_columns(j - FULL)], z_tl.at[old]).start()

            @pl.when(i < PIECES)
            def _():
                @pl.when(i >= SLOTS)
                def _():
                    pl.semaphore_wait(c2, 1)

                for q in range(SPLIT):
                    take(z1.at[there, split(q)], z_r1.at[there, q])
                    zp[slot, split(q), :] = zp[slot, split(q), :] + z1[there, split(q), :]

                    if q == 0:
                        total_send(j, old)
                    else:
                        sum_send(slot, q - 1)
                sum_send(slot, SPLIT - 1)

                @pl.when(i + FIRST_SLOTS < PIECES)
                def _():
                    signal(c1, data(line_end))

            @pl.when(i >= PIECES)
            def _():
                total_send(j, old)

            k = i - LAG_FREE

            @pl.when(jnp.logical_and(k >= 0, k < PIECES))
            def _():
                free = lax.rem(k, SLOTS)
                @pl.when(k < FULL)
                def _():
                    take(z2.at[free], z_ts.at[free])

                take(z2.at[free], z_tl.at[free])

                @pl.when(k + SLOTS < PIECES)
                def _():
                    signal(c2, data(line_across))

    top = LAYERS - 1
    loads_g = [pltpu.make_async_copy(g_ref.at[:, part], gown.at[:, part], sem)
               for part, sem in ((pl.ds(0, cw), ld_rx.at[0]), (pl.ds(cw, hidden - cw), ld_o))]
    for load in loads_g:
        load.start()
    held = ((ha, ld_a), (hr, ld_h))
    for n, (ref, sem) in enumerate(held):
        act_load(top, n, ref, sem).start()
    barrier = pltpu.get_barrier_semaphore()
    for peer in (near_x, near_y, far, partner):
        signal(barrier, model(peer))

    @pl.when(is_end)
    def _():
        signal(barrier, data(line_mid))
        pl.semaphore_wait(barrier, 5)

    @pl.when(is_mid)
    def _():
        signal(barrier, data(line_end))
        signal(barrier, data(line_across))
        pl.semaphore_wait(barrier, 6)

    loads_g[0].wait()
    half_send(0)
    cbuf[0, row_block(me), :] = gown[:, :cw]
    loads_g[1].wait()
    gather_keep(0, gown, 1)
    load_x = pltpu.make_async_copy(x_ref.at[top], xown, ld_o)
    load_x.start()
    for load in weight_loads(top):
        load.start()

    @pl.loop(0, 4)
    def _(b):
        for n, (ref, sem) in enumerate(held):
            act_load(top, 0, ref, sem).wait()
            act_block(2 * b + n, ref)

            @pl.when(b < 3)
            def _():
                act_load(top, 2 * b + n + 2, ref, sem).start()

        @pl.when(b == FIRST_RELAY)
        def _():
            half_relay(0)
            half_send(1)

    half_forward(0)
    half_relay(1)
    gather_send(0, 1, gown, gathered(0, 1))
    load_x.wait()
    take(gown.at[:, pl.ds(0, hidden - cw)], ag_l.at[0])
    half_wait(0)

    @pl.loop(0, PIECES)
    def _(i):
        lp = i // PER_LAYER
        layer = LAYERS - 1 - lp
        s = i // 2
        sl = lax.rem(s, PER_LAYER // 2)
        il = lax.rem(i, PER_LAYER)
        even = lax.rem(i, 2) == 0
        odd = jnp.logical_not(even)
        odd_pair = lax.rem(s, 2) == 1
        even_pair = jnp.logical_not(odd_pair)
        ggid, xgid = 2 * lp, 2 * lp + 1

        @pl.when(jnp.logical_and(i > 0, lax.rem(i, PARTS) == 0))
        def _():
            take(cbuf.at[0], ld_c.at[lax.rem(i // PARTS, 2)])

        piece(i)

        line_step(i)

        def when(*conds):
            return pl.when(functools.reduce(jnp.logical_and, conds))

        @pl.when(i == 0)
        def _():
            half_forward(1)

        @pl.when(i == 1)
        def _():
            half_wait(1)
            pltpu.make_async_copy(cbuf.at[0], gathered(0, 0), first_l).start()

        @when(odd, s < CHUNKS - 1)
        def _():
            gather_relay(0, s + 1, gathered(0, s + 1), ag_s.at[0], ag_f.at[0])

        @pl.when(jnp.logical_or(i == 1, jnp.logical_and(jnp.logical_and(even, s >= 1), s < CHUNKS - 2)))
        def _():
            gather_send(0, s + 2, gown, gathered(0, s + 2))

        @when(even, s >= 1, s < CHUNKS)
        def _():
            gather_forward(0, s, gathered(0, s), ag_f.at[0])

        @when(odd, s >= 1, s < CHUNKS)
        def _():
            gather_wait(0, s, gathered(0, s))

        @when(i == 2 * PARTS - 2)
        def _():
            take(cbuf.at[0, pl.ds(0, 4 * rows)], first_s)
            take(cbuf.at[0], first_l)

        @when(even, sl == X_RUNS[0][2])
        def _():
            gather_keep(xgid, xown)

        for first, count, start, relay, forward in X_RUNS:
            @when(even, sl >= start, sl < start + count)
            def _():
                gather_send(xgid, sl - start + first, xown, gathered(xgid, sl - start + first))

            @when(even, sl >= start + relay, sl < start + relay + count)
            def _():
                gather_relay(xgid, sl - start - relay + first, gathered(xgid, sl - start - relay + first), ag_s.at[xgid], ag_f.at[xgid])

            @when(even, sl >= start + forward, sl < start + forward + count)
            def _():
                gather_forward(xgid, sl - start - forward + first, gathered(xgid, sl - start - forward + first), ag_f.at[xgid])

        @when(even, sl == 15)
        def _():
            take(xown, ag_l.at[xgid])

        @when(even, odd_pair, sl >= 15, sl < 31)
        def _():
            gather_wait(xgid, (sl - 15) // 2, gathered(xgid, (sl - 15) // 2))

        @when(even, s == 25)
        def _():
            gather_keep(2, gown)

        @when(even, s >= 25, s < 25 + CHUNKS)
        def _():
            gather_send(2, s - 25, gown, gathered(2, s - 25))

        @when(even, s >= 27, s < 27 + CHUNKS)
        def _():
            gather_relay(2, s - 27, gathered(2, s - 27), ag_s.at[2], ag_f.at[2])

        @when(even, s >= 29, s < 29 + CHUNKS)
        def _():
            gather_forward(2, s - 29, gathered(2, s - 29), ag_f.at[2])

        @when(odd, s == 30)
        def _():
            take(gown, ag_l.at[2])

        @when(odd, s >= 30, s < 30 + CHUNKS)
        def _():
            gather_wait(2, s - 30, gathered(2, s - 30))

        @when(jnp.logical_or(i == PARTS - 1, jnp.logical_and(i >= PARTS, lax.rem(i, PARTS) == PARTS - 2)), i + 2 < PIECES)
        def _():
            nxt = i // PARTS * PARTS + PARTS
            chunk_load(nxt // PHASE, lax.rem(nxt, PHASE) // PARTS, lax.rem(nxt // PARTS, 2)).start()

        @when(even, sl == UNIT_STEP)
        def _():
            for load in weight_loads(0):
                load.wait()

        @when(even, sl >= UNIT_STEP, sl < UNIT_STEP + 8)
        def _():
            unit_first(sl - UNIT_STEP)

        @when(even, sl > UNIT_STEP + 1, sl <= UNIT_STEP + 9)
        def _():
            unit_finish(lp, sl - UNIT_STEP - 2)

        @when(odd, sl >= UNIT_STEP - 1, sl < UNIT_STEP + 7)
        def _():
            unit_load(ggid, layer, sl - UNIT_STEP + 1)

        @when(odd, sl >= UNIT_STEP, sl < UNIT_STEP + 8)
        def _():
            unit_second(lp, sl - UNIT_STEP)

        @when(il == FINAL_STEP - 1)
        def _():
            take(gb_ref.at[ggid, 0, pl.ds(0, 7 * rows)], ag_s.at[ggid])
            take(gb_ref.at[ggid, pl.ds(0, 3)], ag_s.at[ggid])

            @pl.when(lp > 0)
            def _():
                take(gb_ref.at[ggid, 0, row_block(0)], ag_s.at[ggid])

            new_gradient_load(lp, 0)

        @when(il >= FINAL_STEP, il < FINAL_STEP + 4)
        def _():
            new_gradient(il - FINAL_STEP)

            @pl.when(il < FINAL_STEP + 3)
            def _():
                new_gradient_load(lp, il - FINAL_STEP + 1)

        @when(i == PER_LAYER + FINAL_STEP + 4)
        def _():
            pltpu.make_async_copy(gown, gx_ref, st_gx).start()

        @when(lp == 0, even, sl == 17)
        def _():
            for load in weight_loads(0):
                load.start()

        @when(lp == 0, even, even_pair, sl >= 16)
        def _():
            act_load(0, (sl - 16) // 2, ha, ld_a).start()

        @when(lp == 0, odd, odd_pair, sl >= 16)
        def _():
            act_load(0, 0, ha, ld_a).wait()
            act_block((sl - 16) // 2, ha)

        @when(even, sl == 31)
        def _():
            take(gb_ref.at[xgid, pl.ds(0, 4)], ag_s.at[xgid])

            @pl.when(lp == 0)
            def _():
                pltpu.make_async_copy(x_ref.at[0], xown, ld_o).start()

        @when(lp == 0, odd, sl == 31)
        def _():
            pltpu.make_async_copy(x_ref.at[0], xown, ld_o).wait()

    @pl.loop(PIECES, PIECES + LAG_LAST)
    def _(i):
        line_step(i)

    take(gb_ref.at[0, 0, pl.ds(0, 5 * rows)], ag_f.at[0])
    take(gb_ref.at[0, pl.ds(0, 2)], ag_f.at[0])
    for gid in range(1, 2 * LAYERS):
        take(gb_ref.at[gid, pl.ds(0, 3)], ag_f.at[gid])
    for slot in range(2):
        take(pp.at[slot], pp_s.at[slot])
    for kept in range(8 - SUMS, SUMS):
        take(pm.at[kept], pm_s.at[kept])
    take(gown, st_gx)

    @pl.when(is_end)
    def _():
        for slot in range(SLOTS):
            take(zp.at[slot], zs.at[slot])


def move_kernel(count, *refs):
    sources, targets = refs[:count], refs[count:2 * count]
    buffers, read, written = refs[2 * count:3 * count], refs[-2], refs[-1]
    copies, slot = [], 0
    for source, target, buffer in zip(sources, targets, buffers):
        size = buffer.shape[1]
        for n in range(buffer.shape[0]):
            rows = pl.ds(n * size, size)
            copies.append((pltpu.make_async_copy(source.at[rows], buffer.at[n], read.at[slot]),
                           pltpu.make_async_copy(buffer.at[n], target.at[rows], written.at[slot])))
            slot += 1
    for first, _ in copies:
        first.start()
    for first, _ in copies:
        first.wait()
    for _, second in copies:
        second.start()
    for _, second in copies:
        second.wait()


def move(*arrays):
    flat = [a.reshape(-1, a.shape[-1]) for a in arrays]
    parts = [max(1, a.size * a.dtype.itemsize // MOVE_BYTES) for a in flat]
    any_space = pl.BlockSpec(memory_space=pl.ANY)
    size = sum(a.size * a.dtype.itemsize for a in flat)
    moved = pl.pallas_call(
        functools.partial(move_kernel, len(flat)),
        name="move",
        out_shape=tuple(jax.ShapeDtypeStruct(a.shape, a.dtype) for a in flat),
        in_specs=[any_space] * len(flat),
        out_specs=(any_space,) * len(flat),
        scratch_shapes=[pltpu.VMEM((n, a.shape[0] // n, a.shape[1]), a.dtype) for a, n in zip(flat, parts)]
        + [pltpu.SemaphoreType.DMA((sum(parts),))] * 2,
        compiler_params=pltpu.CompilerParams(vmem_limit_bytes=67043328),
        cost_estimate=pl.CostEstimate(flops=int(size * MOVE_FLOPS), bytes_accessed=2 * size, transcendentals=0),
    )(*flat)
    return [m.reshape(a.shape) for m, a in zip(moved, arrays)]


def solution(mesh):
    def device_step(x_saved, h_saved, w_up, w_down, grad_out):
        layers, hidden, ffn = w_up.shape
        rows = grad_out.shape[1]
        tokens = h_saved.shape[2]
        cw, fb = hidden // CHUNKS, ffn // PARTS
        half_rows = rows // 2
        any_space = pl.BlockSpec(memory_space=pl.ANY)
        dma = pltpu.SemaphoreType.DMA
        vmem = pltpu.VMEM
        grad_x, grad_up, grad_down, rest, _, _ = pl.pallas_call(
            kernel,
            name="backward",
            out_shape=(
                jax.ShapeDtypeStruct((rows, hidden), BF16),
                jax.ShapeDtypeStruct(w_up.shape, F32),
                jax.ShapeDtypeStruct(w_down.shape, F32),
                jax.ShapeDtypeStruct((cw, REST * fb), F32),
                jax.ShapeDtypeStruct((2 * layers, CHUNKS, tokens, cw), BF16),
                jax.ShapeDtypeStruct((layers, 3, rows, hidden), BF16),
            ),
            in_specs=[any_space] * 5,
            out_specs=(any_space,) * 6,
            scratch_shapes=[
                vmem((2, ffn, tokens), BF16),
                vmem((ffn, hidden), BF16),
                vmem((hidden, ffn), BF16),
                vmem((2, tokens, cw), BF16),
                vmem((rows, hidden), BF16),
                vmem((rows, ffn), BF16),
                vmem((rows, ffn), BF16),
                vmem((rows, ffn), BF16),
                vmem((rows, hidden), BF16),
                vmem((rows, hidden), BF16),
                vmem((SUMS, half_rows, hidden), BF16),
                vmem((2, half_rows, hidden), BF16),
                vmem((HELD, half_rows, hidden), BF16),
                vmem((rows, hidden), BF16),
                vmem((SLOTS, fb, cw), F32),
                vmem((FIRST_SLOTS, fb, cw), F32),
                vmem((SLOTS, fb, cw), F32),
                dma((SLOTS,)), dma((FIRST_SLOTS, SPLIT)), dma((SLOTS,)), dma((SLOTS,)), dma((SLOTS,)), dma((LAST_SLOTS,)),
                pltpu.SemaphoreType.REGULAR, pltpu.SemaphoreType.REGULAR, pltpu.SemaphoreType.REGULAR,
                dma((2 * layers, CHUNKS)), dma((2 * layers, CHUNKS)), dma((2 * layers, CHUNKS)), dma((2 * layers, CHUNKS)),
                dma((2 * layers,)), dma((2 * layers,)), dma((2 * layers,)),
                dma((2,)), dma((HELD,)), dma((SUMS,)), dma((6 * layers,)), pltpu.SemaphoreType.REGULAR,
                dma((2,)), dma(()), dma(()), dma(()), dma((2,)), dma(()), dma((3,)), dma(()), dma(()), dma(()), dma((2,)), dma((2,)), dma((2,)), dma((2,)),
            ],
            compiler_params=pltpu.CompilerParams(collective_id=0, has_side_effects=True, vmem_limit_bytes=67043328),
        )(x_saved[:, 0], h_saved[:, 0], w_up, w_down, grad_out[0])
        spot = lax.axis_index("data")
        is_end = (spot == 0) | (spot == 3)
        rest = jnp.where(is_end, lax.ppermute(rest, "data", [(1, 0), (2, 3)]), rest)
        grad_x, grad_up, grad_down = move(grad_x, grad_up, grad_down)
        grad_up = grad_up.at[0, hidden - cw:, ffn - REST * fb:].set(rest)
        return grad_x[None], grad_up, grad_down

    return jax.shard_map(
        device_step,
        mesh=mesh,
        in_specs=(P(None, "data", "model", None), P(None, "data", None, "model"), P(None, None, "model"), P(None, "model", None), P("data", "model", None)),
        out_specs=(P("data", "model", None), P(None, None, "model"), P(None, "model", None)),
        check_vma=False,
    )
```

```python
import functools

import jax
import jax.numpy as jnp
from jax import lax
from jax.experimental import pallas as pl
from jax.experimental.pallas import tpu as pltpu
from jax.sharding import PartitionSpec as P

MESH = pl.DeviceIdType.MESH
F32, BF16 = jnp.float32, jnp.bfloat16
NT = (((1,), (1,)), ((), ()))

LAYERS = 2
CHUNKS = 8
PARTS = 4
PHASE = CHUNKS * PARTS
PER_LAYER = 2 * PHASE
PIECES = LAYERS * PER_LAYER
REST = 2
FULL = PIECES - REST
SLOTS = 16
FIRST_SLOTS = 8
SPLIT = 4
LAST_SLOTS = 32
LAG_SUM = 2
LAG_FREE = 6
LAG_LAST = 20
UNIT_STEPS = 16, 14
X_RUNS = ((0, 5, 6, 3, 8), (5, 3, 19, 4, 5))
FIRST_RELAY = 1
FINAL_STEP = 46
HELD = 3
SUMS = 6

MOVE_BYTES = 1 << 22
MOVE_FLOPS = 10


def gelu_tanh(pre):
    return jnp.tanh(0.7978845608028654 * (pre + 0.044715 * pre * pre * pre))


def gelu(pre):
    return 0.5 * pre * (1.0 + gelu_tanh(pre))


def gelu_slope(pre):
    tanh_val = gelu_tanh(pre)
    return 0.5 * (1.0 + tanh_val) + 0.5 * pre * (1.0 - tanh_val * tanh_val) * 0.7978845608028654 * (1.0 + 0.134145 * pre * pre)


def kernel(x_ref, h_ref, wu_ref, wd_ref, g_ref, gx_ref, up_ref, down_ref, rest_ref, gb_ref, rxh_ref,
           lt, wd, wu, cbuf, gr, hr, dh, ha, gown, xown, pm, pp, pb, rxo, zp, z1, z2,
           zs, z_r1, z_r2, z_ts, z_tl, z_rt, c1, c2, c3,
           ag_x, ag_y, ag_d, ag_p, ag_s, ag_f, ag_l, pp_s, pb_r, pm_s, rx_r, pbc,
           ld_c, ld_g, ld_h, ld_a, ld_w, ld_o, ld_rx, st_gx, first_s, first_l, first_x, first_y, first_d, first_p):
    rows, hidden = gown.shape
    ffn = lt.shape[1]
    half_rows = rows // 2
    cw = hidden // CHUNKS
    fb = ffn // 4

    me = lax.axis_index("model")
    spot = lax.axis_index("data")
    core = lax.rem(me, 2)
    px = lax.rem(me // 2, 2)
    py = me // 4
    partner = me + 1 - 2 * core
    step_x, step_y = 2 * (1 - 2 * px), 4 * (1 - 2 * py)
    near_x, near_y, far = me + step_x, me + step_y, me + step_x + step_y
    is_end = jnp.logical_or(spot == 0, spot == 3)
    is_mid = jnp.logical_not(is_end)
    line_mid = jnp.where(spot < 2, 1, 2)
    line_end = jnp.where(spot < 2, 0, 3)
    line_across = 3 - spot

    def model(i):
        return {"model": i}

    def data(i):
        return {"data": i}

    def signal(sem, where):
        pl.semaphore_signal(sem, inc=1, device_id=where, device_id_type=MESH)

    def remote(src, dst, send, recv, where):
        return pltpu.make_async_remote_copy(src_ref=src, dst_ref=dst, send_sem=send, recv_sem=recv, device_id=where, device_id_type=MESH)

    def take(ref, sem):
        pltpu.make_async_copy(ref, ref, sem).wait()

    def chunk_columns(c):
        return pl.ds(pl.multiple_of(c * cw, cw), cw)

    def row_block(i):
        return pl.ds(pl.multiple_of(i * rows, rows), rows)

    def gather_keep(gid, own, first=0):
        for c in range(first, CHUNKS):
            pltpu.make_async_copy(own.at[:, pl.ds(c * cw, cw)], gb_ref.at[gid, c, row_block(me)], ag_l.at[gid]).start()

    def gather_send(gid, c, own, buf):
        src = own.at[:, chunk_columns(c)]
        dst = buf.at[row_block(me)]
        remote(src, dst, ag_s.at[gid], ag_x.at[gid, c], model(near_x)).start()
        remote(src, dst, ag_s.at[gid], ag_y.at[gid, c], model(near_y)).start()
        remote(src, dst, ag_s.at[gid], ag_p.at[gid, c], model(partner)).start()

    def gather_relay(gid, c, buf, sent, forwarded):
        take(buf.at[row_block(0)], ag_x.at[gid, c])
        take(buf.at[row_block(0)], ag_y.at[gid, c])
        for n, (source, target) in enumerate(((near_x, near_y), (near_y, near_x))):
            @pl.when(core == n)
            def _():
                block = buf.at[row_block(source)]
                remote(block, block, sent, ag_d.at[gid, c], model(target)).start()
        for peer in (near_x, near_y):
            block = buf.at[row_block(peer)]
            remote(block, block, forwarded, ag_p.at[gid, c], model(partner)).start()

    def gather_forward(gid, c, buf, forwarded):
        take(buf.at[row_block(0)], ag_d.at[gid, c])
        block = buf.at[row_block(far)]
        remote(block, block, forwarded, ag_p.at[gid, c], model(partner)).start()

    def gather_wait(gid, c, buf):
        take(buf.at[pl.ds(0, 4 * rows)], ag_p.at[gid, c])

    def gathered(gid, c):
        return gb_ref.at[gid, c]

    def half_block(i, h):
        return cbuf.at[0, row_block(i), pl.ds(h * (cw // 2), cw // 2)]

    def half_send(h):
        src = gown.at[:, pl.ds(h * (cw // 2), cw // 2)]
        for peer, sem in ((near_x, first_x), (near_y, first_y), (partner, first_p)):
            remote(src, half_block(me, h), ag_s.at[0], sem.at[h], model(peer)).start()

    def half_relay(h):
        take(half_block(0, h), first_x.at[h])
        take(half_block(0, h), first_y.at[h])
        for n, (source, target) in enumerate(((near_x, near_y), (near_y, near_x))):
            @pl.when(core == n)
            def _():
                remote(half_block(source, h), half_block(source, h), first_s, first_d.at[h], model(target)).start()
        for peer in (near_x, near_y):
            remote(half_block(peer, h), half_block(peer, h), first_s, first_p.at[h], model(partner)).start()

    def half_forward(h):
        take(half_block(0, h), first_d.at[h])
        remote(half_block(far, h), half_block(far, h), first_s, first_p.at[h], model(partner)).start()

    def half_wait(h):
        take(cbuf.at[0, pl.ds(0, 4 * rows), pl.ds(h * (cw // 2), cw // 2)], first_p.at[h])

    def chunk_load(gid, c, slot):
        return pltpu.make_async_copy(gb_ref.at[gid, c], cbuf.at[slot], ld_c.at[slot])

    def act_load(layer, b, ref, sem):
        return pltpu.make_async_copy(h_ref.at[layer, row_block(b)], ref, sem)

    def act_block(b, ref):
        @pl.loop(0, 4)
        def _(f):
            cols = pl.ds(pl.multiple_of(f * fb, fb), fb)
            a = gelu(ref[:, cols].astype(F32)).astype(BF16).astype(F32)
            lt[0, cols, row_block(b)] = a.T.astype(BF16)

    def weight_loads(layer):
        return (pltpu.make_async_copy(wd_ref.at[layer], wd, ld_w.at[0]), pltpu.make_async_copy(wu_ref.at[layer], wu, ld_w.at[1]))

    def unit_place(u):
        r = lax.rem(u // 2 + 1, 4)
        chip = lax.rem(py + r // 2, 2) * 2 + lax.rem(px + lax.rem(r, 2), 2)
        return r, chip

    def unit_rows(u):
        _, chip = unit_place(u)
        start = (chip * 2 + core) * rows + lax.rem(u, 2) * half_rows
        other = (chip * 2 + 1 - core) * rows + lax.rem(u, 2) * half_rows
        return tuple(pl.ds(pl.multiple_of(s, half_rows), half_rows) for s in (start, other))

    def unit_load(gid, layer, u):
        for n, block in enumerate(unit_rows(u)):
            here = pl.ds(n * half_rows, half_rows)
            for c in range(CHUNKS):
                pltpu.make_async_copy(gb_ref.at[gid, c, block], gr.at[here, pl.ds(c * cw, cw)], ld_g).start()
            pltpu.make_async_copy(h_ref.at[layer, block], hr.at[here], ld_h).start()

    def unit_first(u):
        take(gr, ld_g)
        take(hr, ld_h)
        mine, other = unit_rows(u)

        @pl.loop(0, 4)
        def _(f):
            cols = pl.ds(pl.multiple_of(f * fb, fb), fb)
            d_act = lax.dot_general(gr[...], wd[cols, :], NT, preferred_element_type=F32)
            d_pre = (d_act * gelu_slope(hr[:, cols].astype(F32))).astype(BF16)
            dh[:, cols] = d_pre
            flipped = d_pre.astype(F32).T.astype(BF16)
            lt[1, cols, mine] = flipped[:, :half_rows]
            lt[1, cols, other] = flipped[:, half_rows:]

    def unit_second(lp, u):
        order = lp * 8 + u
        slot = lax.rem(order, 2)
        kept = lax.rem(u, SUMS)

        @pl.when(order >= 2)
        def _():
            take(pp.at[slot], pp_s.at[slot])

        @pl.when(jnp.logical_or(u >= SUMS, jnp.logical_and(lp > 0, u >= 8 - SUMS)))
        def _():
            take(pm.at[kept], pm_s.at[kept])

        @pl.loop(0, CHUNKS)
        def _(d):
            cols = chunk_columns(d)
            part = lax.dot_general(dh[...], wu[cols, :], NT, preferred_element_type=F32).astype(BF16)
            pm[kept, :, cols] = part[:half_rows]
            pp[slot, :, cols] = part[half_rows:]

        @pl.when(order >= HELD)
        def _():
            pl.semaphore_wait(pbc, 1)

        there = lax.rem(order, HELD)
        remote(pp.at[slot], pb.at[there], pp_s.at[slot], pb_r.at[there], model(partner)).start()

    def unit_finish(lp, u):
        order = lp * 8 + u
        slot = lax.rem(order, HELD)
        kept = lax.rem(u, SUMS)
        r, chip = unit_place(u)
        here = pl.ds(pl.multiple_of(lax.rem(u, 2) * half_rows, half_rows), half_rows)
        take(pb.at[slot], pb_r.at[slot])

        @pl.when(r != 0)
        def _():
            @pl.loop(0, CHUNKS)
            def _(d):
                cols = chunk_columns(d)
                pm[kept, :, cols] = (pm[kept, :, cols].astype(F32) + pb[slot, :, cols].astype(F32)).astype(BF16)

            remote(pm.at[kept], rxh_ref.at[lp, r - 1, here], pm_s.at[kept], rx_r.at[lp * 6 + (r - 1) * 2 + lax.rem(u, 2)],
                   model(chip * 2 + core)).start()

        @pl.when(r == 0)
        def _():
            @pl.loop(0, CHUNKS)
            def _(d):
                cols = chunk_columns(d)
                rxo[here, cols] = (pm[kept, :, cols].astype(F32) + pb[slot, :, cols].astype(F32)).astype(BF16)

        @pl.when(order < 8 * LAYERS - HELD)
        def _():
            signal(pbc, model(partner))

    def quarter(n):
        part = rows // 4
        return pl.ds(pl.multiple_of(n * part, part), part)

    def new_gradient_load(lp, n):
        @pl.when(lax.rem(n, 2) == 0)
        def _():
            for r in range(3):
                take(pm.at[0], rx_r.at[lp * 6 + r * 2 + n // 2])

        for r in range(3):
            pltpu.make_async_copy(rxh_ref.at[lp, r, quarter(n)], gr.at[quarter(r)], ld_rx.at[r]).start()

    def new_gradient(n):
        for r in range(3):
            take(gr.at[quarter(0)], ld_rx.at[r])

        @pl.loop(0, CHUNKS)
        def _(d):
            cols = chunk_columns(d)
            total = rxo[quarter(n), cols].astype(F32)
            for r in range(3):
                total += gr[quarter(r), cols].astype(F32)
            gown[quarter(n), cols] = (gown[quarter(n), cols].astype(F32) + total).astype(BF16)

    def split(q):
        return pl.ds(q * (fb // SPLIT), fb // SPLIT)

    def piece_place(i):
        return LAYERS - 1 - i // PER_LAYER, lax.rem(i // PHASE, 2), lax.rem(i, PHASE) // PARTS, lax.rem(i, PARTS)

    def part_columns(n):
        return pl.ds(pl.multiple_of(n * fb, fb), fb)

    def piece(i):
        _, phase, _, n = piece_place(i)
        slot = lax.rem(i, SLOTS)

        @pl.when(jnp.logical_and(is_end, i >= SLOTS))
        def _():
            take(zp.at[slot], zs.at[slot])

        @pl.when(i < PARTS)
        def _():
            wide = pl.ds(pl.multiple_of(lax.rem(i, 2) * 2 * fb, 2 * fb), 2 * fb)

            for h in range(2):
                @pl.when(i // 2 == h)
                def _():
                    part = jnp.dot(lt[0, wide, :], cbuf[0, :, pl.ds(h * (cw // 2), cw // 2)], preferred_element_type=F32)
                    for b in range(2):
                        zp[slot, :, pl.ds(b * (cw // 2), cw // 2)] = part[b * fb:(b + 1) * fb]

        @pl.when(i >= PARTS)
        def _():
            part = jnp.dot(lt[phase, part_columns(n), :], cbuf[lax.rem(i // PARTS, 2)], preferred_element_type=F32)

            @pl.when(phase == 0)
            def _():
                zp[slot] = part

            @pl.when(phase == 1)
            def _():
                zp[slot] = part.T

    def total_place(j):
        layer, _, c, n = piece_place(j)
        return down_ref.at[layer, part_columns(n), chunk_columns(c)], up_ref.at[layer, chunk_columns(c), part_columns(n)]

    def total_copies(j, slot):
        _, phase, _, _ = piece_place(j)
        down, up = total_place(j)
        first = []
        for b in range(2):
            f0 = (lax.rem(j, 2) * 2 + b) * fb
            d0 = j // 2 * (cw // 2)
            first.append((z2.at[slot, :, pl.ds(b * (cw // 2), cw // 2)],
                          down_ref.at[LAYERS - 1, pl.ds(pl.multiple_of(f0, fb), fb), pl.ds(pl.multiple_of(d0, cw // 2), cw // 2)]))
        return ((j < PARTS, first), (jnp.logical_and(j >= PARTS, phase == 0), [(z2.at[slot], down)]), (phase == 1, [(z2.at[slot], up)]))

    def total_send(j, slot):
        @pl.when(jnp.logical_and(j >= 0, j < FULL))
        def _():
            for cond, copies in total_copies(j, slot):
                @pl.when(cond)
                def _():
                    for source, place in copies:
                        remote(source, place, z_ts.at[slot], z_rt.at[lax.rem(j, LAST_SLOTS)], data(line_end)).start()
                        pltpu.make_async_copy(source, place, z_tl.at[slot]).start()

    def sum_send(slot, q):
        remote(zp.at[slot, split(q)], z2.at[slot, split(q)], zs.at[slot], z_r2.at[slot], data(line_across)).start()

    def line_step(i):
        @pl.when(is_end)
        def _():
            @pl.when(i < PIECES)
            def _():
                slot, there = lax.rem(i, SLOTS), lax.rem(i, FIRST_SLOTS)

                @pl.when(i >= FIRST_SLOTS)
                def _():
                    pl.semaphore_wait(c1, 1)

                for q in range(SPLIT):
                    remote(zp.at[slot, split(q)], z1.at[there, split(q)], zs.at[slot], z_r1.at[there, q], data(line_mid)).start()

            j = i - LAG_LAST

            @pl.when(jnp.logical_and(j >= 0, j < FULL))
            def _():
                take(zp.at[0], z_rt.at[lax.rem(j, LAST_SLOTS)])

                @pl.when(j + LAST_SLOTS < FULL)
                def _():
                    signal(c3, data(line_mid))

        @pl.when(is_mid)
        def _():
            slot, there = lax.rem(i, SLOTS), lax.rem(i, FIRST_SLOTS)
            j = i - LAG_SUM
            old = lax.rem(j + SLOTS, SLOTS)

            @pl.when(jnp.logical_and(j >= 0, j < PIECES))
            def _():
                take(z2.at[old], z_r2.at[old])
                z2[old] = z2[old] + zp[old]
                take(zp.at[old], zs.at[old])

                @pl.when(jnp.logical_and(j >= LAST_SLOTS, j < FULL))
                def _():
                    pl.semaphore_wait(c3, 1)

            @pl.when(jnp.logical_and(j >= FULL, j < PIECES))
            def _():
                pltpu.make_async_copy(z2.at[old], rest_ref.at[:, part_columns(j - FULL)], z_tl.at[old]).start()

            @pl.when(i < PIECES)
            def _():
                @pl.when(i >= SLOTS)
                def _():
                    pl.semaphore_wait(c2, 1)

                for q in range(SPLIT):
                    take(z1.at[there, split(q)], z_r1.at[there, q])
                    zp[slot, split(q), :] = zp[slot, split(q), :] + z1[there, split(q), :]

                    if q == 0:
                        total_send(j, old)
                    else:
                        sum_send(slot, q - 1)
                sum_send(slot, SPLIT - 1)

                @pl.when(i + FIRST_SLOTS < PIECES)
                def _():
                    signal(c1, data(line_end))

            @pl.when(i >= PIECES)
            def _():
                total_send(j, old)

            k = i - LAG_FREE

            @pl.when(jnp.logical_and(k >= 0, k < PIECES))
            def _():
                free = lax.rem(k, SLOTS)
                @pl.when(k < FULL)
                def _():
                    take(z2.at[free], z_ts.at[free])

                take(z2.at[free], z_tl.at[free])

                @pl.when(k + SLOTS < PIECES)
                def _():
                    signal(c2, data(line_across))

    top = LAYERS - 1
    loads_g = [pltpu.make_async_copy(g_ref.at[:, part], gown.at[:, part], sem)
               for part, sem in ((pl.ds(0, cw), ld_rx.at[0]), (pl.ds(cw, hidden - cw), ld_o))]
    for load in loads_g:
        load.start()
    held = ((ha, ld_a), (hr, ld_h))
    for n, (ref, sem) in enumerate(held):
        act_load(top, n, ref, sem).start()
    barrier = pltpu.get_barrier_semaphore()
    for peer in (near_x, near_y, far, partner):
        signal(barrier, model(peer))

    @pl.when(is_end)
    def _():
        signal(barrier, data(line_mid))
        pl.semaphore_wait(barrier, 5)

    @pl.when(is_mid)
    def _():
        signal(barrier, data(line_end))
        signal(barrier, data(line_across))
        pl.semaphore_wait(barrier, 6)

    loads_g[0].wait()
    half_send(0)
    cbuf[0, row_block(me), :] = gown[:, :cw]
    loads_g[1].wait()
    gather_keep(0, gown, 1)
    load_x = pltpu.make_async_copy(x_ref.at[top], xown, ld_o)
    load_x.start()
    for load in weight_loads(top):
        load.start()

    @pl.loop(0, 4)
    def _(b):
        for n, (ref, sem) in enumerate(held):
            act_load(top, 0, ref, sem).wait()
            act_block(2 * b + n, ref)

            @pl.when(b < 3)
            def _():
                act_load(top, 2 * b + n + 2, ref, sem).start()

        @pl.when(b == FIRST_RELAY)
        def _():
            half_relay(0)
            half_send(1)

    half_forward(0)
    half_relay(1)
    gather_send(0, 1, gown, gathered(0, 1))
    load_x.wait()
    take(gown.at[:, pl.ds(0, hidden - cw)], ag_l.at[0])
    half_wait(0)

    @pl.loop(0, PIECES)
    def _(i):
        lp = i // PER_LAYER
        layer = LAYERS - 1 - lp
        s = i // 2
        sl = lax.rem(s, PER_LAYER // 2)
        il = lax.rem(i, PER_LAYER)
        even = lax.rem(i, 2) == 0
        odd = jnp.logical_not(even)
        odd_pair = lax.rem(s, 2) == 1
        even_pair = jnp.logical_not(odd_pair)
        ggid, xgid = 2 * lp, 2 * lp + 1

        @pl.when(jnp.logical_and(i > 0, lax.rem(i, PARTS) == 0))
        def _():
            take(cbuf.at[0], ld_c.at[lax.rem(i // PARTS, 2)])

        piece(i)

        line_step(i)

        def when(*conds):
            return pl.when(functools.reduce(jnp.logical_and, conds))

        @pl.when(s < CHUNKS)
        def _():
            @pl.when(i == 0)
            def _():
                half_forward(1)

            @pl.when(i == 1)
            def _():
                half_wait(1)
                pltpu.make_async_copy(cbuf.at[0], gathered(0, 0), first_l).start()

            @when(odd, s < CHUNKS - 1)
            def _():
                gather_relay(0, s + 1, gathered(0, s + 1), ag_s.at[0], ag_f.at[0])

            @pl.when(jnp.logical_or(i == 1, jnp.logical_and(jnp.logical_and(even, s >= 1), s < CHUNKS - 2)))
            def _():
                gather_send(0, s + 2, gown, gathered(0, s + 2))

            @when(even, s >= 1, s < CHUNKS)
            def _():
                gather_forward(0, s, gathered(0, s), ag_f.at[0])

            @when(odd, s >= 1, s < CHUNKS)
            def _():
                gather_wait(0, s, gathered(0, s))

            @when(i == 2 * PARTS - 2)
            def _():
                take(cbuf.at[0, pl.ds(0, 4 * rows)], first_s)
                take(cbuf.at[0], first_l)

        @pl.when(sl >= X_RUNS[0][2])
        def _():
            @when(even, sl == X_RUNS[0][2])
            def _():
                gather_keep(xgid, xown)

            for first, count, start, relay, forward in X_RUNS:
                @when(even, sl >= start, sl < start + count)
                def _():
                    gather_send(xgid, sl - start + first, xown, gathered(xgid, sl - start + first))

                @when(even, sl >= start + relay, sl < start + relay + count)
                def _():
                    gather_relay(xgid, sl - start - relay + first, gathered(xgid, sl - start - relay + first), ag_s.at[xgid], ag_f.at[xgid])

                @when(even, sl >= start + forward, sl < start + forward + count)
                def _():
                    gather_forward(xgid, sl - start - forward + first, gathered(xgid, sl - start - forward + first), ag_f.at[xgid])

            @when(even, sl == 15)
            def _():
                take(xown, ag_l.at[xgid])

            @when(even, odd_pair, sl >= 15, sl < 31)
            def _():
                gather_wait(xgid, (sl - 15) // 2, gathered(xgid, (sl - 15) // 2))

        @pl.when(jnp.logical_and(s >= 25, s < 30 + CHUNKS))
        def _():
            @when(even, s == 25)
            def _():
                gather_keep(2, gown)

            @when(even, s >= 25, s < 25 + CHUNKS)
            def _():
                gather_send(2, s - 25, gown, gathered(2, s - 25))

            @when(even, s >= 27, s < 27 + CHUNKS)
            def _():
                gather_relay(2, s - 27, gathered(2, s - 27), ag_s.at[2], ag_f.at[2])

            @when(even, s >= 29, s < 29 + CHUNKS)
            def _():
                gather_forward(2, s - 29, gathered(2, s - 29), ag_f.at[2])

            @when(odd, s == 30)
            def _():
                take(gown, ag_l.at[2])

            @when(odd, s >= 30, s < 30 + CHUNKS)
            def _():
                gather_wait(2, s - 30, gathered(2, s - 30))

        @when(jnp.logical_or(i == PARTS - 1, jnp.logical_and(i >= PARTS, lax.rem(i, PARTS) == PARTS - 2)), i + 2 < PIECES)
        def _():
            nxt = i // PARTS * PARTS + PARTS
            chunk_load(nxt // PHASE, lax.rem(nxt, PHASE) // PARTS, lax.rem(nxt // PARTS, 2)).start()

        @pl.when(jnp.logical_and(il >= min(UNIT_STEPS) - 1, il < max(UNIT_STEPS) + 24))
        def _():
            spread = lp > 0
            k = il - jnp.where(spread, UNIT_STEPS[1], UNIT_STEPS[0])
            half = jnp.where(spread, 4 * (k // 5) + lax.rem(k + 5, 5), k)
            on = functools.reduce(jnp.logical_and, (k >= 0, half < 16, jnp.logical_or(jnp.logical_not(spread), lax.rem(k + 5, 5) < 4)))
            u = half // 2
            first_half = lax.rem(half + 16, 2) == 0
            last = jnp.where(spread, 20, 16)

            @when(k == -1)
            def _():
                unit_load(ggid, layer, 0)

            @when(k == 0)
            def _():
                for load in weight_loads(0):
                    load.wait()

            @when(on, first_half)
            def _():
                unit_first(u)

            @when(jnp.logical_or(jnp.logical_and(jnp.logical_and(on, first_half), u >= 2), jnp.logical_or(k == last, k == last + 2)))
            def _():
                unit_finish(lp, jnp.where(k >= last, 6 + (k - last) // 2, u - 2))

            @when(on, jnp.logical_not(first_half), u < 7)
            def _():
                unit_load(ggid, layer, u + 1)

            @when(on, jnp.logical_not(first_half))
            def _():
                unit_second(lp, u)

        @pl.when(jnp.logical_and(il >= FINAL_STEP - 1, il < FINAL_STEP + 5))
        def _():
            @when(il == FINAL_STEP - 1)
            def _():
                take(gb_ref.at[ggid, 0, pl.ds(0, 7 * rows)], ag_s.at[ggid])
                take(gb_ref.at[ggid, pl.ds(0, 3)], ag_s.at[ggid])

                @pl.when(lp > 0)
                def _():
                    take(gb_ref.at[ggid, 0, row_block(0)], ag_s.at[ggid])

                new_gradient_load(lp, 0)

            @when(il >= FINAL_STEP, il < FINAL_STEP + 4)
            def _():
                new_gradient(il - FINAL_STEP)

                @pl.when(il < FINAL_STEP + 3)
                def _():
                    new_gradient_load(lp, il - FINAL_STEP + 1)

            @when(i == PER_LAYER + FINAL_STEP + 4)
            def _():
                pltpu.make_async_copy(gown, gx_ref, st_gx).start()

        @pl.when(sl >= 16)
        def _():
            @when(lp == 0, even, sl == 17)
            def _():
                for load in weight_loads(0):
                    load.start()

            @when(lp == 0, even, even_pair, sl >= 16)
            def _():
                act_load(0, (sl - 16) // 2, ha, ld_a).start()

            @when(lp == 0, odd, odd_pair, sl >= 16)
            def _():
                act_load(0, 0, ha, ld_a).wait()
                act_block((sl - 16) // 2, ha)

            @when(even, sl == 31)
            def _():
                take(gb_ref.at[xgid, pl.ds(0, 4)], ag_s.at[xgid])

                @pl.when(lp == 0)
                def _():
                    pltpu.make_async_copy(x_ref.at[0], xown, ld_o).start()

            @when(lp == 0, odd, sl == 31)
            def _():
                pltpu.make_async_copy(x_ref.at[0], xown, ld_o).wait()

    @pl.loop(PIECES, PIECES + LAG_LAST)
    def _(i):
        line_step(i)

    take(gb_ref.at[0, 0, pl.ds(0, 5 * rows)], ag_f.at[0])
    take(gb_ref.at[0, pl.ds(0, 2)], ag_f.at[0])
    for gid in range(1, 2 * LAYERS):
        take(gb_ref.at[gid, pl.ds(0, 3)], ag_f.at[gid])
    for slot in range(2):
        take(pp.at[slot], pp_s.at[slot])
    for kept in range(8 - SUMS, SUMS):
        take(pm.at[kept], pm_s.at[kept])
    take(gown, st_gx)

    @pl.when(is_end)
    def _():
        for slot in range(SLOTS):
            take(zp.at[slot], zs.at[slot])


def move_kernel(count, *refs):
    sources, targets = refs[:count], refs[count:2 * count]
    buffers, read, written = refs[2 * count:3 * count], refs[-2], refs[-1]
    copies, slot = [], 0
    for source, target, buffer in zip(sources, targets, buffers):
        size = buffer.shape[1]
        for n in range(buffer.shape[0]):
            rows = pl.ds(n * size, size)
            copies.append((pltpu.make_async_copy(source.at[rows], buffer.at[n], read.at[slot]),
                           pltpu.make_async_copy(buffer.at[n], target.at[rows], written.at[slot])))
            slot += 1
    for first, _ in copies:
        first.start()
    for first, _ in copies:
        first.wait()
    for _, second in copies:
        second.start()
    for _, second in copies:
        second.wait()


def move(*arrays):
    flat = [a.reshape(-1, a.shape[-1]) for a in arrays]
    parts = [max(1, a.size * a.dtype.itemsize // MOVE_BYTES) for a in flat]
    any_space = pl.BlockSpec(memory_space=pl.ANY)
    size = sum(a.size * a.dtype.itemsize for a in flat)
    moved = pl.pallas_call(
        functools.partial(move_kernel, len(flat)),
        name="move",
        out_shape=tuple(jax.ShapeDtypeStruct(a.shape, a.dtype) for a in flat),
        in_specs=[any_space] * len(flat),
        out_specs=(any_space,) * len(flat),
        scratch_shapes=[pltpu.VMEM((n, a.shape[0] // n, a.shape[1]), a.dtype) for a, n in zip(flat, parts)]
        + [pltpu.SemaphoreType.DMA((sum(parts),))] * 2,
        compiler_params=pltpu.CompilerParams(vmem_limit_bytes=67043328),
        cost_estimate=pl.CostEstimate(flops=int(size * MOVE_FLOPS), bytes_accessed=2 * size, transcendentals=0),
    )(*flat)
    return [m.reshape(a.shape) for m, a in zip(moved, arrays)]


def solution(mesh):
    def device_step(x_saved, h_saved, w_up, w_down, grad_out):
        layers, hidden, ffn = w_up.shape
        rows = grad_out.shape[1]
        tokens = h_saved.shape[2]
        cw, fb = hidden // CHUNKS, ffn // PARTS
        half_rows = rows // 2
        any_space = pl.BlockSpec(memory_space=pl.ANY)
        dma = pltpu.SemaphoreType.DMA
        vmem = pltpu.VMEM
        grad_x, grad_up, grad_down, rest, _, _ = pl.pallas_call(
            kernel,
            name="backward",
            out_shape=(
                jax.ShapeDtypeStruct((rows, hidden), BF16),
                jax.ShapeDtypeStruct(w_up.shape, F32),
                jax.ShapeDtypeStruct(w_down.shape, F32),
                jax.ShapeDtypeStruct((cw, REST * fb), F32),
                jax.ShapeDtypeStruct((2 * layers, CHUNKS, tokens, cw), BF16),
                jax.ShapeDtypeStruct((layers, 3, rows, hidden), BF16),
            ),
            in_specs=[any_space] * 5,
            out_specs=(any_space,) * 6,
            scratch_shapes=[
                vmem((2, ffn, tokens), BF16),
                vmem((ffn, hidden), BF16),
                vmem((hidden, ffn), BF16),
                vmem((2, tokens, cw), BF16),
                vmem((rows, hidden), BF16),
                vmem((rows, ffn), BF16),
                vmem((rows, ffn), BF16),
                vmem((rows, ffn), BF16),
                vmem((rows, hidden), BF16),
                vmem((rows, hidden), BF16),
                vmem((SUMS, half_rows, hidden), BF16),
                vmem((2, half_rows, hidden), BF16),
                vmem((HELD, half_rows, hidden), BF16),
                vmem((rows, hidden), BF16),
                vmem((SLOTS, fb, cw), F32),
                vmem((FIRST_SLOTS, fb, cw), F32),
                vmem((SLOTS, fb, cw), F32),
                dma((SLOTS,)), dma((FIRST_SLOTS, SPLIT)), dma((SLOTS,)), dma((SLOTS,)), dma((SLOTS,)), dma((LAST_SLOTS,)),
                pltpu.SemaphoreType.REGULAR, pltpu.SemaphoreType.REGULAR, pltpu.SemaphoreType.REGULAR,
                dma((2 * layers, CHUNKS)), dma((2 * layers, CHUNKS)), dma((2 * layers, CHUNKS)), dma((2 * layers, CHUNKS)),
                dma((2 * layers,)), dma((2 * layers,)), dma((2 * layers,)),
                dma((2,)), dma((HELD,)), dma((SUMS,)), dma((6 * layers,)), pltpu.SemaphoreType.REGULAR,
                dma((2,)), dma(()), dma(()), dma(()), dma((2,)), dma(()), dma((3,)), dma(()), dma(()), dma(()), dma((2,)), dma((2,)), dma((2,)), dma((2,)),
            ],
            compiler_params=pltpu.CompilerParams(collective_id=0, has_side_effects=True, vmem_limit_bytes=67043328),
        )(x_saved[:, 0], h_saved[:, 0], w_up, w_down, grad_out[0])
        spot = lax.axis_index("data")
        is_end = (spot == 0) | (spot == 3)
        rest = jnp.where(is_end, lax.ppermute(rest, "data", [(1, 0), (2, 3)]), rest)
        grad_x, grad_up, grad_down = move(grad_x, grad_up, grad_down)
        grad_up = grad_up.at[0, hidden - cw:, ffn - REST * fb:].set(rest)
        return grad_x[None], grad_up, grad_down

    return jax.shard_map(
        device_step,
        mesh=mesh,
        in_specs=(P(None, "data", "model", None), P(None, "data", None, "model"), P(None, None, "model"), P(None, "model", None), P("data", "model", None)),
        out_specs=(P("data", "model", None), P(None, None, "model"), P(None, "model", None)),
        check_vma=False,
    )
```

```python
import functools

import jax
import jax.numpy as jnp
from jax import lax
from jax.experimental import pallas as pl
from jax.experimental.pallas import tpu as pltpu
from jax.sharding import PartitionSpec as P

MESH = pl.DeviceIdType.MESH
F32, BF16 = jnp.float32, jnp.bfloat16
NT = (((1,), (1,)), ((), ()))

LAYERS = 2
CHUNKS = 8
PARTS = 4
PHASE = CHUNKS * PARTS
PER_LAYER = 2 * PHASE
PIECES = LAYERS * PER_LAYER
REST = 2
FULL = PIECES - REST
SLOTS = 16
FIRST_SLOTS = 8
SPLIT = 4
LAST_SLOTS = 32
LAG_SUM = 2
LAG_FREE = 6
LAG_LAST = 20
UNIT_STEPS = 16, 14
X_RUNS = ((0, 5, 6, 3, 8), (5, 3, 19, 4, 5))
FIRST_RELAY = 1
FINAL_STEP = 46
HELD = 3
SUMS = 6

MOVE_BYTES = 1 << 22
MOVE_FLOPS = 10


def gelu_tanh(pre):
    return jnp.tanh(0.7978845608028654 * (pre + 0.044715 * pre * pre * pre))


def gelu(pre):
    return 0.5 * pre * (1.0 + gelu_tanh(pre))


def gelu_slope(pre):
    tanh_val = gelu_tanh(pre)
    return 0.5 * (1.0 + tanh_val) + 0.5 * pre * (1.0 - tanh_val * tanh_val) * 0.7978845608028654 * (1.0 + 0.134145 * pre * pre)


def kernel(x_ref, h_ref, wu_ref, wd_ref, g_ref, gx_ref, up_ref, down_ref, rest_ref, gb_ref, rxh_ref,
           lt, wd, wu, cbuf, gr, hr, dh, ha, gown, xown, pm, pp, pb, rxo, zp, z1, z2,
           zs, z_r1, z_r2, z_ts, z_tl, z_rt, c1, c2, c3,
           ag_x, ag_y, ag_d, ag_p, ag_s, ag_f, ag_l, pp_s, pb_r, pm_s, rx_r, pbc,
           ld_c, ld_g, ld_h, ld_a, ld_w, ld_o, ld_rx, st_gx, first_s, first_l, first_x, first_y, first_d, first_p):
    rows, hidden = gown.shape
    ffn = lt.shape[1]
    half_rows = rows // 2
    cw = hidden // CHUNKS
    fb = ffn // 4

    me = lax.axis_index("model")
    spot = lax.axis_index("data")
    core = lax.rem(me, 2)
    px = lax.rem(me // 2, 2)
    py = me // 4
    partner = me + 1 - 2 * core
    step_x, step_y = 2 * (1 - 2 * px), 4 * (1 - 2 * py)
    near_x, near_y, far = me + step_x, me + step_y, me + step_x + step_y
    is_end = jnp.logical_or(spot == 0, spot == 3)
    is_mid = jnp.logical_not(is_end)
    line_mid = jnp.where(spot < 2, 1, 2)
    line_end = jnp.where(spot < 2, 0, 3)
    line_across = 3 - spot

    def model(i):
        return {"model": i}

    def data(i):
        return {"data": i}

    def signal(sem, where):
        pl.semaphore_signal(sem, inc=1, device_id=where, device_id_type=MESH)

    def remote(src, dst, send, recv, where):
        return pltpu.make_async_remote_copy(src_ref=src, dst_ref=dst, send_sem=send, recv_sem=recv, device_id=where, device_id_type=MESH)

    def take(ref, sem):
        pltpu.make_async_copy(ref, ref, sem).wait()

    def chunk_columns(c):
        return pl.ds(pl.multiple_of(c * cw, cw), cw)

    def row_block(i):
        return pl.ds(pl.multiple_of(i * rows, rows), rows)

    def gather_keep(gid, own, first=0):
        for c in range(first, CHUNKS):
            pltpu.make_async_copy(own.at[:, pl.ds(c * cw, cw)], gb_ref.at[gid, c, row_block(me)], ag_l.at[gid]).start()

    def gather_send(gid, c, own, buf):
        src = own.at[:, chunk_columns(c)]
        dst = buf.at[row_block(me)]
        remote(src, dst, ag_s.at[gid], ag_x.at[gid, c], model(near_x)).start()
        remote(src, dst, ag_s.at[gid], ag_y.at[gid, c], model(near_y)).start()
        remote(src, dst, ag_s.at[gid], ag_p.at[gid, c], model(partner)).start()

    def gather_relay(gid, c, buf, sent, forwarded):
        take(buf.at[row_block(0)], ag_x.at[gid, c])
        take(buf.at[row_block(0)], ag_y.at[gid, c])
        for n, (source, target) in enumerate(((near_x, near_y), (near_y, near_x))):
            @pl.when(core == n)
            def _():
                block = buf.at[row_block(source)]
                remote(block, block, sent, ag_d.at[gid, c], model(target)).start()
        for peer in (near_x, near_y):
            block = buf.at[row_block(peer)]
            remote(block, block, forwarded, ag_p.at[gid, c], model(partner)).start()

    def gather_forward(gid, c, buf, forwarded):
        take(buf.at[row_block(0)], ag_d.at[gid, c])
        block = buf.at[row_block(far)]
        remote(block, block, forwarded, ag_p.at[gid, c], model(partner)).start()

    def gather_wait(gid, c, buf):
        take(buf.at[pl.ds(0, 4 * rows)], ag_p.at[gid, c])

    def gathered(gid, c):
        return gb_ref.at[gid, c]

    def half_block(i, h):
        return cbuf.at[0, row_block(i), pl.ds(h * (cw // 2), cw // 2)]

    def half_send(h):
        src = gown.at[:, pl.ds(h * (cw // 2), cw // 2)]
        for peer, sem in ((near_x, first_x), (near_y, first_y), (partner, first_p)):
            remote(src, half_block(me, h), ag_s.at[0], sem.at[h], model(peer)).start()

    def half_relay(h):
        take(half_block(0, h), first_x.at[h])
        take(half_block(0, h), first_y.at[h])
        for n, (source, target) in enumerate(((near_x, near_y), (near_y, near_x))):
            @pl.when(core == n)
            def _():
                remote(half_block(source, h), half_block(source, h), first_s, first_d.at[h], model(target)).start()
        for peer in (near_x, near_y):
            remote(half_block(peer, h), half_block(peer, h), first_s, first_p.at[h], model(partner)).start()

    def half_forward(h):
        take(half_block(0, h), first_d.at[h])
        remote(half_block(far, h), half_block(far, h), first_s, first_p.at[h], model(partner)).start()

    def half_wait(h):
        take(cbuf.at[0, pl.ds(0, 4 * rows), pl.ds(h * (cw // 2), cw // 2)], first_p.at[h])

    def chunk_load(gid, c, slot):
        return pltpu.make_async_copy(gb_ref.at[gid, c], cbuf.at[slot], ld_c.at[slot])

    def act_load(layer, b, ref, sem):
        return pltpu.make_async_copy(h_ref.at[layer, row_block(b)], ref, sem)

    def act_block(b, ref):
        @pl.loop(0, 4)
        def _(f):
            cols = pl.ds(pl.multiple_of(f * fb, fb), fb)
            a = gelu(ref[:, cols].astype(F32)).astype(BF16).astype(F32)
            lt[0, cols, row_block(b)] = a.T.astype(BF16)

    def weight_loads(layer):
        return (pltpu.make_async_copy(wd_ref.at[layer], wd, ld_w.at[0]), pltpu.make_async_copy(wu_ref.at[layer], wu, ld_w.at[1]))

    def unit_place(u):
        r = lax.rem(u // 2 + 1, 4)
        chip = lax.rem(py + r // 2, 2) * 2 + lax.rem(px + lax.rem(r, 2), 2)
        return r, chip

    def unit_rows(u):
        _, chip = unit_place(u)
        start = (chip * 2 + core) * rows + lax.rem(u, 2) * half_rows
        other = (chip * 2 + 1 - core) * rows + lax.rem(u, 2) * half_rows
        return tuple(pl.ds(pl.multiple_of(s, half_rows), half_rows) for s in (start, other))

    def unit_load(gid, layer, u):
        for n, block in enumerate(unit_rows(u)):
            here = pl.ds(n * half_rows, half_rows)
            for c in range(CHUNKS):
                pltpu.make_async_copy(gb_ref.at[gid, c, block], gr.at[here, pl.ds(c * cw, cw)], ld_g).start()
            pltpu.make_async_copy(h_ref.at[layer, block], hr.at[here], ld_h).start()

    def unit_first(u):
        take(gr, ld_g)
        take(hr, ld_h)
        mine, other = unit_rows(u)

        @pl.loop(0, 4)
        def _(f):
            cols = pl.ds(pl.multiple_of(f * fb, fb), fb)
            d_act = lax.dot_general(gr[...], wd[cols, :], NT, preferred_element_type=F32)
            d_pre = (d_act * gelu_slope(hr[:, cols].astype(F32))).astype(BF16)
            dh[:, cols] = d_pre
            flipped = d_pre.astype(F32).T.astype(BF16)
            lt[1, cols, mine] = flipped[:, :half_rows]
            lt[1, cols, other] = flipped[:, half_rows:]

    def unit_second(lp, u):
        order = lp * 8 + u
        slot = lax.rem(order, 2)
        kept = lax.rem(u, SUMS)

        @pl.when(order >= 2)
        def _():
            take(pp.at[slot], pp_s.at[slot])

        @pl.when(jnp.logical_or(u >= SUMS, jnp.logical_and(lp > 0, u >= 8 - SUMS)))
        def _():
            take(pm.at[kept], pm_s.at[kept])

        @pl.loop(0, CHUNKS)
        def _(d):
            cols = chunk_columns(d)
            part = lax.dot_general(dh[...], wu[cols, :], NT, preferred_element_type=F32).astype(BF16)
            pm[kept, :, cols] = part[:half_rows]
            pp[slot, :, cols] = part[half_rows:]

        @pl.when(order >= HELD)
        def _():
            pl.semaphore_wait(pbc, 1)

        there = lax.rem(order, HELD)
        remote(pp.at[slot], pb.at[there], pp_s.at[slot], pb_r.at[there], model(partner)).start()

    def unit_finish(lp, u):
        order = lp * 8 + u
        slot = lax.rem(order, HELD)
        kept = lax.rem(u, SUMS)
        r, chip = unit_place(u)
        here = pl.ds(pl.multiple_of(lax.rem(u, 2) * half_rows, half_rows), half_rows)
        take(pb.at[slot], pb_r.at[slot])

        @pl.when(r != 0)
        def _():
            @pl.loop(0, CHUNKS)
            def _(d):
                cols = chunk_columns(d)
                pm[kept, :, cols] = (pm[kept, :, cols].astype(F32) + pb[slot, :, cols].astype(F32)).astype(BF16)

            remote(pm.at[kept], rxh_ref.at[lp, r - 1, here], pm_s.at[kept], rx_r.at[lp * 6 + (r - 1) * 2 + lax.rem(u, 2)],
                   model(chip * 2 + core)).start()

        @pl.when(r == 0)
        def _():
            @pl.loop(0, CHUNKS)
            def _(d):
                cols = chunk_columns(d)
                rxo[here, cols] = (pm[kept, :, cols].astype(F32) + pb[slot, :, cols].astype(F32)).astype(BF16)

        @pl.when(order < 8 * LAYERS - HELD)
        def _():
            signal(pbc, model(partner))

    def quarter(n):
        part = rows // 4
        return pl.ds(pl.multiple_of(n * part, part), part)

    def new_gradient_load(lp, n):
        @pl.when(lax.rem(n, 2) == 0)
        def _():
            for r in range(3):
                take(pm.at[0], rx_r.at[lp * 6 + r * 2 + n // 2])

        for r in range(3):
            pltpu.make_async_copy(rxh_ref.at[lp, r, quarter(n)], gr.at[quarter(r)], ld_rx.at[r]).start()

    def new_gradient(n):
        for r in range(3):
            take(gr.at[quarter(0)], ld_rx.at[r])

        @pl.loop(0, CHUNKS)
        def _(d):
            cols = chunk_columns(d)
            total = rxo[quarter(n), cols].astype(F32)
            for r in range(3):
                total += gr[quarter(r), cols].astype(F32)
            gown[quarter(n), cols] = (gown[quarter(n), cols].astype(F32) + total).astype(BF16)

    def split(q):
        return pl.ds(q * (fb // SPLIT), fb // SPLIT)

    def piece_place(i):
        return LAYERS - 1 - i // PER_LAYER, lax.rem(i // PHASE, 2), lax.rem(i, PHASE) // PARTS, lax.rem(i, PARTS)

    def part_columns(n):
        return pl.ds(pl.multiple_of(n * fb, fb), fb)

    def piece(i):
        _, phase, _, n = piece_place(i)
        slot = lax.rem(i, SLOTS)

        @pl.when(jnp.logical_and(is_end, i >= SLOTS))
        def _():
            take(zp.at[slot], zs.at[slot])

        @pl.when(i < PARTS)
        def _():
            wide = pl.ds(pl.multiple_of(lax.rem(i, 2) * 2 * fb, 2 * fb), 2 * fb)

            for h in range(2):
                @pl.when(i // 2 == h)
                def _():
                    part = jnp.dot(lt[0, wide, :], cbuf[0, :, pl.ds(h * (cw // 2), cw // 2)], preferred_element_type=F32)
                    for b in range(2):
                        zp[slot, :, pl.ds(b * (cw // 2), cw // 2)] = part[b * fb:(b + 1) * fb]

        @pl.when(i >= PARTS)
        def _():
            part = jnp.dot(lt[phase, part_columns(n), :], cbuf[lax.rem(i // PARTS, 2)], preferred_element_type=F32)

            @pl.when(phase == 0)
            def _():
                zp[slot] = part

            @pl.when(phase == 1)
            def _():
                zp[slot] = part.T

    def total_place(j):
        layer, _, c, n = piece_place(j)
        return down_ref.at[layer, part_columns(n), chunk_columns(c)], up_ref.at[layer, chunk_columns(c), part_columns(n)]

    def total_copies(j, slot):
        _, phase, _, _ = piece_place(j)
        down, up = total_place(j)
        first = []
        for b in range(2):
            f0 = (lax.rem(j, 2) * 2 + b) * fb
            d0 = j // 2 * (cw // 2)
            first.append((z2.at[slot, :, pl.ds(b * (cw // 2), cw // 2)],
                          down_ref.at[LAYERS - 1, pl.ds(pl.multiple_of(f0, fb), fb), pl.ds(pl.multiple_of(d0, cw // 2), cw // 2)]))
        return ((j < PARTS, first), (jnp.logical_and(j >= PARTS, phase == 0), [(z2.at[slot], down)]), (phase == 1, [(z2.at[slot], up)]))

    def total_send(j, slot):
        @pl.when(jnp.logical_and(j >= 0, j < FULL))
        def _():
            for cond, copies in total_copies(j, slot):
                @pl.when(cond)
                def _():
                    for source, place in copies:
                        remote(source, place, z_ts.at[slot], z_rt.at[lax.rem(j, LAST_SLOTS)], data(line_end)).start()
                        pltpu.make_async_copy(source, place, z_tl.at[slot]).start()

    def sum_send(slot, q):
        remote(zp.at[slot, split(q)], z2.at[slot, split(q)], zs.at[slot], z_r2.at[slot], data(line_across)).start()

    def line_step(i):
        @pl.when(is_end)
        def _():
            @pl.when(i < PIECES)
            def _():
                slot, there = lax.rem(i, SLOTS), lax.rem(i, FIRST_SLOTS)

                @pl.when(i >= FIRST_SLOTS)
                def _():
                    pl.semaphore_wait(c1, 1)

                for q in range(SPLIT):
                    remote(zp.at[slot, split(q)], z1.at[there, split(q)], zs.at[slot], z_r1.at[there, q], data(line_mid)).start()

            j = i - LAG_LAST

            @pl.when(jnp.logical_and(j >= 0, j < FULL))
            def _():
                take(zp.at[0], z_rt.at[lax.rem(j, LAST_SLOTS)])

                @pl.when(j + LAST_SLOTS < FULL)
                def _():
                    signal(c3, data(line_mid))

        @pl.when(is_mid)
        def _():
            slot, there = lax.rem(i, SLOTS), lax.rem(i, FIRST_SLOTS)
            j = i - LAG_SUM
            old = lax.rem(j + SLOTS, SLOTS)

            @pl.when(jnp.logical_and(j >= 0, j < PIECES))
            def _():
                take(z2.at[old], z_r2.at[old])
                z2[old] = z2[old] + zp[old]
                take(zp.at[old], zs.at[old])

                @pl.when(jnp.logical_and(j >= LAST_SLOTS, j < FULL))
                def _():
                    pl.semaphore_wait(c3, 1)

            @pl.when(jnp.logical_and(j >= FULL, j < PIECES))
            def _():
                pltpu.make_async_copy(z2.at[old], rest_ref.at[:, part_columns(j - FULL)], z_tl.at[old]).start()

            @pl.when(i < PIECES)
            def _():
                @pl.when(i >= SLOTS)
                def _():
                    pl.semaphore_wait(c2, 1)

                for q in range(SPLIT):
                    take(z1.at[there, split(q)], z_r1.at[there, q])
                    zp[slot, split(q), :] = zp[slot, split(q), :] + z1[there, split(q), :]

                    if q == 0:
                        total_send(j, old)
                    else:
                        sum_send(slot, q - 1)
                sum_send(slot, SPLIT - 1)

                @pl.when(i + FIRST_SLOTS < PIECES)
                def _():
                    signal(c1, data(line_end))

            @pl.when(i >= PIECES)
            def _():
                total_send(j, old)

            k = i - LAG_FREE

            @pl.when(jnp.logical_and(k >= 0, k < PIECES))
            def _():
                free = lax.rem(k, SLOTS)
                @pl.when(k < FULL)
                def _():
                    take(z2.at[free], z_ts.at[free])

                take(z2.at[free], z_tl.at[free])

                @pl.when(k + SLOTS < PIECES)
                def _():
                    signal(c2, data(line_across))

    top = LAYERS - 1
    loads_g = [pltpu.make_async_copy(g_ref.at[:, part], gown.at[:, part], sem)
               for part, sem in ((pl.ds(0, cw), ld_rx.at[0]), (pl.ds(cw, hidden - cw), ld_o))]
    for load in loads_g:
        load.start()
    held = ((ha, ld_a), (hr, ld_h))
    for n, (ref, sem) in enumerate(held):
        act_load(top, n, ref, sem).start()
    barrier = pltpu.get_barrier_semaphore()
    for peer in (near_x, near_y, far, partner):
        signal(barrier, model(peer))

    @pl.when(is_end)
    def _():
        signal(barrier, data(line_mid))
        pl.semaphore_wait(barrier, 5)

    @pl.when(is_mid)
    def _():
        signal(barrier, data(line_end))
        signal(barrier, data(line_across))
        pl.semaphore_wait(barrier, 6)

    loads_g[0].wait()
    half_send(0)
    cbuf[0, row_block(me), :] = gown[:, :cw]
    loads_g[1].wait()
    gather_keep(0, gown, 1)
    load_x = pltpu.make_async_copy(x_ref.at[top], xown, ld_o)
    load_x.start()
    for load in weight_loads(top):
        load.start()

    @pl.loop(0, 4)
    def _(b):
        for n, (ref, sem) in enumerate(held):
            act_load(top, 0, ref, sem).wait()
            act_block(2 * b + n, ref)

            @pl.when(b < 3)
            def _():
                act_load(top, 2 * b + n + 2, ref, sem).start()

        @pl.when(b == FIRST_RELAY)
        def _():
            half_relay(0)
            half_send(1)
            gather_send(0, 1, gown, gathered(0, 1))

    half_forward(0)
    load_x.wait()
    take(gown.at[:, pl.ds(0, hidden - cw)], ag_l.at[0])
    half_wait(0)

    @pl.loop(0, PIECES)
    def _(i):
        lp = i // PER_LAYER
        layer = LAYERS - 1 - lp
        s = i // 2
        sl = lax.rem(s, PER_LAYER // 2)
        il = lax.rem(i, PER_LAYER)
        even = lax.rem(i, 2) == 0
        odd = jnp.logical_not(even)
        odd_pair = lax.rem(s, 2) == 1
        even_pair = jnp.logical_not(odd_pair)
        ggid, xgid = 2 * lp, 2 * lp + 1

        @pl.when(jnp.logical_and(i > 0, lax.rem(i, PARTS) == 0))
        def _():
            take(cbuf.at[0], ld_c.at[lax.rem(i // PARTS, 2)])

        piece(i)

        line_step(i)

        def when(*conds):
            return pl.when(functools.reduce(jnp.logical_and, conds))

        @pl.when(s < CHUNKS)
        def _():
            @pl.when(i == 0)
            def _():
                half_relay(1)
                gather_relay(0, 1, gathered(0, 1), ag_s.at[0], ag_f.at[0])

            @pl.when(i == 1)
            def _():
                half_forward(1)
                half_wait(1)
                pltpu.make_async_copy(cbuf.at[0], gathered(0, 0), first_l).start()

            @when(odd, s >= 1, s < CHUNKS - 1)
            def _():
                gather_relay(0, s + 1, gathered(0, s + 1), ag_s.at[0], ag_f.at[0])

            @when(even, s < CHUNKS - 2)
            def _():
                gather_send(0, s + 2, gown, gathered(0, s + 2))

            @when(even, s >= 1, s < CHUNKS)
            def _():
                gather_forward(0, s, gathered(0, s), ag_f.at[0])

            @when(odd, s >= 1, s < CHUNKS)
            def _():
                gather_wait(0, s, gathered(0, s))

            @when(i == 2 * PARTS - 2)
            def _():
                take(cbuf.at[0, pl.ds(0, 4 * rows)], first_s)
                take(cbuf.at[0], first_l)

        @pl.when(sl >= X_RUNS[0][2])
        def _():
            @when(even, sl == X_RUNS[0][2])
            def _():
                gather_keep(xgid, xown)

            for first, count, start, relay, forward in X_RUNS:
                @when(even, sl >= start, sl < start + count)
                def _():
                    gather_send(xgid, sl - start + first, xown, gathered(xgid, sl - start + first))

                @when(even, sl >= start + relay, sl < start + relay + count)
                def _():
                    gather_relay(xgid, sl - start - relay + first, gathered(xgid, sl - start - relay + first), ag_s.at[xgid], ag_f.at[xgid])

                @when(even, sl >= start + forward, sl < start + forward + count)
                def _():
                    gather_forward(xgid, sl - start - forward + first, gathered(xgid, sl - start - forward + first), ag_f.at[xgid])

            @when(even, sl == 15)
            def _():
                take(xown, ag_l.at[xgid])

            @when(even, odd_pair, sl >= 15, sl < 31)
            def _():
                gather_wait(xgid, (sl - 15) // 2, gathered(xgid, (sl - 15) // 2))

        @pl.when(jnp.logical_and(s >= 25, s < 30 + CHUNKS))
        def _():
            @when(even, s == 25)
            def _():
                gather_keep(2, gown)

            @when(even, s >= 25, s < 25 + CHUNKS)
            def _():
                gather_send(2, s - 25, gown, gathered(2, s - 25))

            @when(even, s >= 27, s < 27 + CHUNKS)
            def _():
                gather_relay(2, s - 27, gathered(2, s - 27), ag_s.at[2], ag_f.at[2])

            @when(even, s >= 29, s < 29 + CHUNKS)
            def _():
                gather_forward(2, s - 29, gathered(2, s - 29), ag_f.at[2])

            @when(odd, s == 30)
            def _():
                take(gown, ag_l.at[2])

            @when(odd, s >= 30, s < 30 + CHUNKS)
            def _():
                gather_wait(2, s - 30, gathered(2, s - 30))

        @when(jnp.logical_or(i == PARTS - 1, jnp.logical_and(i >= PARTS, lax.rem(i, PARTS) == PARTS - 2)), i + 2 < PIECES)
        def _():
            nxt = i // PARTS * PARTS + PARTS
            chunk_load(nxt // PHASE, lax.rem(nxt, PHASE) // PARTS, lax.rem(nxt // PARTS, 2)).start()

        @pl.when(jnp.logical_and(il >= min(UNIT_STEPS) - 1, il < max(UNIT_STEPS) + 24))
        def _():
            spread = lp > 0
            k = il - jnp.where(spread, UNIT_STEPS[1], UNIT_STEPS[0])
            half = jnp.where(spread, 4 * (k // 5) + lax.rem(k + 5, 5), k)
            on = functools.reduce(jnp.logical_and, (k >= 0, half < 16, jnp.logical_or(jnp.logical_not(spread), lax.rem(k + 5, 5) < 4)))
            u = half // 2
            first_half = lax.rem(half + 16, 2) == 0
            last = jnp.where(spread, 20, 16)

            @when(k == -1)
            def _():
                unit_load(ggid, layer, 0)

            @when(k == 0)
            def _():
                for load in weight_loads(0):
                    load.wait()

            @when(on, first_half)
            def _():
                unit_first(u)

            @when(jnp.logical_or(jnp.logical_and(jnp.logical_and(on, first_half), u >= 2), jnp.logical_or(k == last, k == last + 2)))
            def _():
                unit_finish(lp, jnp.where(k >= last, 6 + (k - last) // 2, u - 2))

            @when(on, jnp.logical_not(first_half), u < 7)
            def _():
                unit_load(ggid, layer, u + 1)

            @when(on, jnp.logical_not(first_half))
            def _():
                unit_second(lp, u)

        @pl.when(jnp.logical_and(il >= FINAL_STEP - 1, il < FINAL_STEP + 5))
        def _():
            @when(il == FINAL_STEP - 1)
            def _():
                take(gb_ref.at[ggid, 0, pl.ds(0, 7 * rows)], ag_s.at[ggid])
                take(gb_ref.at[ggid, pl.ds(0, 3)], ag_s.at[ggid])

                @pl.when(lp > 0)
                def _():
                    take(gb_ref.at[ggid, 0, row_block(0)], ag_s.at[ggid])

                new_gradient_load(lp, 0)

            @when(il >= FINAL_STEP, il < FINAL_STEP + 4)
            def _():
                new_gradient(il - FINAL_STEP)

                @pl.when(il < FINAL_STEP + 3)
                def _():
                    new_gradient_load(lp, il - FINAL_STEP + 1)

            @when(i == PER_LAYER + FINAL_STEP + 4)
            def _():
                pltpu.make_async_copy(gown, gx_ref, st_gx).start()

        @pl.when(sl >= 16)
        def _():
            @when(lp == 0, even, sl == 17)
            def _():
                for load in weight_loads(0):
                    load.start()

            @when(lp == 0, even, even_pair, sl >= 16)
            def _():
                act_load(0, (sl - 16) // 2, ha, ld_a).start()

            @when(lp == 0, odd, odd_pair, sl >= 16)
            def _():
                act_load(0, 0, ha, ld_a).wait()
                act_block((sl - 16) // 2, ha)

            @when(even, sl == 31)
            def _():
                take(gb_ref.at[xgid, pl.ds(0, 4)], ag_s.at[xgid])

                @pl.when(lp == 0)
                def _():
                    pltpu.make_async_copy(x_ref.at[0], xown, ld_o).start()

            @when(lp == 0, odd, sl == 31)
            def _():
                pltpu.make_async_copy(x_ref.at[0], xown, ld_o).wait()

    @pl.loop(PIECES, PIECES + LAG_LAST)
    def _(i):
        line_step(i)

    take(gb_ref.at[0, 0, pl.ds(0, 5 * rows)], ag_f.at[0])
    take(gb_ref.at[0, pl.ds(0, 2)], ag_f.at[0])
    for gid in range(1, 2 * LAYERS):
        take(gb_ref.at[gid, pl.ds(0, 3)], ag_f.at[gid])
    for slot in range(2):
        take(pp.at[slot], pp_s.at[slot])
    for kept in range(8 - SUMS, SUMS):
        take(pm.at[kept], pm_s.at[kept])
    take(gown, st_gx)

    @pl.when(is_end)
    def _():
        for slot in range(SLOTS):
            take(zp.at[slot], zs.at[slot])


def move_kernel(count, *refs):
    sources, targets = refs[:count], refs[count:2 * count]
    buffers, read, written = refs[2 * count:3 * count], refs[-2], refs[-1]
    copies, slot = [], 0
    for source, target, buffer in zip(sources, targets, buffers):
        size = buffer.shape[1]
        for n in range(buffer.shape[0]):
            rows = pl.ds(n * size, size)
            copies.append((pltpu.make_async_copy(source.at[rows], buffer.at[n], read.at[slot]),
                           pltpu.make_async_copy(buffer.at[n], target.at[rows], written.at[slot])))
            slot += 1
    for first, _ in copies:
        first.start()
    for first, _ in copies:
        first.wait()
    for _, second in copies:
        second.start()
    for _, second in copies:
        second.wait()


def move(*arrays):
    flat = [a.reshape(-1, a.shape[-1]) for a in arrays]
    parts = [max(1, a.size * a.dtype.itemsize // MOVE_BYTES) for a in flat]
    any_space = pl.BlockSpec(memory_space=pl.ANY)
    size = sum(a.size * a.dtype.itemsize for a in flat)
    moved = pl.pallas_call(
        functools.partial(move_kernel, len(flat)),
        name="move",
        out_shape=tuple(jax.ShapeDtypeStruct(a.shape, a.dtype) for a in flat),
        in_specs=[any_space] * len(flat),
        out_specs=(any_space,) * len(flat),
        scratch_shapes=[pltpu.VMEM((n, a.shape[0] // n, a.shape[1]), a.dtype) for a, n in zip(flat, parts)]
        + [pltpu.SemaphoreType.DMA((sum(parts),))] * 2,
        compiler_params=pltpu.CompilerParams(vmem_limit_bytes=67043328),
        cost_estimate=pl.CostEstimate(flops=int(size * MOVE_FLOPS), bytes_accessed=2 * size, transcendentals=0),
    )(*flat)
    return [m.reshape(a.shape) for m, a in zip(moved, arrays)]


def solution(mesh):
    def device_step(x_saved, h_saved, w_up, w_down, grad_out):
        layers, hidden, ffn = w_up.shape
        rows = grad_out.shape[1]
        tokens = h_saved.shape[2]
        cw, fb = hidden // CHUNKS, ffn // PARTS
        half_rows = rows // 2
        any_space = pl.BlockSpec(memory_space=pl.ANY)
        dma = pltpu.SemaphoreType.DMA
        vmem = pltpu.VMEM
        grad_x, grad_up, grad_down, rest, _, _ = pl.pallas_call(
            kernel,
            name="backward",
            out_shape=(
                jax.ShapeDtypeStruct((rows, hidden), BF16),
                jax.ShapeDtypeStruct(w_up.shape, F32),
                jax.ShapeDtypeStruct(w_down.shape, F32),
                jax.ShapeDtypeStruct((cw, REST * fb), F32),
                jax.ShapeDtypeStruct((2 * layers, CHUNKS, tokens, cw), BF16),
                jax.ShapeDtypeStruct((layers, 3, rows, hidden), BF16),
            ),
            in_specs=[any_space] * 5,
            out_specs=(any_space,) * 6,
            scratch_shapes=[
                vmem((2, ffn, tokens), BF16),
                vmem((ffn, hidden), BF16),
                vmem((hidden, ffn), BF16),
                vmem((2, tokens, cw), BF16),
                vmem((rows, hidden), BF16),
                vmem((rows, ffn), BF16),
                vmem((rows, ffn), BF16),
                vmem((rows, ffn), BF16),
                vmem((rows, hidden), BF16),
                vmem((rows, hidden), BF16),
                vmem((SUMS, half_rows, hidden), BF16),
                vmem((2, half_rows, hidden), BF16),
                vmem((HELD, half_rows, hidden), BF16),
                vmem((rows, hidden), BF16),
                vmem((SLOTS, fb, cw), F32),
                vmem((FIRST_SLOTS, fb, cw), F32),
                vmem((SLOTS, fb, cw), F32),
                dma((SLOTS,)), dma((FIRST_SLOTS, SPLIT)), dma((SLOTS,)), dma((SLOTS,)), dma((SLOTS,)), dma((LAST_SLOTS,)),
                pltpu.SemaphoreType.REGULAR, pltpu.SemaphoreType.REGULAR, pltpu.SemaphoreType.REGULAR,
                dma((2 * layers, CHUNKS)), dma((2 * layers, CHUNKS)), dma((2 * layers, CHUNKS)), dma((2 * layers, CHUNKS)),
                dma((2 * layers,)), dma((2 * layers,)), dma((2 * layers,)),
                dma((2,)), dma((HELD,)), dma((SUMS,)), dma((6 * layers,)), pltpu.SemaphoreType.REGULAR,
                dma((2,)), dma(()), dma(()), dma(()), dma((2,)), dma(()), dma((3,)), dma(()), dma(()), dma(()), dma((2,)), dma((2,)), dma((2,)), dma((2,)),
            ],
            compiler_params=pltpu.CompilerParams(collective_id=0, has_side_effects=True, vmem_limit_bytes=67043328),
        )(x_saved[:, 0], h_saved[:, 0], w_up, w_down, grad_out[0])
        spot = lax.axis_index("data")
        is_end = (spot == 0) | (spot == 3)
        rest = jnp.where(is_end, lax.ppermute(rest, "data", [(1, 0), (2, 3)]), rest)
        grad_x, grad_up, grad_down = move(grad_x, grad_up, grad_down)
        grad_up = grad_up.at[0, hidden - cw:, ffn - REST * fb:].set(rest)
        return grad_x[None], grad_up, grad_down

    return jax.shard_map(
        device_step,
        mesh=mesh,
        in_specs=(P(None, "data", "model", None), P(None, "data", None, "model"), P(None, None, "model"), P(None, "model", None), P("data", "model", None)),
        out_specs=(P("data", "model", None), P(None, None, "model"), P(None, "model", None)),
        check_vma=False,
    )
```

```python
import functools

import jax
import jax.numpy as jnp
from jax import lax
from jax.experimental import pallas as pl
from jax.experimental.pallas import tpu as pltpu
from jax.sharding import PartitionSpec as P

MESH = pl.DeviceIdType.MESH
F32, BF16 = jnp.float32, jnp.bfloat16
NT = (((1,), (1,)), ((), ()))

LAYERS = 2
CHUNKS = 8
PARTS = 4
PHASE = CHUNKS * PARTS
PER_LAYER = 2 * PHASE
PIECES = LAYERS * PER_LAYER
REST = 2
FULL = PIECES - REST
SLOTS = 16
FIRST_SLOTS = 8
SPLIT = 4
LAST_SLOTS = 32
LAG_SUM = 2
LAG_FREE = 6
LAG_LAST = 20
UNIT_STEPS = 16, 14
X_RUNS = ((0, 5, 6, 3, 8), (5, 3, 19, 4, 5))
FIRST_RELAY = 1
FINAL_STEP = 48
HELD = 3
SUMS = 6

MOVE_BYTES = 1 << 22
MOVE_FLOPS = 10


def gelu_tanh(pre):
    return jnp.tanh(0.7978845608028654 * (pre + 0.044715 * pre * pre * pre))


def gelu(pre):
    return 0.5 * pre * (1.0 + gelu_tanh(pre))


def gelu_slope(pre):
    tanh_val = gelu_tanh(pre)
    return 0.5 * (1.0 + tanh_val) + 0.5 * pre * (1.0 - tanh_val * tanh_val) * 0.7978845608028654 * (1.0 + 0.134145 * pre * pre)


def kernel(x_ref, h_ref, wu_ref, wd_ref, g_ref, gx_ref, up_ref, down_ref, rest_ref, gb_ref, rxh_ref,
           lt, wd, wu, cbuf, gr, hr, dh, ha, gown, xown, pm, pp, pb, rxo, zp, z1, z2,
           zs, z_r1, z_r2, z_ts, z_tl, z_rt, c1, c2, c3,
           ag_x, ag_y, ag_d, ag_p, ag_s, ag_f, ag_l, pp_s, pb_r, pm_s, rx_r, pbc,
           ld_c, ld_g, ld_h, ld_a, ld_w, ld_o, ld_rx, st_gx, first_s, first_l, first_x, first_y, first_d, first_p):
    rows, hidden = gown.shape
    ffn = lt.shape[1]
    half_rows = rows // 2
    cw = hidden // CHUNKS
    fb = ffn // 4

    me = lax.axis_index("model")
    spot = lax.axis_index("data")
    core = lax.rem(me, 2)
    px = lax.rem(me // 2, 2)
    py = me // 4
    partner = me + 1 - 2 * core
    step_x, step_y = 2 * (1 - 2 * px), 4 * (1 - 2 * py)
    near_x, near_y, far = me + step_x, me + step_y, me + step_x + step_y
    is_end = jnp.logical_or(spot == 0, spot == 3)
    is_mid = jnp.logical_not(is_end)
    line_mid = jnp.where(spot < 2, 1, 2)
    line_end = jnp.where(spot < 2, 0, 3)
    line_across = 3 - spot

    def model(i):
        return {"model": i}

    def data(i):
        return {"data": i}

    def signal(sem, where):
        pl.semaphore_signal(sem, inc=1, device_id=where, device_id_type=MESH)

    def remote(src, dst, send, recv, where):
        return pltpu.make_async_remote_copy(src_ref=src, dst_ref=dst, send_sem=send, recv_sem=recv, device_id=where, device_id_type=MESH)

    def take(ref, sem):
        pltpu.make_async_copy(ref, ref, sem).wait()

    def chunk_columns(c):
        return pl.ds(pl.multiple_of(c * cw, cw), cw)

    def row_block(i):
        return pl.ds(pl.multiple_of(i * rows, rows), rows)

    def gather_keep(gid, own, first=0):
        for c in range(first, CHUNKS):
            pltpu.make_async_copy(own.at[:, pl.ds(c * cw, cw)], gb_ref.at[gid, c, row_block(me)], ag_l.at[gid]).start()

    def gather_send(gid, c, own, buf):
        src = own.at[:, chunk_columns(c)]
        dst = buf.at[row_block(me)]
        remote(src, dst, ag_s.at[gid], ag_x.at[gid, c], model(near_x)).start()
        remote(src, dst, ag_s.at[gid], ag_y.at[gid, c], model(near_y)).start()
        remote(src, dst, ag_s.at[gid], ag_p.at[gid, c], model(partner)).start()

    def gather_relay(gid, c, buf, sent, forwarded):
        take(buf.at[row_block(0)], ag_x.at[gid, c])
        take(buf.at[row_block(0)], ag_y.at[gid, c])
        for n, (source, target) in enumerate(((near_x, near_y), (near_y, near_x))):
            @pl.when(core == n)
            def _():
                block = buf.at[row_block(source)]
                remote(block, block, sent, ag_d.at[gid, c], model(target)).start()
        for peer in (near_x, near_y):
            block = buf.at[row_block(peer)]
            remote(block, block, forwarded, ag_p.at[gid, c], model(partner)).start()

    def gather_forward(gid, c, buf, forwarded):
        take(buf.at[row_block(0)], ag_d.at[gid, c])
        block = buf.at[row_block(far)]
        remote(block, block, forwarded, ag_p.at[gid, c], model(partner)).start()

    def gather_wait(gid, c, buf):
        take(buf.at[pl.ds(0, 4 * rows)], ag_p.at[gid, c])

    def gathered(gid, c):
        return gb_ref.at[gid, c]

    def half_block(i, h):
        return cbuf.at[0, row_block(i), pl.ds(h * (cw // 2), cw // 2)]

    def half_send(h):
        src = gown.at[:, pl.ds(h * (cw // 2), cw // 2)]
        for peer, sem in ((near_x, first_x), (near_y, first_y), (partner, first_p)):
            remote(src, half_block(me, h), ag_s.at[0], sem.at[h], model(peer)).start()

    def half_relay(h):
        take(half_block(0, h), first_x.at[h])
        take(half_block(0, h), first_y.at[h])
        for n, (source, target) in enumerate(((near_x, near_y), (near_y, near_x))):
            @pl.when(core == n)
            def _():
                remote(half_block(source, h), half_block(source, h), first_s, first_d.at[h], model(target)).start()
        for peer in (near_x, near_y):
            remote(half_block(peer, h), half_block(peer, h), first_s, first_p.at[h], model(partner)).start()

    def half_forward(h):
        take(half_block(0, h), first_d.at[h])
        remote(half_block(far, h), half_block(far, h), first_s, first_p.at[h], model(partner)).start()

    def half_wait(h):
        take(cbuf.at[0, pl.ds(0, 4 * rows), pl.ds(h * (cw // 2), cw // 2)], first_p.at[h])

    def chunk_load(gid, c, slot):
        return pltpu.make_async_copy(gb_ref.at[gid, c], cbuf.at[slot], ld_c.at[slot])

    def act_load(layer, b, ref, sem):
        return pltpu.make_async_copy(h_ref.at[layer, row_block(b)], ref, sem)

    def act_block(b, ref):
        @pl.loop(0, 4)
        def _(f):
            cols = pl.ds(pl.multiple_of(f * fb, fb), fb)
            a = gelu(ref[:, cols].astype(F32)).astype(BF16).astype(F32)
            lt[0, cols, row_block(b)] = a.T.astype(BF16)

    def weight_loads(layer):
        return (pltpu.make_async_copy(wd_ref.at[layer], wd, ld_w.at[0]), pltpu.make_async_copy(wu_ref.at[layer], wu, ld_w.at[1]))

    def unit_place(u):
        r = lax.rem(u // 2 + 1, 4)
        chip = lax.rem(py + r // 2, 2) * 2 + lax.rem(px + lax.rem(r, 2), 2)
        return r, chip

    def unit_rows(u):
        _, chip = unit_place(u)
        start = (chip * 2 + core) * rows + lax.rem(u, 2) * half_rows
        other = (chip * 2 + 1 - core) * rows + lax.rem(u, 2) * half_rows
        return tuple(pl.ds(pl.multiple_of(s, half_rows), half_rows) for s in (start, other))

    def unit_load(gid, layer, u):
        for n, block in enumerate(unit_rows(u)):
            here = pl.ds(n * half_rows, half_rows)
            for c in range(CHUNKS):
                pltpu.make_async_copy(gb_ref.at[gid, c, block], gr.at[here, pl.ds(c * cw, cw)], ld_g).start()
            pltpu.make_async_copy(h_ref.at[layer, block], hr.at[here], ld_h).start()

    def unit_first(u):
        take(gr, ld_g)
        take(hr, ld_h)
        mine, other = unit_rows(u)

        @pl.loop(0, 4)
        def _(f):
            cols = pl.ds(pl.multiple_of(f * fb, fb), fb)
            d_act = lax.dot_general(gr[...], wd[cols, :], NT, preferred_element_type=F32)
            d_pre = (d_act * gelu_slope(hr[:, cols].astype(F32))).astype(BF16)
            dh[:, cols] = d_pre
            flipped = d_pre.astype(F32).T.astype(BF16)
            lt[1, cols, mine] = flipped[:, :half_rows]
            lt[1, cols, other] = flipped[:, half_rows:]

    def unit_second(lp, u):
        order = lp * 8 + u
        slot = lax.rem(order, 2)
        kept = lax.rem(u, SUMS)

        @pl.when(order >= 2)
        def _():
            take(pp.at[slot], pp_s.at[slot])

        @pl.when(jnp.logical_or(u >= SUMS, jnp.logical_and(lp > 0, u >= 8 - SUMS)))
        def _():
            take(pm.at[kept], pm_s.at[kept])

        @pl.loop(0, CHUNKS)
        def _(d):
            cols = chunk_columns(d)
            part = lax.dot_general(dh[...], wu[cols, :], NT, preferred_element_type=F32).astype(BF16)
            pm[kept, :, cols] = part[:half_rows]
            pp[slot, :, cols] = part[half_rows:]

        @pl.when(order >= HELD)
        def _():
            pl.semaphore_wait(pbc, 1)

        there = lax.rem(order, HELD)
        remote(pp.at[slot], pb.at[there], pp_s.at[slot], pb_r.at[there], model(partner)).start()

    def unit_finish(lp, u):
        order = lp * 8 + u
        slot = lax.rem(order, HELD)
        kept = lax.rem(u, SUMS)
        r, chip = unit_place(u)
        here = pl.ds(pl.multiple_of(lax.rem(u, 2) * half_rows, half_rows), half_rows)
        take(pb.at[slot], pb_r.at[slot])

        @pl.when(r != 0)
        def _():
            @pl.loop(0, CHUNKS)
            def _(d):
                cols = chunk_columns(d)
                pm[kept, :, cols] = (pm[kept, :, cols].astype(F32) + pb[slot, :, cols].astype(F32)).astype(BF16)

            remote(pm.at[kept], rxh_ref.at[lp, r - 1, here], pm_s.at[kept], rx_r.at[lp * 6 + (r - 1) * 2 + lax.rem(u, 2)],
                   model(chip * 2 + core)).start()

        @pl.when(r == 0)
        def _():
            @pl.loop(0, CHUNKS)
            def _(d):
                cols = chunk_columns(d)
                rxo[here, cols] = (pm[kept, :, cols].astype(F32) + pb[slot, :, cols].astype(F32)).astype(BF16)

        @pl.when(order < 8 * LAYERS - HELD)
        def _():
            signal(pbc, model(partner))

    def quarter(n):
        part = rows // 4
        return pl.ds(pl.multiple_of(n * part, part), part)

    def new_gradient_load(lp, n):
        @pl.when(lax.rem(n, 2) == 0)
        def _():
            for r in range(3):
                take(pm.at[0], rx_r.at[lp * 6 + r * 2 + n // 2])

        for r in range(3):
            pltpu.make_async_copy(rxh_ref.at[lp, r, quarter(n)], gr.at[quarter(r)], ld_rx.at[r]).start()

    def new_gradient(n):
        for r in range(3):
            take(gr.at[quarter(0)], ld_rx.at[r])

        @pl.loop(0, CHUNKS)
        def _(d):
            cols = chunk_columns(d)
            total = rxo[quarter(n), cols].astype(F32)
            for r in range(3):
                total += gr[quarter(r), cols].astype(F32)
            gown[quarter(n), cols] = (gown[quarter(n), cols].astype(F32) + total).astype(BF16)

    def split(q):
        return pl.ds(q * (fb // SPLIT), fb // SPLIT)

    def piece_place(i):
        return LAYERS - 1 - i // PER_LAYER, lax.rem(i // PHASE, 2), lax.rem(i, PHASE) // PARTS, lax.rem(i, PARTS)

    def part_columns(n):
        return pl.ds(pl.multiple_of(n * fb, fb), fb)

    def piece(i):
        _, phase, _, n = piece_place(i)
        slot = lax.rem(i, SLOTS)

        @pl.when(jnp.logical_and(is_end, i >= SLOTS))
        def _():
            take(zp.at[slot], zs.at[slot])

        @pl.when(i < PARTS)
        def _():
            wide = pl.ds(pl.multiple_of(lax.rem(i, 2) * 2 * fb, 2 * fb), 2 * fb)

            for h in range(2):
                @pl.when(i // 2 == h)
                def _():
                    part = jnp.dot(lt[0, wide, :], cbuf[0, :, pl.ds(h * (cw // 2), cw // 2)], preferred_element_type=F32)
                    for b in range(2):
                        zp[slot, :, pl.ds(b * (cw // 2), cw // 2)] = part[b * fb:(b + 1) * fb]

        @pl.when(i >= PARTS)
        def _():
            part = jnp.dot(lt[phase, part_columns(n), :], cbuf[lax.rem(i // PARTS, 2)], preferred_element_type=F32)

            @pl.when(phase == 0)
            def _():
                zp[slot] = part

            @pl.when(phase == 1)
            def _():
                zp[slot] = part.T

    def total_place(j):
        layer, _, c, n = piece_place(j)
        return down_ref.at[layer, part_columns(n), chunk_columns(c)], up_ref.at[layer, chunk_columns(c), part_columns(n)]

    def total_copies(j, slot):
        _, phase, _, _ = piece_place(j)
        down, up = total_place(j)
        first = []
        for b in range(2):
            f0 = (lax.rem(j, 2) * 2 + b) * fb
            d0 = j // 2 * (cw // 2)
            first.append((z2.at[slot, :, pl.ds(b * (cw // 2), cw // 2)],
                          down_ref.at[LAYERS - 1, pl.ds(pl.multiple_of(f0, fb), fb), pl.ds(pl.multiple_of(d0, cw // 2), cw // 2)]))
        return ((j < PARTS, first), (jnp.logical_and(j >= PARTS, phase == 0), [(z2.at[slot], down)]), (phase == 1, [(z2.at[slot], up)]))

    def total_send(j, slot):
        @pl.when(jnp.logical_and(j >= 0, j < FULL))
        def _():
            for cond, copies in total_copies(j, slot):
                @pl.when(cond)
                def _():
                    for source, place in copies:
                        remote(source, place, z_ts.at[slot], z_rt.at[lax.rem(j, LAST_SLOTS)], data(line_end)).start()
                        pltpu.make_async_copy(source, place, z_tl.at[slot]).start()

    def sum_send(slot, q):
        remote(zp.at[slot, split(q)], z2.at[slot, split(q)], zs.at[slot], z_r2.at[slot], data(line_across)).start()

    def line_step(i):
        @pl.when(is_end)
        def _():
            @pl.when(i < PIECES)
            def _():
                slot, there = lax.rem(i, SLOTS), lax.rem(i, FIRST_SLOTS)

                @pl.when(i >= FIRST_SLOTS)
                def _():
                    pl.semaphore_wait(c1, 1)

                for q in range(SPLIT):
                    remote(zp.at[slot, split(q)], z1.at[there, split(q)], zs.at[slot], z_r1.at[there, q], data(line_mid)).start()

            j = i - LAG_LAST

            @pl.when(jnp.logical_and(j >= 0, j < FULL))
            def _():
                take(zp.at[0], z_rt.at[lax.rem(j, LAST_SLOTS)])

                @pl.when(j + LAST_SLOTS < FULL)
                def _():
                    signal(c3, data(line_mid))

        @pl.when(is_mid)
        def _():
            slot, there = lax.rem(i, SLOTS), lax.rem(i, FIRST_SLOTS)
            j = i - LAG_SUM
            old = lax.rem(j + SLOTS, SLOTS)

            @pl.when(jnp.logical_and(j >= 0, j < PIECES))
            def _():
                take(z2.at[old], z_r2.at[old])
                z2[old] = z2[old] + zp[old]
                take(zp.at[old], zs.at[old])

                @pl.when(jnp.logical_and(j >= LAST_SLOTS, j < FULL))
                def _():
                    pl.semaphore_wait(c3, 1)

            @pl.when(jnp.logical_and(j >= FULL, j < PIECES))
            def _():
                pltpu.make_async_copy(z2.at[old], rest_ref.at[:, part_columns(j - FULL)], z_tl.at[old]).start()

            @pl.when(i < PIECES)
            def _():
                @pl.when(i >= SLOTS)
                def _():
                    pl.semaphore_wait(c2, 1)

                for q in range(SPLIT):
                    take(z1.at[there, split(q)], z_r1.at[there, q])
                    zp[slot, split(q), :] = zp[slot, split(q), :] + z1[there, split(q), :]

                    if q == 0:
                        total_send(j, old)
                    else:
                        sum_send(slot, q - 1)
                sum_send(slot, SPLIT - 1)

                @pl.when(i + FIRST_SLOTS < PIECES)
                def _():
                    signal(c1, data(line_end))

            @pl.when(i >= PIECES)
            def _():
                total_send(j, old)

            k = i - LAG_FREE

            @pl.when(jnp.logical_and(k >= 0, k < PIECES))
            def _():
                free = lax.rem(k, SLOTS)
                @pl.when(k < FULL)
                def _():
                    take(z2.at[free], z_ts.at[free])

                take(z2.at[free], z_tl.at[free])

                @pl.when(k + SLOTS < PIECES)
                def _():
                    signal(c2, data(line_across))

    top = LAYERS - 1
    loads_g = [pltpu.make_async_copy(g_ref.at[:, part], gown.at[:, part], sem)
               for part, sem in ((pl.ds(0, cw), ld_rx.at[0]), (pl.ds(cw, hidden - cw), ld_o))]
    for load in loads_g:
        load.start()
    held = ((ha, ld_a), (hr, ld_h))
    for n, (ref, sem) in enumerate(held):
        act_load(top, n, ref, sem).start()
    barrier = pltpu.get_barrier_semaphore()
    for peer in (near_x, near_y, far, partner):
        signal(barrier, model(peer))

    @pl.when(is_end)
    def _():
        signal(barrier, data(line_mid))
        pl.semaphore_wait(barrier, 5)

    @pl.when(is_mid)
    def _():
        signal(barrier, data(line_end))
        signal(barrier, data(line_across))
        pl.semaphore_wait(barrier, 6)

    loads_g[0].wait()
    half_send(0)
    cbuf[0, row_block(me), :] = gown[:, :cw]
    loads_g[1].wait()
    gather_keep(0, gown, 1)
    load_x = pltpu.make_async_copy(x_ref.at[top], xown, ld_o)
    load_x.start()
    for load in weight_loads(top):
        load.start()

    @pl.loop(0, 4)
    def _(b):
        for n, (ref, sem) in enumerate(held):
            act_load(top, 0, ref, sem).wait()
            act_block(2 * b + n, ref)

            @pl.when(b < 3)
            def _():
                act_load(top, 2 * b + n + 2, ref, sem).start()

        @pl.when(b == FIRST_RELAY)
        def _():
            half_relay(0)
            half_send(1)
            gather_send(0, 1, gown, gathered(0, 1))

    half_forward(0)
    load_x.wait()
    take(gown.at[:, pl.ds(0, hidden - cw)], ag_l.at[0])
    half_wait(0)

    @pl.loop(0, PIECES)
    def _(i):
        lp = i // PER_LAYER
        layer = LAYERS - 1 - lp
        s = i // 2
        sl = lax.rem(s, PER_LAYER // 2)
        il = lax.rem(i, PER_LAYER)
        even = lax.rem(i, 2) == 0
        odd = jnp.logical_not(even)
        odd_pair = lax.rem(s, 2) == 1
        even_pair = jnp.logical_not(odd_pair)
        ggid, xgid = 2 * lp, 2 * lp + 1

        @pl.when(jnp.logical_and(i > 0, lax.rem(i, PARTS) == 0))
        def _():
            take(cbuf.at[0], ld_c.at[lax.rem(i // PARTS, 2)])

        piece(i)

        line_step(i)

        def when(*conds):
            return pl.when(functools.reduce(jnp.logical_and, conds))

        @pl.when(s < CHUNKS)
        def _():
            @pl.when(i == 0)
            def _():
                half_relay(1)
                gather_relay(0, 1, gathered(0, 1), ag_s.at[0], ag_f.at[0])

            @pl.when(i == 1)
            def _():
                half_forward(1)
                half_wait(1)
                pltpu.make_async_copy(cbuf.at[0], gathered(0, 0), first_l).start()

            @when(odd, s >= 1, s < CHUNKS - 1)
            def _():
                gather_relay(0, s + 1, gathered(0, s + 1), ag_s.at[0], ag_f.at[0])

            @when(even, s < CHUNKS - 2)
            def _():
                gather_send(0, s + 2, gown, gathered(0, s + 2))

            @when(even, s >= 1, s < CHUNKS)
            def _():
                gather_forward(0, s, gathered(0, s), ag_f.at[0])

            @when(odd, s >= 1, s < CHUNKS)
            def _():
                gather_wait(0, s, gathered(0, s))

            @when(i == 2 * PARTS - 2)
            def _():
                take(cbuf.at[0, pl.ds(0, 4 * rows)], first_s)
                take(cbuf.at[0], first_l)

        @pl.when(sl >= X_RUNS[0][2])
        def _():
            @when(even, sl == X_RUNS[0][2])
            def _():
                gather_keep(xgid, xown)

            for first, count, start, relay, forward in X_RUNS:
                @when(even, sl >= start, sl < start + count)
                def _():
                    gather_send(xgid, sl - start + first, xown, gathered(xgid, sl - start + first))

                @when(even, sl >= start + relay, sl < start + relay + count)
                def _():
                    gather_relay(xgid, sl - start - relay + first, gathered(xgid, sl - start - relay + first), ag_s.at[xgid], ag_f.at[xgid])

                @when(even, sl >= start + forward, sl < start + forward + count)
                def _():
                    gather_forward(xgid, sl - start - forward + first, gathered(xgid, sl - start - forward + first), ag_f.at[xgid])

            @when(even, sl == 15)
            def _():
                take(xown, ag_l.at[xgid])

            @when(even, odd_pair, sl >= 15, sl < 31)
            def _():
                gather_wait(xgid, (sl - 15) // 2, gathered(xgid, (sl - 15) // 2))

        @pl.when(jnp.logical_and(s >= 26, s < 31 + CHUNKS))
        def _():
            @when(even, s == 26)
            def _():
                gather_keep(2, gown)

            @when(even, s >= 26, s < 26 + CHUNKS)
            def _():
                gather_send(2, s - 26, gown, gathered(2, s - 26))

            @when(even, s >= 28, s < 28 + CHUNKS)
            def _():
                gather_relay(2, s - 28, gathered(2, s - 28), ag_s.at[2], ag_f.at[2])

            @when(even, s >= 30, s < 30 + CHUNKS)
            def _():
                gather_forward(2, s - 30, gathered(2, s - 30), ag_f.at[2])

            @when(even, s == 31)
            def _():
                take(gown, ag_l.at[2])

            @when(even, s >= 31, s < 31 + CHUNKS)
            def _():
                gather_wait(2, s - 31, gathered(2, s - 31))

        @when(jnp.logical_or(i == PARTS - 1, jnp.logical_and(i >= PARTS, lax.rem(i, PARTS) == PARTS - 2)), i + 2 < PIECES)
        def _():
            nxt = i // PARTS * PARTS + PARTS
            chunk_load(nxt // PHASE, lax.rem(nxt, PHASE) // PARTS, lax.rem(nxt // PARTS, 2)).start()

        @pl.when(jnp.logical_and(il >= min(UNIT_STEPS) - 1, il < max(UNIT_STEPS) + 24))
        def _():
            spread = lp > 0
            k = il - jnp.where(spread, UNIT_STEPS[1], UNIT_STEPS[0])
            half = jnp.where(spread, 4 * (k // 5) + lax.rem(k + 5, 5), k)
            on = functools.reduce(jnp.logical_and, (k >= 0, half < 16, jnp.logical_or(jnp.logical_not(spread), lax.rem(k + 5, 5) < 4)))
            u = half // 2
            first_half = lax.rem(half + 16, 2) == 0
            last = jnp.where(spread, 20, 16)

            @when(k == -1)
            def _():
                unit_load(ggid, layer, 0)

            @when(k == 0)
            def _():
                for load in weight_loads(0):
                    load.wait()

            @when(on, first_half)
            def _():
                unit_first(u)

            @when(jnp.logical_or(jnp.logical_and(jnp.logical_and(on, first_half), u >= 2), jnp.logical_or(k == last, k == last + 2)))
            def _():
                unit_finish(lp, jnp.where(k >= last, 6 + (k - last) // 2, u - 2))

            @when(on, jnp.logical_not(first_half), u < 7)
            def _():
                unit_load(ggid, layer, u + 1)

            @when(on, jnp.logical_not(first_half))
            def _():
                unit_second(lp, u)

        @pl.when(jnp.logical_and(il >= FINAL_STEP - 1, il < FINAL_STEP + 5))
        def _():
            @when(il == FINAL_STEP - 1)
            def _():
                take(gb_ref.at[ggid, 0, pl.ds(0, 7 * rows)], ag_s.at[ggid])
                take(gb_ref.at[ggid, pl.ds(0, 3)], ag_s.at[ggid])

                @pl.when(lp > 0)
                def _():
                    take(gb_ref.at[ggid, 0, row_block(0)], ag_s.at[ggid])

                new_gradient_load(lp, 0)

            @when(il >= FINAL_STEP, il < FINAL_STEP + 4)
            def _():
                new_gradient(il - FINAL_STEP)

                @pl.when(il < FINAL_STEP + 3)
                def _():
                    new_gradient_load(lp, il - FINAL_STEP + 1)

            @when(i == PER_LAYER + FINAL_STEP + 4)
            def _():
                pltpu.make_async_copy(gown, gx_ref, st_gx).start()

        @pl.when(sl >= 16)
        def _():
            @when(lp == 0, even, sl == 17)
            def _():
                for load in weight_loads(0):
                    load.start()

            @when(lp == 0, even, even_pair, sl >= 16)
            def _():
                act_load(0, (sl - 16) // 2, ha, ld_a).start()

            @when(lp == 0, odd, odd_pair, sl >= 16)
            def _():
                act_load(0, 0, ha, ld_a).wait()
                act_block((sl - 16) // 2, ha)

            @when(even, sl == 31)
            def _():
                take(gb_ref.at[xgid, pl.ds(0, 4)], ag_s.at[xgid])

                @pl.when(lp == 0)
                def _():
                    pltpu.make_async_copy(x_ref.at[0], xown, ld_o).start()

            @when(lp == 0, odd, sl == 31)
            def _():
                pltpu.make_async_copy(x_ref.at[0], xown, ld_o).wait()

    @pl.loop(PIECES, PIECES + LAG_LAST)
    def _(i):
        line_step(i)

    take(gb_ref.at[0, 0, pl.ds(0, 5 * rows)], ag_f.at[0])
    take(gb_ref.at[0, pl.ds(0, 2)], ag_f.at[0])
    for gid in range(1, 2 * LAYERS):
        take(gb_ref.at[gid, pl.ds(0, 3)], ag_f.at[gid])
    for slot in range(2):
        take(pp.at[slot], pp_s.at[slot])
    for kept in range(8 - SUMS, SUMS):
        take(pm.at[kept], pm_s.at[kept])
    take(gown, st_gx)

    @pl.when(is_end)
    def _():
        for slot in range(SLOTS):
            take(zp.at[slot], zs.at[slot])


def move_kernel(count, *refs):
    sources, targets = refs[:count], refs[count:2 * count]
    buffers, read, written = refs[2 * count:3 * count], refs[-2], refs[-1]
    copies, slot = [], 0
    for source, target, buffer in zip(sources, targets, buffers):
        size = buffer.shape[1]
        for n in range(buffer.shape[0]):
            rows = pl.ds(n * size, size)
            copies.append((pltpu.make_async_copy(source.at[rows], buffer.at[n], read.at[slot]),
                           pltpu.make_async_copy(buffer.at[n], target.at[rows], written.at[slot])))
            slot += 1
    for first, _ in copies:
        first.start()
    for first, _ in copies:
        first.wait()
    for _, second in copies:
        second.start()
    for _, second in copies:
        second.wait()


def move(*arrays):
    flat = [a.reshape(-1, a.shape[-1]) for a in arrays]
    parts = [max(1, a.size * a.dtype.itemsize // MOVE_BYTES) for a in flat]
    any_space = pl.BlockSpec(memory_space=pl.ANY)
    size = sum(a.size * a.dtype.itemsize for a in flat)
    moved = pl.pallas_call(
        functools.partial(move_kernel, len(flat)),
        name="move",
        out_shape=tuple(jax.ShapeDtypeStruct(a.shape, a.dtype) for a in flat),
        in_specs=[any_space] * len(flat),
        out_specs=(any_space,) * len(flat),
        scratch_shapes=[pltpu.VMEM((n, a.shape[0] // n, a.shape[1]), a.dtype) for a, n in zip(flat, parts)]
        + [pltpu.SemaphoreType.DMA((sum(parts),))] * 2,
        compiler_params=pltpu.CompilerParams(vmem_limit_bytes=67043328),
        cost_estimate=pl.CostEstimate(flops=int(size * MOVE_FLOPS), bytes_accessed=2 * size, transcendentals=0),
    )(*flat)
    return [m.reshape(a.shape) for m, a in zip(moved, arrays)]


def solution(mesh):
    def device_step(x_saved, h_saved, w_up, w_down, grad_out):
        layers, hidden, ffn = w_up.shape
        rows = grad_out.shape[1]
        tokens = h_saved.shape[2]
        cw, fb = hidden // CHUNKS, ffn // PARTS
        half_rows = rows // 2
        any_space = pl.BlockSpec(memory_space=pl.ANY)
        dma = pltpu.SemaphoreType.DMA
        vmem = pltpu.VMEM
        grad_x, grad_up, grad_down, rest, _, _ = pl.pallas_call(
            kernel,
            name="backward",
            out_shape=(
                jax.ShapeDtypeStruct((rows, hidden), BF16),
                jax.ShapeDtypeStruct(w_up.shape, F32),
                jax.ShapeDtypeStruct(w_down.shape, F32),
                jax.ShapeDtypeStruct((cw, REST * fb), F32),
                jax.ShapeDtypeStruct((2 * layers, CHUNKS, tokens, cw), BF16),
                jax.ShapeDtypeStruct((layers, 3, rows, hidden), BF16),
            ),
            in_specs=[any_space] * 5,
            out_specs=(any_space,) * 6,
            scratch_shapes=[
                vmem((2, ffn, tokens), BF16),
                vmem((ffn, hidden), BF16),
                vmem((hidden, ffn), BF16),
                vmem((2, tokens, cw), BF16),
                vmem((rows, hidden), BF16),
                vmem((rows, ffn), BF16),
                vmem((rows, ffn), BF16),
                vmem((rows, ffn), BF16),
                vmem((rows, hidden), BF16),
                vmem((rows, hidden), BF16),
                vmem((SUMS, half_rows, hidden), BF16),
                vmem((2, half_rows, hidden), BF16),
                vmem((HELD, half_rows, hidden), BF16),
                vmem((rows, hidden), BF16),
                vmem((SLOTS, fb, cw), F32),
                vmem((FIRST_SLOTS, fb, cw), F32),
                vmem((SLOTS, fb, cw), F32),
                dma((SLOTS,)), dma((FIRST_SLOTS, SPLIT)), dma((SLOTS,)), dma((SLOTS,)), dma((SLOTS,)), dma((LAST_SLOTS,)),
                pltpu.SemaphoreType.REGULAR, pltpu.SemaphoreType.REGULAR, pltpu.SemaphoreType.REGULAR,
                dma((2 * layers, CHUNKS)), dma((2 * layers, CHUNKS)), dma((2 * layers, CHUNKS)), dma((2 * layers, CHUNKS)),
                dma((2 * layers,)), dma((2 * layers,)), dma((2 * layers,)),
                dma((2,)), dma((HELD,)), dma((SUMS,)), dma((6 * layers,)), pltpu.SemaphoreType.REGULAR,
                dma((2,)), dma(()), dma(()), dma(()), dma((2,)), dma(()), dma((3,)), dma(()), dma(()), dma(()), dma((2,)), dma((2,)), dma((2,)), dma((2,)),
            ],
            compiler_params=pltpu.CompilerParams(collective_id=0, has_side_effects=True, vmem_limit_bytes=67043328),
        )(x_saved[:, 0], h_saved[:, 0], w_up, w_down, grad_out[0])
        spot = lax.axis_index("data")
        is_end = (spot == 0) | (spot == 3)
        rest = jnp.where(is_end, lax.ppermute(rest, "data", [(1, 0), (2, 3)]), rest)
        grad_x, grad_up, grad_down = move(grad_x, grad_up, grad_down)
        grad_up = grad_up.at[0, hidden - cw:, ffn - REST * fb:].set(rest)
        return grad_x[None], grad_up, grad_down

    return jax.shard_map(
        device_step,
        mesh=mesh,
        in_specs=(P(None, "data", "model", None), P(None, "data", None, "model"), P(None, None, "model"), P(None, "model", None), P("data", "model", None)),
        out_specs=(P("data", "model", None), P(None, None, "model"), P(None, "model", None)),
        check_vma=False,
    )
```
